32 devices in a mesh: dp: 2 (over core), row: 4 (over y, x), col: 4 (over z).
Axes of the slice: x: 2, y: 2, z: 4, core: 2. Of those that a mesh axis runs over, the one named last changes fastest.
Arguments:
- block_input: float32 [4096, 2048], P(('dp', 'row'), 'col'), as said below
- out_grad: float32 [4096, 2048], P(('dp', 'row'), 'col'), may hold values from -6 to 6
- ln1_gain: float32 [2048], P('col'), may hold values from 0.25 to 1.75
- ln1_bias: float32 [2048], P('col'), may hold values from -1.75 to 1.75
- ln2_gain: float32 [2048], P('col'), may hold values from 0.25 to 1.75
- ln2_bias: float32 [2048], P('col'), may hold values from -1.75 to 1.75
- w_qkv: bfloat16 [2048, 6144], P('row', 'col'), as said below
- b_qkv: float32 [6144], P('col'), may hold values from -3 to 3
- w_dense: bfloat16 [2048, 2048], P('col', 'row'), may hold values from -0.5 to 0.5
- b_dense: float32 [2048], P('col'), may hold values from -1.75 to 1.75
- w_fc: bfloat16 [2048, 8192], P('row', 'col'), may hold values from -0.125 to 0.125
- b_fc: float32 [8192], P('col'), may hold values from -3 to 3
- w_proj: bfloat16 [8192, 2048], P('col', 'row'), may hold values from -0.0625 to 0.0625
- b_proj: float32 [2048], P('col'), may hold values from -1.75 to 1.75
Outputs:
- block_output: float32 [4096, 2048], P(('dp', 'row'), 'col')
- input_grad: float32 [4096, 2048], P(('dp', 'row'), 'col')
- grad_ln1_gain: float32 [2048], P('col')
- grad_ln1_bias: float32 [2048], P('col')
- grad_ln2_gain: float32 [2048], P('col')
- grad_ln2_bias: float32 [2048], P('col')
- grad_w_qkv: float32 [2048, 6144], P('row', 'col')
- grad_b_qkv: float32 [6144], P('col')
- grad_w_dense: float32 [2048, 2048], P('col', 'row')
- grad_b_dense: float32 [2048], P('col')
- grad_w_fc: float32 [2048, 8192], P('row', 'col')
- grad_b_fc: float32 [8192], P('col')
- grad_w_proj: float32 [8192, 2048], P('col', 'row')
- grad_b_proj: float32 [2048], P('col')
The draws below stay inside these ranges and needn't reach their ends.
Inputs may be any that keep to these rules, and one draw needn't show every extreme that they name: `block_input`: finite real values. `w_qkv`: finite real values.
All inputs are finite; a program needn't handle non-finite values.
Results may differ from the reference program's by a relative error of at most 0.011.
Values may be sent and summed in bfloat16 or wider, within the bound.
A program may use at most 320 MiB of HBM per device.

```python
import math
import jax
import jax.numpy as jnp
from jax import lax

D = 2048
FF = 8192
HEADS = 8
HD = 256
ROT = 64
SEQ = 512
TOKENS = 4096


def draw_block_input(key, part):
    key_base, key_rows = jax.random.split(key, 2)
    position = jnp.arange(D, dtype=jnp.float32) / D
    base = jnp.clip(jax.random.normal(key_base, (TOKENS, D), jnp.float32), -4.0, 4.0)
    feature_scale = 10.0 ** (position - 0.5)
    row_scale = jnp.exp(jax.random.uniform(key_rows, (TOKENS, 1), jnp.float32, math.log(0.32), math.log(3.2)))
    return row_scale * feature_scale[None, :] * base


def draw_w_qkv(key, part):
    key_base = jax.random.fold_in(key, 0)
    shape = (D, HEADS, 3, HD)
    factor = D ** (-0.5)
    base = jnp.clip(jax.random.normal(key_base, shape, jnp.float32), -6.0, 6.0) * factor
    return base.reshape(D, 3 * D).astype(jnp.bfloat16)


def level_of(rng, shape, shards, smallest, largest):
    def one(dim, shards_of):
        steps = jax.random.uniform(jax.random.fold_in(jax.random.fold_in(rng, 6), dim), (shards_of,), jnp.float32, smallest / len(shards), largest / len(shards))
        return jnp.repeat(jnp.exp(steps), shape[dim] // shards_of).reshape((-1,) + (1,) * (len(shape) - dim - 1))

    loudness = one(*shards[0])
    for cut in shards[1:]:
        loudness = loudness * one(*cut)
    return loudness


def noise(stream_key, dims, scale, reach, shards=(), kind=jnp.bfloat16):
    gain = level_of(stream_key, dims, shards, -0.22, 0.18) if shards else 1.0
    entries = jax.random.normal(stream_key, dims, jnp.float32) * scale * gain
    return jnp.minimum(jnp.maximum(entries, -reach), reach).astype(kind)


def setup_inputs(seed: int = 0) -> dict:
    streams_of = jax.random.split(jax.random.key(seed), 15)
    block_input = draw_block_input(jax.random.fold_in(streams_of[14], 71), 0)
    out_grad = noise(streams_of[1], (TOKENS, D), 1.0, 6.0, ((0, 8), (1, 4)), jnp.float32)
    ln1_gain = jnp.clip(1.0 + 0.15 * jax.random.normal(streams_of[2], (D,), jnp.float32), 0.25, 1.75)
    ln1_bias = noise(streams_of[3], (D,), 0.3, 1.75, ((0, 4),), jnp.float32)
    ln2_gain = jnp.clip(1.0 + 0.15 * jax.random.normal(streams_of[4], (D,), jnp.float32), 0.25, 1.75)
    ln2_bias = noise(streams_of[5], (D,), 0.3, 1.75, ((0, 4),), jnp.float32)
    w_qkv = draw_w_qkv(jax.random.fold_in(streams_of[14], 71), 0)
    b_qkv = noise(streams_of[7], (3 * D,), 0.5, 3.0, ((0, 4),), jnp.float32)
    w_dense = noise(streams_of[8], (D, D), (D // 16) ** -0.5, 0.5, ((0, 4), (1, 4)))
    b_dense = noise(streams_of[9], (D,), 0.3, 1.75, ((0, 4),), jnp.float32)
    w_fc = noise(streams_of[10], (D, FF), D ** -0.5, 0.125, ((0, 4), (1, 4)))
    b_fc = noise(streams_of[11], (FF,), 0.5, 3.0, ((0, 4),), jnp.float32)
    w_proj = noise(streams_of[12], (FF, D), FF ** -0.5, 0.0625, ((0, 4), (1, 4)))
    b_proj = noise(streams_of[13], (D,), 0.3, 1.75, ((0, 4),), jnp.float32)
    return dict(block_input=block_input, out_grad=out_grad, ln1_gain=ln1_gain, ln1_bias=ln1_bias, ln2_gain=ln2_gain, ln2_bias=ln2_bias, w_qkv=w_qkv, b_qkv=b_qkv, w_dense=w_dense, b_dense=b_dense, w_fc=w_fc, b_fc=b_fc, w_proj=w_proj, b_proj=b_proj)


epsilon = 1e-05

def angle_tables(length):
    half_rot = ROT // 2
    position = jnp.arange(length, dtype=jnp.float32)
    exponent = jnp.arange(half_rot, dtype=jnp.float32) * (2.0 / ROT)
    frequency = 10000.0 ** (-exponent)
    angles = position[:, None] * frequency[None, :]
    return (jnp.cos(angles), jnp.sin(angles))

def rotate_fwd(values, cosine, sine_vals):
    half_rot = ROT // 2
    first = values[..., :half_rot]
    second = values[..., half_rot:ROT]
    cos_part = cosine[:, None, :]
    sin_part = sine_vals[:, None, :]
    return jnp.concatenate([first * cos_part - second * sin_part, second * cos_part + first * sin_part, values[..., ROT:]], axis=-1)

def rotate_back(grads, cosine, sine_vals):
    half_rot = ROT // 2
    first = grads[..., :half_rot]
    second = grads[..., half_rot:ROT]
    cos_part = cosine[:, None, :]
    sin_part = sine_vals[:, None, :]
    return jnp.concatenate([first * cos_part + second * sin_part, second * cos_part - first * sin_part, grads[..., ROT:]], axis=-1)

def gelu_value(pre_act):
    return 0.5 * pre_act * (1.0 + lax.erf(pre_act * 0.7071067811865476))

def gelu_slope(pre_act):
    return 0.5 * (1.0 + lax.erf(pre_act * 0.7071067811865476)) + pre_act * 0.3989422804014327 * jnp.exp(-0.5 * pre_act * pre_act)

def reference(block_input, out_grad, ln1_gain, ln1_bias, ln2_gain, ln2_bias, w_qkv, b_qkv, w_dense, b_dense, w_fc, b_fc, w_proj, b_proj):
    seq_count = TOKENS // SEQ
    cosine, sine_vals = angle_tables(SEQ)
    scale = 1.0 / math.sqrt(HD)
    causal = jnp.arange(SEQ)[:, None] >= jnp.arange(SEQ)[None, :]

    def step_fn(totals, inputs):
        rows, grad_rows = inputs
        mean_row = lax.optimization_barrier(jnp.mean(rows, axis=1, keepdims=True))
        var_row = lax.optimization_barrier(jnp.mean(rows * rows, axis=1, keepdims=True)) - mean_row * mean_row
        inv_std = lax.rsqrt(var_row + epsilon)
        x_hat = (rows - mean_row) * inv_std
        normed_one = (x_hat * ln1_gain + ln1_bias).astype(jnp.bfloat16)
        normed_two = (x_hat * ln2_gain + ln2_bias).astype(jnp.bfloat16)
        qkv_pre = (jnp.dot(normed_one, w_qkv, preferred_element_type=jnp.float32) + b_qkv).reshape(SEQ, HEADS, 3, HD)
        query = rotate_fwd(qkv_pre[:, :, 0], cosine, sine_vals).astype(jnp.bfloat16)
        keys = rotate_fwd(qkv_pre[:, :, 1], cosine, sine_vals).astype(jnp.bfloat16)
        values = qkv_pre[:, :, 2].astype(jnp.bfloat16)
        query_f = query.astype(jnp.float32)
        keys_f = keys.astype(jnp.float32)
        values_f = values.astype(jnp.float32)
        scores = jnp.einsum('qhd,khd->hqk', query_f, keys_f) * scale
        masked = jnp.where(causal[None], scores, -1e+30)
        row_max = lax.optimization_barrier(jnp.max(masked, axis=-1, keepdims=True))
        exp_sum = lax.optimization_barrier(jnp.sum(jnp.where(causal[None], jnp.exp(masked - row_max), 0.0), axis=-1, keepdims=True))
        log_total = row_max + jnp.log(exp_sum)
        probs = jnp.where(causal[None], jnp.exp(masked - log_total), 0.0)
        probs_low = probs.astype(jnp.bfloat16)
        attended = jnp.einsum('hqk,khd->qhd', probs_low.astype(jnp.float32), values_f).astype(jnp.bfloat16)
        attn_out = attended.reshape(SEQ, D)
        fc_pre = jnp.dot(normed_two, w_fc, preferred_element_type=jnp.float32) + b_fc
        gelu_out = gelu_value(fc_pre).astype(jnp.bfloat16)
        branch_sum = jnp.dot(attn_out, w_dense, preferred_element_type=jnp.float32) + jnp.dot(gelu_out, w_proj, preferred_element_type=jnp.float32)
        out_rows = rows + branch_sum + b_dense + b_proj
        grad_low = grad_rows.astype(jnp.bfloat16)
        dense_grad = jnp.dot(attn_out.T, grad_low, preferred_element_type=jnp.float32)
        proj_grad = jnp.dot(gelu_out.T, grad_low, preferred_element_type=jnp.float32)
        out_bias_grad = lax.optimization_barrier(jnp.sum(grad_rows, axis=0))
        attn_grad = jnp.dot(grad_low, w_dense.T, preferred_element_type=jnp.float32).astype(jnp.bfloat16)
        fc_grad = jnp.dot(grad_low, w_proj.T, preferred_element_type=jnp.float32) * gelu_slope(fc_pre)
        fc_bias_grad = lax.optimization_barrier(jnp.sum(fc_grad, axis=0))
        fc_grad_low = fc_grad.astype(jnp.bfloat16)
        head_grad = attn_grad.reshape(SEQ, HEADS, HD).astype(jnp.float32)
        value_grad = jnp.einsum('hqk,qhd->khd', probs_low.astype(jnp.float32), head_grad)
        prob_grad = jnp.einsum('qhd,khd->hqk', head_grad, values_f)
        delta_row = jnp.transpose(lax.optimization_barrier(jnp.sum(head_grad * attended.astype(jnp.float32), axis=-1)), (1, 0))[:, :, None]
        score_grad = (probs * (prob_grad - delta_row) * scale).astype(jnp.bfloat16).astype(jnp.float32)
        query_grad = rotate_back(jnp.einsum('hqk,khd->qhd', score_grad, keys_f), cosine, sine_vals)
        key_grad = rotate_back(jnp.einsum('hqk,qhd->khd', score_grad, query_f), cosine, sine_vals)
        qkv_grad = jnp.stack([query_grad, key_grad, value_grad], axis=2).reshape(SEQ, 3 * D)
        qkv_bias_grad = lax.optimization_barrier(jnp.sum(qkv_grad, axis=0))
        qkv_grad_low = qkv_grad.astype(jnp.bfloat16)
        qkv_weight_grad = jnp.dot(normed_one.T, qkv_grad_low, preferred_element_type=jnp.float32)
        fc_weight_grad = jnp.dot(normed_two.T, fc_grad_low, preferred_element_type=jnp.float32)
        grad_one = jnp.dot(qkv_grad_low, w_qkv.T, preferred_element_type=jnp.float32)
        grad_two = jnp.dot(fc_grad_low, w_fc.T, preferred_element_type=jnp.float32)
        hat_grad = grad_one * ln1_gain + grad_two * ln2_gain
        in_rows = grad_rows + inv_std * (hat_grad - lax.optimization_barrier(jnp.mean(hat_grad, axis=1, keepdims=True)) - x_hat * lax.optimization_barrier(jnp.mean(hat_grad * x_hat, axis=1, keepdims=True)))
        terms = (lax.optimization_barrier(jnp.sum(grad_one * x_hat, axis=0)), lax.optimization_barrier(jnp.sum(grad_one, axis=0)), lax.optimization_barrier(jnp.sum(grad_two * x_hat, axis=0)), lax.optimization_barrier(jnp.sum(grad_two, axis=0)), qkv_weight_grad, qkv_bias_grad, dense_grad, out_bias_grad, fc_weight_grad, fc_bias_grad, proj_grad)
        new_totals = tuple((old + new for old, new in zip(totals, terms)))
        return (new_totals, (out_rows, in_rows))
    zero_width = jnp.zeros((D,), jnp.float32)
    initial = (zero_width, zero_width, zero_width, zero_width, jnp.zeros((D, 3 * D), jnp.float32), jnp.zeros((3 * D,), jnp.float32), jnp.zeros((D, D), jnp.float32), zero_width, jnp.zeros((D, FF), jnp.float32), jnp.zeros((FF,), jnp.float32), jnp.zeros((FF, D), jnp.float32))
    totals, (out_all, in_all) = lax.scan(step_fn, initial, (block_input.reshape(seq_count, SEQ, D), out_grad.reshape(seq_count, SEQ, D)))
    return (out_all.reshape(TOKENS, D), in_all.reshape(TOKENS, D), totals[0], totals[1], totals[2], totals[3], totals[4], totals[5], totals[6], totals[7], totals[8], totals[9], totals[10], totals[7])
```

```python
import functools
import math

import jax
import jax.numpy as jnp
import numpy as np
from jax import lax
from jax.experimental import pallas as pl
from jax.experimental.pallas import tpu as pltpu
from jax.sharding import PartitionSpec as P

D = 2048
HD = 256
ROT = 64
SEQ = 512


epsilon = 1e-05
contract_last = (((1,), (1,)), ((), ()))
contract_first = (((0,), (0,)), ((), ()))


def angle_tables(length):
    half_rot = ROT // 2
    position = jnp.arange(length, dtype=jnp.float32)
    exponent = jnp.arange(half_rot, dtype=jnp.float32) * (2.0 / ROT)
    frequency = 10000.0 ** (-exponent)
    angles = position[:, None] * frequency[None, :]
    return (jnp.cos(angles), jnp.sin(angles))


def rotate_fwd(values, cosine, sine_vals):
    half_rot = ROT // 2
    first = values[..., :half_rot]
    second = values[..., half_rot:ROT]
    cos_part = cosine[:, None, :]
    sin_part = sine_vals[:, None, :]
    return jnp.concatenate(
        [
            first * cos_part - second * sin_part,
            second * cos_part + first * sin_part,
            values[..., ROT:],
        ],
        axis=-1,
    )


def rotate_back(grads, cosine, sine_vals):
    half_rot = ROT // 2
    first = grads[..., :half_rot]
    second = grads[..., half_rot:ROT]
    cos_part = cosine[:, None, :]
    sin_part = sine_vals[:, None, :]
    return jnp.concatenate(
        [
            first * cos_part + second * sin_part,
            second * cos_part - first * sin_part,
            grads[..., ROT:],
        ],
        axis=-1,
    )


def gelu_value(pre_act):
    return 0.5 * pre_act * (1.0 + lax.erf(pre_act * 0.7071067811865476))


def gelu_slope(pre_act):
    return 0.5 * (
        1.0 + lax.erf(pre_act * 0.7071067811865476)
    ) + pre_act * 0.3989422804014327 * jnp.exp(-0.5 * pre_act * pre_act)


def shards(
    block_input,
    out_grad,
    ln1_gain,
    ln1_bias,
    ln2_gain,
    ln2_bias,
    w_qkv,
    b_qkv,
    w_dense,
    b_dense,
    w_fc,
    b_fc,
    w_proj,
    b_proj,
):
    tok_rows = block_input.shape[0]
    seq_count = tok_rows // SEQ
    qkv_cols = w_qkv.shape[1]
    fc_cols = w_fc.shape[1]
    local_heads = qkv_cols // (3 * HD)
    head_cols = local_heads * HD
    scale = 1.0 / math.sqrt(HD)
    cosine, sine_vals = angle_tables(SEQ)
    causal = jnp.arange(SEQ)[:, None] >= jnp.arange(SEQ)[None, :]
    row_total, square_total = lax.psum(
        (jnp.sum(block_input, axis=1), jnp.sum(block_input * block_input, axis=1)), "col"
    )
    mean_row = (row_total / D)[:, None]
    var_row = (square_total / D)[:, None] - mean_row * mean_row
    inv_std = lax.rsqrt(var_row + epsilon)
    x_hat = (block_input - mean_row) * inv_std
    normed_one = (x_hat * ln1_gain + ln1_bias).astype(jnp.bfloat16)
    normed_two = (x_hat * ln2_gain + ln2_bias).astype(jnp.bfloat16)
    wide_one, wide_two = (
        lax.all_gather(normed_one, "col", axis=1, tiled=True),
        lax.all_gather(normed_two, "col", axis=1, tiled=True),
    )
    part_one = wide_one
    part_two = wide_two
    qkv_pre = jnp.dot(
        part_one,
        lax.all_gather(w_qkv, "row", axis=0, tiled=True),
        preferred_element_type=jnp.float32,
    )
    fc_pre = jnp.dot(
        part_two,
        lax.all_gather(w_fc, "row", axis=0, tiled=True),
        preferred_element_type=jnp.float32,
    )
    qkv_pre = qkv_pre + b_qkv
    fc_pre = fc_pre + b_fc

    def forward_seq(block):
        query = rotate_fwd(block[:, :, 0], cosine, sine_vals).astype(jnp.bfloat16)
        keys = rotate_fwd(block[:, :, 1], cosine, sine_vals).astype(jnp.bfloat16)
        values = block[:, :, 2].astype(jnp.bfloat16)
        scores = jnp.einsum("qhd,khd->hqk", query, keys, preferred_element_type=jnp.float32) * scale
        masked = jnp.where(causal[None], scores, -1e30)
        row_max = jnp.max(masked, axis=-1, keepdims=True)
        exp_sum = jnp.sum(
            jnp.where(causal[None], jnp.exp(masked - row_max), 0.0), axis=-1, keepdims=True
        )
        log_total = row_max + jnp.log(exp_sum)
        probs_low = jnp.where(causal[None], jnp.exp(masked - log_total), 0.0).astype(jnp.bfloat16)
        attended = jnp.einsum(
            "hqk,khd->qhd", probs_low, values, preferred_element_type=jnp.float32
        ).astype(jnp.bfloat16)
        return (query, keys, values, attended, log_total)

    query, keys, values, attended, log_total = lax.map(
        forward_seq, qkv_pre.reshape(seq_count, SEQ, local_heads, 3, HD)
    )
    attn_out = attended.reshape(tok_rows, head_cols)
    gelu_out = gelu_value(fc_pre).astype(jnp.bfloat16)
    out_stack = jnp.concatenate([w_dense, w_proj], axis=0)
    shard_piece = lax.all_gather(out_stack, "row", axis=1, tiled=True)
    mixed = jnp.dot(
        attn_out, shard_piece[:head_cols], preferred_element_type=jnp.float32
    ) + jnp.dot(gelu_out, shard_piece[head_cols:], preferred_element_type=jnp.float32)
    branch_sum = lax.psum_scatter(mixed, "col", scatter_dimension=1, tiled=True)
    block_output = block_input + branch_sum + b_dense + b_proj
    grad_low = out_grad.astype(jnp.bfloat16)
    wide_grad = lax.all_gather(grad_low, "col", axis=1, tiled=True)
    both_grad = lax.dot_general(
        wide_grad,
        lax.all_gather(out_stack, "row", axis=1, tiled=True),
        contract_last,
        preferred_element_type=jnp.float32,
    )
    attn_grad = both_grad[:, :head_cols]
    gelu_grad = both_grad[:, head_cols:]
    attn_grad_low = attn_grad.astype(jnp.bfloat16)
    fc_grad = gelu_grad * gelu_slope(fc_pre)
    fc_bias_grad = jnp.sum(fc_grad, axis=0)
    fc_grad_low = fc_grad.astype(jnp.bfloat16)

    def backward_seq(items):
        query_s, keys_s, values_s, attended_s, log_s, head_grad = items
        scores = (
            jnp.einsum("qhd,khd->hqk", query_s, keys_s, preferred_element_type=jnp.float32) * scale
        )
        probs = jnp.where(
            causal[None], jnp.exp(jnp.where(causal[None], scores, -1e30) - log_s), 0.0
        )
        probs_low = probs.astype(jnp.bfloat16)
        value_grad = jnp.einsum(
            "hqk,qhd->khd", probs_low, head_grad, preferred_element_type=jnp.float32
        )
        prob_grad = jnp.einsum(
            "qhd,khd->hqk", head_grad, values_s, preferred_element_type=jnp.float32
        )
        delta_row = jnp.transpose(
            jnp.sum(head_grad.astype(jnp.float32) * attended_s.astype(jnp.float32), axis=-1), (1, 0)
        )[:, :, None]
        score_grad = (probs * (prob_grad - delta_row) * scale).astype(jnp.bfloat16)
        query_grad = jnp.einsum(
            "hqk,khd->qhd", score_grad, keys_s, preferred_element_type=jnp.float32
        )
        key_grad = jnp.einsum(
            "hqk,qhd->khd", score_grad, query_s, preferred_element_type=jnp.float32
        )
        return jnp.stack(
            [
                rotate_back(query_grad, cosine, sine_vals),
                rotate_back(key_grad, cosine, sine_vals),
                value_grad,
            ],
            axis=2,
        )

    head_grads = attn_grad_low.reshape(seq_count, SEQ, local_heads, HD)
    qkv_grad = lax.map(
        backward_seq, (query, keys, values, attended, log_total, head_grads)
    ).reshape(tok_rows, qkv_cols)
    qkv_bias_grad = jnp.sum(qkv_grad, axis=0)
    qkv_grad_low = qkv_grad.astype(jnp.bfloat16)
    in_stack = jnp.concatenate([w_qkv, w_fc], axis=1)
    shard_piece = lax.all_gather(in_stack, "row", axis=0, tiled=True)
    norm_grads = jnp.stack(
        [
            lax.dot_general(
                qkv_grad_low,
                shard_piece[:, :qkv_cols],
                contract_last,
                preferred_element_type=jnp.float32,
            ),
            lax.dot_general(
                fc_grad_low,
                shard_piece[:, qkv_cols:],
                contract_last,
                preferred_element_type=jnp.float32,
            ),
        ]
    )
    part_one = wide_one
    part_two = wide_two
    row_part = lax.psum_scatter(
        jnp.concatenate(
            [
                lax.dot_general(
                    part_one, qkv_grad_low, contract_first, preferred_element_type=jnp.float32
                ),
                lax.dot_general(
                    part_two, fc_grad_low, contract_first, preferred_element_type=jnp.float32
                ),
                lax.dot_general(
                    wide_grad, attn_out, contract_first, preferred_element_type=jnp.float32
                ),
                lax.dot_general(
                    wide_grad, gelu_out, contract_first, preferred_element_type=jnp.float32
                ),
            ],
            axis=1,
        ),
        "row",
        scatter_dimension=0,
        tiled=True,
    )
    grad_rows = lax.psum(row_part, "dp")
    qkv_total = grad_rows[:, :qkv_cols]
    fc_total = grad_rows[:, qkv_cols : qkv_cols + fc_cols]
    dense_total = grad_rows[:, qkv_cols + fc_cols : qkv_cols + fc_cols + head_cols].T
    proj_total = grad_rows[:, qkv_cols + fc_cols + head_cols :].T
    norm_local = lax.psum_scatter(norm_grads, "col", scatter_dimension=2, tiled=True)
    grad_one = norm_local[0]
    grad_two = norm_local[1]
    hat_grad = grad_one * ln1_gain + grad_two * ln2_gain
    total_hat, total_cross = lax.psum(
        (jnp.sum(hat_grad, axis=1), jnp.sum(hat_grad * x_hat, axis=1)), "col"
    )
    input_grad = out_grad + inv_std * (
        hat_grad - (total_hat / D)[:, None] - x_hat * (total_cross / D)[:, None]
    )
    gain_one, shift_one, gain_two, shift_two, qkv_bias_total, fc_bias_total, out_bias_total = (
        lax.psum(
            (
                jnp.sum(grad_one * x_hat, axis=0),
                jnp.sum(grad_one, axis=0),
                jnp.sum(grad_two * x_hat, axis=0),
                jnp.sum(grad_two, axis=0),
                qkv_bias_grad,
                fc_bias_grad,
                jnp.sum(out_grad, axis=0),
            ),
            ("dp", "row"),
        )
    )
    return (
        block_output,
        input_grad,
        gain_one,
        shift_one,
        gain_two,
        shift_two,
        qkv_total,
        qkv_bias_total,
        dense_total,
        out_bias_total,
        fc_total,
        fc_bias_total,
        proj_total,
        out_bias_total,
    )


f32 = jnp.float32
bf16 = jnp.bfloat16
MESH = pl.DeviceIdType.MESH
VMEM = pltpu.VMEM
Q = 256
HALF = 4 * Q


def flip(a, b):
    return a + b - 2 * a * b


def span(start, size):
    return pl.ds(pl.multiple_of(start, size), size)


def mm(a, b):
    return jnp.dot(a, b, preferred_element_type=f32)


def mm_nt(a, b):
    return lax.dot_general(a, b, (((1,), (1,)), ((), ())), preferred_element_type=f32)


def mm_tn(a, b):
    return lax.dot_general(a, b, (((0,), (0,)), ((), ())), preferred_element_type=f32)


class Net:
    def __init__(self, send_sems, recv_sems, local_sems):
        self.k = lax.axis_index("dp")
        self.r = lax.axis_index("row")
        self.c = lax.axis_index("col")
        k, r, c = self.k, self.r, self.c
        self.core = (1 - k, r, c)
        self.x = (k, r + 1 - 2 * (r % 2), c)
        self.y = (k, r + 2 - 4 * (r // 2), c)
        near = c + 1 - 2 * (c % 2)
        self.z = (None, (k, r, near), (k, r, c + 2 - 4 * (c // 2)), (k, r, 3 - c))
        self.middle = flip(c % 2, c // 2) == 1
        self.send_sems, self.recv_sems, self.local_sems = send_sems, recv_sems, local_sems
        self.remote_count = 0
        self.local_count = 0
        self.pending = []

    def mix(self, j):
        return flip(j % 2, flip(self.c % 2, self.r % 2)) + 2 * flip(
            j // 2, flip(self.c // 2, self.r // 2)
        )

    def barrier(self):
        sem = pltpu.get_barrier_semaphore()
        peers = (self.core, self.x, self.y) + self.z[1:]
        for peer in peers:
            pl.semaphore_signal(sem, inc=1, device_id=peer, device_id_type=MESH)
        pl.semaphore_wait(sem, len(peers))

    def slot(self):
        self.remote_count += 1
        return self.remote_count - 1

    def remote(self, src, dst, peer):
        slot = self.slot()
        copy = pltpu.make_async_remote_copy(
            src_ref=src,
            dst_ref=dst,
            send_sem=self.send_sems.at[slot],
            recv_sem=self.recv_sems.at[slot],
            device_id=peer,
            device_id_type=MESH,
        )
        copy.start()
        self.pending.append(copy)
        return copy

    def local(self, src, dst):
        copy = pltpu.make_async_copy(src, dst, self.local_sems.at[self.local_count])
        self.local_count += 1
        copy.start()
        return copy

    def drain(self):
        for copy in self.pending:
            copy.wait_send()


class Gather:
    def __init__(self, net, shard, full, by_rows):
        self.net, self.shard, self.full, self.by_rows = net, shard, full, by_rows
        self.depth = Q // 2 if by_rows else shard.shape[0] // 2
        self.placed = []

    def own(self, half, part=None):
        if self.by_rows:
            if part is None:
                return self.shard.at[span(half * Q, Q), :]
            return self.shard.at[span(half * Q + part * self.depth, self.depth), :]
        rows = slice(None) if part is None else pl.ds(part * self.depth, self.depth)
        return self.shard.at[rows, span(half * Q, Q)]

    def chunk(self, s, i, part=None):
        start = s * HALF + i * Q
        if self.by_rows:
            if part is None:
                return self.full.at[pl.ds(start, Q), :]
            return self.full.at[pl.ds(start + part * self.depth, self.depth), :]
        rows = slice(None) if part is None else pl.ds(part * self.depth, self.depth)
        return self.full.at[rows, pl.ds(start, Q)]

    def place_own(self):
        net = self.net
        self.placed = [
            net.local(self.own(net.k), self.chunk(0, 0)),
            net.local(self.own(1 - net.k), self.chunk(1, 0)),
        ]

    def send_own(self):
        net, k = self.net, self.net.k
        self.y0 = net.remote(self.own(k, 0), self.chunk(0, 2, 0), net.y)
        self.x1 = net.remote(self.own(k, 1), self.chunk(0, 1, 1), net.x)
        self.y1 = net.remote(self.own(k, 1), self.chunk(0, 2, 1), net.y)
        self.x0 = net.remote(self.own(k, 0), self.chunk(0, 1, 0), net.x)

    def forward(self):
        net = self.net
        self.y0.wait_recv()
        self.d0 = net.remote(self.chunk(0, 2, 0), self.chunk(0, 3, 0), net.x)
        self.x1.wait_recv()
        self.d1 = net.remote(self.chunk(0, 1, 1), self.chunk(0, 3, 1), net.y)

    def swap_near(self):
        net = self.net
        self.x0.wait_recv()
        self.c1 = net.remote(self.chunk(0, 1), self.chunk(1, 1), net.core)
        self.y1.wait_recv()
        self.c2 = net.remote(self.chunk(0, 2), self.chunk(1, 2), net.core)

    def swap_far(self):
        net = self.net
        self.d0.wait_recv()
        self.d1.wait_recv()
        self.c3 = net.remote(self.chunk(0, 3), self.chunk(1, 3), net.core)

    def ready(self):
        for copy in (self.c1, self.c2, self.c3):
            copy.wait_recv()
        for copy in self.placed:
            copy.wait()


class Line:
    def __init__(self, net, slots):
        self.net, self.slots = net, slots
        self.ids = [None] + [net.slot() for _ in range(3)]
        self.sends = []

    def copy(self, src, dst, peer, send):
        net = self.net
        return pltpu.make_async_remote_copy(
            src_ref=self.slots.at[src],
            dst_ref=self.slots.at[dst],
            send_sem=net.send_sems.at[send],
            recv_sem=net.recv_sems.at[self.ids[dst]],
            device_id=peer,
            device_id_type=MESH,
        )

    def start(self):
        net = self.net
        first = self.copy(0, 1, net.z[1], self.ids[1])
        first.start()
        net.pending.append(first)
        self.hops = [
            self.copy(0, 3, net.z[3], self.ids[2]),
            self.copy(1, 2, net.z[3], self.ids[3]),
            self.copy(3, 2, net.z[1], net.slot()),
            self.copy(2, 3, net.z[1], net.slot()),
        ]

        @pl.when(net.middle)
        def _():
            self.hops[0].start()

    def arrived(self, slot):
        return self.copy(0, slot, self.net.z[1], self.ids[slot])

    def step(self, number):
        slot = (1, 3, 2)[number]

        @pl.when(self.net.middle)
        def _():
            self.arrived(slot).wait_recv()
            self.hops[number + 1].start()

    def ready(self):
        @pl.when(jnp.logical_not(self.net.middle))
        def _():
            for slot in (1, 2, 3):
                self.arrived(slot).wait_recv()

    def drain(self):
        @pl.when(self.net.middle)
        def _():
            for hop in self.hops:
                hop.wait_send()


def turn(low, tables, sign):
    swing = tables[1] * pltpu.roll(low, 96, 1) + tables[2] * pltpu.roll(low, 32, 1)
    return low * tables[0] + sign * swing


def gather_kernel(
    x, og, norms, w_qkv, w_dense, w_fc, w_proj, b_qkv, b_fc, tables,
    o_proj, o_fc, o_dense, o_h2, o_dy, o_dys, o_g, o_slope, o_attn, o_hat, o_xh,
    r_proj, r_qkv, r_dense, o_stats, o_vecs, o_bias,
    g_qkv, g_dense, g_fc, xs, dys_in, pks, stats, rows, h1c, h1s, h2c, h2s, dyc, dys, xh,
    qb, kb, vb, probs, probs_low, score_low, oc, dob, dqc, gc, slope, hat, stage, r_q, r_d,
    send_sems, recv_sems, local_sems, stage_sems,
):
    tok = x.shape[0]
    heads = qb.shape[0]
    scale = 1.0 / math.sqrt(HD)
    net = Net(send_sems, recv_sems, local_sems)
    net.barrier()
    qkv = Gather(net, w_qkv, g_qkv, True)
    dense = Gather(net, w_dense, g_dense, False)
    fc = Gather(net, w_fc, g_fc, True)
    proj = Gather(net, w_proj, o_proj, False)
    qkv.send_own()
    dense.send_own()

    step = 128
    lane = lax.broadcasted_iota(jnp.int32, (step, 128), 1)
    o_bias[...] = jnp.zeros_like(o_bias)

    def local_norm(n, _):
        at = span(n * step, step)
        block = x[at, :]
        mean = jnp.mean(block, axis=1, keepdims=True)
        centred = block - mean
        var = jnp.mean(centred * centred, axis=1, keepdims=True)
        xs[0, at, :] = (centred * lax.rsqrt(var + epsilon)).astype(bf16)
        stats[at, :] = jnp.where(lane == 0, mean, jnp.where(lane == 1, var, 0.0))
        return 0

    lax.fori_loop(0, tok // step, local_norm, 0)
    pks[0] = stats[...].T[0:8]
    pks[0, 2:6, :] = norms[...]
    packs = [net.remote(pks.at[0], pks.at[j], net.z[j]) for j in (1, 2, 3)]
    x_line = Line(net, xs)
    x_line.start()
    for weight in (qkv, dense, fc):
        weight.place_own()

    def local_grad(n, _):
        at = span(n * step, step)
        block = og[at, :]
        dys_in[0, at, :] = block.astype(bf16)
        o_bias[1:2, 0:512] += jnp.sum(block, axis=0, keepdims=True)
        return 0

    lax.fori_loop(0, tok // step, local_grad, 0)
    qkv.forward()
    x_line.step(0)
    x_line.step(1)
    fc.send_own()
    dense.forward()
    qkv.swap_near()
    x_line.step(2)
    y_line = Line(net, dys_in)
    y_line.start()
    dense.swap_near()
    qkv.swap_far()
    dense.swap_far()

    for pack in packs:
        pack.wait_recv()
    means = [pks[j, 0:1, :] for j in range(4)]
    vars_ = [pks[j, 1:2, :] for j in range(4)]
    mu = (means[0] + means[1] + means[2] + means[3]) * 0.25
    spread = [vars_[j] + (means[j] - mu) * (means[j] - mu) for j in range(4)]
    rstd = lax.rsqrt((spread[0] + spread[1] + spread[2] + spread[3]) * 0.25 + epsilon)
    rows[...] = jnp.zeros_like(rows)
    for j in range(4):
        rows[j : j + 1, :] = jnp.sqrt(vars_[j] + epsilon) * rstd
        rows[4 + j : 5 + j, :] = (means[j] - mu) * rstd
    rows[8:9, :] = mu
    rows[9:10, :] = rstd
    stats[...] = rows[...].T
    o_stats[...] = stats[...]
    x_line.ready()
    for s in range(2):
        for j in range(4):
            lanes = span(flip(s, net.k) * Q, Q)
            dest = span(net.mix(j) * Q, Q)
            wide = span(s * HALF + net.mix(j) * Q, Q)
            o_vecs[0:4, wide] = pks[j, 2:6, lanes]

            def norm(n, _, s=s, j=j, lanes=lanes, dest=dest, wide=wide):
                at = span(n * step, step)
                hat_x = xs[j, at, lanes].astype(f32) * stats[at, j : j + 1] + stats[at, 4 + j : 5 + j]
                xh[at, wide] = hat_x.astype(bf16)
                one = hat_x * pks[j, 2:3, lanes] + pks[j, 3:4, lanes]
                two = hat_x * pks[j, 4:5, lanes] + pks[j, 5:6, lanes]
                (h1s if s else h1c)[at, dest] = one.astype(bf16)
                (h2s if s else h2c)[at, dest] = two.astype(bf16)
                return 0

            lax.fori_loop(0, tok // step, norm, 0)
    swaps = [
        net.remote(h1s, h1c.at[pl.ds(tok, tok), :], net.core),
        net.remote(h2s, h2c.at[pl.ds(tok, tok), :], net.core),
    ]
    mine = pl.ds(0, tok)
    theirs = pl.ds(tok, tok)
    fc.forward()
    y_line.step(0)
    qkv.ready()

    def project(n, _):
        cols = span(n * 3 * HD, 3 * HD)
        acc = mm(h1c[mine, :], g_qkv[0:HALF, cols]) + mm(h1s[...], g_qkv[HALF:, cols])
        acc = acc + b_qkv[:, cols]
        qb[n, :, 0:128] = turn(acc[:, 0:128], tables, 1.0).astype(bf16)
        qb[n, :, 128:HD] = acc[:, 128:HD].astype(bf16)
        kb[n, :, 0:128] = turn(acc[:, HD : HD + 128], tables, 1.0).astype(bf16)
        kb[n, :, 128:HD] = acc[:, HD + 128 : 2 * HD].astype(bf16)
        vb[n] = acc[:, 2 * HD :].astype(bf16)
        return 0

    lax.fori_loop(0, heads, project, 0)
    proj.send_own()
    y_line.step(1)

    chunks = tok // step

    def attend(n, _):
        head, chunk = n // chunks, n % chunks
        at = span(chunk * step, step)
        scores = mm_nt(qb[head, at, :], kb[head]) * scale
        token = lax.broadcasted_iota(jnp.int32, (step, tok), 0) + chunk * step
        allowed = token >= lax.broadcasted_iota(jnp.int32, (step, tok), 1)
        scores = jnp.where(allowed, scores, -1e30)
        top = jnp.max(scores, axis=1, keepdims=True)
        raised = jnp.where(allowed, jnp.exp(scores - top), 0.0)
        weight = raised / jnp.sum(raised, axis=1, keepdims=True)
        probs[head, at, :] = weight
        low = weight.astype(bf16)
        probs_low[head, at, :] = low
        oc[at, span(head * HD, HD)] = mm(low, vb[head]).astype(bf16)
        return 0

    lax.fori_loop(0, heads * chunks, attend, 0)
    swaps.append(net.remote(oc.at[mine, :], oc.at[theirs, :], net.core))
    outs = [net.local(oc.at[mine, :], o_attn)]
    fc.swap_near()
    y_line.step(2)
    fc.swap_far()
    fc.ready()
    outs.append(net.local(g_fc, o_fc))

    def expand(n, _):
        cols = span(n * 512, 512)
        a = mm(h2c[mine, :], g_fc[0:HALF, cols]) + mm(h2s[...], g_fc[HALF:, cols])
        a = a + b_fc[:, cols]
        rise = 0.5 * (1.0 + lax.erf(a * 0.7071067811865476))
        gc[mine, cols] = (a * rise).astype(bf16)
        slope[:, cols] = (rise + a * 0.3989422804014327 * jnp.exp(-0.5 * a * a)).astype(bf16)
        return 0

    lax.fori_loop(0, gc.shape[1] // 512, expand, 0)
    swaps.append(net.remote(gc.at[mine, :], gc.at[theirs, :], net.core))
    outs.append(net.local(gc.at[mine, :], o_g))
    outs.append(net.local(slope, o_slope))
    outs.append(net.local(xh, o_xh))
    proj.forward()

    y_line.ready()
    for s in range(2):
        for j in range(4):
            lanes = span(flip(s, net.k) * Q, Q)
            dest = span(net.mix(j) * Q, Q)
            (dys if s else dyc)[mine, dest] = dys_in[j, :, lanes]
    swaps.append(net.remote(dys, dyc.at[theirs, :], net.core))
    outs.append(net.local(dyc.at[mine, :], o_dy))
    outs.append(net.local(dys, o_dys))
    dense.ready()
    outs.append(net.local(g_dense, o_dense))
    dob[...] = (
        mm_nt(dyc[mine, :], g_dense[:, 0:HALF]) + mm_nt(dys[...], g_dense[:, HALF:])
    ).astype(bf16)

    def keep(head, part, at, value, rotated):
        base = head * 3 * HD + part * HD
        if rotated:
            low = turn(value[:, 0:128], [tables[t, at, :] for t in range(3)], -1.0)
            dqc[at, pl.ds(pl.multiple_of(base, 128), 128)] = low.astype(bf16)
            o_bias[0:1, pl.ds(pl.multiple_of(base, 128), 128)] += jnp.sum(low, axis=0, keepdims=True)
            value, base, width = value[:, 128:], base + 128, 128
        else:
            width = HD
        cols = pl.ds(pl.multiple_of(base, 128), width)
        dqc[at, cols] = value.astype(bf16)
        o_bias[0:1, cols] += jnp.sum(value, axis=0, keepdims=True)

    def attend_back(head, _):
        cols = span(head * HD, HD)

        def chunk_back(n, _):
            at = span(n * step, step)
            grad = dob[at, cols]
            delta = jnp.sum(grad.astype(f32) * oc[at, cols].astype(f32), axis=1, keepdims=True)
            spread = mm_nt(grad, vb[head]) - delta
            low = (probs[head, at, :] * spread * scale).astype(bf16)
            score_low[at, :] = low
            keep(head, 0, at, mm(low, kb[head]), True)
            return 0

        lax.fori_loop(0, chunks, chunk_back, 0)
        whole = pl.ds(0, tok)
        keep(head, 1, whole, mm_tn(score_low[...], qb[head]), True)
        keep(head, 2, whole, mm_tn(probs_low[head], dob[:, cols]), False)
        return 0

    lax.fori_loop(0, heads, attend_back, 0)
    swaps.append(net.remote(dqc.at[mine, :], dqc.at[theirs, :], net.core))
    for copy in swaps:
        copy.wait_recv()
    outs.append(net.local(h2c, o_h2))
    proj.swap_near()

    def grad_proj(n, _):
        cols = span(n * 512, 512)
        part = mm_tn(gc[:, cols], dyc[...]).astype(bf16)
        slot = n % 2
        copy = pltpu.make_async_copy(stage.at[slot], r_proj.at[cols, :], stage_sems.at[slot])

        @pl.when(n >= 2)
        def _():
            copy.wait()

        stage[slot] = part
        copy.start()
        return 0

    lax.fori_loop(0, gc.shape[1] // 512, grad_proj, 0)
    for slot in range(2):
        pltpu.make_async_copy(stage.at[slot], r_proj.at[0:512, :], stage_sems.at[slot]).wait()

    def grad_qkv(n, _):
        cols = span(n * 512, 512)
        r_q[:, cols] = mm_tn(h1c[...], dqc[:, cols]).astype(bf16)
        return 0

    lax.fori_loop(0, dqc.shape[1] // 512, grad_qkv, 0)
    outs.append(net.local(r_q, r_qkv))
    r_d[...] = mm_tn(oc[...], dyc[...]).astype(bf16)
    outs.append(net.local(r_d, r_dense))
    proj.swap_far()

    def grad_norm(n, _):
        cols = span(n * 512, 512)
        grad = mm_nt(dqc[mine, :], g_qkv[cols, :])
        hat[:, cols] = (grad * o_vecs[0:1, cols]).astype(bf16)
        o_vecs[4:5, cols] = jnp.sum(grad * xh[:, cols].astype(f32), axis=0, keepdims=True)
        o_vecs[5:6, cols] = jnp.sum(grad, axis=0, keepdims=True)
        return 0

    lax.fori_loop(0, 2 * HALF // 512, grad_norm, 0)
    o_vecs[6:8, :] = jnp.zeros((2, 2 * HALF), f32)
    outs.append(net.local(hat, o_hat))
    proj.ready()
    for copy in outs:
        copy.wait()
    net.drain()
    x_line.drain()
    y_line.drain()


def call_gather(x, og, norms, w_qkv, w_dense, w_fc, w_proj, b_qkv, b_fc, tables):
    tok = x.shape[0]
    n_qkv, n_attn, n_fc = w_qkv.shape[1], w_dense.shape[0], w_fc.shape[1]
    heads = n_attn // HD
    wide = 2 * HALF
    any_spec = pl.BlockSpec(memory_space=pl.ANY)
    vmem = pl.BlockSpec(memory_space=VMEM)
    shape = jax.ShapeDtypeStruct
    outs = [
        shape((n_fc, wide), bf16), shape((wide, n_fc), bf16), shape((n_attn, wide), bf16),
        shape((2 * tok, HALF), bf16), shape((tok, HALF), bf16), shape((tok, HALF), bf16),
        shape((tok, n_fc), bf16), shape((tok, n_fc), bf16), shape((tok, n_attn), bf16),
        shape((tok, wide), bf16), shape((tok, wide), bf16),
        shape((n_fc, HALF), bf16), shape((HALF, n_qkv), bf16), shape((n_attn, HALF), bf16),
        shape((tok, 128), f32), shape((8, wide), f32), shape((8, wide), f32),
    ]
    scratch = [
        VMEM((wide, n_qkv), bf16), VMEM((n_attn, wide), bf16), VMEM((wide, n_fc), bf16),
        VMEM((4, tok, 512), bf16), VMEM((4, tok, 512), bf16), VMEM((4, 8, tok), f32),
        VMEM((tok, 128), f32), VMEM((128, tok), f32),
        VMEM((2 * tok, HALF), bf16), VMEM((tok, HALF), bf16),
        VMEM((2 * tok, HALF), bf16), VMEM((tok, HALF), bf16),
        VMEM((2 * tok, HALF), bf16), VMEM((tok, HALF), bf16), VMEM((tok, wide), bf16),
        VMEM((heads, tok, HD), bf16), VMEM((heads, tok, HD), bf16), VMEM((heads, tok, HD), bf16),
        VMEM((heads, tok, tok), f32), VMEM((heads, tok, tok), bf16), VMEM((tok, tok), bf16),
        VMEM((2 * tok, n_attn), bf16), VMEM((tok, n_attn), bf16), VMEM((2 * tok, n_qkv), bf16),
        VMEM((2 * tok, n_fc), bf16), VMEM((tok, n_fc), bf16), VMEM((tok, wide), bf16),
        VMEM((2, 512, HALF), bf16), VMEM((HALF, n_qkv), bf16), VMEM((n_attn, HALF), bf16),
        pltpu.SemaphoreType.DMA((64,)), pltpu.SemaphoreType.DMA((64,)),
        pltpu.SemaphoreType.DMA((32,)), pltpu.SemaphoreType.DMA((2,)),
    ]
    return pl.pallas_call(
        gather_kernel,
        name="gather_and_forward",
        out_shape=outs,
        in_specs=[vmem] * 3 + [any_spec] * 4 + [vmem] * 3,
        out_specs=[any_spec] * 14 + [vmem] * 3,
        scratch_shapes=scratch,
        compiler_params=pltpu.CompilerParams(
            collective_id=1, has_side_effects=True, vmem_limit_bytes=67043328
        ),
    )(x, og, norms, w_qkv, w_dense, w_fc, w_proj, b_qkv, b_fc, tables)


class Reduce:
    def __init__(self, net, partial, part, joined, near, far, by_rows):
        self.net, self.partial, self.by_rows = net, partial, by_rows
        self.part, self.joined, self.near, self.far = part, joined, near, far
        self.depth = Q // 2 if by_rows else partial.shape[0] // 2

    def chunk(self, i, half):
        if self.by_rows:
            return self.partial.at[pl.ds(i * Q + half * self.depth, self.depth), :]
        return self.partial.at[pl.ds(half * self.depth, self.depth), pl.ds(i * Q, Q)]

    def whole(self):
        if self.by_rows:
            return self.partial.at[pl.ds(0, Q), :]
        return self.partial.at[:, pl.ds(0, Q)]

    def rows(self, half):
        return pl.ds(half * self.depth, self.depth)

    def start(self):
        net = self.net
        self.loads = [
            net.local(self.chunk(2, 0), self.part.at[0]),
            net.local(self.chunk(1, 1), self.part.at[1]),
        ]
        self.a = net.remote(self.chunk(3, 0), self.joined.at[0], net.x)
        self.b = net.remote(self.chunk(3, 1), self.joined.at[1], net.y)
        self.near_a = net.remote(self.chunk(1, 0), self.near.at[self.rows(0), :], net.x)
        self.near_b = net.remote(self.chunk(2, 1), self.near.at[self.rows(1), :], net.y)

    def join(self):
        net = self.net
        hops = []
        for half, copy, peer in ((0, self.a, net.y), (1, self.b, net.x)):
            self.loads[half].wait()
            copy.wait_recv()
            tile = 64

            def add(n, _, half=half):
                at = span(n * tile, tile)
                total = self.joined[half, at, :].astype(f32) + self.part[half, at, :].astype(f32)
                self.part[half, at, :] = total.astype(bf16)
                return 0

            lax.fori_loop(0, self.depth // tile, add, 0)
            hops.append(net.remote(self.part.at[half], self.far.at[self.rows(half), :], peer))
        self.far_a, self.far_b = hops

    def finish(self, buffers, total, out):
        net = self.net
        loads = [net.local(self.whole(), buffers[0])]
        for copy in (self.near_a, self.near_b):
            copy.wait_recv()
        loads.append(net.local(self.near, buffers[1]))
        for copy in (self.far_a, self.far_b):
            copy.wait_recv()
        loads.append(net.local(self.far, buffers[2]))
        for copy in loads:
            copy.wait()
        tile = 64

        def add(n, _):
            at = span(n * tile, tile)
            parts = [buffer[at, :].astype(f32) for buffer in buffers]
            total[at, :] = parts[0] + parts[1] + parts[2]
            return 0

        lax.fori_loop(0, total.shape[0] // tile, add, 0)
        if self.by_rows:
            place = out.at[span(net.k * Q, Q), :]
        else:
            place = out.at[:, span(net.k * Q, Q)]
        return [net.local(total, place)], [net.remote(total, place, net.core)]


def reduce_kernel(
    w_proj, i_proj, i_fc, i_dense, i_h2, i_dy, i_dys, i_g, i_slope, i_attn, i_hat, i_xh,
    r_proj, r_qkv, r_dense, vecs, bias,
    o_proj, o_qkv, o_fc, o_dense, n_proj, f_proj, n_qkv, f_qkv, n_fc, f_fc, n_dense, f_dense,
    o_branch, o_hat, o_stats, o_small,
    g_proj, g_fc, g_dense, g, slope, attn, hat, xh, dy, dys, h2c, dab,
    out_send, out_recv, hat_send, hat_recv, p_proj, j_proj, p_qkv, j_qkv, p_fc, j_fc, p_dense, j_dense,
    part_fc, t_proj, t_qkv, t_fc, t_dense, packs, stats, sums, small,
    send_sems, recv_sems, local_sems,
):
    tok = g.shape[0]
    net = Net(send_sems, recv_sems, local_sems)
    net.barrier()
    proj = Reduce(net, r_proj, p_proj, j_proj, n_proj, f_proj, False)
    qkv = Reduce(net, r_qkv, p_qkv, j_qkv, n_qkv, f_qkv, True)
    fc = Reduce(net, part_fc, p_fc, j_fc, n_fc, f_fc, True)
    dense = Reduce(net, r_dense, p_dense, j_dense, n_dense, f_dense, False)
    load_g = [net.local(i_g, g), net.local(i_attn, attn), net.local(i_dense, g_dense)]
    for s, half in ((0, net.k), (1, 1 - net.k)):
        load_g.append(net.local(w_proj.at[:, span(half * Q, Q)], g_proj.at[:, pl.ds(s * HALF, Q)]))
        rest = pl.ds(s * HALF + Q, HALF - Q)
        load_g.append(net.local(i_proj.at[:, rest], g_proj.at[:, rest]))
    proj.start()
    load_dy = [net.local(i_dy, dy), net.local(i_dys, dys), net.local(i_slope, slope)]
    load_fc = [net.local(i_fc, g_fc), net.local(i_hat, hat), net.local(i_xh, xh)]
    load_h2 = net.local(i_h2, h2c)
    for copy in load_g:
        copy.wait()

    def lanes_of(s):
        return span(flip(s, net.k) * Q, Q)

    def project(j, _):
        for s in range(2):
            cols = span(s * HALF + net.mix(j) * Q, Q)
            out = mm(g[...], g_proj[:, cols]) + mm(attn[...], g_dense[:, cols])
            out_send[j, :, lanes_of(s)] = out.astype(bf16)
        return 0

    lax.fori_loop(0, 4, project, 0)
    out_copies = [net.remote(out_send.at[j], out_recv.at[j - 1], net.z[j]) for j in (1, 2, 3)]
    for copy in load_dy:
        copy.wait()
    mine = pl.ds(0, tok)
    theirs = pl.ds(tok, tok)
    sums[...] = jnp.zeros_like(sums)

    def back_fc(n, _):
        cols = span(n * 512, 512)
        grad = mm_nt(dy[...], g_proj[cols, 0:HALF]) + mm_nt(dys[...], g_proj[cols, HALF:])
        grad = grad * slope[:, cols].astype(f32)
        sums[0:1, cols] = jnp.sum(grad, axis=0, keepdims=True)
        dab[mine, cols] = grad.astype(bf16)
        return 0

    lax.fori_loop(0, g.shape[1] // 512, back_fc, 0)
    swap = net.remote(dab.at[mine, :], dab.at[theirs, :], net.core)
    proj.join()
    qkv.start()
    for copy in load_fc:
        copy.wait()
    stats[...] = jnp.zeros_like(stats)
    lane = lax.broadcasted_iota(jnp.int32, (tok, 128), 1)

    def back_norm(j, _):
        for s in range(2):
            lanes = lanes_of(s)
            cols = span(s * HALF + net.mix(j) * Q, Q)
            grad = mm_nt(dab[mine, :], g_fc[cols, :])
            hats = xh[:, cols].astype(f32)
            packs[j, 2:3, lanes] = vecs[4:5, cols]
            packs[j, 3:4, lanes] = vecs[5:6, cols]
            packs[j, 4:5, lanes] = jnp.sum(grad * hats, axis=0, keepdims=True)
            packs[j, 5:6, lanes] = jnp.sum(grad, axis=0, keepdims=True)
            joint = hat[:, cols].astype(f32) + grad * vecs[2:3, cols]
            hat_send[j, :, lanes] = joint.astype(bf16)
            one = jnp.sum(joint, axis=1, keepdims=True)
            two = jnp.sum(joint * hats, axis=1, keepdims=True)
            stats[...] += jnp.where(lane == 0, one, jnp.where(lane == 1, two, 0.0))
        return 0

    lax.fori_loop(0, 4, back_norm, 0)
    turned = stats[...].T
    for j in range(4):
        packs[j, 0:2, :] = turned[0:2]
        packs[j, 6:8, :] = jnp.zeros((2, tok), f32)
    pack_copies = [net.remote(packs.at[j], packs.at[3 + j], net.z[j]) for j in (1, 2, 3)]
    hat_copies = [net.remote(hat_send.at[j], hat_recv.at[j - 1], net.z[j]) for j in (1, 2, 3)]
    load_h2.wait()
    swap.wait_recv()

    def grad_fc(n, _):
        cols = span(n * 512, 512)
        part_fc[:, cols] = mm_tn(h2c[...], dab[:, cols]).astype(bf16)
        return 0

    lax.fori_loop(0, dab.shape[1] // 512, grad_fc, 0)
    outs = []

    def wide(n, columns):
        return g_proj.at[pl.ds(n * Q, Q), pl.ds(0, columns)]

    def tall(n, count):
        return g_proj.at[pl.ds(0, count), pl.ds(n * Q, Q)]

    fc.start()
    local, remote = proj.finish([tall(n, r_proj.shape[0]) for n in range(3)], t_proj, o_proj)
    outs += local
    far = remote
    qkv.join()
    dense.start()
    for copy in pack_copies:
        copy.wait_recv()
    total = packs[0] + packs[4] + packs[5] + packs[6]
    stats[...] = jnp.zeros_like(stats)
    turned_rows = jnp.concatenate([total, jnp.zeros((120, tok), f32)], axis=0)
    o_stats[...] = turned_rows.T
    small[0, 0:4, :] = total[2:6, :]
    for n in range(3):
        small[0, 4 + n : 5 + n, :] = bias[0:1, n * 512 : n * 512 + 512]
    for n in range(4):
        small[0, 7 + n : 8 + n, :] = sums[0:1, n * 512 : n * 512 + 512]
    small[0, 11:12, :] = bias[1:2, 0:512]
    small[0, 12:16, :] = jnp.zeros((4, 512), f32)
    for hop, peer in enumerate((net.core, net.x, net.y)):
        net.remote(small.at[hop], small.at[4 + hop], peer).wait_recv()
        small[hop + 1] = small[hop] + small[4 + hop]
    o_small[...] = small[3]
    for copy in out_copies:
        copy.wait_recv()

    def sum_out(n, _):
        at = span(n * 64, 64)
        value = out_send[0, at, :].astype(f32)
        for j in range(3):
            value = value + out_recv[j, at, :].astype(f32)
        o_branch[at, :] = value
        return 0

    lax.fori_loop(0, tok // 64, sum_out, 0)
    local, remote = qkv.finish([wide(n, r_qkv.shape[1]) for n in range(3)], t_qkv, o_qkv)
    outs += local
    far += remote
    fc.join()
    for copy in hat_copies:
        copy.wait_recv()

    def sum_hat(n, _):
        at = span(n * 64, 64)
        value = hat_send[0, at, :].astype(f32)
        for j in range(3):
            value = value + hat_recv[j, at, :].astype(f32)
        o_hat[at, :] = value
        return 0

    lax.fori_loop(0, tok // 64, sum_hat, 0)
    dense.join()
    local, remote = fc.finish([wide(n, part_fc.shape[1]) for n in range(3)], t_fc, o_fc)
    outs += local
    far += remote
    local, remote = dense.finish([tall(n, r_dense.shape[0]) for n in range(3)], t_dense, o_dense)
    outs += local
    far += remote
    for copy in outs:
        copy.wait()
    for copy in far:
        copy.wait_recv()
    net.drain()


def call_reduce(w_proj, gathered, vecs, bias):
    tok, wide = gathered[9].shape
    n_fc, n_attn = gathered[0].shape[0], gathered[2].shape[0]
    n_qkv = gathered[12].shape[1]
    any_spec = pl.BlockSpec(memory_space=pl.ANY)
    vmem = pl.BlockSpec(memory_space=VMEM)
    shape = jax.ShapeDtypeStruct
    pieces = ((n_fc, Q), (Q, n_qkv), (Q, n_fc), (n_attn, Q))
    outs = [
        shape((n_fc, 2 * Q), f32), shape((2 * Q, n_qkv), f32),
        shape((2 * Q, n_fc), f32), shape((n_attn, 2 * Q), f32),
    ]
    outs += [shape(piece, bf16) for piece in pieces for _ in range(2)]
    outs += [shape((tok, 512), f32), shape((tok, 512), f32), shape((tok, 128), f32)]
    outs += [shape((16, 512), f32)]
    scratch = [
        VMEM((n_fc, wide), bf16), VMEM((wide, n_fc), bf16), VMEM((n_attn, wide), bf16),
        VMEM((tok, n_fc), bf16), VMEM((tok, n_fc), bf16), VMEM((tok, n_attn), bf16),
        VMEM((tok, wide), bf16), VMEM((tok, wide), bf16), VMEM((tok, HALF), bf16),
        VMEM((tok, HALF), bf16), VMEM((2 * tok, HALF), bf16), VMEM((2 * tok, n_fc), bf16),
        VMEM((4, tok, 512), bf16), VMEM((3, tok, 512), bf16),
        VMEM((4, tok, 512), bf16), VMEM((3, tok, 512), bf16),
    ]
    for rows, cols in pieces:
        scratch += [VMEM((2, rows // 2, cols), bf16)] * 2
    scratch += [VMEM((HALF, n_fc), bf16)]
    scratch += [VMEM(piece, f32) for piece in pieces]
    scratch += [
        VMEM((7, 8, tok), f32), VMEM((tok, 128), f32), VMEM((8, n_fc), f32), VMEM((7, 16, 512), f32),
        pltpu.SemaphoreType.DMA((48,)), pltpu.SemaphoreType.DMA((48,)), pltpu.SemaphoreType.DMA((48,)),
    ]
    return pl.pallas_call(
        reduce_kernel,
        name="backward_and_reduce",
        out_shape=outs,
        in_specs=[any_spec] * 15 + [vmem] * 2,
        out_specs=[any_spec] * 12 + [vmem] * 4,
        scratch_shapes=scratch,
        compiler_params=pltpu.CompilerParams(
            collective_id=2, has_side_effects=True, vmem_limit_bytes=67043328
        ),
    )(w_proj, *gathered, vecs, bias)


def turn_tables(length):
    half_rot = ROT // 2
    frequency = (10000.0 ** (-np.arange(half_rot, dtype=np.float32) * (2.0 / ROT))).astype(np.float32)
    angles = np.arange(length, dtype=np.float32)[:, None] * frequency[None, :]
    tables = np.zeros((3, length, 128), np.float32)
    tables[0] = 1.0
    tables[0, :, :half_rot] = tables[0, :, half_rot:ROT] = np.cos(angles)
    tables[1, :, :half_rot] = -np.sin(angles)
    tables[2, :, half_rot:ROT] = np.sin(angles)
    return tables


def fused_shards(
    block_input, out_grad, ln1_gain, ln1_bias, ln2_gain, ln2_bias,
    w_qkv, b_qkv, w_dense, b_dense, w_fc, b_fc, w_proj, b_proj,
):
    norms = jnp.stack([ln1_gain, ln1_bias, ln2_gain, ln2_bias])
    *gathered, stats, vecs, bias = call_gather(
        block_input, out_grad, norms, w_qkv, w_dense, w_fc, w_proj,
        b_qkv[None, :], b_fc[None, :], turn_tables(SEQ),
    )
    reduced = call_reduce(w_proj, gathered, vecs, bias)
    proj_total, qkv_total, fc_total, dense_total = reduced[:4]
    branch, hat_grad, totals, small = reduced[12:]
    block_output = block_input + branch + (b_dense + b_proj)
    x_hat = (block_input - stats[:, 8:9]) * stats[:, 9:10]
    input_grad = out_grad + stats[:, 9:10] * (
        hat_grad - totals[:, 0:1] * (1.0 / D) - x_hat * (totals[:, 1:2] * (1.0 / D))
    )
    return (
        block_output, input_grad, small[0], small[1], small[2], small[3],
        qkv_total, small[4:7].reshape(-1), dense_total, small[11],
        fc_total, small[7:11].reshape(-1), proj_total, small[11],
    )


def solution(mesh):
    sizes = tuple(mesh.shape[name] for name in ("dp", "row", "col"))
    body = fused_shards if sizes == (2, 4, 4) else shards
    return jax.shard_map(
        body,
        mesh=mesh,
        in_specs=(
            P(("dp", "row"), "col"),
            P(("dp", "row"), "col"),
            P("col"),
            P("col"),
            P("col"),
            P("col"),
            P("row", "col"),
            P("col"),
            P("col", "row"),
            P("col"),
            P("row", "col"),
            P("col"),
            P("col", "row"),
            P("col"),
        ),
        out_specs=(
            P(("dp", "row"), "col"),
            P(("dp", "row"), "col"),
            P("col"),
            P("col"),
            P("col"),
            P("col"),
            P("row", "col"),
            P("col"),
            P("col", "row"),
            P("col"),
            P("row", "col"),
            P("col"),
            P("col", "row"),
            P("col"),
        ),
        check_vma=False,
    )
```

```python
import functools
import math

import jax
import jax.numpy as jnp
import numpy as np
from jax import lax
from jax.experimental import pallas as pl
from jax.experimental.pallas import tpu as pltpu
from jax.sharding import PartitionSpec as P

D = 2048
HD = 256
ROT = 64
SEQ = 512


epsilon = 1e-05
contract_last = (((1,), (1,)), ((), ()))
contract_first = (((0,), (0,)), ((), ()))


def angle_tables(length):
    half_rot = ROT // 2
    position = jnp.arange(length, dtype=jnp.float32)
    exponent = jnp.arange(half_rot, dtype=jnp.float32) * (2.0 / ROT)
    frequency = 10000.0 ** (-exponent)
    angles = position[:, None] * frequency[None, :]
    return (jnp.cos(angles), jnp.sin(angles))


def rotate_fwd(values, cosine, sine_vals):
    half_rot = ROT // 2
    first = values[..., :half_rot]
    second = values[..., half_rot:ROT]
    cos_part = cosine[:, None, :]
    sin_part = sine_vals[:, None, :]
    return jnp.concatenate(
        [
            first * cos_part - second * sin_part,
            second * cos_part + first * sin_part,
            values[..., ROT:],
        ],
        axis=-1,
    )


def rotate_back(grads, cosine, sine_vals):
    half_rot = ROT // 2
    first = grads[..., :half_rot]
    second = grads[..., half_rot:ROT]
    cos_part = cosine[:, None, :]
    sin_part = sine_vals[:, None, :]
    return jnp.concatenate(
        [
            first * cos_part + second * sin_part,
            second * cos_part - first * sin_part,
            grads[..., ROT:],
        ],
        axis=-1,
    )


def gelu_value(pre_act):
    return 0.5 * pre_act * (1.0 + lax.erf(pre_act * 0.7071067811865476))


def gelu_slope(pre_act):
    return 0.5 * (
        1.0 + lax.erf(pre_act * 0.7071067811865476)
    ) + pre_act * 0.3989422804014327 * jnp.exp(-0.5 * pre_act * pre_act)


def shards(
    block_input,
    out_grad,
    ln1_gain,
    ln1_bias,
    ln2_gain,
    ln2_bias,
    w_qkv,
    b_qkv,
    w_dense,
    b_dense,
    w_fc,
    b_fc,
    w_proj,
    b_proj,
):
    tok_rows = block_input.shape[0]
    seq_count = tok_rows // SEQ
    qkv_cols = w_qkv.shape[1]
    fc_cols = w_fc.shape[1]
    local_heads = qkv_cols // (3 * HD)
    head_cols = local_heads * HD
    scale = 1.0 / math.sqrt(HD)
    cosine, sine_vals = angle_tables(SEQ)
    causal = jnp.arange(SEQ)[:, None] >= jnp.arange(SEQ)[None, :]
    row_total, square_total = lax.psum(
        (jnp.sum(block_input, axis=1), jnp.sum(block_input * block_input, axis=1)), "col"
    )
    mean_row = (row_total / D)[:, None]
    var_row = (square_total / D)[:, None] - mean_row * mean_row
    inv_std = lax.rsqrt(var_row + epsilon)
    x_hat = (block_input - mean_row) * inv_std
    normed_one = (x_hat * ln1_gain + ln1_bias).astype(jnp.bfloat16)
    normed_two = (x_hat * ln2_gain + ln2_bias).astype(jnp.bfloat16)
    wide_one, wide_two = (
        lax.all_gather(normed_one, "col", axis=1, tiled=True),
        lax.all_gather(normed_two, "col", axis=1, tiled=True),
    )
    part_one = wide_one
    part_two = wide_two
    qkv_pre = jnp.dot(
        part_one,
        lax.all_gather(w_qkv, "row", axis=0, tiled=True),
        preferred_element_type=jnp.float32,
    )
    fc_pre = jnp.dot(
        part_two,
        lax.all_gather(w_fc, "row", axis=0, tiled=True),
        preferred_element_type=jnp.float32,
    )
    qkv_pre = qkv_pre + b_qkv
    fc_pre = fc_pre + b_fc

    def forward_seq(block):
        query = rotate_fwd(block[:, :, 0], cosine, sine_vals).astype(jnp.bfloat16)
        keys = rotate_fwd(block[:, :, 1], cosine, sine_vals).astype(jnp.bfloat16)
        values = block[:, :, 2].astype(jnp.bfloat16)
        scores = jnp.einsum("qhd,khd->hqk", query, keys, preferred_element_type=jnp.float32) * scale
        masked = jnp.where(causal[None], scores, -1e30)
        row_max = jnp.max(masked, axis=-1, keepdims=True)
        exp_sum = jnp.sum(
            jnp.where(causal[None], jnp.exp(masked - row_max), 0.0), axis=-1, keepdims=True
        )
        log_total = row_max + jnp.log(exp_sum)
        probs_low = jnp.where(causal[None], jnp.exp(masked - log_total), 0.0).astype(jnp.bfloat16)
        attended = jnp.einsum(
            "hqk,khd->qhd", probs_low, values, preferred_element_type=jnp.float32
        ).astype(jnp.bfloat16)
        return (query, keys, values, attended, log_total)

    query, keys, values, attended, log_total = lax.map(
        forward_seq, qkv_pre.reshape(seq_count, SEQ, local_heads, 3, HD)
    )
    attn_out = attended.reshape(tok_rows, head_cols)
    gelu_out = gelu_value(fc_pre).astype(jnp.bfloat16)
    out_stack = jnp.concatenate([w_dense, w_proj], axis=0)
    shard_piece = lax.all_gather(out_stack, "row", axis=1, tiled=True)
    mixed = jnp.dot(
        attn_out, shard_piece[:head_cols], preferred_element_type=jnp.float32
    ) + jnp.dot(gelu_out, shard_piece[head_cols:], preferred_element_type=jnp.float32)
    branch_sum = lax.psum_scatter(mixed, "col", scatter_dimension=1, tiled=True)
    block_output = block_input + branch_sum + b_dense + b_proj
    grad_low = out_grad.astype(jnp.bfloat16)
    wide_grad = lax.all_gather(grad_low, "col", axis=1, tiled=True)
    both_grad = lax.dot_general(
        wide_grad,
        lax.all_gather(out_stack, "row", axis=1, tiled=True),
        contract_last,
        preferred_element_type=jnp.float32,
    )
    attn_grad = both_grad[:, :head_cols]
    gelu_grad = both_grad[:, head_cols:]
    attn_grad_low = attn_grad.astype(jnp.bfloat16)
    fc_grad = gelu_grad * gelu_slope(fc_pre)
    fc_bias_grad = jnp.sum(fc_grad, axis=0)
    fc_grad_low = fc_grad.astype(jnp.bfloat16)

    def backward_seq(items):
        query_s, keys_s, values_s, attended_s, log_s, head_grad = items
        scores = (
            jnp.einsum("qhd,khd->hqk", query_s, keys_s, preferred_element_type=jnp.float32) * scale
        )
        probs = jnp.where(
            causal[None], jnp.exp(jnp.where(causal[None], scores, -1e30) - log_s), 0.0
        )
        probs_low = probs.astype(jnp.bfloat16)
        value_grad = jnp.einsum(
            "hqk,qhd->khd", probs_low, head_grad, preferred_element_type=jnp.float32
        )
        prob_grad = jnp.einsum(
            "qhd,khd->hqk", head_grad, values_s, preferred_element_type=jnp.float32
        )
        delta_row = jnp.transpose(
            jnp.sum(head_grad.astype(jnp.float32) * attended_s.astype(jnp.float32), axis=-1), (1, 0)
        )[:, :, None]
        score_grad = (probs * (prob_grad - delta_row) * scale).astype(jnp.bfloat16)
        query_grad = jnp.einsum(
            "hqk,khd->qhd", score_grad, keys_s, preferred_element_type=jnp.float32
        )
        key_grad = jnp.einsum(
            "hqk,qhd->khd", score_grad, query_s, preferred_element_type=jnp.float32
        )
        return jnp.stack(
            [
                rotate_back(query_grad, cosine, sine_vals),
                rotate_back(key_grad, cosine, sine_vals),
                value_grad,
            ],
            axis=2,
        )

    head_grads = attn_grad_low.reshape(seq_count, SEQ, local_heads, HD)
    qkv_grad = lax.map(
        backward_seq, (query, keys, values, attended, log_total, head_grads)
    ).reshape(tok_rows, qkv_cols)
    qkv_bias_grad = jnp.sum(qkv_grad, axis=0)
    qkv_grad_low = qkv_grad.astype(jnp.bfloat16)
    in_stack = jnp.concatenate([w_qkv, w_fc], axis=1)
    shard_piece = lax.all_gather(in_stack, "row", axis=0, tiled=True)
    norm_grads = jnp.stack(
        [
            lax.dot_general(
                qkv_grad_low,
                shard_piece[:, :qkv_cols],
                contract_last,
                preferred_element_type=jnp.float32,
            ),
            lax.dot_general(
                fc_grad_low,
                shard_piece[:, qkv_cols:],
                contract_last,
                preferred_element_type=jnp.float32,
            ),
        ]
    )
    part_one = wide_one
    part_two = wide_two
    row_part = lax.psum_scatter(
        jnp.concatenate(
            [
                lax.dot_general(
                    part_one, qkv_grad_low, contract_first, preferred_element_type=jnp.float32
                ),
                lax.dot_general(
                    part_two, fc_grad_low, contract_first, preferred_element_type=jnp.float32
                ),
                lax.dot_general(
                    wide_grad, attn_out, contract_first, preferred_element_type=jnp.float32
                ),
                lax.dot_general(
                    wide_grad, gelu_out, contract_first, preferred_element_type=jnp.float32
                ),
            ],
            axis=1,
        ),
        "row",
        scatter_dimension=0,
        tiled=True,
    )
    grad_rows = lax.psum(row_part, "dp")
    qkv_total = grad_rows[:, :qkv_cols]
    fc_total = grad_rows[:, qkv_cols : qkv_cols + fc_cols]
    dense_total = grad_rows[:, qkv_cols + fc_cols : qkv_cols + fc_cols + head_cols].T
    proj_total = grad_rows[:, qkv_cols + fc_cols + head_cols :].T
    norm_local = lax.psum_scatter(norm_grads, "col", scatter_dimension=2, tiled=True)
    grad_one = norm_local[0]
    grad_two = norm_local[1]
    hat_grad = grad_one * ln1_gain + grad_two * ln2_gain
    total_hat, total_cross = lax.psum(
        (jnp.sum(hat_grad, axis=1), jnp.sum(hat_grad * x_hat, axis=1)), "col"
    )
    input_grad = out_grad + inv_std * (
        hat_grad - (total_hat / D)[:, None] - x_hat * (total_cross / D)[:, None]
    )
    gain_one, shift_one, gain_two, shift_two, qkv_bias_total, fc_bias_total, out_bias_total = (
        lax.psum(
            (
                jnp.sum(grad_one * x_hat, axis=0),
                jnp.sum(grad_one, axis=0),
                jnp.sum(grad_two * x_hat, axis=0),
                jnp.sum(grad_two, axis=0),
                qkv_bias_grad,
                fc_bias_grad,
                jnp.sum(out_grad, axis=0),
            ),
            ("dp", "row"),
        )
    )
    return (
        block_output,
        input_grad,
        gain_one,
        shift_one,
        gain_two,
        shift_two,
        qkv_total,
        qkv_bias_total,
        dense_total,
        out_bias_total,
        fc_total,
        fc_bias_total,
        proj_total,
        out_bias_total,
    )


f32 = jnp.float32
bf16 = jnp.bfloat16
MESH = pl.DeviceIdType.MESH
VMEM = pltpu.VMEM
Q = 256
HALF = 4 * Q


def flip(a, b):
    return a + b - 2 * a * b


def span(start, size):
    return pl.ds(pl.multiple_of(start, size), size)


def mm(a, b):
    return jnp.dot(a, b, preferred_element_type=f32)


def mm_nt(a, b):
    return lax.dot_general(a, b, (((1,), (1,)), ((), ())), preferred_element_type=f32)


def mm_tn(a, b):
    return lax.dot_general(a, b, (((0,), (0,)), ((), ())), preferred_element_type=f32)


class Net:
    def __init__(self, send_sems, recv_sems, local_sems):
        self.k = lax.axis_index("dp")
        self.r = lax.axis_index("row")
        self.c = lax.axis_index("col")
        k, r, c = self.k, self.r, self.c
        self.core = (1 - k, r, c)
        self.x = (k, r + 1 - 2 * (r % 2), c)
        self.y = (k, r + 2 - 4 * (r // 2), c)
        near = c + 1 - 2 * (c % 2)
        self.z = (None, (k, r, near), (k, r, c + 2 - 4 * (c // 2)), (k, r, 3 - c))
        self.middle = flip(c % 2, c // 2) == 1
        self.send_sems, self.recv_sems, self.local_sems = send_sems, recv_sems, local_sems
        self.remote_count = 0
        self.local_count = 0
        self.pending = []

    def mix(self, j):
        return flip(j % 2, flip(self.c % 2, self.r % 2)) + 2 * flip(
            j // 2, flip(self.c // 2, self.r // 2)
        )

    def barrier(self):
        sem = pltpu.get_barrier_semaphore()
        peers = (self.core, self.x, self.y) + self.z[1:]
        for peer in peers:
            pl.semaphore_signal(sem, inc=1, device_id=peer, device_id_type=MESH)
        pl.semaphore_wait(sem, len(peers))

    def slot(self):
        self.remote_count += 1
        return self.remote_count - 1

    def remote(self, src, dst, peer):
        slot = self.slot()
        copy = pltpu.make_async_remote_copy(
            src_ref=src,
            dst_ref=dst,
            send_sem=self.send_sems.at[slot],
            recv_sem=self.recv_sems.at[slot],
            device_id=peer,
            device_id_type=MESH,
        )
        copy.start()
        self.pending.append(copy)
        return copy

    def local(self, src, dst):
        copy = pltpu.make_async_copy(src, dst, self.local_sems.at[self.local_count])
        self.local_count += 1
        copy.start()
        return copy

    def sent(self, copy):
        copy.wait_send()
        self.pending = [other for other in self.pending if other is not copy]

    def drain(self):
        for copy in self.pending:
            copy.wait_send()


class Gather:
    def __init__(self, net, shard, full, by_rows):
        self.net, self.shard, self.full, self.by_rows = net, shard, full, by_rows
        self.depth = Q // 2 if by_rows else shard.shape[0] // 2
        self.placed = []

    def own(self, half, part=None):
        if self.by_rows:
            if part is None:
                return self.shard.at[span(half * Q, Q), :]
            return self.shard.at[span(half * Q + part * self.depth, self.depth), :]
        rows = slice(None) if part is None else pl.ds(part * self.depth, self.depth)
        return self.shard.at[rows, span(half * Q, Q)]

    def chunk(self, s, i, part=None):
        start = s * HALF + i * Q
        if self.by_rows:
            if part is None:
                return self.full.at[pl.ds(start, Q), :]
            return self.full.at[pl.ds(start + part * self.depth, self.depth), :]
        rows = slice(None) if part is None else pl.ds(part * self.depth, self.depth)
        return self.full.at[rows, pl.ds(start, Q)]

    def place_own(self):
        net = self.net
        self.placed = [
            net.local(self.own(net.k), self.chunk(0, 0)),
            net.local(self.own(1 - net.k), self.chunk(1, 0)),
        ]

    def send_own(self):
        net, k = self.net, self.net.k
        self.y0 = net.remote(self.own(k, 0), self.chunk(0, 2, 0), net.y)
        self.x1 = net.remote(self.own(k, 1), self.chunk(0, 1, 1), net.x)
        self.y1 = net.remote(self.own(k, 1), self.chunk(0, 2, 1), net.y)
        self.x0 = net.remote(self.own(k, 0), self.chunk(0, 1, 0), net.x)

    def forward(self):
        net = self.net
        self.y0.wait_recv()
        self.d0 = net.remote(self.chunk(0, 2, 0), self.chunk(0, 3, 0), net.x)
        self.x1.wait_recv()
        self.d1 = net.remote(self.chunk(0, 1, 1), self.chunk(0, 3, 1), net.y)

    def swap_near(self):
        net = self.net
        self.x0.wait_recv()
        self.c1 = net.remote(self.chunk(0, 1), self.chunk(1, 1), net.core)
        self.y1.wait_recv()
        self.c2 = net.remote(self.chunk(0, 2), self.chunk(1, 2), net.core)

    def swap_far(self):
        net = self.net
        self.d0.wait_recv()
        self.d1.wait_recv()
        self.c3 = net.remote(self.chunk(0, 3), self.chunk(1, 3), net.core)

    def ready(self):
        for copy in (self.c1, self.c2, self.c3):
            copy.wait_recv()
        for copy in self.placed:
            copy.wait()

    def release(self):
        for copy in (self.d0, self.d1, self.c1, self.c2, self.c3):
            self.net.sent(copy)


class Line:
    def __init__(self, net, slots):
        self.net, self.slots = net, slots
        self.ids = [None] + [net.slot() for _ in range(3)]
        self.sends = []

    def copy(self, src, dst, peer, send):
        net = self.net
        return pltpu.make_async_remote_copy(
            src_ref=self.slots.at[src],
            dst_ref=self.slots.at[dst],
            send_sem=net.send_sems.at[send],
            recv_sem=net.recv_sems.at[self.ids[dst]],
            device_id=peer,
            device_id_type=MESH,
        )

    def start(self):
        net = self.net
        self.first = self.copy(0, 1, net.z[1], self.ids[1])
        self.first.start()
        self.hops = [
            self.copy(0, 3, net.z[3], self.ids[2]),
            self.copy(1, 2, net.z[3], self.ids[3]),
            self.copy(3, 2, net.z[1], net.slot()),
            self.copy(2, 3, net.z[1], net.slot()),
        ]

        @pl.when(net.middle)
        def _():
            self.hops[0].start()

    def arrived(self, slot):
        return self.copy(0, slot, self.net.z[1], self.ids[slot])

    def step(self, number):
        slot = (1, 3, 2)[number]

        @pl.when(self.net.middle)
        def _():
            self.arrived(slot).wait_recv()
            self.hops[number + 1].start()

    def ready(self):
        @pl.when(jnp.logical_not(self.net.middle))
        def _():
            for slot in (1, 2, 3):
                self.arrived(slot).wait_recv()

    def drain(self):
        self.first.wait_send()

        @pl.when(self.net.middle)
        def _():
            for hop in self.hops:
                hop.wait_send()


def turn(low, tables, sign):
    swing = tables[1] * pltpu.roll(low, 96, 1) + tables[2] * pltpu.roll(low, 32, 1)
    return low * tables[0] + sign * swing


class Tiles:
    def __init__(self, slots, sems):
        self.slots, self.sems = slots, sems

    def write(self, count, product, place, depth):
        def body(n, _):
            slot = n % 2
            source = self.slots.at[slot, pl.ds(0, depth), :]
            copy = pltpu.make_async_copy(source, place(n), self.sems.at[slot])

            @pl.when(n >= 2)
            def _():
                copy.wait()

            self.slots[slot, 0:depth, :] = product(n).astype(bf16)
            copy.start()
            return 0

        lax.fori_loop(0, count, body, 0)
        for slot in range(2):
            source = self.slots.at[slot, pl.ds(0, depth), :]
            pltpu.make_async_copy(source, place(slot), self.sems.at[slot]).wait()


class Reduce:
    def __init__(self, net, partial, joined, near, far, by_rows):
        self.net, self.partial, self.by_rows = net, partial, by_rows
        self.joined, self.near, self.far = joined, near, far
        self.depth = Q // 2 if by_rows else partial.shape[0] // 2

    def chunk(self, i, half):
        if self.by_rows:
            return self.partial.at[pl.ds(i * Q + half * self.depth, self.depth), :]
        return self.partial.at[pl.ds(half * self.depth, self.depth), pl.ds(i * Q, Q)]

    def whole(self):
        if self.by_rows:
            return self.partial.at[pl.ds(0, Q), :]
        return self.partial.at[:, pl.ds(0, Q)]

    def rows(self, half):
        return pl.ds(half * self.depth, self.depth)

    def start(self):
        net = self.net
        self.a = net.remote(self.chunk(3, 0), self.joined.at[0], net.x)
        self.b = net.remote(self.chunk(3, 1), self.joined.at[1], net.y)
        self.near_a = net.remote(self.chunk(1, 0), self.near.at[self.rows(0), :], net.x)
        self.near_b = net.remote(self.chunk(2, 1), self.near.at[self.rows(1), :], net.y)

    def join(self, parts):
        net = self.net
        loads = [net.local(self.chunk(2, 0), parts[0]), net.local(self.chunk(1, 1), parts[1])]
        hops = []
        for half, copy, peer in ((0, self.a, net.y), (1, self.b, net.x)):
            loads[half].wait()
            copy.wait_recv()
            tile = 64

            def add(n, _, half=half):
                at = span(n * tile, tile)
                total = self.joined[half, at, :].astype(f32) + parts[half][at, :].astype(f32)
                self.joined[half, at, :] = total.astype(bf16)
                return 0

            lax.fori_loop(0, self.depth // tile, add, 0)
            hops.append(net.remote(self.joined.at[half], self.far.at[self.rows(half), :], peer))
        self.far_a, self.far_b = hops

    def finish(self, buffers, out):
        net = self.net
        loads = [net.local(self.whole(), buffers[0])]
        for copy in (self.near_a, self.near_b):
            copy.wait_recv()
        loads.append(net.local(self.near, buffers[1]))
        for copy in (self.far_a, self.far_b):
            copy.wait_recv()
        loads.append(net.local(self.far, buffers[2]))
        for copy in loads:
            copy.wait()
        tile = 64

        def add(n, _):
            at = span(n * tile, tile)
            parts = [buffer[at, :].astype(f32) for buffer in buffers[:3]]
            buffers[3][at, :] = (parts[0] + parts[1] + parts[2]).astype(bf16)
            return 0

        lax.fori_loop(0, self.near.shape[0] // tile, add, 0)
        if self.by_rows:
            place = out.at[span(net.k * Q, Q), :]
        else:
            place = out.at[:, span(net.k * Q, Q)]
        self.here = net.local(buffers[3], place)
        self.there = net.remote(buffers[3], place, net.core)

    def done(self):
        self.here.wait()
        self.there.wait_recv()


def block_kernel(
    x, og, gain_1, bias_1, gain_2, bias_2, w_qkv, w_dense, w_fc, w_proj, b_qkv, b_fc, tables,
    o_proj, o_qkv, o_fc, o_dense, o_branch, o_hat,
    all_proj, r_proj, r_qkv, r_fc, r_dense,
    n_proj, f_proj, n_qkv, f_qkv, n_fc, f_fc, n_dense, f_dense,
    o_stats, o_small,
    g_qkv, g_dense, g_fc, g_tail, xs, ys, pks, stats, rows, h1c, h1s, h2c, h2s, dyc, dys, xh,
    qb, kb, vb, probs, probs_low, score_low, oc, dob, dqc, gc, slope, dabt, stage,
    out_recv, hat_recv, j_proj, j_qkv, j_fc, j_dense, vecs, bias, packs, small,
    send_sems, recv_sems, local_sems, stage_sems,
):
    tok = x.shape[0]
    heads = qb.shape[0]
    width = gc.shape[1]
    scale = 1.0 / math.sqrt(HD)
    net = Net(send_sems, recv_sems, local_sems)
    net.barrier()
    qkv = Gather(net, w_qkv, g_qkv, True)
    dense = Gather(net, w_dense, g_dense, False)
    fc = Gather(net, w_fc, g_fc, True)
    proj = Gather(net, w_proj, all_proj, False)
    qkv.send_own()
    dense.send_own()
    load_x = net.local(x, probs.at[0])
    load_og = net.local(og, probs.at[1])
    tiles = Tiles(stage, stage_sems)
    mine = pl.ds(0, tok)
    theirs = pl.ds(tok, tok)

    step = 128
    lane = lax.broadcasted_iota(jnp.int32, (step, 128), 1)
    load_x.wait()

    def local_norm(n, _):
        at = span(n * step, step)
        block = probs[0, at, :]
        mean = jnp.mean(block, axis=1, keepdims=True)
        centred = block - mean
        var = jnp.mean(centred * centred, axis=1, keepdims=True)
        stats[at, :] = jnp.where(lane == 0, mean, jnp.where(lane == 1, var, 0.0))
        return 0

    lax.fori_loop(0, tok // step, local_norm, 0)
    pks[0] = stats[...].T[0:8]
    for n, vector in enumerate((gain_1, bias_1, gain_2, bias_2)):
        pks[0, 2 + n : 3 + n, :] = vector[...].reshape(1, 512)
    packed = [net.remote(pks.at[0], pks.at[j], net.z[j]) for j in (1, 2, 3)]
    for weight in (qkv, dense, fc):
        weight.place_own()
    bias[...] = jnp.zeros_like(bias)
    bias[3:4, 0 : b_qkv.shape[0]] = b_qkv[...].reshape(1, b_qkv.shape[0])
    bias[4:5, :] = b_fc[...].reshape(1, width)
    rows[...] = jnp.zeros_like(rows)
    load_og.wait()

    def local_grad(n, _):
        at = span(n * step, step)
        block = probs[1, at, :]
        ys[0, at, :] = block.astype(bf16)
        bias[1:2, 0:512] += jnp.sum(block, axis=0, keepdims=True)
        return 0

    lax.fori_loop(0, tok // step, local_grad, 0)
    for pack in packed:
        pack.wait_recv()
    means = [pks[j, 0:1, :] for j in range(4)]
    mu = (means[0] + means[1] + means[2] + means[3]) * 0.25
    spread = [pks[j, 1:2, :] + (means[j] - mu) * (means[j] - mu) for j in range(4)]
    rows[0:1, :] = mu
    rows[1:2, :] = lax.rsqrt((spread[0] + spread[1] + spread[2] + spread[3]) * 0.25 + epsilon)
    stats[...] = rows[...].T

    def own_norm(n, _):
        at = span(n * step, step)
        hats = (probs[0, at, :] - stats[at, 0:1]) * stats[at, 1:2]
        xs[0, at, :] = (hats * pks[0, 2:3, :] + pks[0, 3:4, :]).astype(bf16)
        return 0

    lax.fori_loop(0, tok // step, own_norm, 0)
    x_line = Line(net, xs)
    y_line = Line(net, ys)
    x_line.start()
    qkv.forward()
    x_line.step(0)
    x_line.step(1)
    fc.send_own()
    dense.forward()
    qkv.swap_near()
    x_line.step(2)
    y_line.start()
    dense.swap_near()
    qkv.swap_far()
    dense.swap_far()
    x_line.ready()

    for s in range(2):
        for j in range(4):
            lanes = span(flip(s, net.k) * Q, Q)
            dest = span(net.mix(j) * Q, Q)
            wide = span(s * HALF + net.mix(j) * Q, Q)
            vecs[0:4, wide] = pks[j, 2:6, lanes]

            def norm(n, _, s=s, j=j, lanes=lanes, dest=dest, wide=wide):
                at = span(n * step, step)
                one = xs[j, at, lanes]
                hats = (one.astype(f32) - pks[j, 3:4, lanes]) * (1.0 / pks[j, 2:3, lanes])
                xh[at, wide] = hats.astype(bf16)
                (h1s if s else h1c)[at, dest] = one
                two = hats * pks[j, 4:5, lanes] + pks[j, 5:6, lanes]
                (h2s if s else h2c)[at, dest] = two.astype(bf16)
                return 0

            lax.fori_loop(0, tok // step, norm, 0)
    swap_h1 = net.remote(h1s, h1c.at[theirs, :], net.core)
    swap_h2 = net.remote(h2s, h2c.at[theirs, :], net.core)
    fc.forward()
    proj.send_own()
    y_line.step(0)
    qkv.ready()

    def project(n, _):
        cols = span(n * 3 * HD, 3 * HD)
        acc = mm(h1c[mine, :], g_qkv[0:HALF, cols]) + mm(h1s[...], g_qkv[HALF:, cols])
        acc = acc + bias[3:4, cols]
        qb[n, :, 0:128] = turn(acc[:, 0:128], tables, 1.0).astype(bf16)
        qb[n, :, 128:HD] = acc[:, 128:HD].astype(bf16)
        kb[n, :, 0:128] = turn(acc[:, HD : HD + 128], tables, 1.0).astype(bf16)
        kb[n, :, 128:HD] = acc[:, HD + 128 : 2 * HD].astype(bf16)
        vb[n] = acc[:, 2 * HD :].astype(bf16)
        return 0

    lax.fori_loop(0, heads, project, 0)
    y_line.step(1)
    chunks = tok // step

    def attend(n, _):
        head, chunk = n // chunks, n % chunks
        at = span(chunk * step, step)
        scores = mm_nt(qb[head, at, :], kb[head]) * scale
        token = lax.broadcasted_iota(jnp.int32, (step, tok), 0) + chunk * step
        allowed = token >= lax.broadcasted_iota(jnp.int32, (step, tok), 1)
        scores = jnp.where(allowed, scores, -1e30)
        top = jnp.max(scores, axis=1, keepdims=True)
        raised = jnp.where(allowed, jnp.exp(scores - top), 0.0)
        weight = raised / jnp.sum(raised, axis=1, keepdims=True)
        probs[head, at, :] = weight
        low = weight.astype(bf16)
        probs_low[head, at, :] = low
        oc[at, span(head * HD, HD)] = mm(low, vb[head]).astype(bf16)
        return 0

    lax.fori_loop(0, heads * chunks, attend, 0)
    swap_o = net.remote(oc.at[mine, :], oc.at[theirs, :], net.core)
    fc.swap_near()
    y_line.step(2)
    fc.swap_far()
    fc.ready()

    def expand(n, _):
        cols = span(n * 512, 512)
        a = mm(h2c[mine, :], g_fc[0:HALF, cols]) + mm(h2s[...], g_fc[HALF:, cols])
        a = a + bias[4:5, cols]
        rise = 0.5 * (1.0 + lax.erf(a * 0.7071067811865476))
        gc[mine, cols] = (a * rise).astype(bf16)
        slope[:, cols] = (rise + a * 0.3989422804014327 * jnp.exp(-0.5 * a * a)).astype(bf16)
        return 0

    lax.fori_loop(0, width // 512, expand, 0)
    swap_g = net.remote(gc.at[mine, :], gc.at[theirs, :], net.core)
    proj.forward()
    y_line.ready()
    for s in range(2):
        for j in range(4):
            lanes = span(flip(s, net.k) * Q, Q)
            dest = span(net.mix(j) * Q, Q)
            (dys if s else dyc)[mine, dest] = ys[j, :, lanes]
    swap_dy = net.remote(dys, dyc.at[theirs, :], net.core)
    dense.ready()
    dob[...] = (
        mm_nt(dyc[mine, :], g_dense[:, 0:HALF]) + mm_nt(dys[...], g_dense[:, HALF:])
    ).astype(bf16)

    red_proj = Reduce(net, r_proj, j_proj, n_proj, f_proj, False)
    red_qkv = Reduce(net, r_qkv, j_qkv, n_qkv, f_qkv, True)
    red_fc = Reduce(net, r_fc, j_fc, n_fc, f_fc, True)
    red_dense = Reduce(net, r_dense, j_dense, n_dense, f_dense, False)
    swap_g.wait_recv()
    swap_dy.wait_recv()
    tall = width // 2
    tiles.write(
        4,
        lambda n: mm_tn(gc[:, span(n // 2 * tall, tall)], dyc[:, span(n % 2 * 512, 512)]),
        lambda n: r_proj.at[span(n // 2 * tall, tall), span(n % 2 * 512, 512)],
        tall,
    )
    proj.swap_near()
    red_proj.start()

    def keep(head, part, at, value, rotated):
        base = head * 3 * HD + part * HD
        if rotated:
            low = turn(value[:, 0:128], [tables[t, at, :] for t in range(3)], -1.0)
            dqc[at, pl.ds(pl.multiple_of(base, 128), 128)] = low.astype(bf16)
            bias[0:1, pl.ds(pl.multiple_of(base, 128), 128)] += jnp.sum(low, axis=0, keepdims=True)
            value, base, size = value[:, 128:], base + 128, 128
        else:
            size = HD
        cols = pl.ds(pl.multiple_of(base, 128), size)
        dqc[at, cols] = value.astype(bf16)
        bias[0:1, cols] += jnp.sum(value, axis=0, keepdims=True)

    def attend_back(head, _):
        cols = span(head * HD, HD)

        def chunk_back(n, _):
            at = span(n * step, step)
            grad = dob[at, cols]
            delta = jnp.sum(grad.astype(f32) * oc[at, cols].astype(f32), axis=1, keepdims=True)
            spread = mm_nt(grad, vb[head]) - delta
            low = (probs[head, at, :] * spread * scale).astype(bf16)
            score_low[at, :] = low
            keep(head, 0, at, mm(low, kb[head]), True)
            return 0

        lax.fori_loop(0, chunks, chunk_back, 0)
        keep(head, 1, mine, mm_tn(score_low[...], qb[head]), True)
        keep(head, 2, mine, mm_tn(probs_low[head], dob[:, cols]), False)
        return 0

    lax.fori_loop(0, heads, attend_back, 0)
    swap_dq = net.remote(dqc.at[mine, :], dqc.at[theirs, :], net.core)
    swap_o.wait_recv()
    attn = oc.shape[1]
    tiles.write(
        2,
        lambda n: mm_tn(oc[...], dyc[:, span(n * 512, 512)]),
        lambda n: r_dense.at[:, span(n * 512, 512)],
        attn,
    )
    swap_h1.wait_recv()
    swap_dq.wait_recv()
    tiles.write(
        dqc.shape[1] // 512,
        lambda n: mm_tn(h1c[...], dqc[:, span(n * 512, 512)]),
        lambda n: r_qkv.at[:, span(n * 512, 512)],
        HALF,
    )
    red_qkv.start()
    proj.swap_far()

    net.sent(swap_h1)
    net.sent(swap_h2)
    for s in range(2):

        def back_first(n, _, s=s):
            wide = span(s * HALF + n * 512, 512)
            grad = mm_nt(dqc[mine, :], g_qkv[wide, :])
            (h2s if s else h1s)[:, span(n * 512, 512)] = (grad * vecs[0:1, wide]).astype(bf16)
            vecs[4:5, wide] = jnp.sum(grad * xh[:, wide].astype(f32), axis=0, keepdims=True)
            vecs[5:6, wide] = jnp.sum(grad, axis=0, keepdims=True)
            return 0

        lax.fori_loop(0, HALF // 512, back_first, 0)

    proj.ready()
    qkv.release()
    loads = [
        net.local(w_proj.at[:, span(net.k * Q, Q)], g_qkv.at[:, pl.ds(0, Q)]),
        net.local(w_proj.at[:, span((1 - net.k) * Q, Q)], g_qkv.at[:, pl.ds(HALF, Q)]),
        net.local(all_proj.at[:, pl.ds(Q, 3 * Q)], g_qkv.at[:, pl.ds(Q, 3 * Q)]),
        net.local(all_proj.at[:, pl.ds(5 * Q, Q)], g_qkv.at[:, pl.ds(5 * Q, Q)]),
        net.local(all_proj.at[:, pl.ds(6 * Q, 2 * Q)], g_tail),
    ]
    for copy in loads:
        copy.wait()
    x_line.drain()
    y_line.drain()

    def put_out(p, product):
        s, i = p // 4, p % 4
        out = product + mm(oc[mine, :], g_dense[:, span(p * Q, Q)])
        xs[net.mix(i), :, span(flip(s, net.k) * Q, Q)] = out.astype(bf16)

    def project_head(p, _):
        put_out(p, mm(gc[mine, :], g_qkv[:, span(p * Q, Q)]))
        return 0

    def project_tail(p, _):
        put_out(6 + p, mm(gc[mine, :], g_tail[:, span(p * Q, Q)]))
        return 0

    lax.fori_loop(0, 6, project_head, 0)
    lax.fori_loop(0, 2, project_tail, 0)
    out_copies = [net.remote(xs.at[j], out_recv.at[j - 1], net.z[j]) for j in (1, 2, 3)]

    def back_fc(n, _):
        cols = span(n * 512, 512)
        grad = mm_nt(dyc[mine, :], g_qkv[cols, 0:HALF])
        grad = grad + mm_nt(dys[:, 0:512], g_qkv[cols, HALF : 6 * Q])
        grad = grad + mm_nt(dys[:, 512:], g_tail[cols, :])
        grad = grad * slope[:, cols].astype(f32)
        bias[2:3, cols] = jnp.sum(grad, axis=0, keepdims=True)
        slope[:, cols] = grad.astype(bf16)
        return 0

    lax.fori_loop(0, width // 512, back_fc, 0)
    dab = slope
    swap_da = net.remote(dab, dabt, net.core)
    red_proj.join([g_tail.at[pl.ds(0, tall), pl.ds(0, Q)], g_tail.at[pl.ds(tall, tall), pl.ds(0, Q)]])
    stats[...] = jnp.zeros_like(stats)
    lane = lax.broadcasted_iota(jnp.int32, (tok, 128), 1)

    def back_norm(j, _):
        for s in range(2):
            lanes = span(flip(s, net.k) * Q, Q)
            dest = span(net.mix(j) * Q, Q)
            wide = span(s * HALF + net.mix(j) * Q, Q)
            grad = mm_nt(dab[...], g_fc[wide, :])
            hats = xh[:, wide].astype(f32)
            packs[j, 2:4, lanes] = vecs[4:6, wide]
            packs[j, 4:5, lanes] = jnp.sum(grad * hats, axis=0, keepdims=True)
            packs[j, 5:6, lanes] = jnp.sum(grad, axis=0, keepdims=True)
            joint = (h2s if s else h1s)[:, dest].astype(f32) + grad * vecs[2:3, wide]
            ys[j, :, lanes] = joint.astype(bf16)
            one = jnp.sum(joint, axis=1, keepdims=True)
            two = jnp.sum(joint * hats, axis=1, keepdims=True)
            stats[...] += jnp.where(lane == 0, one, jnp.where(lane == 1, two, 0.0))
        return 0

    lax.fori_loop(0, 4, back_norm, 0)
    turned = stats[...].T
    for j in range(4):
        packs[j, 0:2, :] = turned[0:2]
        packs[j, 6:8, :] = jnp.zeros((2, tok), f32)
    pack_copies = [net.remote(packs.at[j], packs.at[3 + j], net.z[j]) for j in (1, 2, 3)]
    hat_copies = [net.remote(ys.at[j], hat_recv.at[j - 1], net.z[j]) for j in (1, 2, 3)]
    swap_h2.wait_recv()
    swap_da.wait_recv()

    def grad_fc(n):
        cols = span(n * 512, 512)
        return mm_tn(h2c[mine, :], dab[:, cols]) + mm_tn(h2c[theirs, :], dabt[:, cols])

    tiles.write(width // 512, grad_fc, lambda n: r_fc.at[:, span(n * 512, 512)], HALF)
    red_fc.start()

    fc.release()

    def strips(base, n, columns):
        return g_fc.at[pl.ds(base + n * Q, Q), pl.ds(0, columns)]

    halves = [g_fc.at[pl.ds(7 * Q + n * (Q // 2), Q // 2), pl.ds(0, 6 * Q)] for n in range(2)]
    red_qkv.join(halves)
    red_dense.start()
    red_proj.finish([g_qkv.at[:, pl.ds(n * Q, Q)] for n in range(4)], o_proj)
    for copy in pack_copies:
        copy.wait_recv()
    total = packs[0] + packs[4] + packs[5] + packs[6]
    rows[2:4, :] = total[0:2, :]
    o_stats[...] = rows[...].T
    small[0, 0:4, :] = total[2:6, :]
    for n in range(3):
        small[0, 4 + n : 5 + n, :] = bias[0:1, n * 512 : n * 512 + 512]
    for n in range(4):
        small[0, 7 + n : 8 + n, :] = bias[2:3, n * 512 : n * 512 + 512]
    small[0, 11:12, :] = bias[1:2, 0:512]
    small[0, 12:16, :] = jnp.zeros((4, 512), f32)
    for hop, peer in enumerate((net.core, net.x, net.y)):
        net.remote(small.at[hop], small.at[4 + hop], peer).wait_recv()
        small[hop + 1] = small[hop] + small[4 + hop]
    o_small[...] = small[3]

    def sum_blocks(sent, received, total):
        def body(n, _):
            at = span(n * 64, 64)
            value = sent[0, at, :].astype(f32)
            for j in range(3):
                value = value + received[j, at, :].astype(f32)
            total[at, :] = value
            return 0

        lax.fori_loop(0, tok // 64, body, 0)

    for copy in out_copies:
        copy.wait_recv()
    sum_blocks(xs, out_recv, probs.at[0])
    keep_branch = net.local(probs.at[0], o_branch)
    red_fc.join([g_fc.at[pl.ds(6 * Q + n * (Q // 2), Q // 2), :] for n in range(2)])
    red_qkv.finish([strips(0, n, 6 * Q) for n in range(4)], o_qkv)
    dense_parts = [g_tail.at[pl.ds(n * attn, attn), pl.ds(Q, Q)] for n in range(4)]
    red_dense.join([g_tail.at[pl.ds(n * attn // 2, attn // 2), pl.ds(0, Q)] for n in range(2)])
    red_fc.finish([strips(4 * Q, n, 8 * Q) for n in range(4)], o_fc)
    red_dense.finish(dense_parts, o_dense)
    for copy in hat_copies:
        copy.wait_recv()
    sum_blocks(ys, hat_recv, probs.at[1])
    keep_hat = net.local(probs.at[1], o_hat)
    for weight in (red_proj, red_qkv, red_fc, red_dense):
        weight.done()
    keep_branch.wait()
    keep_hat.wait()
    net.drain()


def call_block(*args):
    x, w_qkv, w_dense = args[0], args[6], args[7]
    tok = x.shape[0]
    n_qkv, n_attn, n_fc = w_qkv.shape[1], w_dense.shape[0], args[8].shape[1]
    heads = n_attn // HD
    wide = 2 * HALF
    any_spec = pl.BlockSpec(memory_space=pl.ANY)
    vmem = pl.BlockSpec(memory_space=VMEM)
    shape = jax.ShapeDtypeStruct
    pieces = ((n_fc, Q), (Q, n_qkv), (Q, n_fc), (n_attn, Q))
    outs = [
        shape((n_fc, 2 * Q), bf16), shape((2 * Q, n_qkv), bf16),
        shape((2 * Q, n_fc), bf16), shape((n_attn, 2 * Q), bf16),
        shape((tok, 512), f32), shape((tok, 512), f32),
        shape((n_fc, wide), bf16), shape((n_fc, HALF), bf16), shape((HALF, n_qkv), bf16),
        shape((HALF, n_fc), bf16), shape((n_attn, HALF), bf16),
    ]
    outs += [shape(piece, bf16) for piece in pieces for _ in range(2)]
    outs += [shape((tok, 128), f32), shape((16, 512), f32)]
    scratch = [
        VMEM((wide, n_qkv), bf16), VMEM((n_attn, wide), bf16), VMEM((wide, n_fc), bf16),
        VMEM((n_fc, 2 * Q), bf16),
        VMEM((4, tok, 512), bf16), VMEM((4, tok, 512), bf16), VMEM((4, 8, tok), f32),
        VMEM((tok, 128), f32), VMEM((128, tok), f32),
        VMEM((2 * tok, HALF), bf16), VMEM((tok, HALF), bf16),
        VMEM((2 * tok, HALF), bf16), VMEM((tok, HALF), bf16),
        VMEM((2 * tok, HALF), bf16), VMEM((tok, HALF), bf16), VMEM((tok, wide), bf16),
        VMEM((heads, tok, HD), bf16), VMEM((heads, tok, HD), bf16), VMEM((heads, tok, HD), bf16),
        VMEM((heads, tok, tok), f32), VMEM((heads, tok, tok), bf16), VMEM((tok, tok), bf16),
        VMEM((2 * tok, n_attn), bf16), VMEM((tok, n_attn), bf16), VMEM((2 * tok, n_qkv), bf16),
        VMEM((2 * tok, n_fc), bf16), VMEM((tok, n_fc), bf16), VMEM((tok, n_fc), bf16),
        VMEM((2, HALF, 512), bf16),
        VMEM((3, tok, 512), bf16), VMEM((3, tok, 512), bf16),
    ]
    scratch += [VMEM((2,) + ((r // 2, c)), bf16) for r, c in pieces]
    scratch += [
        VMEM((8, wide), f32), VMEM((8, n_fc), f32), VMEM((7, 8, tok), f32), VMEM((7, 16, 512), f32),
        pltpu.SemaphoreType.DMA((96,)), pltpu.SemaphoreType.DMA((96,)),
        pltpu.SemaphoreType.DMA((64,)), pltpu.SemaphoreType.DMA((2,)),
    ]
    return pl.pallas_call(
        block_kernel,
        name="block",
        out_shape=outs,
        in_specs=[any_spec] * 2 + [vmem] * 4 + [any_spec] * 4 + [vmem] * 3,
        out_specs=[any_spec] * 19 + [vmem] * 2,
        scratch_shapes=scratch,
        compiler_params=pltpu.CompilerParams(
            collective_id=1, has_side_effects=True, vmem_limit_bytes=67043328
        ),
    )(*args)


def turn_tables(length):
    half_rot = ROT // 2
    frequency = (10000.0 ** (-np.arange(half_rot, dtype=np.float32) * (2.0 / ROT))).astype(np.float32)
    angles = np.arange(length, dtype=np.float32)[:, None] * frequency[None, :]
    tables = np.zeros((3, length, 128), np.float32)
    tables[0] = 1.0
    tables[0, :, :half_rot] = tables[0, :, half_rot:ROT] = np.cos(angles)
    tables[1, :, :half_rot] = -np.sin(angles)
    tables[2, :, half_rot:ROT] = np.sin(angles)
    return tables


def fused_shards(
    block_input, out_grad, ln1_gain, ln1_bias, ln2_gain, ln2_bias,
    w_qkv, b_qkv, w_dense, b_dense, w_fc, b_fc, w_proj, b_proj,
):
    results = call_block(
        block_input, out_grad, ln1_gain, ln1_bias, ln2_gain, ln2_bias,
        w_qkv, w_dense, w_fc, w_proj, b_qkv, b_fc, turn_tables(SEQ),
    )
    proj_total, qkv_total, fc_total, dense_total = (part.astype(f32) for part in results[:4])
    branch, hat_grad = results[4:6]
    stats, small = results[19:]
    mu, rstd, total, cross = (stats[:, n : n + 1] for n in range(4))
    block_output = block_input + branch + (b_dense + b_proj)
    x_hat = (block_input - mu) * rstd
    input_grad = out_grad + rstd * (hat_grad - total * (1.0 / D) - x_hat * (cross * (1.0 / D)))
    return (
        block_output, input_grad, small[0], small[1], small[2], small[3],
        qkv_total, small[4:7].reshape(-1), dense_total, small[11],
        fc_total, small[7:11].reshape(-1), proj_total, small[11],
    )


def solution(mesh):
    sizes = tuple(mesh.shape[name] for name in ("dp", "row", "col"))
    body = fused_shards if sizes == (2, 4, 4) else shards
    return jax.shard_map(
        body,
        mesh=mesh,
        in_specs=(
            P(("dp", "row"), "col"),
            P(("dp", "row"), "col"),
            P("col"),
            P("col"),
            P("col"),
            P("col"),
            P("row", "col"),
            P("col"),
            P("col", "row"),
            P("col"),
            P("row", "col"),
            P("col"),
            P("col", "row"),
            P("col"),
        ),
        out_specs=(
            P(("dp", "row"), "col"),
            P(("dp", "row"), "col"),
            P("col"),
            P("col"),
            P("col"),
            P("col"),
            P("row", "col"),
            P("col"),
            P("col", "row"),
            P("col"),
            P("row", "col"),
            P("col"),
            P("col", "row"),
            P("col"),
        ),
        check_vma=False,
    )
```

```python
import functools
import math

import jax
import jax.numpy as jnp
import numpy as np
from jax import lax
from jax.experimental import pallas as pl
from jax.experimental.pallas import tpu as pltpu
from jax.sharding import PartitionSpec as P

D = 2048
HD = 256
ROT = 64
SEQ = 512


epsilon = 1e-05
contract_last = (((1,), (1,)), ((), ()))
contract_first = (((0,), (0,)), ((), ()))


def angle_tables(length):
    half_rot = ROT // 2
    position = jnp.arange(length, dtype=jnp.float32)
    exponent = jnp.arange(half_rot, dtype=jnp.float32) * (2.0 / ROT)
    frequency = 10000.0 ** (-exponent)
    angles = position[:, None] * frequency[None, :]
    return (jnp.cos(angles), jnp.sin(angles))


def rotate_fwd(values, cosine, sine_vals):
    half_rot = ROT // 2
    first = values[..., :half_rot]
    second = values[..., half_rot:ROT]
    cos_part = cosine[:, None, :]
    sin_part = sine_vals[:, None, :]
    return jnp.concatenate(
        [
            first * cos_part - second * sin_part,
            second * cos_part + first * sin_part,
            values[..., ROT:],
        ],
        axis=-1,
    )


def rotate_back(grads, cosine, sine_vals):
    half_rot = ROT // 2
    first = grads[..., :half_rot]
    second = grads[..., half_rot:ROT]
    cos_part = cosine[:, None, :]
    sin_part = sine_vals[:, None, :]
    return jnp.concatenate(
        [
            first * cos_part + second * sin_part,
            second * cos_part - first * sin_part,
            grads[..., ROT:],
        ],
        axis=-1,
    )


def gelu_value(pre_act):
    return 0.5 * pre_act * (1.0 + lax.erf(pre_act * 0.7071067811865476))


def gelu_slope(pre_act):
    return 0.5 * (
        1.0 + lax.erf(pre_act * 0.7071067811865476)
    ) + pre_act * 0.3989422804014327 * jnp.exp(-0.5 * pre_act * pre_act)


def shards(
    block_input,
    out_grad,
    ln1_gain,
    ln1_bias,
    ln2_gain,
    ln2_bias,
    w_qkv,
    b_qkv,
    w_dense,
    b_dense,
    w_fc,
    b_fc,
    w_proj,
    b_proj,
):
    tok_rows = block_input.shape[0]
    seq_count = tok_rows // SEQ
    qkv_cols = w_qkv.shape[1]
    fc_cols = w_fc.shape[1]
    local_heads = qkv_cols // (3 * HD)
    head_cols = local_heads * HD
    scale = 1.0 / math.sqrt(HD)
    cosine, sine_vals = angle_tables(SEQ)
    causal = jnp.arange(SEQ)[:, None] >= jnp.arange(SEQ)[None, :]
    row_total, square_total = lax.psum(
        (jnp.sum(block_input, axis=1), jnp.sum(block_input * block_input, axis=1)), "col"
    )
    mean_row = (row_total / D)[:, None]
    var_row = (square_total / D)[:, None] - mean_row * mean_row
    inv_std = lax.rsqrt(var_row + epsilon)
    x_hat = (block_input - mean_row) * inv_std
    normed_one = (x_hat * ln1_gain + ln1_bias).astype(jnp.bfloat16)
    normed_two = (x_hat * ln2_gain + ln2_bias).astype(jnp.bfloat16)
    wide_one, wide_two = (
        lax.all_gather(normed_one, "col", axis=1, tiled=True),
        lax.all_gather(normed_two, "col", axis=1, tiled=True),
    )
    part_one = wide_one
    part_two = wide_two
    qkv_pre = jnp.dot(
        part_one,
        lax.all_gather(w_qkv, "row", axis=0, tiled=True),
        preferred_element_type=jnp.float32,
    )
    fc_pre = jnp.dot(
        part_two,
        lax.all_gather(w_fc, "row", axis=0, tiled=True),
        preferred_element_type=jnp.float32,
    )
    qkv_pre = qkv_pre + b_qkv
    fc_pre = fc_pre + b_fc

    def forward_seq(block):
        query = rotate_fwd(block[:, :, 0], cosine, sine_vals).astype(jnp.bfloat16)
        keys = rotate_fwd(block[:, :, 1], cosine, sine_vals).astype(jnp.bfloat16)
        values = block[:, :, 2].astype(jnp.bfloat16)
        scores = jnp.einsum("qhd,khd->hqk", query, keys, preferred_element_type=jnp.float32) * scale
        masked = jnp.where(causal[None], scores, -1e30)
        row_max = jnp.max(masked, axis=-1, keepdims=True)
        exp_sum = jnp.sum(
            jnp.where(causal[None], jnp.exp(masked - row_max), 0.0), axis=-1, keepdims=True
        )
        log_total = row_max + jnp.log(exp_sum)
        probs_low = jnp.where(causal[None], jnp.exp(masked - log_total), 0.0).astype(jnp.bfloat16)
        attended = jnp.einsum(
            "hqk,khd->qhd", probs_low, values, preferred_element_type=jnp.float32
        ).astype(jnp.bfloat16)
        return (query, keys, values, attended, log_total)

    query, keys, values, attended, log_total = lax.map(
        forward_seq, qkv_pre.reshape(seq_count, SEQ, local_heads, 3, HD)
    )
    attn_out = attended.reshape(tok_rows, head_cols)
    gelu_out = gelu_value(fc_pre).astype(jnp.bfloat16)
    out_stack = jnp.concatenate([w_dense, w_proj], axis=0)
    shard_piece = lax.all_gather(out_stack, "row", axis=1, tiled=True)
    mixed = jnp.dot(
        attn_out, shard_piece[:head_cols], preferred_element_type=jnp.float32
    ) + jnp.dot(gelu_out, shard_piece[head_cols:], preferred_element_type=jnp.float32)
    branch_sum = lax.psum_scatter(mixed, "col", scatter_dimension=1, tiled=True)
    block_output = block_input + branch_sum + b_dense + b_proj
    grad_low = out_grad.astype(jnp.bfloat16)
    wide_grad = lax.all_gather(grad_low, "col", axis=1, tiled=True)
    both_grad = lax.dot_general(
        wide_grad,
        lax.all_gather(out_stack, "row", axis=1, tiled=True),
        contract_last,
        preferred_element_type=jnp.float32,
    )
    attn_grad = both_grad[:, :head_cols]
    gelu_grad = both_grad[:, head_cols:]
    attn_grad_low = attn_grad.astype(jnp.bfloat16)
    fc_grad = gelu_grad * gelu_slope(fc_pre)
    fc_bias_grad = jnp.sum(fc_grad, axis=0)
    fc_grad_low = fc_grad.astype(jnp.bfloat16)

    def backward_seq(items):
        query_s, keys_s, values_s, attended_s, log_s, head_grad = items
        scores = (
            jnp.einsum("qhd,khd->hqk", query_s, keys_s, preferred_element_type=jnp.float32) * scale
        )
        probs = jnp.where(
            causal[None], jnp.exp(jnp.where(causal[None], scores, -1e30) - log_s), 0.0
        )
        probs_low = probs.astype(jnp.bfloat16)
        value_grad = jnp.einsum(
            "hqk,qhd->khd", probs_low, head_grad, preferred_element_type=jnp.float32
        )
        prob_grad = jnp.einsum(
            "qhd,khd->hqk", head_grad, values_s, preferred_element_type=jnp.float32
        )
        delta_row = jnp.transpose(
            jnp.sum(head_grad.astype(jnp.float32) * attended_s.astype(jnp.float32), axis=-1), (1, 0)
        )[:, :, None]
        score_grad = (probs * (prob_grad - delta_row) * scale).astype(jnp.bfloat16)
        query_grad = jnp.einsum(
            "hqk,khd->qhd", score_grad, keys_s, preferred_element_type=jnp.float32
        )
        key_grad = jnp.einsum(
            "hqk,qhd->khd", score_grad, query_s, preferred_element_type=jnp.float32
        )
        return jnp.stack(
            [
                rotate_back(query_grad, cosine, sine_vals),
                rotate_back(key_grad, cosine, sine_vals),
                value_grad,
            ],
            axis=2,
        )

    head_grads = attn_grad_low.reshape(seq_count, SEQ, local_heads, HD)
    qkv_grad = lax.map(
        backward_seq, (query, keys, values, attended, log_total, head_grads)
    ).reshape(tok_rows, qkv_cols)
    qkv_bias_grad = jnp.sum(qkv_grad, axis=0)
    qkv_grad_low = qkv_grad.astype(jnp.bfloat16)
    in_stack = jnp.concatenate([w_qkv, w_fc], axis=1)
    shard_piece = lax.all_gather(in_stack, "row", axis=0, tiled=True)
    norm_grads = jnp.stack(
        [
            lax.dot_general(
                qkv_grad_low,
                shard_piece[:, :qkv_cols],
                contract_last,
                preferred_element_type=jnp.float32,
            ),
            lax.dot_general(
                fc_grad_low,
                shard_piece[:, qkv_cols:],
                contract_last,
                preferred_element_type=jnp.float32,
            ),
        ]
    )
    part_one = wide_one
    part_two = wide_two
    row_part = lax.psum_scatter(
        jnp.concatenate(
            [
                lax.dot_general(
                    part_one, qkv_grad_low, contract_first, preferred_element_type=jnp.float32
                ),
                lax.dot_general(
                    part_two, fc_grad_low, contract_first, preferred_element_type=jnp.float32
                ),
                lax.dot_general(
                    wide_grad, attn_out, contract_first, preferred_element_type=jnp.float32
                ),
                lax.dot_general(
                    wide_grad, gelu_out, contract_first, preferred_element_type=jnp.float32
                ),
            ],
            axis=1,
        ),
        "row",
        scatter_dimension=0,
        tiled=True,
    )
    grad_rows = lax.psum(row_part, "dp")
    qkv_total = grad_rows[:, :qkv_cols]
    fc_total = grad_rows[:, qkv_cols : qkv_cols + fc_cols]
    dense_total = grad_rows[:, qkv_cols + fc_cols : qkv_cols + fc_cols + head_cols].T
    proj_total = grad_rows[:, qkv_cols + fc_cols + head_cols :].T
    norm_local = lax.psum_scatter(norm_grads, "col", scatter_dimension=2, tiled=True)
    grad_one = norm_local[0]
    grad_two = norm_local[1]
    hat_grad = grad_one * ln1_gain + grad_two * ln2_gain
    total_hat, total_cross = lax.psum(
        (jnp.sum(hat_grad, axis=1), jnp.sum(hat_grad * x_hat, axis=1)), "col"
    )
    input_grad = out_grad + inv_std * (
        hat_grad - (total_hat / D)[:, None] - x_hat * (total_cross / D)[:, None]
    )
    gain_one, shift_one, gain_two, shift_two, qkv_bias_total, fc_bias_total, out_bias_total = (
        lax.psum(
            (
                jnp.sum(grad_one * x_hat, axis=0),
                jnp.sum(grad_one, axis=0),
                jnp.sum(grad_two * x_hat, axis=0),
                jnp.sum(grad_two, axis=0),
                qkv_bias_grad,
                fc_bias_grad,
                jnp.sum(out_grad, axis=0),
            ),
            ("dp", "row"),
        )
    )
    return (
        block_output,
        input_grad,
        gain_one,
        shift_one,
        gain_two,
        shift_two,
        qkv_total,
        qkv_bias_total,
        dense_total,
        out_bias_total,
        fc_total,
        fc_bias_total,
        proj_total,
        out_bias_total,
    )


f32 = jnp.float32
bf16 = jnp.bfloat16
MESH = pl.DeviceIdType.MESH
VMEM = pltpu.VMEM
Q = 256
HALF = 4 * Q


def flip(a, b):
    return a + b - 2 * a * b


def span(start, size):
    return pl.ds(pl.multiple_of(start, size), size)


def mm(a, b):
    return jnp.dot(a, b, preferred_element_type=f32)


def mm_nt(a, b):
    return lax.dot_general(a, b, (((1,), (1,)), ((), ())), preferred_element_type=f32)


def mm_tn(a, b):
    return lax.dot_general(a, b, (((0,), (0,)), ((), ())), preferred_element_type=f32)


class Net:
    def __init__(self, send_sems, recv_sems, local_sems):
        self.k = lax.axis_index("dp")
        self.r = lax.axis_index("row")
        self.c = lax.axis_index("col")
        k, r, c = self.k, self.r, self.c
        self.core = (1 - k, r, c)
        self.x = (k, r + 1 - 2 * (r % 2), c)
        self.y = (k, r + 2 - 4 * (r // 2), c)
        near = c + 1 - 2 * (c % 2)
        self.z = (None, (k, r, near), (k, r, c + 2 - 4 * (c // 2)), (k, r, 3 - c))
        self.middle = flip(c % 2, c // 2) == 1
        self.send_sems, self.recv_sems, self.local_sems = send_sems, recv_sems, local_sems
        self.remote_count = 0
        self.local_count = 0
        self.pending = []

    def mix(self, j):
        return flip(j % 2, flip(self.c % 2, self.r % 2)) + 2 * flip(
            j // 2, flip(self.c // 2, self.r // 2)
        )

    def barrier(self):
        sem = pltpu.get_barrier_semaphore()
        peers = (self.core, self.x, self.y) + self.z[1:]
        for peer in peers:
            pl.semaphore_signal(sem, inc=1, device_id=peer, device_id_type=MESH)
        pl.semaphore_wait(sem, len(peers))

    def slot(self):
        self.remote_count += 1
        return self.remote_count - 1

    def remote(self, src, dst, peer):
        slot = self.slot()
        copy = pltpu.make_async_remote_copy(
            src_ref=src,
            dst_ref=dst,
            send_sem=self.send_sems.at[slot],
            recv_sem=self.recv_sems.at[slot],
            device_id=peer,
            device_id_type=MESH,
        )
        copy.start()
        self.pending.append(copy)
        return copy

    def local(self, src, dst):
        copy = pltpu.make_async_copy(src, dst, self.local_sems.at[self.local_count])
        self.local_count += 1
        copy.start()
        return copy

    def sent(self, copy):
        copy.wait_send()
        self.pending = [other for other in self.pending if other is not copy]

    def drain(self):
        for copy in self.pending:
            copy.wait_send()


class Gather:
    def __init__(self, net, shard, full, by_rows):
        self.net, self.shard, self.full, self.by_rows = net, shard, full, by_rows
        self.depth = Q // 2 if by_rows else shard.shape[0] // 2
        self.placed = []

    def own(self, half, part=None):
        if self.by_rows:
            if part is None:
                return self.shard.at[span(half * Q, Q), :]
            return self.shard.at[span(half * Q + part * self.depth, self.depth), :]
        rows = slice(None) if part is None else pl.ds(part * self.depth, self.depth)
        return self.shard.at[rows, span(half * Q, Q)]

    def chunk(self, s, i, part=None):
        start = s * HALF + i * Q
        if self.by_rows:
            if part is None:
                return self.full.at[pl.ds(start, Q), :]
            return self.full.at[pl.ds(start + part * self.depth, self.depth), :]
        rows = slice(None) if part is None else pl.ds(part * self.depth, self.depth)
        return self.full.at[rows, pl.ds(start, Q)]

    def place_own(self):
        net = self.net
        self.placed = [
            net.local(self.own(net.k), self.chunk(0, 0)),
            net.local(self.own(1 - net.k), self.chunk(1, 0)),
        ]

    def send_own(self):
        net, k = self.net, self.net.k
        self.y0 = net.remote(self.own(k, 0), self.chunk(0, 2, 0), net.y)
        self.x1 = net.remote(self.own(k, 1), self.chunk(0, 1, 1), net.x)
        self.y1 = net.remote(self.own(k, 1), self.chunk(0, 2, 1), net.y)
        self.x0 = net.remote(self.own(k, 0), self.chunk(0, 1, 0), net.x)

    def forward(self):
        net = self.net
        self.y0.wait_recv()
        self.d0 = net.remote(self.chunk(0, 2, 0), self.chunk(0, 3, 0), net.x)
        self.x1.wait_recv()
        self.d1 = net.remote(self.chunk(0, 1, 1), self.chunk(0, 3, 1), net.y)

    def swap_near(self):
        net = self.net
        self.x0.wait_recv()
        self.c1 = net.remote(self.chunk(0, 1), self.chunk(1, 1), net.core)
        self.y1.wait_recv()
        self.c2 = net.remote(self.chunk(0, 2), self.chunk(1, 2), net.core)

    def swap_far(self):
        net = self.net
        self.d0.wait_recv()
        self.d1.wait_recv()
        self.c3 = net.remote(self.chunk(0, 3), self.chunk(1, 3), net.core)

    def ready(self):
        for copy in (self.c1, self.c2, self.c3):
            copy.wait_recv()
        for copy in self.placed:
            copy.wait()

    def release(self):
        for copy in (self.d0, self.d1, self.c1, self.c2, self.c3):
            self.net.sent(copy)


class Line:
    def __init__(self, net, slots):
        self.net, self.slots = net, slots
        self.ids = [None] + [net.slot() for _ in range(3)]
        self.sends = []

    def copy(self, src, dst, peer, send):
        net = self.net
        return pltpu.make_async_remote_copy(
            src_ref=self.slots.at[src],
            dst_ref=self.slots.at[dst],
            send_sem=net.send_sems.at[send],
            recv_sem=net.recv_sems.at[self.ids[dst]],
            device_id=peer,
            device_id_type=MESH,
        )

    def start(self):
        net = self.net
        self.first = self.copy(0, 1, net.z[1], self.ids[1])
        self.first.start()
        self.hops = [
            self.copy(0, 3, net.z[3], self.ids[2]),
            self.copy(1, 2, net.z[3], self.ids[3]),
            self.copy(3, 2, net.z[1], net.slot()),
            self.copy(2, 3, net.z[1], net.slot()),
        ]

        @pl.when(net.middle)
        def _():
            self.hops[0].start()

    def arrived(self, slot):
        return self.copy(0, slot, self.net.z[1], self.ids[slot])

    def step(self, number):
        slot = (1, 3, 2)[number]

        @pl.when(self.net.middle)
        def _():
            self.arrived(slot).wait_recv()
            self.hops[number + 1].start()

    def ready(self):
        @pl.when(jnp.logical_not(self.net.middle))
        def _():
            for slot in (1, 2, 3):
                self.arrived(slot).wait_recv()

    def drain(self):
        self.first.wait_send()

        @pl.when(self.net.middle)
        def _():
            for hop in self.hops:
                hop.wait_send()


class Fold:
    def __init__(self, net, blocks, inbox):
        self.net, self.blocks, self.inbox = net, blocks, inbox
        hops = ((3, None, 0), (2, None, 1), (1, None, 2), (None, 0, 3), (None, 1, 4), (None, 3, 0))
        self.copies = []
        for n, (block, slot, dest) in enumerate(hops):
            number = net.slot()
            self.copies.append(
                pltpu.make_async_remote_copy(
                    src_ref=blocks.at[block] if slot is None else inbox.at[slot],
                    dst_ref=inbox.at[dest],
                    send_sem=net.send_sems.at[number],
                    recv_sem=net.recv_sems.at[number],
                    device_id=net.z[3] if n in (3, 4) else net.z[1],
                    device_id_type=MESH,
                )
            )

    def start(self):
        @pl.when(jnp.logical_not(self.net.middle))
        def _():
            for copy in self.copies[:3]:
                copy.start()

    def step(self, number):
        slot, block = ((0, 2), (1, 3), (3, 1))[number]
        inbox, blocks = self.inbox, self.blocks

        @pl.when(self.net.middle)
        def _():
            self.copies[(0, 1, 3)[number]].wait_recv()

            def add(n, _):
                at = span(n * 64, 64)
                total = inbox[slot, at, :].astype(f32) + blocks[block, at, :].astype(f32)
                inbox[slot, at, :] = total.astype(bf16)
                return 0

            lax.fori_loop(0, inbox.shape[1] // 64, add, 0)
            self.copies[3 + number].start()

    def total(self, use):
        def gather(*slots):
            def add(n, _):
                at = span(n * 64, 64)
                value = self.blocks[0, at, :].astype(f32)
                for slot in slots:
                    value = value + self.inbox[slot, at, :].astype(f32)
                use(at, value)
                return 0

            lax.fori_loop(0, self.inbox.shape[1] // 64, add, 0)

        @pl.when(self.net.middle)
        def _():
            self.copies[2].wait_recv()
            self.copies[4].wait_recv()
            gather(2, 4)

        @pl.when(jnp.logical_not(self.net.middle))
        def _():
            self.copies[5].wait_recv()
            gather(0)

    def drain(self):
        @pl.when(self.net.middle)
        def _():
            for copy in self.copies[3:]:
                copy.wait_send()

        @pl.when(jnp.logical_not(self.net.middle))
        def _():
            for copy in self.copies[:3]:
                copy.wait_send()


def turn(low, tables, sign):
    lane = lax.broadcasted_iota(jnp.int32, low.shape, 1)
    swung = jnp.where(lane < ROT // 2, pltpu.roll(low, 96, 1), pltpu.roll(low, 32, 1))
    return low * tables[0] + sign * (tables[1] * swung)


class Tiles:
    def __init__(self, slots, sems):
        self.slots, self.sems = slots, sems

    def write(self, count, product, place, depth):
        def body(n, _):
            slot = n % 2
            source = self.slots.at[slot, pl.ds(0, depth), :]
            copy = pltpu.make_async_copy(source, place(n), self.sems.at[slot])

            @pl.when(n >= 2)
            def _():
                copy.wait()

            self.slots[slot, 0:depth, :] = product(n).astype(bf16)
            copy.start()
            return 0

        lax.fori_loop(0, count, body, 0)
        for slot in range(2):
            source = self.slots.at[slot, pl.ds(0, depth), :]
            pltpu.make_async_copy(source, place(slot), self.sems.at[slot]).wait()


class Reduce:
    def __init__(self, net, partial, joined, near, far, by_rows, in_vmem=False):
        self.in_vmem = in_vmem
        self.net, self.partial, self.by_rows = net, partial, by_rows
        self.joined, self.near, self.far = joined, near, far
        self.depth = Q // 2 if by_rows else partial.shape[0] // 2

    def chunk(self, i, half):
        if self.by_rows:
            return self.partial.at[pl.ds(i * Q + half * self.depth, self.depth), :]
        return self.partial.at[pl.ds(half * self.depth, self.depth), pl.ds(i * Q, Q)]

    def whole(self):
        if self.by_rows:
            return self.partial.at[pl.ds(0, Q), :]
        return self.partial.at[:, pl.ds(0, Q)]

    def rows(self, half):
        return pl.ds(half * self.depth, self.depth)

    def start(self):
        net = self.net
        self.a = net.remote(self.chunk(3, 0), self.joined.at[0], net.x)
        self.b = net.remote(self.chunk(3, 1), self.joined.at[1], net.y)
        self.near_a = net.remote(self.chunk(1, 0), self.near.at[self.rows(0), :], net.x)
        self.near_b = net.remote(self.chunk(2, 1), self.near.at[self.rows(1), :], net.y)

    def join(self, parts):
        net = self.net
        loads = [net.local(self.chunk(2, 0), parts[0]), net.local(self.chunk(1, 1), parts[1])]
        hops = []
        for half, copy, peer in ((0, self.a, net.y), (1, self.b, net.x)):
            loads[half].wait()
            copy.wait_recv()
            tile = 64

            def add(n, _, half=half):
                at = span(n * tile, tile)
                total = self.joined[half, at, :].astype(f32) + parts[half][at, :].astype(f32)
                self.joined[half, at, :] = total.astype(bf16)
                return 0

            lax.fori_loop(0, self.depth // tile, add, 0)
            hops.append(net.remote(self.joined.at[half], self.far.at[self.rows(half), :], peer))
        self.far_a, self.far_b = hops

    def prepare(self, buffers):
        net = self.net
        self.buffers = list(buffers)
        self.loads = [net.local(self.whole(), buffers[0])]
        for copy in (self.near_a, self.near_b):
            copy.wait_recv()
        if self.in_vmem:
            self.buffers[1:3] = [self.near, self.far]
        else:
            self.loads.append(net.local(self.near, buffers[1]))

    def finish(self, out):
        net, buffers = self.net, self.buffers
        for copy in (self.far_a, self.far_b):
            copy.wait_recv()
        if not self.in_vmem:
            self.loads.append(net.local(self.far, buffers[2]))
        for copy in self.loads:
            copy.wait()
        tile = 64

        def add(n, _):
            at = span(n * tile, tile)
            parts = [buffer[at, :].astype(f32) for buffer in buffers[:3]]
            buffers[3][at, :] = (parts[0] + parts[1] + parts[2]).astype(bf16)
            return 0

        lax.fori_loop(0, self.near.shape[0] // tile, add, 0)
        if self.by_rows:
            place = out.at[span(net.k * Q, Q), :]
        else:
            place = out.at[:, span(net.k * Q, Q)]
        self.here = net.local(buffers[3], place)
        self.there = net.remote(buffers[3], place, net.core)

    def done(self):
        self.here.wait()
        self.there.wait_recv()


def block_kernel(
    x, og, w_qkv, w_dense, w_fc, w_proj, t_turn,
    gain_1, bias_1, gain_2, bias_2, b_qkv, b_fc, b_dense, b_proj,
    o_proj, o_qkv, o_fc, o_dense, o_block, o_input, o_small,
    all_proj, r_proj, r_qkv, r_fc, r_dense, n_proj, f_proj, n_qkv, f_qkv, n_fc, f_fc,
    g_qkv, g_dense, g_fc, g_tail, xs, ys, pks, stats, rows, h1c, h1s, h2c, h2s, dyc, dys, xh,
    qb, kb, vb, probs, probs_low, oc, dob, dqc, gc, slope, dabt, stage,
    out_recv, hat_recv, j_proj, j_qkv, j_fc, j_dense, n_dense, f_dense, tables, vecs, bias, packs, small,
    send_sems, recv_sems, local_sems, stage_sems,
):
    tok = x.shape[0]
    heads = qb.shape[0]
    width = gc.shape[1]
    scale = 1.0 / math.sqrt(HD)
    net = Net(send_sems, recv_sems, local_sems)
    net.barrier()
    qkv = Gather(net, w_qkv, g_qkv, True)
    dense = Gather(net, w_dense, g_dense, False)
    fc = Gather(net, w_fc, g_fc, True)
    proj = Gather(net, w_proj, all_proj, False)
    qkv.send_own()
    dense.send_own()
    load_x = net.local(x, probs.at[0])
    load_og = net.local(og, probs.at[1])
    load_turn = net.local(t_turn, tables)
    tiles = Tiles(stage, stage_sems)
    mine = pl.ds(0, tok)
    theirs = pl.ds(tok, tok)

    step = 128
    lane = lax.broadcasted_iota(jnp.int32, (step, 128), 1)
    load_x.wait()

    def local_norm(n, _):
        at = span(n * step, step)
        block = probs[0, at, :]
        mean = jnp.mean(block, axis=1, keepdims=True)
        centred = block - mean
        var = jnp.mean(centred * centred, axis=1, keepdims=True)
        stats[at, :] = jnp.where(lane == 0, mean, jnp.where(lane == 1, var, 0.0))
        return 0

    lax.fori_loop(0, tok // step, local_norm, 0)
    pks[0] = stats[...].T[0:8]
    for n, vector in enumerate((gain_1, bias_1, gain_2, bias_2)):
        pks[0, 2 + n : 3 + n, :] = vector[...].reshape(1, 512)
    packed = [net.remote(pks.at[0], pks.at[j], net.z[j]) for j in (1, 2, 3)]
    for weight in (qkv, dense, fc):
        weight.place_own()
    bias[...] = jnp.zeros_like(bias)
    bias[3:4, 0 : b_qkv.shape[0]] = b_qkv[...].reshape(1, b_qkv.shape[0])
    bias[4:5, :] = b_fc[...].reshape(1, width)
    bias[5:6, 0:512] = (b_dense[...] + b_proj[...]).reshape(1, 512)
    rows[...] = jnp.zeros_like(rows)
    load_og.wait()

    def local_grad(n, _):
        at = span(n * step, step)
        block = probs[1, at, :]
        ys[0, at, :] = block.astype(bf16)
        bias[1:2, 0:512] += jnp.sum(block, axis=0, keepdims=True)
        return 0

    lax.fori_loop(0, tok // step, local_grad, 0)
    for pack in packed:
        pack.wait_recv()
    means = [pks[j, 0:1, :] for j in range(4)]
    mu = (means[0] + means[1] + means[2] + means[3]) * 0.25
    spread = [pks[j, 1:2, :] + (means[j] - mu) * (means[j] - mu) for j in range(4)]
    rows[0:1, :] = mu
    rows[1:2, :] = lax.rsqrt((spread[0] + spread[1] + spread[2] + spread[3]) * 0.25 + epsilon)
    stats[...] = rows[...].T

    def own_norm(n, _):
        at = span(n * step, step)
        hats = (probs[0, at, :] - stats[at, 0:1]) * stats[at, 1:2]
        xs[0, at, :] = (hats * pks[0, 2:3, :] + pks[0, 3:4, :]).astype(bf16)
        return 0

    lax.fori_loop(0, tok // step, own_norm, 0)
    x_line = Line(net, xs)
    y_line = Line(net, ys)
    x_line.start()
    qkv.forward()
    x_line.step(0)
    x_line.step(1)
    fc.send_own()
    dense.forward()
    qkv.swap_near()
    x_line.step(2)
    y_line.start()
    dense.swap_near()
    qkv.swap_far()
    dense.swap_far()
    x_line.ready()

    for s in range(2):
        for j in range(4):
            lanes = span(flip(s, net.k) * Q, Q)
            dest = span(net.mix(j) * Q, Q)
            wide = span(s * HALF + net.mix(j) * Q, Q)
            vecs[0:4, wide] = pks[j, 2:6, lanes]

            def norm(n, _, s=s, j=j, lanes=lanes, dest=dest, wide=wide):
                at = span(n * step, step)
                one = xs[j, at, lanes]
                hats = (one.astype(f32) - pks[j, 3:4, lanes]) * (1.0 / pks[j, 2:3, lanes])
                xh[at, wide] = hats.astype(bf16)
                (h1s if s else h1c)[at, dest] = one
                two = hats * pks[j, 4:5, lanes] + pks[j, 5:6, lanes]
                (h2s if s else h2c)[at, dest] = two.astype(bf16)
                return 0

            lax.fori_loop(0, tok // step, norm, 0)
    swap_h1 = net.remote(h1s, h1c.at[theirs, :], net.core)
    swap_h2 = net.remote(h2s, h2c.at[theirs, :], net.core)
    fc.forward()
    proj.send_own()
    y_line.step(0)
    load_turn.wait()
    qkv.ready()

    def project(n, _):
        cols = span(n * 3 * HD, 3 * HD)
        acc = mm(h1c[mine, :], g_qkv[0:HALF, cols]) + mm(h1s[...], g_qkv[HALF:, cols])
        acc = acc + bias[3:4, cols]
        qb[n, :, 0:128] = turn(acc[:, 0:128], tables, 1.0).astype(bf16)
        qb[n, :, 128:HD] = acc[:, 128:HD].astype(bf16)
        kb[n, :, 0:128] = turn(acc[:, HD : HD + 128], tables, 1.0).astype(bf16)
        kb[n, :, 128:HD] = acc[:, HD + 128 : 2 * HD].astype(bf16)
        vb[n] = acc[:, 2 * HD :].astype(bf16)
        return 0

    lax.fori_loop(0, heads, project, 0)
    y_line.step(1)
    chunks = tok // step

    def attend(n, _):
        head, chunk = n // chunks, n % chunks
        at = span(chunk * step, step)
        scores = mm_nt(qb[head, at, :], kb[head]) * scale
        token = lax.broadcasted_iota(jnp.int32, (step, tok), 0) + chunk * step
        allowed = token >= lax.broadcasted_iota(jnp.int32, (step, tok), 1)
        scores = jnp.where(allowed, scores, -1e30)
        top = jnp.max(scores, axis=1, keepdims=True)
        raised = jnp.where(allowed, jnp.exp(scores - top), 0.0)
        weight = raised / jnp.sum(raised, axis=1, keepdims=True)
        probs[head, at, :] = weight
        low = weight.astype(bf16)
        probs_low[head, at, :] = low
        oc[at, span(head * HD, HD)] = mm(low, vb[head]).astype(bf16)
        return 0

    lax.fori_loop(0, heads * chunks, attend, 0)
    swap_o = net.remote(oc.at[mine, :], oc.at[theirs, :], net.core)
    fc.swap_near()
    y_line.step(2)
    fc.swap_far()
    fc.ready()

    def expand(n, _):
        cols = span(n * 512, 512)
        a = mm(h2c[mine, :], g_fc[0:HALF, cols]) + mm(h2s[...], g_fc[HALF:, cols])
        a = a + bias[4:5, cols]
        rise = 0.5 * (1.0 + lax.erf(a * 0.7071067811865476))
        gc[mine, cols] = (a * rise).astype(bf16)
        slope[:, cols] = (rise + a * 0.3989422804014327 * jnp.exp(-0.5 * a * a)).astype(bf16)
        return 0

    lax.fori_loop(0, width // 512, expand, 0)
    swap_g = net.remote(gc.at[mine, :], gc.at[theirs, :], net.core)
    proj.forward()
    y_line.ready()
    for s in range(2):
        for j in range(4):
            lanes = span(flip(s, net.k) * Q, Q)
            dest = span(net.mix(j) * Q, Q)
            (dys if s else dyc)[mine, dest] = ys[j, :, lanes]
    swap_dy = net.remote(dys, dyc.at[theirs, :], net.core)
    dense.ready()
    dob[...] = (
        mm_nt(dyc[mine, :], g_dense[:, 0:HALF]) + mm_nt(dys[...], g_dense[:, HALF:])
    ).astype(bf16)

    red_proj = Reduce(net, r_proj, j_proj, n_proj, f_proj, False)
    red_qkv = Reduce(net, r_qkv, j_qkv, n_qkv, f_qkv, True)
    red_fc = Reduce(net, r_fc, j_fc, n_fc, f_fc, True)
    red_dense = Reduce(net, r_dense, j_dense, n_dense, f_dense, False, True)
    swap_g.wait_recv()
    swap_dy.wait_recv()
    tall = width // 2
    tiles.write(
        4,
        lambda n: mm_tn(gc[:, span(n // 2 * tall, tall)], dyc[:, span(n % 2 * 512, 512)]),
        lambda n: r_proj.at[span(n // 2 * tall, tall), span(n % 2 * 512, 512)],
        tall,
    )
    proj.swap_near()
    red_proj.start()

    def keep(head, part, at, value, rotated):
        base = head * 3 * HD + part * HD
        if rotated:
            low = turn(value[:, 0:128], [tables[t, at, :] for t in range(2)], -1.0)
            dqc[at, pl.ds(pl.multiple_of(base, 128), 128)] = low.astype(bf16)
            bias[0:1, pl.ds(pl.multiple_of(base, 128), 128)] += jnp.sum(low, axis=0, keepdims=True)
            value, base, size = value[:, 128:], base + 128, 128
        else:
            size = HD
        cols = pl.ds(pl.multiple_of(base, 128), size)
        dqc[at, cols] = value.astype(bf16)
        bias[0:1, cols] += jnp.sum(value, axis=0, keepdims=True)

    def attend_back(head, _):
        cols = span(head * HD, HD)

        def chunk_back(n, _):
            at = span(n * step, step)
            grad = dob[at, cols]
            delta = jnp.sum(grad.astype(f32) * oc[at, cols].astype(f32), axis=1, keepdims=True)
            spread = mm_nt(grad, vb[head]) - delta
            low = (probs[head, at, :] * spread * scale).astype(bf16)
            probs_low[head, at, :] = low
            keep(head, 0, at, mm(low, kb[head]), True)
            return 0

        keep(head, 2, mine, mm_tn(probs_low[head], dob[:, cols]), False)
        lax.fori_loop(0, chunks, chunk_back, 0)
        keep(head, 1, mine, mm_tn(probs_low[head], qb[head]), True)
        return 0

    lax.fori_loop(0, heads, attend_back, 0)
    swap_dq = net.remote(dqc.at[mine, :], dqc.at[theirs, :], net.core)
    net.sent(swap_h1)
    net.sent(swap_h2)
    for s in range(2):

        def back_first(n, _, s=s):
            wide = span(s * HALF + n * 512, 512)
            grad = mm_nt(dqc[mine, :], g_qkv[wide, :])
            (h2s if s else h1s)[:, span(n * 512, 512)] = (grad * vecs[0:1, wide]).astype(bf16)
            vecs[4:5, wide] = jnp.sum(grad * xh[:, wide].astype(f32), axis=0, keepdims=True)
            vecs[5:6, wide] = jnp.sum(grad, axis=0, keepdims=True)
            return 0

        lax.fori_loop(0, HALF // 512, back_first, 0)

    proj.swap_far()
    proj.ready()
    qkv.release()
    loads = [
        net.local(w_proj.at[:, span(net.k * Q, Q)], g_qkv.at[:, pl.ds(0, Q)]),
        net.local(w_proj.at[:, span((1 - net.k) * Q, Q)], g_qkv.at[:, pl.ds(HALF, Q)]),
        net.local(all_proj.at[:, pl.ds(Q, 3 * Q)], g_qkv.at[:, pl.ds(Q, 3 * Q)]),
        net.local(all_proj.at[:, pl.ds(5 * Q, Q)], g_qkv.at[:, pl.ds(5 * Q, Q)]),
        net.local(all_proj.at[:, pl.ds(6 * Q, 2 * Q)], g_tail),
    ]
    swap_o.wait_recv()
    attn = oc.shape[1]
    tiles.write(
        2,
        lambda n: mm_tn(oc[...], dyc[:, span(n * 512, 512)]),
        lambda n: r_dense.at[:, span(n * 512, 512)],
        attn,
    )
    swap_h1.wait_recv()
    swap_dq.wait_recv()
    tiles.write(
        dqc.shape[1] // 512,
        lambda n: mm_tn(h1c[...], dqc[:, span(n * 512, 512)]),
        lambda n: r_qkv.at[:, span(n * 512, 512)],
        HALF,
    )
    red_qkv.start()
    red_dense.start()

    for copy in loads:
        copy.wait()
    x_line.drain()
    y_line.drain()

    def put_out(p, product):
        s, i = p // 4, p % 4
        out = product + mm(oc[mine, :], g_dense[:, span(p * Q, Q)])
        xs[net.mix(i), :, span(flip(s, net.k) * Q, Q)] = out.astype(bf16)

    def project_head(p, _):
        put_out(p, mm(gc[mine, :], g_qkv[:, span(p * Q, Q)]))
        return 0

    def project_tail(p, _):
        put_out(6 + p, mm(gc[mine, :], g_tail[:, span(p * Q, Q)]))
        return 0

    lax.fori_loop(0, 6, project_head, 0)
    lax.fori_loop(0, 2, project_tail, 0)
    out_fold = Fold(net, xs, out_recv)
    out_fold.start()

    def back_fc(n, _):
        cols = span(n * 512, 512)
        grad = mm_nt(dyc[mine, :], g_qkv[cols, 0:HALF])
        grad = grad + mm_nt(dys[:, 0:512], g_qkv[cols, HALF : 6 * Q])
        grad = grad + mm_nt(dys[:, 512:], g_tail[cols, :])
        grad = grad * slope[:, cols].astype(f32)
        bias[2:3, cols] = jnp.sum(grad, axis=0, keepdims=True)
        slope[:, cols] = grad.astype(bf16)
        return 0

    lax.fori_loop(0, width // 512, back_fc, 0)
    dab = slope
    swap_da = net.remote(dab, dabt, net.core)
    red_proj.join([g_tail.at[pl.ds(0, tall), pl.ds(0, Q)], g_tail.at[pl.ds(tall, tall), pl.ds(0, Q)]])
    stats[...] = jnp.zeros_like(stats)
    lane = lax.broadcasted_iota(jnp.int32, (tok, 128), 1)

    def back_norm(j, _):
        for s in range(2):
            lanes = span(flip(s, net.k) * Q, Q)
            dest = span(net.mix(j) * Q, Q)
            wide = span(s * HALF + net.mix(j) * Q, Q)
            grad = mm_nt(dab[...], g_fc[wide, :])
            hats = xh[:, wide].astype(f32)
            packs[j, 2:4, lanes] = vecs[4:6, wide]
            packs[j, 4:5, lanes] = jnp.sum(grad * hats, axis=0, keepdims=True)
            packs[j, 5:6, lanes] = jnp.sum(grad, axis=0, keepdims=True)
            joint = (h2s if s else h1s)[:, dest].astype(f32) + grad * vecs[2:3, wide]
            ys[j, :, lanes] = joint.astype(bf16)
            one = jnp.sum(joint, axis=1, keepdims=True)
            two = jnp.sum(joint * hats, axis=1, keepdims=True)
            stats[...] += jnp.where(lane == 0, one, jnp.where(lane == 1, two, 0.0))
        return 0

    lax.fori_loop(0, 4, back_norm, 0)

    fc.release()
    red_qkv.join(
        [g_fc.at[pl.ds(7 * Q + n * (Q // 2), Q // 2), pl.ds(0, 6 * Q)] for n in range(2)]
    )
    turned = stats[...].T
    for j in range(4):
        packs[j, 0:2, :] = turned[0:2]
        packs[j, 6:8, :] = jnp.zeros((2, tok), f32)
    pack_copies = [net.remote(packs.at[j], packs.at[3 + j], net.z[j]) for j in (1, 2, 3)]
    hat_fold = Fold(net, ys, hat_recv)
    hat_fold.start()
    out_fold.step(0)
    swap_h2.wait_recv()
    swap_da.wait_recv()

    def grad_fc(n):
        cols = span(n * 512, 512)
        return mm_tn(h2c[mine, :], dab[:, cols]) + mm_tn(h2c[theirs, :], dabt[:, cols])

    tiles.write(width // 512, grad_fc, lambda n: r_fc.at[:, span(n * 512, 512)], HALF)
    red_fc.start()
    out_fold.step(1)

    def strips(base, n, columns):
        return g_fc.at[pl.ds(base + n * Q, Q), pl.ds(0, columns)]

    out_fold.step(2)
    for copy in pack_copies:
        copy.wait_recv()
    total = packs[0] + packs[4] + packs[5] + packs[6]
    rows[2:4, :] = total[0:2, :]
    stats[...] = rows[...].T
    me = net.k * 4 + net.r
    small[me, 0:4, :] = total[2:6, :]
    for n in range(3):
        small[me, 4 + n : 5 + n, :] = bias[0:1, n * 512 : n * 512 + 512]
    for n in range(4):
        small[me, 7 + n : 8 + n, :] = bias[2:3, n * 512 : n * 512 + 512]
    small[me, 11:12, :] = bias[1:2, 0:512]
    small[me, 12:16, :] = jnp.zeros((4, 512), f32)
    small_copies = []
    for n in range(1, 8):
        row = flip(net.r % 2, n % 2) + 2 * flip(net.r // 2, n // 2 % 2)
        peer = (flip(net.k, n // 4), row, net.c)
        small_copies.append(net.remote(small.at[me], small.at[me], peer))
    reload_x = net.local(x, probs.at[1])
    red_proj.prepare([g_qkv.at[:, pl.ds(n * Q, Q)] for n in range(4)])
    red_proj.finish(o_proj)
    reload_x.wait()

    def close_out(at, value):
        probs[0, at, :] = probs[1, at, :] + value + bias[5:6, 0:512]

    out_fold.total(close_out)
    keep_block = net.local(probs.at[0], o_block)
    hat_fold.step(0)
    red_fc.join([g_fc.at[pl.ds(6 * Q + n * (Q // 2), Q // 2), :] for n in range(2)])
    hat_fold.step(1)
    hat_fold.step(2)
    keep_block.wait()
    reload_og = net.local(og, probs.at[0])
    red_qkv.prepare([strips(0, n, 6 * Q) for n in range(4)])
    red_qkv.finish(o_qkv)
    red_dense.join([g_tail.at[pl.ds(n * attn // 2, attn // 2), pl.ds(0, Q)] for n in range(2)])
    red_fc.prepare([strips(4 * Q, n, 8 * Q) for n in range(4)])
    red_dense.prepare([g_tail.at[pl.ds(n * attn, attn), pl.ds(Q, Q)] for n in range(4)])
    for copy in small_copies:
        copy.wait_recv()
    grand = small[0]
    for n in range(1, 8):
        grand = grand + small[n]
    small[8] = grand
    keep_small = net.local(small.at[8], o_small)
    reload_og.wait()

    def close_hat(at, value):
        mu, rstd = stats[at, 0:1], stats[at, 1:2]
        hats = (probs[1, at, :] - mu) * rstd
        mean, cross = stats[at, 2:3] * (1.0 / D), stats[at, 3:4] * (1.0 / D)
        probs[0, at, :] += rstd * (value - mean - hats * cross)

    hat_fold.total(close_hat)
    keep_input = net.local(probs.at[0], o_input)
    red_fc.finish(o_fc)
    red_dense.finish(o_dense)
    for weight in (red_proj, red_qkv, red_fc, red_dense):
        weight.done()
    keep_small.wait()
    keep_input.wait()
    out_fold.drain()
    hat_fold.drain()
    net.drain()


def call_block(*args):
    x, w_qkv, w_dense, w_fc = args[0], args[2], args[3], args[4]
    tok = x.shape[0]
    n_qkv, n_attn, n_fc = w_qkv.shape[1], w_dense.shape[0], w_fc.shape[1]
    heads = n_attn // HD
    wide = 2 * HALF
    any_spec = pl.BlockSpec(memory_space=pl.ANY)
    vmem = pl.BlockSpec(memory_space=VMEM)
    shape = jax.ShapeDtypeStruct
    pieces = ((n_fc, Q), (Q, n_qkv), (Q, n_fc), (n_attn, Q))
    outs = [
        shape((n_fc, 2 * Q), bf16), shape((2 * Q, n_qkv), bf16),
        shape((2 * Q, n_fc), bf16), shape((n_attn, 2 * Q), bf16),
        shape((tok, 512), f32), shape((tok, 512), f32), shape((16, 512), f32),
        shape((n_fc, wide), bf16), shape((n_fc, HALF), bf16), shape((HALF, n_qkv), bf16),
        shape((HALF, n_fc), bf16), shape((n_attn, HALF), bf16),
    ]
    outs += [shape(piece, bf16) for piece in pieces[:3] for _ in range(2)]
    scratch = [
        VMEM((wide, n_qkv), bf16), VMEM((n_attn, wide), bf16), VMEM((wide, n_fc), bf16),
        VMEM((n_fc, 2 * Q), bf16),
        VMEM((4, tok, 512), bf16), VMEM((4, tok, 512), bf16), VMEM((4, 8, tok), f32),
        VMEM((tok, 128), f32), VMEM((128, tok), f32),
        VMEM((2 * tok, HALF), bf16), VMEM((tok, HALF), bf16),
        VMEM((2 * tok, HALF), bf16), VMEM((tok, HALF), bf16),
        VMEM((2 * tok, HALF), bf16), VMEM((tok, HALF), bf16), VMEM((tok, wide), bf16),
        VMEM((heads, tok, HD), bf16), VMEM((heads, tok, HD), bf16), VMEM((heads, tok, HD), bf16),
        VMEM((heads, tok, tok), f32), VMEM((heads, tok, tok), bf16),
        VMEM((2 * tok, n_attn), bf16), VMEM((tok, n_attn), bf16), VMEM((2 * tok, n_qkv), bf16),
        VMEM((2 * tok, n_fc), bf16), VMEM((tok, n_fc), bf16), VMEM((tok, n_fc), bf16),
        VMEM((2, HALF, 512), bf16),
        VMEM((5, tok, 512), bf16), VMEM((5, tok, 512), bf16),
    ]
    scratch += [VMEM((2,) + ((r // 2, c)), bf16) for r, c in pieces]
    scratch += [VMEM(pieces[3], bf16)] * 2
    scratch += [
        VMEM((2, tok, 128), f32),
        VMEM((8, wide), f32), VMEM((8, n_fc), f32), VMEM((7, 8, tok), f32), VMEM((9, 16, 512), f32),
        pltpu.SemaphoreType.DMA((128,)), pltpu.SemaphoreType.DMA((128,)),
        pltpu.SemaphoreType.DMA((64,)), pltpu.SemaphoreType.DMA((2,)),
    ]
    return pl.pallas_call(
        block_kernel,
        name="block",
        out_shape=outs,
        in_specs=[any_spec] * 7 + [vmem] * 8,
        out_specs=[any_spec] * len(outs),
        scratch_shapes=scratch,
        compiler_params=pltpu.CompilerParams(
            collective_id=1, has_side_effects=True, vmem_limit_bytes=67043328
        ),
    )(*args)


def turn_tables(length):
    half_rot = ROT // 2
    frequency = (10000.0 ** (-np.arange(half_rot, dtype=np.float32) * (2.0 / ROT))).astype(np.float32)
    angles = np.arange(length, dtype=np.float32)[:, None] * frequency[None, :]
    tables = np.zeros((2, length, 128), np.float32)
    tables[0] = 1.0
    tables[0, :, :half_rot] = tables[0, :, half_rot:ROT] = np.cos(angles)
    tables[1, :, :half_rot] = -np.sin(angles)
    tables[1, :, half_rot:ROT] = np.sin(angles)
    return tables


def close_kernel(cuts, *refs):
    count = len(cuts)
    sources, small = refs[:count], refs[count]
    outs, vectors = refs[count + 1 : 2 * count + 1], refs[2 * count + 1 : 2 * count + 9]
    lows, wides = refs[2 * count + 9 : 3 * count + 9], refs[3 * count + 9 : -2]
    in_sems, out_sems = refs[-2:]
    loads, stores = [], []
    for n, cut in enumerate(cuts):
        rows = sources[n].shape[0] // cut
        for part in range(cut):
            at = pl.ds(part * rows, rows)
            number = len(loads)
            wide = lows[n] if n >= len(wides) else wides[n]
            loads.append(
                pltpu.make_async_copy(sources[n].at[at, :], lows[n].at[at, :], in_sems.at[number])
            )
            stores.append(
                (n, at, pltpu.make_async_copy(wide.at[at, :], outs[n].at[at, :], out_sems.at[number]))
            )
    for copy in loads:
        copy.start()
    for row, (vector, length) in zip((0, 1, 2, 3, 4, 7, 11, 11), ((v, v.shape[0]) for v in vectors)):
        for n in range(length // 512):
            vector[n * 512 : n * 512 + 512] = small[row + n, :]
    for load, (n, at, store) in zip(loads, stores):
        load.wait()
        if n < len(wides):
            wides[n][at, :] = lows[n][at, :].astype(f32)
        store.start()
    for _, _, store in stores:
        store.wait()


def call_close(proj, qkv, fc, dense, block, grad, small):
    any_spec = pl.BlockSpec(memory_space=pl.ANY)
    vmem = pl.BlockSpec(memory_space=VMEM)
    shape = jax.ShapeDtypeStruct
    arrays = (fc, proj, qkv, dense, block, grad)
    cuts = (4, 4, 2, 1, 2, 2)
    outs = [shape(a.shape, f32) for a in arrays]
    lengths = [512] * 4 + [qkv.shape[1], fc.shape[1], 512, 512]
    outs += [shape((length,), f32) for length in lengths]
    return pl.pallas_call(
        functools.partial(close_kernel, cuts),
        name="close",
        out_shape=outs,
        in_specs=[any_spec] * 6 + [vmem],
        out_specs=[any_spec] * 6 + [vmem] * 8,
        scratch_shapes=[VMEM(a.shape, a.dtype) for a in arrays]
        + [VMEM(a.shape, f32) for a in arrays[:4]]
        + [pltpu.SemaphoreType.DMA((sum(cuts),)), pltpu.SemaphoreType.DMA((sum(cuts),))],
        compiler_params=pltpu.CompilerParams(vmem_limit_bytes=60 << 20),
    )(*arrays, small)


def fused_shards(
    block_input, out_grad, ln1_gain, ln1_bias, ln2_gain, ln2_bias,
    w_qkv, b_qkv, w_dense, b_dense, w_fc, b_fc, w_proj, b_proj,
):
    results = call_block(
        block_input, out_grad, w_qkv, w_dense, w_fc, w_proj, turn_tables(SEQ),
        ln1_gain, ln1_bias, ln2_gain, ln2_bias, b_qkv, b_fc, b_dense, b_proj,
    )
    fc, proj, qkv, dense, block, grad, *vectors = call_close(*results[:7])
    gain_1, shift_1, gain_2, shift_2, qkv_bias, fc_bias, dense_bias, proj_bias = vectors
    return (
        block, grad, gain_1, shift_1, gain_2, shift_2, qkv, qkv_bias, dense, dense_bias,
        fc, fc_bias, proj, proj_bias,
    )


def solution(mesh):
    sizes = tuple(mesh.shape[name] for name in ("dp", "row", "col"))
    body = fused_shards if sizes == (2, 4, 4) else shards
    return jax.shard_map(
        body,
        mesh=mesh,
        in_specs=(
            P(("dp", "row"), "col"),
            P(("dp", "row"), "col"),
            P("col"),
            P("col"),
            P("col"),
            P("col"),
            P("row", "col"),
            P("col"),
            P("col", "row"),
            P("col"),
            P("row", "col"),
            P("col"),
            P("col", "row"),
            P("col"),
        ),
        out_specs=(
            P(("dp", "row"), "col"),
            P(("dp", "row"), "col"),
            P("col"),
            P("col"),
            P("col"),
            P("col"),
            P("row", "col"),
            P("col"),
            P("col", "row"),
            P("col"),
            P("row", "col"),
            P("col"),
            P("col", "row"),
            P("col"),
        ),
        check_vma=False,
    )
```

```python
import functools
import math

import jax
import jax.numpy as jnp
import numpy as np
from jax import lax
from jax.experimental import pallas as pl
from jax.experimental.pallas import tpu as pltpu
from jax.sharding import PartitionSpec as P

D = 2048
HD = 256
ROT = 64
SEQ = 512


epsilon = 1e-05
contract_last = (((1,), (1,)), ((), ()))
contract_first = (((0,), (0,)), ((), ()))


def angle_tables(length):
    half_rot = ROT // 2
    position = jnp.arange(length, dtype=jnp.float32)
    exponent = jnp.arange(half_rot, dtype=jnp.float32) * (2.0 / ROT)
    frequency = 10000.0 ** (-exponent)
    angles = position[:, None] * frequency[None, :]
    return (jnp.cos(angles), jnp.sin(angles))


def rotate_fwd(values, cosine, sine_vals):
    half_rot = ROT // 2
    first = values[..., :half_rot]
    second = values[..., half_rot:ROT]
    cos_part = cosine[:, None, :]
    sin_part = sine_vals[:, None, :]
    return jnp.concatenate(
        [
            first * cos_part - second * sin_part,
            second * cos_part + first * sin_part,
            values[..., ROT:],
        ],
        axis=-1,
    )


def rotate_back(grads, cosine, sine_vals):
    half_rot = ROT // 2
    first = grads[..., :half_rot]
    second = grads[..., half_rot:ROT]
    cos_part = cosine[:, None, :]
    sin_part = sine_vals[:, None, :]
    return jnp.concatenate(
        [
            first * cos_part + second * sin_part,
            second * cos_part - first * sin_part,
            grads[..., ROT:],
        ],
        axis=-1,
    )


def gelu_value(pre_act):
    return 0.5 * pre_act * (1.0 + lax.erf(pre_act * 0.7071067811865476))


def gelu_slope(pre_act):
    return 0.5 * (
        1.0 + lax.erf(pre_act * 0.7071067811865476)
    ) + pre_act * 0.3989422804014327 * jnp.exp(-0.5 * pre_act * pre_act)


def shards(
    block_input,
    out_grad,
    ln1_gain,
    ln1_bias,
    ln2_gain,
    ln2_bias,
    w_qkv,
    b_qkv,
    w_dense,
    b_dense,
    w_fc,
    b_fc,
    w_proj,
    b_proj,
):
    tok_rows = block_input.shape[0]
    seq_count = tok_rows // SEQ
    qkv_cols = w_qkv.shape[1]
    fc_cols = w_fc.shape[1]
    local_heads = qkv_cols // (3 * HD)
    head_cols = local_heads * HD
    scale = 1.0 / math.sqrt(HD)
    cosine, sine_vals = angle_tables(SEQ)
    causal = jnp.arange(SEQ)[:, None] >= jnp.arange(SEQ)[None, :]
    row_total, square_total = lax.psum(
        (jnp.sum(block_input, axis=1), jnp.sum(block_input * block_input, axis=1)), "col"
    )
    mean_row = (row_total / D)[:, None]
    var_row = (square_total / D)[:, None] - mean_row * mean_row
    inv_std = lax.rsqrt(var_row + epsilon)
    x_hat = (block_input - mean_row) * inv_std
    normed_one = (x_hat * ln1_gain + ln1_bias).astype(jnp.bfloat16)
    normed_two = (x_hat * ln2_gain + ln2_bias).astype(jnp.bfloat16)
    wide_one, wide_two = (
        lax.all_gather(normed_one, "col", axis=1, tiled=True),
        lax.all_gather(normed_two, "col", axis=1, tiled=True),
    )
    part_one = wide_one
    part_two = wide_two
    qkv_pre = jnp.dot(
        part_one,
        lax.all_gather(w_qkv, "row", axis=0, tiled=True),
        preferred_element_type=jnp.float32,
    )
    fc_pre = jnp.dot(
        part_two,
        lax.all_gather(w_fc, "row", axis=0, tiled=True),
        preferred_element_type=jnp.float32,
    )
    qkv_pre = qkv_pre + b_qkv
    fc_pre = fc_pre + b_fc

    def forward_seq(block):
        query = rotate_fwd(block[:, :, 0], cosine, sine_vals).astype(jnp.bfloat16)
        keys = rotate_fwd(block[:, :, 1], cosine, sine_vals).astype(jnp.bfloat16)
        values = block[:, :, 2].astype(jnp.bfloat16)
        scores = jnp.einsum("qhd,khd->hqk", query, keys, preferred_element_type=jnp.float32) * scale
        masked = jnp.where(causal[None], scores, -1e30)
        row_max = jnp.max(masked, axis=-1, keepdims=True)
        exp_sum = jnp.sum(
            jnp.where(causal[None], jnp.exp(masked - row_max), 0.0), axis=-1, keepdims=True
        )
        log_total = row_max + jnp.log(exp_sum)
        probs_low = jnp.where(causal[None], jnp.exp(masked - log_total), 0.0).astype(jnp.bfloat16)
        attended = jnp.einsum(
            "hqk,khd->qhd", probs_low, values, preferred_element_type=jnp.float32
        ).astype(jnp.bfloat16)
        return (query, keys, values, attended, log_total)

    query, keys, values, attended, log_total = lax.map(
        forward_seq, qkv_pre.reshape(seq_count, SEQ, local_heads, 3, HD)
    )
    attn_out = attended.reshape(tok_rows, head_cols)
    gelu_out = gelu_value(fc_pre).astype(jnp.bfloat16)
    out_stack = jnp.concatenate([w_dense, w_proj], axis=0)
    shard_piece = lax.all_gather(out_stack, "row", axis=1, tiled=True)
    mixed = jnp.dot(
        attn_out, shard_piece[:head_cols], preferred_element_type=jnp.float32
    ) + jnp.dot(gelu_out, shard_piece[head_cols:], preferred_element_type=jnp.float32)
    branch_sum = lax.psum_scatter(mixed, "col", scatter_dimension=1, tiled=True)
    block_output = block_input + branch_sum + b_dense + b_proj
    grad_low = out_grad.astype(jnp.bfloat16)
    wide_grad = lax.all_gather(grad_low, "col", axis=1, tiled=True)
    both_grad = lax.dot_general(
        wide_grad,
        lax.all_gather(out_stack, "row", axis=1, tiled=True),
        contract_last,
        preferred_element_type=jnp.float32,
    )
    attn_grad = both_grad[:, :head_cols]
    gelu_grad = both_grad[:, head_cols:]
    attn_grad_low = attn_grad.astype(jnp.bfloat16)
    fc_grad = gelu_grad * gelu_slope(fc_pre)
    fc_bias_grad = jnp.sum(fc_grad, axis=0)
    fc_grad_low = fc_grad.astype(jnp.bfloat16)

    def backward_seq(items):
        query_s, keys_s, values_s, attended_s, log_s, head_grad = items
        scores = (
            jnp.einsum("qhd,khd->hqk", query_s, keys_s, preferred_element_type=jnp.float32) * scale
        )
        probs = jnp.where(
            causal[None], jnp.exp(jnp.where(causal[None], scores, -1e30) - log_s), 0.0
        )
        probs_low = probs.astype(jnp.bfloat16)
        value_grad = jnp.einsum(
            "hqk,qhd->khd", probs_low, head_grad, preferred_element_type=jnp.float32
        )
        prob_grad = jnp.einsum(
            "qhd,khd->hqk", head_grad, values_s, preferred_element_type=jnp.float32
        )
        delta_row = jnp.transpose(
            jnp.sum(head_grad.astype(jnp.float32) * attended_s.astype(jnp.float32), axis=-1), (1, 0)
        )[:, :, None]
        score_grad = (probs * (prob_grad - delta_row) * scale).astype(jnp.bfloat16)
        query_grad = jnp.einsum(
            "hqk,khd->qhd", score_grad, keys_s, preferred_element_type=jnp.float32
        )
        key_grad = jnp.einsum(
            "hqk,qhd->khd", score_grad, query_s, preferred_element_type=jnp.float32
        )
        return jnp.stack(
            [
                rotate_back(query_grad, cosine, sine_vals),
                rotate_back(key_grad, cosine, sine_vals),
                value_grad,
            ],
            axis=2,
        )

    head_grads = attn_grad_low.reshape(seq_count, SEQ, local_heads, HD)
    qkv_grad = lax.map(
        backward_seq, (query, keys, values, attended, log_total, head_grads)
    ).reshape(tok_rows, qkv_cols)
    qkv_bias_grad = jnp.sum(qkv_grad, axis=0)
    qkv_grad_low = qkv_grad.astype(jnp.bfloat16)
    in_stack = jnp.concatenate([w_qkv, w_fc], axis=1)
    shard_piece = lax.all_gather(in_stack, "row", axis=0, tiled=True)
    norm_grads = jnp.stack(
        [
            lax.dot_general(
                qkv_grad_low,
                shard_piece[:, :qkv_cols],
                contract_last,
                preferred_element_type=jnp.float32,
            ),
            lax.dot_general(
                fc_grad_low,
                shard_piece[:, qkv_cols:],
                contract_last,
                preferred_element_type=jnp.float32,
            ),
        ]
    )
    part_one = wide_one
    part_two = wide_two
    row_part = lax.psum_scatter(
        jnp.concatenate(
            [
                lax.dot_general(
                    part_one, qkv_grad_low, contract_first, preferred_element_type=jnp.float32
                ),
                lax.dot_general(
                    part_two, fc_grad_low, contract_first, preferred_element_type=jnp.float32
                ),
                lax.dot_general(
                    wide_grad, attn_out, contract_first, preferred_element_type=jnp.float32
                ),
                lax.dot_general(
                    wide_grad, gelu_out, contract_first, preferred_element_type=jnp.float32
                ),
            ],
            axis=1,
        ),
        "row",
        scatter_dimension=0,
        tiled=True,
    )
    grad_rows = lax.psum(row_part, "dp")
    qkv_total = grad_rows[:, :qkv_cols]
    fc_total = grad_rows[:, qkv_cols : qkv_cols + fc_cols]
    dense_total = grad_rows[:, qkv_cols + fc_cols : qkv_cols + fc_cols + head_cols].T
    proj_total = grad_rows[:, qkv_cols + fc_cols + head_cols :].T
    norm_local = lax.psum_scatter(norm_grads, "col", scatter_dimension=2, tiled=True)
    grad_one = norm_local[0]
    grad_two = norm_local[1]
    hat_grad = grad_one * ln1_gain + grad_two * ln2_gain
    total_hat, total_cross = lax.psum(
        (jnp.sum(hat_grad, axis=1), jnp.sum(hat_grad * x_hat, axis=1)), "col"
    )
    input_grad = out_grad + inv_std * (
        hat_grad - (total_hat / D)[:, None] - x_hat * (total_cross / D)[:, None]
    )
    gain_one, shift_one, gain_two, shift_two, qkv_bias_total, fc_bias_total, out_bias_total = (
        lax.psum(
            (
                jnp.sum(grad_one * x_hat, axis=0),
                jnp.sum(grad_one, axis=0),
                jnp.sum(grad_two * x_hat, axis=0),
                jnp.sum(grad_two, axis=0),
                qkv_bias_grad,
                fc_bias_grad,
                jnp.sum(out_grad, axis=0),
            ),
            ("dp", "row"),
        )
    )
    return (
        block_output,
        input_grad,
        gain_one,
        shift_one,
        gain_two,
        shift_two,
        qkv_total,
        qkv_bias_total,
        dense_total,
        out_bias_total,
        fc_total,
        fc_bias_total,
        proj_total,
        out_bias_total,
    )


f32 = jnp.float32
bf16 = jnp.bfloat16
MESH = pl.DeviceIdType.MESH
VMEM = pltpu.VMEM
Q = 256
HALF = 4 * Q


def flip(a, b):
    return a + b - 2 * a * b


def span(start, size):
    return pl.ds(pl.multiple_of(start, size), size)


def mm(a, b):
    return jnp.dot(a, b, preferred_element_type=f32)


def mm_nt(a, b):
    return lax.dot_general(a, b, (((1,), (1,)), ((), ())), preferred_element_type=f32)


def mm_tn(a, b):
    return lax.dot_general(a, b, (((0,), (0,)), ((), ())), preferred_element_type=f32)


class Net:
    def __init__(self, send_sems, recv_sems, local_sems):
        self.k = lax.axis_index("dp")
        self.r = lax.axis_index("row")
        self.c = lax.axis_index("col")
        k, r, c = self.k, self.r, self.c
        self.core = (1 - k, r, c)
        self.x = (k, r + 1 - 2 * (r % 2), c)
        self.y = (k, r + 2 - 4 * (r // 2), c)
        near = c + 1 - 2 * (c % 2)
        self.z = (None, (k, r, near), (k, r, c + 2 - 4 * (c // 2)), (k, r, 3 - c))
        self.middle = flip(c % 2, c // 2) == 1
        self.send_sems, self.recv_sems, self.local_sems = send_sems, recv_sems, local_sems
        self.remote_count = 0
        self.local_count = 0
        self.pending = []

    def mix(self, j):
        return flip(j % 2, flip(self.c % 2, self.r % 2)) + 2 * flip(
            j // 2, flip(self.c // 2, self.r // 2)
        )

    def barrier(self):
        sem = pltpu.get_barrier_semaphore()
        peers = (self.core, self.x, self.y) + self.z[1:]
        for peer in peers:
            pl.semaphore_signal(sem, inc=1, device_id=peer, device_id_type=MESH)
        pl.semaphore_wait(sem, len(peers))

    def slot(self):
        self.remote_count += 1
        return self.remote_count - 1

    def remote(self, src, dst, peer):
        slot = self.slot()
        copy = pltpu.make_async_remote_copy(
            src_ref=src,
            dst_ref=dst,
            send_sem=self.send_sems.at[slot],
            recv_sem=self.recv_sems.at[slot],
            device_id=peer,
            device_id_type=MESH,
        )
        copy.start()
        self.pending.append(copy)
        return copy

    def local(self, src, dst):
        copy = pltpu.make_async_copy(src, dst, self.local_sems.at[self.local_count])
        self.local_count += 1
        copy.start()
        return copy

    def sent(self, copy):
        copy.wait_send()
        self.pending = [other for other in self.pending if other is not copy]

    def drain(self):
        for copy in self.pending:
            copy.wait_send()


class Gather:
    def __init__(self, net, shard, full, by_rows):
        self.net, self.shard, self.full, self.by_rows = net, shard, full, by_rows
        self.depth = Q // 2 if by_rows else shard.shape[0] // 2
        self.placed = []

    def own(self, half, part=None):
        if self.by_rows:
            if part is None:
                return self.shard.at[span(half * Q, Q), :]
            return self.shard.at[span(half * Q + part * self.depth, self.depth), :]
        rows = slice(None) if part is None else pl.ds(part * self.depth, self.depth)
        return self.shard.at[rows, span(half * Q, Q)]

    def chunk(self, s, i, part=None):
        start = s * HALF + i * Q
        if self.by_rows:
            if part is None:
                return self.full.at[pl.ds(start, Q), :]
            return self.full.at[pl.ds(start + part * self.depth, self.depth), :]
        rows = slice(None) if part is None else pl.ds(part * self.depth, self.depth)
        return self.full.at[rows, pl.ds(start, Q)]

    def place_own(self):
        net = self.net
        self.placed = [
            net.local(self.own(net.k), self.chunk(0, 0)),
            net.local(self.own(1 - net.k), self.chunk(1, 0)),
        ]

    def send_own(self):
        net, k = self.net, self.net.k
        self.y0 = net.remote(self.own(k, 0), self.chunk(0, 2, 0), net.y)
        self.x1 = net.remote(self.own(k, 1), self.chunk(0, 1, 1), net.x)
        self.y1 = net.remote(self.own(k, 1), self.chunk(0, 2, 1), net.y)
        self.x0 = net.remote(self.own(k, 0), self.chunk(0, 1, 0), net.x)

    def forward(self):
        net = self.net
        self.y0.wait_recv()
        self.d0 = net.remote(self.chunk(0, 2, 0), self.chunk(0, 3, 0), net.x)
        self.x1.wait_recv()
        self.d1 = net.remote(self.chunk(0, 1, 1), self.chunk(0, 3, 1), net.y)

    def swap_near(self):
        net = self.net
        self.x0.wait_recv()
        self.c1 = net.remote(self.chunk(0, 1), self.chunk(1, 1), net.core)
        self.y1.wait_recv()
        self.c2 = net.remote(self.chunk(0, 2), self.chunk(1, 2), net.core)

    def swap_far(self):
        net = self.net
        self.d0.wait_recv()
        self.d1.wait_recv()
        self.c3 = net.remote(self.chunk(0, 3), self.chunk(1, 3), net.core)

    def ready(self):
        for copy in (self.c1, self.c2, self.c3):
            copy.wait_recv()
        for copy in self.placed:
            copy.wait()

    def release(self):
        for copy in (self.d0, self.d1, self.c1, self.c2, self.c3):
            self.net.sent(copy)


class Line:
    def __init__(self, net, slots):
        self.net, self.slots = net, slots
        self.ids = [None] + [net.slot() for _ in range(3)]
        self.sends = []

    def copy(self, src, dst, peer, send):
        net = self.net
        return pltpu.make_async_remote_copy(
            src_ref=self.slots.at[src],
            dst_ref=self.slots.at[dst],
            send_sem=net.send_sems.at[send],
            recv_sem=net.recv_sems.at[self.ids[dst]],
            device_id=peer,
            device_id_type=MESH,
        )

    def start(self):
        net = self.net
        self.first = self.copy(0, 1, net.z[1], self.ids[1])
        self.first.start()
        self.hops = [
            self.copy(0, 3, net.z[3], self.ids[2]),
            self.copy(1, 2, net.z[3], self.ids[3]),
            self.copy(3, 2, net.z[1], net.slot()),
            self.copy(2, 3, net.z[1], net.slot()),
        ]

        @pl.when(net.middle)
        def _():
            self.hops[0].start()

    def arrived(self, slot):
        return self.copy(0, slot, self.net.z[1], self.ids[slot])

    def step(self, number):
        slot = (1, 3, 2)[number]

        @pl.when(self.net.middle)
        def _():
            self.arrived(slot).wait_recv()
            self.hops[number + 1].start()

    def ready(self):
        @pl.when(jnp.logical_not(self.net.middle))
        def _():
            for slot in (1, 2, 3):
                self.arrived(slot).wait_recv()

    def drain(self):
        self.first.wait_send()

        @pl.when(self.net.middle)
        def _():
            for hop in self.hops:
                hop.wait_send()


class Fold:
    def __init__(self, net, blocks, inbox):
        self.net, self.blocks, self.inbox = net, blocks, inbox
        hops = ((3, None, 0), (2, None, 1), (1, None, 2), (None, 0, 3), (None, 1, 4), (None, 3, 0))
        self.copies = []
        for n, (block, slot, dest) in enumerate(hops):
            number = net.slot()
            self.copies.append(
                pltpu.make_async_remote_copy(
                    src_ref=blocks.at[block] if slot is None else inbox.at[slot],
                    dst_ref=inbox.at[dest],
                    send_sem=net.send_sems.at[number],
                    recv_sem=net.recv_sems.at[number],
                    device_id=net.z[3] if n in (3, 4) else net.z[1],
                    device_id_type=MESH,
                )
            )

    def start(self, first, last):
        @pl.when(jnp.logical_not(self.net.middle))
        def _():
            for copy in self.copies[first:last]:
                copy.start()

    def step(self, number):
        slot, block = ((0, 2), (1, 3), (3, 1))[number]
        inbox, blocks = self.inbox, self.blocks

        @pl.when(self.net.middle)
        def _():
            self.copies[(0, 1, 3)[number]].wait_recv()

            def add(n, _):
                at = span(n * 64, 64)
                total = inbox[slot, at, :].astype(f32) + blocks[block, at, :].astype(f32)
                inbox[slot, at, :] = total.astype(bf16)
                return 0

            lax.fori_loop(0, inbox.shape[1] // 64, add, 0)
            self.copies[3 + number].start()

    def total(self, use):
        def gather(*slots):
            def add(n, _):
                at = span(n * 64, 64)
                value = self.blocks[0, at, :].astype(f32)
                for slot in slots:
                    value = value + self.inbox[slot, at, :].astype(f32)
                use(at, value)
                return 0

            lax.fori_loop(0, self.inbox.shape[1] // 64, add, 0)

        @pl.when(self.net.middle)
        def _():
            self.copies[2].wait_recv()
            self.copies[4].wait_recv()
            gather(2, 4)

        @pl.when(jnp.logical_not(self.net.middle))
        def _():
            self.copies[5].wait_recv()
            gather(0)

    def drain(self):
        @pl.when(self.net.middle)
        def _():
            for copy in self.copies[3:]:
                copy.wait_send()

        @pl.when(jnp.logical_not(self.net.middle))
        def _():
            for copy in self.copies[:3]:
                copy.wait_send()


def turn(low, tables, sign):
    lane = lax.broadcasted_iota(jnp.int32, low.shape, 1)
    swung = jnp.where(lane < ROT // 2, pltpu.roll(low, 96, 1), pltpu.roll(low, 32, 1))
    return low * tables[0] + sign * (tables[1] * swung)


class Tiles:
    def __init__(self, slots, sems):
        self.slots, self.sems = slots, sems

    def write(self, count, product, place, depth):
        def body(n, _):
            slot = n % 2
            source = self.slots.at[slot, pl.ds(0, depth), :]
            copy = pltpu.make_async_copy(source, place(n), self.sems.at[slot])

            @pl.when(n >= 2)
            def _():
                copy.wait()

            self.slots[slot, 0:depth, :] = product(n).astype(bf16)
            copy.start()
            return 0

        lax.fori_loop(0, count, body, 0)
        for slot in range(2):
            source = self.slots.at[slot, pl.ds(0, depth), :]
            pltpu.make_async_copy(source, place(slot), self.sems.at[slot]).wait()


class Reduce:
    def __init__(self, net, partial, joined, near, far, by_rows, in_vmem=False):
        self.in_vmem = in_vmem
        self.net, self.partial, self.by_rows = net, partial, by_rows
        self.joined, self.near, self.far = joined, near, far
        self.depth = Q // 2 if by_rows else partial.shape[0] // 2

    def chunk(self, i, half):
        if self.by_rows:
            return self.partial.at[pl.ds(i * Q + half * self.depth, self.depth), :]
        return self.partial.at[pl.ds(half * self.depth, self.depth), pl.ds(i * Q, Q)]

    def whole(self):
        if self.by_rows:
            return self.partial.at[pl.ds(0, Q), :]
        return self.partial.at[:, pl.ds(0, Q)]

    def rows(self, half):
        return pl.ds(half * self.depth, self.depth)

    def start(self):
        net = self.net
        self.a = net.remote(self.chunk(3, 0), self.joined.at[0], net.x)
        self.b = net.remote(self.chunk(3, 1), self.joined.at[1], net.y)
        self.near_a = net.remote(self.chunk(1, 0), self.near.at[self.rows(0), :], net.x)
        self.near_b = net.remote(self.chunk(2, 1), self.near.at[self.rows(1), :], net.y)

    def join(self, parts):
        net = self.net
        loads = [net.local(self.chunk(2, 0), parts[0]), net.local(self.chunk(1, 1), parts[1])]
        hops = []
        for half, copy, peer in ((0, self.a, net.y), (1, self.b, net.x)):
            loads[half].wait()
            copy.wait_recv()
            tile = 64

            def add(n, _, half=half):
                at = span(n * tile, tile)
                total = self.joined[half, at, :].astype(f32) + parts[half][at, :].astype(f32)
                self.joined[half, at, :] = total.astype(bf16)
                return 0

            lax.fori_loop(0, self.depth // tile, add, 0)
            hops.append(net.remote(self.joined.at[half], self.far.at[self.rows(half), :], peer))
        self.far_a, self.far_b = hops

    def prepare(self, buffers):
        net = self.net
        self.buffers = list(buffers)
        self.loads = [net.local(self.whole(), buffers[0])]
        for copy in (self.near_a, self.near_b):
            copy.wait_recv()
        if self.in_vmem:
            self.buffers[1:3] = [self.near, self.far]
        else:
            self.loads.append(net.local(self.near, buffers[1]))

    def finish(self, out):
        net, buffers = self.net, self.buffers
        for copy in (self.far_a, self.far_b):
            copy.wait_recv()
        if not self.in_vmem:
            self.loads.append(net.local(self.far, buffers[2]))
        for copy in self.loads:
            copy.wait()
        tile = 64
        self.here, self.there = [], []
        for half in range(2):

            def add(n, _, half=half):
                at = span(half * self.depth + n * tile, tile)
                parts = [buffer[at, :].astype(f32) for buffer in buffers[:3]]
                buffers[3][at, :] = (parts[0] + parts[1] + parts[2]).astype(bf16)
                return 0

            lax.fori_loop(0, self.depth // tile, add, 0)
            source = buffers[3].at[self.rows(half), :]
            if self.by_rows:
                place = out.at[span(net.k * Q + half * self.depth, self.depth), :]
            else:
                place = out.at[self.rows(half), span(net.k * Q, Q)]
            self.here.append(net.local(source, place))
            self.there.append(net.remote(source, place, net.core))

    def done(self):
        for copy in self.here:
            copy.wait()
        for copy in self.there:
            copy.wait_recv()


def block_kernel(
    x, og, w_qkv, w_dense, w_fc, w_proj, t_turn,
    i_gain_1, i_bias_1, i_gain_2, i_bias_2, i_b_qkv, i_b_fc, i_b_dense, i_b_proj,
    o_proj, o_qkv, o_fc, o_dense, o_block, o_input, o_small,
    all_proj, r_proj, r_qkv, r_fc, r_dense, n_proj, f_proj, n_qkv, f_qkv, n_fc, f_fc,
    g_qkv, g_dense, g_fc, g_tail, xs, ys, pks, stats, rows, h1c, h1s, h2c, h2s, dyc, dys, xh,
    qb, kb, vb, probs, probs_low, oc, dob, dqc, gc, slope, dabt, stage,
    out_recv, hat_recv, j_proj, j_qkv, j_fc, j_dense, n_dense, f_dense, tables, vecs, bias, packs, small,
    gain_1, bias_1, gain_2, bias_2, b_qkv, b_fc, b_dense, b_proj,
    send_sems, recv_sems, local_sems, stage_sems,
):
    tok = x.shape[0]
    heads = qb.shape[0]
    width = gc.shape[1]
    scale = 1.0 / math.sqrt(HD)
    net = Net(send_sems, recv_sems, local_sems)
    net.barrier()
    qkv = Gather(net, w_qkv, g_qkv, True)
    dense = Gather(net, w_dense, g_dense, False)
    fc = Gather(net, w_fc, g_fc, True)
    proj = Gather(net, w_proj, all_proj, False)
    qkv.send_own()
    dense.send_own()
    load_x = net.local(x, probs.at[0])
    vectors = [
        net.local(i_gain_1, gain_1), net.local(i_bias_1, bias_1), net.local(i_gain_2, gain_2),
        net.local(i_bias_2, bias_2), net.local(i_b_qkv, b_qkv), net.local(i_b_fc, b_fc),
        net.local(i_b_dense, b_dense), net.local(i_b_proj, b_proj),
    ]
    load_og = net.local(og, probs.at[1])
    load_turn = net.local(t_turn, tables)
    tiles = Tiles(stage, stage_sems)
    mine = pl.ds(0, tok)
    theirs = pl.ds(tok, tok)

    step = 128
    lane = lax.broadcasted_iota(jnp.int32, (step, 128), 1)
    load_x.wait()

    def local_norm(n, _):
        at = span(n * step, step)
        block = probs[0, at, :]
        mean = jnp.mean(block, axis=1, keepdims=True)
        centred = block - mean
        var = jnp.mean(centred * centred, axis=1, keepdims=True)
        stats[at, :] = jnp.where(lane == 0, mean, jnp.where(lane == 1, var, 0.0))
        return 0

    lax.fori_loop(0, tok // step, local_norm, 0)
    pks[0] = stats[...].T[0:8]
    for copy in vectors:
        copy.wait()
    for n, vector in enumerate((gain_1, bias_1, gain_2, bias_2)):
        pks[0, 2 + n : 3 + n, :] = vector[...].reshape(1, 512)
    packed = [net.remote(pks.at[0], pks.at[j], net.z[j]) for j in (1, 2, 3)]
    for weight in (qkv, dense, fc):
        weight.place_own()
    bias[...] = jnp.zeros_like(bias)
    bias[3:4, 0 : b_qkv.shape[0]] = b_qkv[...].reshape(1, b_qkv.shape[0])
    bias[4:5, :] = b_fc[...].reshape(1, width)
    bias[5:6, 0:512] = (b_dense[...] + b_proj[...]).reshape(1, 512)
    rows[...] = jnp.zeros_like(rows)
    load_og.wait()

    def local_grad(n, _):
        at = span(n * step, step)
        block = probs[1, at, :]
        ys[0, at, :] = block.astype(bf16)
        bias[1:2, 0:512] += jnp.sum(block, axis=0, keepdims=True)
        return 0

    lax.fori_loop(0, tok // step, local_grad, 0)
    for pack in packed:
        pack.wait_recv()
    means = [pks[j, 0:1, :] for j in range(4)]
    mu = (means[0] + means[1] + means[2] + means[3]) * 0.25
    spread = [pks[j, 1:2, :] + (means[j] - mu) * (means[j] - mu) for j in range(4)]
    rows[0:1, :] = mu
    rows[1:2, :] = lax.rsqrt((spread[0] + spread[1] + spread[2] + spread[3]) * 0.25 + epsilon)
    stats[...] = rows[...].T

    def own_norm(n, _):
        at = span(n * step, step)
        hats = (probs[0, at, :] - stats[at, 0:1]) * stats[at, 1:2]
        xs[0, at, :] = (hats * pks[0, 2:3, :] + pks[0, 3:4, :]).astype(bf16)
        return 0

    lax.fori_loop(0, tok // step, own_norm, 0)
    x_line = Line(net, xs)
    y_line = Line(net, ys)
    x_line.start()
    qkv.forward()
    x_line.step(0)
    x_line.step(1)
    fc.send_own()
    dense.forward()
    qkv.swap_near()
    x_line.step(2)
    y_line.start()
    dense.swap_near()
    qkv.swap_far()
    x_line.ready()
    fc.forward()
    proj.send_own()

    for s in range(2):
        for j in range(4):
            lanes = span(flip(s, net.k) * Q, Q)
            dest = span(net.mix(j) * Q, Q)
            wide = span(s * HALF + net.mix(j) * Q, Q)
            vecs[0:4, wide] = pks[j, 2:6, lanes]

            def norm(n, _, s=s, j=j, lanes=lanes, dest=dest, wide=wide):
                at = span(n * step, step)
                one = xs[j, at, lanes]
                hats = (one.astype(f32) - pks[j, 3:4, lanes]) * (1.0 / pks[j, 2:3, lanes])
                xh[at, wide] = hats.astype(bf16)
                (h1s if s else h1c)[at, dest] = one
                two = hats * pks[j, 4:5, lanes] + pks[j, 5:6, lanes]
                (h2s if s else h2c)[at, dest] = two.astype(bf16)
                return 0

            lax.fori_loop(0, tok // step, norm, 0)
    swap_h1 = net.remote(h1s, h1c.at[theirs, :], net.core)
    swap_h2 = net.remote(h2s, h2c.at[theirs, :], net.core)
    y_line.step(0)
    load_turn.wait()
    qkv.ready()

    def project(n, _):
        cols = span(n * 3 * HD, 3 * HD)
        acc = mm(h1c[mine, :], g_qkv[0:HALF, cols]) + mm(h1s[...], g_qkv[HALF:, cols])
        acc = acc + bias[3:4, cols]
        qb[n, :, 0:128] = turn(acc[:, 0:128], tables, 1.0).astype(bf16)
        qb[n, :, 128:HD] = acc[:, 128:HD].astype(bf16)
        kb[n, :, 0:128] = turn(acc[:, HD : HD + 128], tables, 1.0).astype(bf16)
        kb[n, :, 128:HD] = acc[:, HD + 128 : 2 * HD].astype(bf16)
        vb[n] = acc[:, 2 * HD :].astype(bf16)
        return 0

    lax.fori_loop(0, heads, project, 0)
    y_line.step(1)
    chunks = tok // step

    def attend(n, _):
        head, chunk = n // chunks, n % chunks
        at = span(chunk * step, step)
        scores = mm_nt(qb[head, at, :], kb[head]) * scale
        token = lax.broadcasted_iota(jnp.int32, (step, tok), 0) + chunk * step
        allowed = token >= lax.broadcasted_iota(jnp.int32, (step, tok), 1)
        scores = jnp.where(allowed, scores, -1e30)
        top = jnp.max(scores, axis=1, keepdims=True)
        raised = jnp.where(allowed, jnp.exp(scores - top), 0.0)
        weight = raised / jnp.sum(raised, axis=1, keepdims=True)
        probs[head, at, :] = weight
        low = weight.astype(bf16)
        probs_low[head, at, :] = low
        oc[at, span(head * HD, HD)] = mm(low, vb[head]).astype(bf16)
        return 0

    lax.fori_loop(0, heads * chunks, attend, 0)
    swap_o = net.remote(oc.at[mine, :], oc.at[theirs, :], net.core)
    dense.swap_far()
    fc.swap_near()
    y_line.step(2)
    fc.swap_far()
    fc.ready()

    def expand(n, _):
        cols = span(n * 512, 512)
        a = mm(h2c[mine, :], g_fc[0:HALF, cols]) + mm(h2s[...], g_fc[HALF:, cols])
        a = a + bias[4:5, cols]
        rise = 0.5 * (1.0 + lax.erf(a * 0.7071067811865476))
        gc[mine, cols] = (a * rise).astype(bf16)
        slope[:, cols] = (rise + a * 0.3989422804014327 * jnp.exp(-0.5 * a * a)).astype(bf16)
        return 0

    lax.fori_loop(0, width // 1024, expand, 0)
    proj.forward()
    lax.fori_loop(width // 1024, width // 512, expand, 0)
    swap_g = net.remote(gc.at[mine, :], gc.at[theirs, :], net.core)
    y_line.ready()
    for s in range(2):
        for j in range(4):
            lanes = span(flip(s, net.k) * Q, Q)
            dest = span(net.mix(j) * Q, Q)
            (dys if s else dyc)[mine, dest] = ys[j, :, lanes]
    swap_dy = net.remote(dys, dyc.at[theirs, :], net.core)
    dense.ready()
    dob[...] = (
        mm_nt(dyc[mine, :], g_dense[:, 0:HALF]) + mm_nt(dys[...], g_dense[:, HALF:])
    ).astype(bf16)

    red_proj = Reduce(net, r_proj, j_proj, n_proj, f_proj, False)
    red_qkv = Reduce(net, r_qkv, j_qkv, n_qkv, f_qkv, True)
    red_fc = Reduce(net, r_fc, j_fc, n_fc, f_fc, True)
    red_dense = Reduce(net, r_dense, j_dense, n_dense, f_dense, False, True)
    swap_g.wait_recv()
    swap_dy.wait_recv()
    tall = width // 2
    tiles.write(
        4,
        lambda n: mm_tn(gc[:, span(n // 2 * tall, tall)], dyc[:, span(n % 2 * 512, 512)]),
        lambda n: r_proj.at[span(n // 2 * tall, tall), span(n % 2 * 512, 512)],
        tall,
    )
    proj.swap_near()
    red_proj.start()

    def keep(head, part, at, value, rotated):
        base = head * 3 * HD + part * HD
        if rotated:
            low = turn(value[:, 0:128], [tables[t, at, :] for t in range(2)], -1.0)
            dqc[at, pl.ds(pl.multiple_of(base, 128), 128)] = low.astype(bf16)
            bias[0:1, pl.ds(pl.multiple_of(base, 128), 128)] += jnp.sum(low, axis=0, keepdims=True)
            value, base, size = value[:, 128:], base + 128, 128
        else:
            size = HD
        cols = pl.ds(pl.multiple_of(base, 128), size)
        dqc[at, cols] = value.astype(bf16)
        bias[0:1, cols] += jnp.sum(value, axis=0, keepdims=True)

    def attend_back(head, _):
        cols = span(head * HD, HD)

        def chunk_back(n, _):
            at = span(n * step, step)
            grad = dob[at, cols]
            delta = jnp.sum(grad.astype(f32) * oc[at, cols].astype(f32), axis=1, keepdims=True)
            spread = mm_nt(grad, vb[head]) - delta
            low = (probs[head, at, :] * spread * scale).astype(bf16)
            probs_low[head, at, :] = low
            keep(head, 0, at, mm(low, kb[head]), True)
            return 0

        keep(head, 2, mine, mm_tn(probs_low[head], dob[:, cols]), False)
        lax.fori_loop(0, chunks, chunk_back, 0)
        keep(head, 1, mine, mm_tn(probs_low[head], qb[head]), True)
        return 0

    lax.fori_loop(0, heads, attend_back, 0)
    proj.swap_far()
    swap_dq = net.remote(dqc.at[mine, :], dqc.at[theirs, :], net.core)
    net.sent(swap_h1)
    net.sent(swap_h2)
    for s in range(2):

        def back_first(n, _, s=s):
            wide = span(s * HALF + n * 512, 512)
            grad = mm_nt(dqc[mine, :], g_qkv[wide, :])
            (h2s if s else h1s)[:, span(n * 512, 512)] = (grad * vecs[0:1, wide]).astype(bf16)
            vecs[4:5, wide] = jnp.sum(grad * xh[:, wide].astype(f32), axis=0, keepdims=True)
            vecs[5:6, wide] = jnp.sum(grad, axis=0, keepdims=True)
            return 0

        lax.fori_loop(0, HALF // 512, back_first, 0)

    proj.ready()
    qkv.release()
    loads = [
        net.local(w_proj.at[:, span(net.k * Q, Q)], g_qkv.at[:, pl.ds(0, Q)]),
        net.local(w_proj.at[:, span((1 - net.k) * Q, Q)], g_qkv.at[:, pl.ds(HALF, Q)]),
        net.local(all_proj.at[:, pl.ds(Q, 3 * Q)], g_qkv.at[:, pl.ds(Q, 3 * Q)]),
        net.local(all_proj.at[:, pl.ds(5 * Q, Q)], g_qkv.at[:, pl.ds(5 * Q, Q)]),
        net.local(all_proj.at[:, pl.ds(6 * Q, 2 * Q)], g_tail),
    ]
    swap_o.wait_recv()
    attn = oc.shape[1]
    tiles.write(
        2,
        lambda n: mm_tn(oc[...], dyc[:, span(n * 512, 512)]),
        lambda n: r_dense.at[:, span(n * 512, 512)],
        attn,
    )
    swap_h1.wait_recv()
    swap_dq.wait_recv()
    tiles.write(
        dqc.shape[1] // 512,
        lambda n: mm_tn(h1c[...], dqc[:, span(n * 512, 512)]),
        lambda n: r_qkv.at[:, span(n * 512, 512)],
        HALF,
    )
    red_qkv.start()
    red_dense.start()

    for copy in loads:
        copy.wait()
    x_line.drain()
    y_line.drain()

    def put_out(p, product):
        s, i = p // 4, p % 4
        out = product + mm(oc[mine, :], g_dense[:, span(p * Q, Q)])
        xs[net.mix(i), :, span(flip(s, net.k) * Q, Q)] = out.astype(bf16)

    def project_head(p, _):
        put_out(p, mm(gc[mine, :], g_qkv[:, span(p * Q, Q)]))
        return 0

    def project_tail(p, _):
        put_out(6 + p, mm(gc[mine, :], g_tail[:, span(p * Q, Q)]))
        return 0

    lax.fori_loop(0, 6, project_head, 0)
    lax.fori_loop(0, 2, project_tail, 0)
    out_fold = Fold(net, xs, out_recv)
    out_fold.start(0, 2)

    def back_fc(n, _):
        cols = span(n * 512, 512)
        grad = mm_nt(dyc[mine, :], g_qkv[cols, 0:HALF])
        grad = grad + mm_nt(dys[:, 0:512], g_qkv[cols, HALF : 6 * Q])
        grad = grad + mm_nt(dys[:, 512:], g_tail[cols, :])
        grad = grad * slope[:, cols].astype(f32)
        bias[2:3, cols] = jnp.sum(grad, axis=0, keepdims=True)
        slope[:, cols] = grad.astype(bf16)
        return 0

    lax.fori_loop(0, width // 512, back_fc, 0)
    dab = slope
    swap_da = net.remote(dab, dabt, net.core)
    red_proj.join([g_tail.at[pl.ds(0, tall), pl.ds(0, Q)], g_tail.at[pl.ds(tall, tall), pl.ds(0, Q)]])
    stats[...] = jnp.zeros_like(stats)
    lane = lax.broadcasted_iota(jnp.int32, (tok, 128), 1)

    def back_norm(j, _):
        for s in range(2):
            lanes = span(flip(s, net.k) * Q, Q)
            dest = span(net.mix(j) * Q, Q)
            wide = span(s * HALF + net.mix(j) * Q, Q)
            grad = mm_nt(dab[...], g_fc[wide, :])
            hats = xh[:, wide].astype(f32)
            packs[j, 2:4, lanes] = vecs[4:6, wide]
            packs[j, 4:5, lanes] = jnp.sum(grad * hats, axis=0, keepdims=True)
            packs[j, 5:6, lanes] = jnp.sum(grad, axis=0, keepdims=True)
            joint = (h2s if s else h1s)[:, dest].astype(f32) + grad * vecs[2:3, wide]
            ys[j, :, lanes] = joint.astype(bf16)
            one = jnp.sum(joint, axis=1, keepdims=True)
            two = jnp.sum(joint * hats, axis=1, keepdims=True)
            stats[...] += jnp.where(lane == 0, one, jnp.where(lane == 1, two, 0.0))
        return 0

    lax.fori_loop(0, 4, back_norm, 0)

    fc.release()
    red_qkv.join(
        [g_fc.at[pl.ds(7 * Q + n * (Q // 2), Q // 2), pl.ds(0, 6 * Q)] for n in range(2)]
    )
    turned = stats[...].T
    for j in range(4):
        packs[j, 0:2, :] = turned[0:2]
        packs[j, 6:8, :] = jnp.zeros((2, tok), f32)
    pack_copies = [net.remote(packs.at[j], packs.at[3 + j], net.z[j]) for j in (1, 2, 3)]
    hat_fold = Fold(net, ys, hat_recv)
    hat_fold.start(0, 2)
    out_fold.start(2, 3)
    hat_fold.start(2, 3)
    out_fold.step(0)
    swap_h2.wait_recv()
    swap_da.wait_recv()

    def grad_fc(n):
        cols = span(n * 512, 512)
        return mm_tn(h2c[mine, :], dab[:, cols]) + mm_tn(h2c[theirs, :], dabt[:, cols])

    tiles.write(width // 512, grad_fc, lambda n: r_fc.at[:, span(n * 512, 512)], HALF)
    red_fc.start()
    out_fold.step(1)

    def strips(base, n, columns):
        return g_fc.at[pl.ds(base + n * Q, Q), pl.ds(0, columns)]

    out_fold.step(2)
    for copy in pack_copies:
        copy.wait_recv()
    total = packs[0] + packs[4] + packs[5] + packs[6]
    rows[2:4, :] = total[0:2, :]
    stats[...] = rows[...].T
    me = net.k * 4 + net.r
    small[me, 0:4, :] = total[2:6, :]
    for n in range(3):
        small[me, 4 + n : 5 + n, :] = bias[0:1, n * 512 : n * 512 + 512]
    for n in range(4):
        small[me, 7 + n : 8 + n, :] = bias[2:3, n * 512 : n * 512 + 512]
    small[me, 11:12, :] = bias[1:2, 0:512]
    small[me, 12:16, :] = jnp.zeros((4, 512), f32)
    small_copies = []
    for n in range(1, 8):
        row = flip(net.r % 2, n % 2) + 2 * flip(net.r // 2, n // 2 % 2)
        peer = (flip(net.k, n // 4), row, net.c)
        small_copies.append(net.remote(small.at[me], small.at[me], peer))
    reload_x = net.local(x, probs.at[1])
    red_proj.prepare([g_qkv.at[:, pl.ds(n * Q, Q)] for n in range(4)])
    red_proj.finish(o_proj)
    hat_fold.step(0)
    red_fc.join([g_fc.at[pl.ds(6 * Q + n * (Q // 2), Q // 2), :] for n in range(2)])
    hat_fold.step(1)
    hat_fold.step(2)
    reload_x.wait()

    def close_out(at, value):
        probs[0, at, :] = probs[1, at, :] + value + bias[5:6, 0:512]

    out_fold.total(close_out)
    keep_block = net.local(probs.at[0], o_block)
    keep_block.wait()
    reload_og = net.local(og, probs.at[0])
    red_qkv.prepare([strips(0, n, 6 * Q) for n in range(4)])
    red_qkv.finish(o_qkv)
    red_dense.join([g_tail.at[pl.ds(n * attn // 2, attn // 2), pl.ds(0, Q)] for n in range(2)])
    red_fc.prepare([strips(4 * Q, n, 8 * Q) for n in range(4)])
    red_dense.prepare([g_tail.at[pl.ds(n * attn, attn), pl.ds(Q, Q)] for n in range(4)])
    for copy in small_copies:
        copy.wait_recv()
    grand = small[0]
    for n in range(1, 8):
        grand = grand + small[n]
    small[8] = grand
    keep_small = net.local(small.at[8], o_small)
    reload_og.wait()

    def close_hat(at, value):
        mu, rstd = stats[at, 0:1], stats[at, 1:2]
        hats = (probs[1, at, :] - mu) * rstd
        mean, cross = stats[at, 2:3] * (1.0 / D), stats[at, 3:4] * (1.0 / D)
        probs[0, at, :] += rstd * (value - mean - hats * cross)

    hat_fold.total(close_hat)
    keep_input = net.local(probs.at[0], o_input)
    red_fc.finish(o_fc)
    red_dense.finish(o_dense)
    for weight in (red_proj, red_qkv, red_fc, red_dense):
        weight.done()
    keep_small.wait()
    keep_input.wait()
    out_fold.drain()
    hat_fold.drain()
    net.drain()


def call_block(*args):
    x, w_qkv, w_dense, w_fc = args[0], args[2], args[3], args[4]
    tok = x.shape[0]
    n_qkv, n_attn, n_fc = w_qkv.shape[1], w_dense.shape[0], w_fc.shape[1]
    heads = n_attn // HD
    wide = 2 * HALF
    any_spec = pl.BlockSpec(memory_space=pl.ANY)
    shape = jax.ShapeDtypeStruct
    pieces = ((n_fc, Q), (Q, n_qkv), (Q, n_fc), (n_attn, Q))
    outs = [
        shape((n_fc, 2 * Q), bf16), shape((2 * Q, n_qkv), bf16),
        shape((2 * Q, n_fc), bf16), shape((n_attn, 2 * Q), bf16),
        shape((tok, 512), f32), shape((tok, 512), f32), shape((16, 512), f32),
        shape((n_fc, wide), bf16), shape((n_fc, HALF), bf16), shape((HALF, n_qkv), bf16),
        shape((HALF, n_fc), bf16), shape((n_attn, HALF), bf16),
    ]
    outs += [shape(piece, bf16) for piece in pieces[:3] for _ in range(2)]
    scratch = [
        VMEM((wide, n_qkv), bf16), VMEM((n_attn, wide), bf16), VMEM((wide, n_fc), bf16),
        VMEM((n_fc, 2 * Q), bf16),
        VMEM((4, tok, 512), bf16), VMEM((4, tok, 512), bf16), VMEM((4, 8, tok), f32),
        VMEM((tok, 128), f32), VMEM((128, tok), f32),
        VMEM((2 * tok, HALF), bf16), VMEM((tok, HALF), bf16),
        VMEM((2 * tok, HALF), bf16), VMEM((tok, HALF), bf16),
        VMEM((2 * tok, HALF), bf16), VMEM((tok, HALF), bf16), VMEM((tok, wide), bf16),
        VMEM((heads, tok, HD), bf16), VMEM((heads, tok, HD), bf16), VMEM((heads, tok, HD), bf16),
        VMEM((heads, tok, tok), f32), VMEM((heads, tok, tok), bf16),
        VMEM((2 * tok, n_attn), bf16), VMEM((tok, n_attn), bf16), VMEM((2 * tok, n_qkv), bf16),
        VMEM((2 * tok, n_fc), bf16), VMEM((tok, n_fc), bf16), VMEM((tok, n_fc), bf16),
        VMEM((2, HALF, 512), bf16),
        VMEM((5, tok, 512), bf16), VMEM((5, tok, 512), bf16),
    ]
    scratch += [VMEM((2,) + ((r // 2, c)), bf16) for r, c in pieces]
    scratch += [VMEM(pieces[3], bf16)] * 2
    scratch += [
        VMEM((2, tok, 128), f32),
        VMEM((8, wide), f32), VMEM((8, n_fc), f32), VMEM((7, 8, tok), f32), VMEM((9, 16, 512), f32),
        VMEM((512,), f32), VMEM((512,), f32), VMEM((512,), f32), VMEM((512,), f32),
        VMEM((n_qkv,), f32), VMEM((n_fc,), f32), VMEM((512,), f32), VMEM((512,), f32),
        pltpu.SemaphoreType.DMA((128,)), pltpu.SemaphoreType.DMA((128,)),
        pltpu.SemaphoreType.DMA((64,)), pltpu.SemaphoreType.DMA((2,)),
    ]
    return pl.pallas_call(
        block_kernel,
        name="block",
        out_shape=outs,
        in_specs=[any_spec] * 15,
        out_specs=[any_spec] * len(outs),
        scratch_shapes=scratch,
        compiler_params=pltpu.CompilerParams(
            collective_id=1, has_side_effects=True, vmem_limit_bytes=67043328
        ),
    )(*args)


def turn_tables(length):
    half_rot = ROT // 2
    frequency = (10000.0 ** (-np.arange(half_rot, dtype=np.float32) * (2.0 / ROT))).astype(np.float32)
    angles = np.arange(length, dtype=np.float32)[:, None] * frequency[None, :]
    tables = np.zeros((2, length, 128), np.float32)
    tables[0] = 1.0
    tables[0, :, :half_rot] = tables[0, :, half_rot:ROT] = np.cos(angles)
    tables[1, :, :half_rot] = -np.sin(angles)
    tables[1, :, half_rot:ROT] = np.sin(angles)
    return tables


def close_kernel(cuts, *refs):
    count = len(cuts)
    refs = list(refs)
    sources, small = [refs.pop(0) for _ in cuts], refs.pop(0)
    outs, vectors = [refs.pop(0) for _ in cuts], [refs.pop(0) for _ in range(8)]
    lows, sums = [refs.pop(0) for _ in cuts], refs.pop(0)
    wides, lines = [refs.pop(0) for _ in range(4)], [refs.pop(0) for _ in range(8)]
    in_sems, out_sems = refs
    loads, stores = [], []
    for n, cut in enumerate(cuts):
        rows = sources[n].shape[0] // cut
        for part in range(cut):
            at = pl.ds(part * rows, rows)
            number = len(loads)
            wide = wides[n] if n < len(wides) else lows[n]
            loads.append(
                pltpu.make_async_copy(sources[n].at[at, :], lows[n].at[at, :], in_sems.at[number])
            )
            stores.append(
                (n, at, pltpu.make_async_copy(wide.at[at, :], outs[n].at[at, :], out_sems.at[number]))
            )
    total = len(loads)
    load_small = pltpu.make_async_copy(small, sums, in_sems.at[total])
    for copy in loads:
        copy.start()
    load_small.start()
    for load, (n, at, store) in zip(loads, stores):
        load.wait()
        if n < len(wides):
            wides[n][at, :] = lows[n][at, :].astype(f32)
        store.start()
    load_small.wait()
    last = []
    for n, (row, line, vector) in enumerate(zip((0, 1, 2, 3, 4, 7, 11, 11), lines, vectors)):
        for part in range(line.shape[0] // 512):
            line[part * 512 : part * 512 + 512] = sums[row + part, :]
        last.append(pltpu.make_async_copy(line, vector, out_sems.at[total + n]))
        last[-1].start()
    for _, _, store in stores:
        store.wait()
    for copy in last:
        copy.wait()


def call_close(proj, qkv, fc, dense, block, grad, small):
    any_spec = pl.BlockSpec(memory_space=pl.ANY)
    shape = jax.ShapeDtypeStruct
    arrays = (fc, proj, qkv, dense, block, grad)
    cuts = (4, 4, 2, 1, 2, 2)
    outs = [shape(a.shape, f32) for a in arrays]
    lengths = [512] * 4 + [qkv.shape[1], fc.shape[1], 512, 512]
    outs += [shape((length,), f32) for length in lengths]
    return pl.pallas_call(
        functools.partial(close_kernel, cuts),
        name="close",
        out_shape=outs,
        in_specs=[any_spec] * 7,
        out_specs=[any_spec] * 14,
        scratch_shapes=[VMEM(a.shape, a.dtype) for a in (*arrays, small)]
        + [VMEM(a.shape, f32) for a in arrays[:4]]
        + [VMEM((length,), f32) for length in lengths]
        + [pltpu.SemaphoreType.DMA((sum(cuts) + 8,)), pltpu.SemaphoreType.DMA((sum(cuts) + 8,))],
        compiler_params=pltpu.CompilerParams(vmem_limit_bytes=60 << 20),
    )(*arrays, small)


def fused_shards(
    block_input, out_grad, ln1_gain, ln1_bias, ln2_gain, ln2_bias,
    w_qkv, b_qkv, w_dense, b_dense, w_fc, b_fc, w_proj, b_proj,
):
    results = call_block(
        block_input, out_grad, w_qkv, w_dense, w_fc, w_proj, turn_tables(SEQ),
        ln1_gain, ln1_bias, ln2_gain, ln2_bias, b_qkv, b_fc, b_dense, b_proj,
    )
    fc, proj, qkv, dense, block, grad, *vectors = call_close(*results[:7])
    gain_1, shift_1, gain_2, shift_2, qkv_bias, fc_bias, dense_bias, proj_bias = vectors
    return (
        block, grad, gain_1, shift_1, gain_2, shift_2, qkv, qkv_bias, dense, dense_bias,
        fc, fc_bias, proj, proj_bias,
    )


def solution(mesh):
    sizes = tuple(mesh.shape[name] for name in ("dp", "row", "col"))
    body = fused_shards if sizes == (2, 4, 4) else shards
    return jax.shard_map(
        body,
        mesh=mesh,
        in_specs=(
            P(("dp", "row"), "col"),
            P(("dp", "row"), "col"),
            P("col"),
            P("col"),
            P("col"),
            P("col"),
            P("row", "col"),
            P("col"),
            P("col", "row"),
            P("col"),
            P("row", "col"),
            P("col"),
            P("col", "row"),
            P("col"),
        ),
        out_specs=(
            P(("dp", "row"), "col"),
            P(("dp", "row"), "col"),
            P("col"),
            P("col"),
            P("col"),
            P("col"),
            P("row", "col"),
            P("col"),
            P("col", "row"),
            P("col"),
            P("row", "col"),
            P("col"),
            P("col", "row"),
            P("col"),
        ),
        check_vma=False,
    )
```

```python
import functools
import math

import jax
import jax.numpy as jnp
import numpy as np
from jax import lax
from jax.experimental import pallas as pl
from jax.experimental.pallas import tpu as pltpu
from jax.sharding import PartitionSpec as P

D = 2048
HD = 256
ROT = 64
SEQ = 512


epsilon = 1e-05
contract_last = (((1,), (1,)), ((), ()))
contract_first = (((0,), (0,)), ((), ()))


def angle_tables(length):
    half_rot = ROT // 2
    position = jnp.arange(length, dtype=jnp.float32)
    exponent = jnp.arange(half_rot, dtype=jnp.float32) * (2.0 / ROT)
    frequency = 10000.0 ** (-exponent)
    angles = position[:, None] * frequency[None, :]
    return (jnp.cos(angles), jnp.sin(angles))


def rotate_fwd(values, cosine, sine_vals):
    half_rot = ROT // 2
    first = values[..., :half_rot]
    second = values[..., half_rot:ROT]
    cos_part = cosine[:, None, :]
    sin_part = sine_vals[:, None, :]
    return jnp.concatenate(
        [
            first * cos_part - second * sin_part,
            second * cos_part + first * sin_part,
            values[..., ROT:],
        ],
        axis=-1,
    )


def rotate_back(grads, cosine, sine_vals):
    half_rot = ROT // 2
    first = grads[..., :half_rot]
    second = grads[..., half_rot:ROT]
    cos_part = cosine[:, None, :]
    sin_part = sine_vals[:, None, :]
    return jnp.concatenate(
        [
            first * cos_part + second * sin_part,
            second * cos_part - first * sin_part,
            grads[..., ROT:],
        ],
        axis=-1,
    )


def gelu_value(pre_act):
    return 0.5 * pre_act * (1.0 + lax.erf(pre_act * 0.7071067811865476))


def gelu_slope(pre_act):
    return 0.5 * (
        1.0 + lax.erf(pre_act * 0.7071067811865476)
    ) + pre_act * 0.3989422804014327 * jnp.exp(-0.5 * pre_act * pre_act)


def shards(
    block_input,
    out_grad,
    ln1_gain,
    ln1_bias,
    ln2_gain,
    ln2_bias,
    w_qkv,
    b_qkv,
    w_dense,
    b_dense,
    w_fc,
    b_fc,
    w_proj,
    b_proj,
):
    tok_rows = block_input.shape[0]
    seq_count = tok_rows // SEQ
    qkv_cols = w_qkv.shape[1]
    fc_cols = w_fc.shape[1]
    local_heads = qkv_cols // (3 * HD)
    head_cols = local_heads * HD
    scale = 1.0 / math.sqrt(HD)
    cosine, sine_vals = angle_tables(SEQ)
    causal = jnp.arange(SEQ)[:, None] >= jnp.arange(SEQ)[None, :]
    row_total, square_total = lax.psum(
        (jnp.sum(block_input, axis=1), jnp.sum(block_input * block_input, axis=1)), "col"
    )
    mean_row = (row_total / D)[:, None]
    var_row = (square_total / D)[:, None] - mean_row * mean_row
    inv_std = lax.rsqrt(var_row + epsilon)
    x_hat = (block_input - mean_row) * inv_std
    normed_one = (x_hat * ln1_gain + ln1_bias).astype(jnp.bfloat16)
    normed_two = (x_hat * ln2_gain + ln2_bias).astype(jnp.bfloat16)
    wide_one, wide_two = (
        lax.all_gather(normed_one, "col", axis=1, tiled=True),
        lax.all_gather(normed_two, "col", axis=1, tiled=True),
    )
    part_one = wide_one
    part_two = wide_two
    qkv_pre = jnp.dot(
        part_one,
        lax.all_gather(w_qkv, "row", axis=0, tiled=True),
        preferred_element_type=jnp.float32,
    )
    fc_pre = jnp.dot(
        part_two,
        lax.all_gather(w_fc, "row", axis=0, tiled=True),
        preferred_element_type=jnp.float32,
    )
    qkv_pre = qkv_pre + b_qkv
    fc_pre = fc_pre + b_fc

    def forward_seq(block):
        query = rotate_fwd(block[:, :, 0], cosine, sine_vals).astype(jnp.bfloat16)
        keys = rotate_fwd(block[:, :, 1], cosine, sine_vals).astype(jnp.bfloat16)
        values = block[:, :, 2].astype(jnp.bfloat16)
        scores = jnp.einsum("qhd,khd->hqk", query, keys, preferred_element_type=jnp.float32) * scale
        masked = jnp.where(causal[None], scores, -1e30)
        row_max = jnp.max(masked, axis=-1, keepdims=True)
        exp_sum = jnp.sum(
            jnp.where(causal[None], jnp.exp(masked - row_max), 0.0), axis=-1, keepdims=True
        )
        log_total = row_max + jnp.log(exp_sum)
        probs_low = jnp.where(causal[None], jnp.exp(masked - log_total), 0.0).astype(jnp.bfloat16)
        attended = jnp.einsum(
            "hqk,khd->qhd", probs_low, values, preferred_element_type=jnp.float32
        ).astype(jnp.bfloat16)
        return (query, keys, values, attended, log_total)

    query, keys, values, attended, log_total = lax.map(
        forward_seq, qkv_pre.reshape(seq_count, SEQ, local_heads, 3, HD)
    )
    attn_out = attended.reshape(tok_rows, head_cols)
    gelu_out = gelu_value(fc_pre).astype(jnp.bfloat16)
    out_stack = jnp.concatenate([w_dense, w_proj], axis=0)
    shard_piece = lax.all_gather(out_stack, "row", axis=1, tiled=True)
    mixed = jnp.dot(
        attn_out, shard_piece[:head_cols], preferred_element_type=jnp.float32
    ) + jnp.dot(gelu_out, shard_piece[head_cols:], preferred_element_type=jnp.float32)
    branch_sum = lax.psum_scatter(mixed, "col", scatter_dimension=1, tiled=True)
    block_output = block_input + branch_sum + b_dense + b_proj
    grad_low = out_grad.astype(jnp.bfloat16)
    wide_grad = lax.all_gather(grad_low, "col", axis=1, tiled=True)
    both_grad = lax.dot_general(
        wide_grad,
        lax.all_gather(out_stack, "row", axis=1, tiled=True),
        contract_last,
        preferred_element_type=jnp.float32,
    )
    attn_grad = both_grad[:, :head_cols]
    gelu_grad = both_grad[:, head_cols:]
    attn_grad_low = attn_grad.astype(jnp.bfloat16)
    fc_grad = gelu_grad * gelu_slope(fc_pre)
    fc_bias_grad = jnp.sum(fc_grad, axis=0)
    fc_grad_low = fc_grad.astype(jnp.bfloat16)

    def backward_seq(items):
        query_s, keys_s, values_s, attended_s, log_s, head_grad = items
        scores = (
            jnp.einsum("qhd,khd->hqk", query_s, keys_s, preferred_element_type=jnp.float32) * scale
        )
        probs = jnp.where(
            causal[None], jnp.exp(jnp.where(causal[None], scores, -1e30) - log_s), 0.0
        )
        probs_low = probs.astype(jnp.bfloat16)
        value_grad = jnp.einsum(
            "hqk,qhd->khd", probs_low, head_grad, preferred_element_type=jnp.float32
        )
        prob_grad = jnp.einsum(
            "qhd,khd->hqk", head_grad, values_s, preferred_element_type=jnp.float32
        )
        delta_row = jnp.transpose(
            jnp.sum(head_grad.astype(jnp.float32) * attended_s.astype(jnp.float32), axis=-1), (1, 0)
        )[:, :, None]
        score_grad = (probs * (prob_grad - delta_row) * scale).astype(jnp.bfloat16)
        query_grad = jnp.einsum(
            "hqk,khd->qhd", score_grad, keys_s, preferred_element_type=jnp.float32
        )
        key_grad = jnp.einsum(
            "hqk,qhd->khd", score_grad, query_s, preferred_element_type=jnp.float32
        )
        return jnp.stack(
            [
                rotate_back(query_grad, cosine, sine_vals),
                rotate_back(key_grad, cosine, sine_vals),
                value_grad,
            ],
            axis=2,
        )

    head_grads = attn_grad_low.reshape(seq_count, SEQ, local_heads, HD)
    qkv_grad = lax.map(
        backward_seq, (query, keys, values, attended, log_total, head_grads)
    ).reshape(tok_rows, qkv_cols)
    qkv_bias_grad = jnp.sum(qkv_grad, axis=0)
    qkv_grad_low = qkv_grad.astype(jnp.bfloat16)
    in_stack = jnp.concatenate([w_qkv, w_fc], axis=1)
    shard_piece = lax.all_gather(in_stack, "row", axis=0, tiled=True)
    norm_grads = jnp.stack(
        [
            lax.dot_general(
                qkv_grad_low,
                shard_piece[:, :qkv_cols],
                contract_last,
                preferred_element_type=jnp.float32,
            ),
            lax.dot_general(
                fc_grad_low,
                shard_piece[:, qkv_cols:],
                contract_last,
                preferred_element_type=jnp.float32,
            ),
        ]
    )
    part_one = wide_one
    part_two = wide_two
    row_part = lax.psum_scatter(
        jnp.concatenate(
            [
                lax.dot_general(
                    part_one, qkv_grad_low, contract_first, preferred_element_type=jnp.float32
                ),
                lax.dot_general(
                    part_two, fc_grad_low, contract_first, preferred_element_type=jnp.float32
                ),
                lax.dot_general(
                    wide_grad, attn_out, contract_first, preferred_element_type=jnp.float32
                ),
                lax.dot_general(
                    wide_grad, gelu_out, contract_first, preferred_element_type=jnp.float32
                ),
            ],
            axis=1,
        ),
        "row",
        scatter_dimension=0,
        tiled=True,
    )
    grad_rows = lax.psum(row_part, "dp")
    qkv_total = grad_rows[:, :qkv_cols]
    fc_total = grad_rows[:, qkv_cols : qkv_cols + fc_cols]
    dense_total = grad_rows[:, qkv_cols + fc_cols : qkv_cols + fc_cols + head_cols].T
    proj_total = grad_rows[:, qkv_cols + fc_cols + head_cols :].T
    norm_local = lax.psum_scatter(norm_grads, "col", scatter_dimension=2, tiled=True)
    grad_one = norm_local[0]
    grad_two = norm_local[1]
    hat_grad = grad_one * ln1_gain + grad_two * ln2_gain
    total_hat, total_cross = lax.psum(
        (jnp.sum(hat_grad, axis=1), jnp.sum(hat_grad * x_hat, axis=1)), "col"
    )
    input_grad = out_grad + inv_std * (
        hat_grad - (total_hat / D)[:, None] - x_hat * (total_cross / D)[:, None]
    )
    gain_one, shift_one, gain_two, shift_two, qkv_bias_total, fc_bias_total, out_bias_total = (
        lax.psum(
            (
                jnp.sum(grad_one * x_hat, axis=0),
                jnp.sum(grad_one, axis=0),
                jnp.sum(grad_two * x_hat, axis=0),
                jnp.sum(grad_two, axis=0),
                qkv_bias_grad,
                fc_bias_grad,
                jnp.sum(out_grad, axis=0),
            ),
            ("dp", "row"),
        )
    )
    return (
        block_output,
        input_grad,
        gain_one,
        shift_one,
        gain_two,
        shift_two,
        qkv_total,
        qkv_bias_total,
        dense_total,
        out_bias_total,
        fc_total,
        fc_bias_total,
        proj_total,
        out_bias_total,
    )


f32 = jnp.float32
bf16 = jnp.bfloat16
MESH = pl.DeviceIdType.MESH
VMEM = pltpu.VMEM
Q = 256
HALF = 4 * Q


def flip(a, b):
    return a + b - 2 * a * b


def span(start, size):
    return pl.ds(pl.multiple_of(start, size), size)


def mm(a, b):
    return jnp.dot(a, b, preferred_element_type=f32)


def mm_nt(a, b):
    return lax.dot_general(a, b, (((1,), (1,)), ((), ())), preferred_element_type=f32)


def mm_tn(a, b):
    return lax.dot_general(a, b, (((0,), (0,)), ((), ())), preferred_element_type=f32)


class Net:
    def __init__(self, send_sems, recv_sems, local_sems):
        self.k = lax.axis_index("dp")
        self.r = lax.axis_index("row")
        self.c = lax.axis_index("col")
        k, r, c = self.k, self.r, self.c
        self.core = (1 - k, r, c)
        self.x = (k, r + 1 - 2 * (r % 2), c)
        self.y = (k, r + 2 - 4 * (r // 2), c)
        near = c + 1 - 2 * (c % 2)
        self.z = (None, (k, r, near), (k, r, c + 2 - 4 * (c // 2)), (k, r, 3 - c))
        self.middle = flip(c % 2, c // 2) == 1
        self.send_sems, self.recv_sems, self.local_sems = send_sems, recv_sems, local_sems
        self.remote_count = 0
        self.local_count = 0
        self.pending = []

    def mix(self, j):
        return flip(j % 2, flip(self.c % 2, self.r % 2)) + 2 * flip(
            j // 2, flip(self.c // 2, self.r // 2)
        )

    def barrier(self):
        sem = pltpu.get_barrier_semaphore()

        def greet(peer):
            pl.semaphore_signal(sem, inc=1, device_id=peer, device_id_type=MESH)

        for peer in (self.x, self.y, self.core, self.z[1]):
            greet(peer)

        @pl.when(self.middle)
        def _():
            greet(self.z[3])
            pl.semaphore_wait(sem, 5)

        @pl.when(jnp.logical_not(self.middle))
        def _():
            pl.semaphore_wait(sem, 4)

    def slot(self):
        self.remote_count += 1
        return self.remote_count - 1

    def remote(self, src, dst, peer):
        slot = self.slot()
        copy = pltpu.make_async_remote_copy(
            src_ref=src,
            dst_ref=dst,
            send_sem=self.send_sems.at[slot],
            recv_sem=self.recv_sems.at[slot],
            device_id=peer,
            device_id_type=MESH,
        )
        copy.start()
        self.pending.append(copy)
        return copy

    def local(self, src, dst):
        copy = pltpu.make_async_copy(src, dst, self.local_sems.at[self.local_count])
        self.local_count += 1
        copy.start()
        return copy

    def sent(self, copy):
        copy.wait_send()
        self.pending = [other for other in self.pending if other is not copy]

    def drain(self):
        for copy in self.pending:
            copy.wait_send()


class Gather:
    def __init__(self, net, shard, full, by_rows):
        self.net, self.shard, self.full, self.by_rows = net, shard, full, by_rows
        self.depth = Q // 2 if by_rows else shard.shape[0] // 2
        self.placed = []

    def own(self, half, part=None):
        if self.by_rows:
            if part is None:
                return self.shard.at[span(half * Q, Q), :]
            return self.shard.at[span(half * Q + part * self.depth, self.depth), :]
        rows = slice(None) if part is None else pl.ds(part * self.depth, self.depth)
        return self.shard.at[rows, span(half * Q, Q)]

    def chunk(self, s, i, part=None):
        start = s * HALF + i * Q
        if self.by_rows:
            if part is None:
                return self.full.at[pl.ds(start, Q), :]
            return self.full.at[pl.ds(start + part * self.depth, self.depth), :]
        rows = slice(None) if part is None else pl.ds(part * self.depth, self.depth)
        return self.full.at[rows, pl.ds(start, Q)]

    def place_own(self):
        net = self.net
        self.placed = [
            net.local(self.own(net.k), self.chunk(0, 0)),
            net.local(self.own(1 - net.k), self.chunk(1, 0)),
        ]

    def send_own(self):
        net, k = self.net, self.net.k
        self.y0 = net.remote(self.own(k, 0), self.chunk(0, 2, 0), net.y)
        self.x1 = net.remote(self.own(k, 1), self.chunk(0, 1, 1), net.x)
        self.y1 = net.remote(self.own(k, 1), self.chunk(0, 2, 1), net.y)
        self.x0 = net.remote(self.own(k, 0), self.chunk(0, 1, 0), net.x)

    def forward(self):
        net = self.net
        self.y0.wait_recv()
        self.d0 = net.remote(self.chunk(0, 2, 0), self.chunk(0, 3, 0), net.x)
        self.x1.wait_recv()
        self.d1 = net.remote(self.chunk(0, 1, 1), self.chunk(0, 3, 1), net.y)

    def swap_near(self):
        net = self.net
        self.x0.wait_recv()
        self.c1 = net.remote(self.chunk(0, 1), self.chunk(1, 1), net.core)
        self.y1.wait_recv()
        self.c2 = net.remote(self.chunk(0, 2), self.chunk(1, 2), net.core)

    def swap_far(self):
        net = self.net
        self.d0.wait_recv()
        self.d1.wait_recv()
        self.c3 = net.remote(self.chunk(0, 3), self.chunk(1, 3), net.core)

    def ready(self):
        for copy in (self.c1, self.c2, self.c3):
            copy.wait_recv()
        for copy in self.placed:
            copy.wait()

    def release(self):
        for copy in (self.d0, self.d1, self.c1, self.c2, self.c3):
            self.net.sent(copy)


class Line:
    def __init__(self, net, slots):
        self.net, self.slots = net, slots
        self.ids = [None] + [net.slot() for _ in range(3)]
        self.sends = []

    def copy(self, src, dst, peer, send):
        net = self.net
        return pltpu.make_async_remote_copy(
            src_ref=self.slots.at[src],
            dst_ref=self.slots.at[dst],
            send_sem=net.send_sems.at[send],
            recv_sem=net.recv_sems.at[self.ids[dst]],
            device_id=peer,
            device_id_type=MESH,
        )

    def start(self):
        net = self.net
        self.first = self.copy(0, 1, net.z[1], self.ids[1])
        self.first.start()
        self.hops = [
            self.copy(0, 3, net.z[3], self.ids[2]),
            self.copy(1, 2, net.z[3], self.ids[3]),
            self.copy(3, 2, net.z[1], net.slot()),
            self.copy(2, 3, net.z[1], net.slot()),
        ]

        @pl.when(net.middle)
        def _():
            self.hops[0].start()

    def arrived(self, slot):
        return self.copy(0, slot, self.net.z[1], self.ids[slot])

    def step(self, number):
        slot = (1, 3, 2)[number]

        @pl.when(self.net.middle)
        def _():
            self.arrived(slot).wait_recv()
            self.hops[number + 1].start()

    def ready(self):
        @pl.when(jnp.logical_not(self.net.middle))
        def _():
            for slot in (1, 2, 3):
                self.arrived(slot).wait_recv()

    def drain(self):
        self.first.wait_send()

        @pl.when(self.net.middle)
        def _():
            for hop in self.hops:
                hop.wait_send()


class Fold:
    def __init__(self, net, blocks, inbox):
        self.net, self.blocks, self.inbox = net, blocks, inbox
        hops = ((3, None, 0), (2, None, 1), (1, None, 2), (None, 0, 3), (None, 1, 4), (None, 3, 0))
        self.copies = []
        for n, (block, slot, dest) in enumerate(hops):
            number = net.slot()
            self.copies.append(
                pltpu.make_async_remote_copy(
                    src_ref=blocks.at[block] if slot is None else inbox.at[slot],
                    dst_ref=inbox.at[dest],
                    send_sem=net.send_sems.at[number],
                    recv_sem=net.recv_sems.at[number],
                    device_id=net.z[3] if n in (3, 4) else net.z[1],
                    device_id_type=MESH,
                )
            )

    def start(self, first, last):
        @pl.when(jnp.logical_not(self.net.middle))
        def _():
            for copy in self.copies[first:last]:
                copy.start()

    def step(self, number):
        slot, block = ((0, 2), (1, 3), (3, 1))[number]
        inbox, blocks = self.inbox, self.blocks

        @pl.when(self.net.middle)
        def _():
            self.copies[(0, 1, 3)[number]].wait_recv()

            def add(n, _):
                at = span(n * 64, 64)
                total = inbox[slot, at, :].astype(f32) + blocks[block, at, :].astype(f32)
                inbox[slot, at, :] = total.astype(bf16)
                return 0

            lax.fori_loop(0, inbox.shape[1] // 64, add, 0)
            self.copies[3 + number].start()

    def total(self, use):
        def gather(*slots):
            def add(n, _):
                at = span(n * 64, 64)
                value = self.blocks[0, at, :].astype(f32)
                for slot in slots:
                    value = value + self.inbox[slot, at, :].astype(f32)
                use(at, value)
                return 0

            lax.fori_loop(0, self.inbox.shape[1] // 64, add, 0)

        @pl.when(self.net.middle)
        def _():
            self.copies[2].wait_recv()
            self.copies[4].wait_recv()
            gather(2, 4)

        @pl.when(jnp.logical_not(self.net.middle))
        def _():
            self.copies[5].wait_recv()
            gather(0)

    def drain(self):
        @pl.when(self.net.middle)
        def _():
            for copy in self.copies[3:]:
                copy.wait_send()

        @pl.when(jnp.logical_not(self.net.middle))
        def _():
            for copy in self.copies[:3]:
                copy.wait_send()


def turn(low, tables, sign):
    lane = lax.broadcasted_iota(jnp.int32, low.shape, 1)
    swung = jnp.where(lane < ROT // 2, pltpu.roll(low, 96, 1), pltpu.roll(low, 32, 1))
    return low * tables[0] + sign * (tables[1] * swung)


class Tiles:
    def __init__(self, slots, sems):
        self.slots, self.sems = slots, sems

    def write(self, count, product, place, depth):
        def body(n, _):
            slot = n % 2
            source = self.slots.at[slot, pl.ds(0, depth), :]
            copy = pltpu.make_async_copy(source, place(n), self.sems.at[slot])

            @pl.when(n >= 2)
            def _():
                copy.wait()

            self.slots[slot, 0:depth, :] = product(n).astype(bf16)
            copy.start()
            return 0

        lax.fori_loop(0, count, body, 0)
        for slot in range(2):
            source = self.slots.at[slot, pl.ds(0, depth), :]
            pltpu.make_async_copy(source, place(slot), self.sems.at[slot]).wait()


class Reduce:
    def __init__(self, net, partial, joined, near, far, by_rows, in_vmem=False):
        self.in_vmem = in_vmem
        self.net, self.partial, self.by_rows = net, partial, by_rows
        self.joined, self.near, self.far = joined, near, far
        self.depth = Q // 2 if by_rows else partial.shape[0] // 2

    def chunk(self, i, half):
        if self.by_rows:
            return self.partial.at[pl.ds(i * Q + half * self.depth, self.depth), :]
        return self.partial.at[pl.ds(half * self.depth, self.depth), pl.ds(i * Q, Q)]

    def whole(self):
        if self.by_rows:
            return self.partial.at[pl.ds(0, Q), :]
        return self.partial.at[:, pl.ds(0, Q)]

    def rows(self, half):
        return pl.ds(half * self.depth, self.depth)

    def start(self):
        net = self.net
        self.a = net.remote(self.chunk(3, 0), self.joined.at[0], net.x)
        self.b = net.remote(self.chunk(3, 1), self.joined.at[1], net.y)
        self.near_a = net.remote(self.chunk(1, 0), self.near.at[self.rows(0), :], net.x)
        self.near_b = net.remote(self.chunk(2, 1), self.near.at[self.rows(1), :], net.y)

    def join(self, parts):
        net = self.net
        loads = [net.local(self.chunk(2, 0), parts[0]), net.local(self.chunk(1, 1), parts[1])]
        hops = []
        for half, copy, peer in ((0, self.a, net.y), (1, self.b, net.x)):
            loads[half].wait()
            copy.wait_recv()
            tile = 64

            def add(n, _, half=half):
                at = span(n * tile, tile)
                total = self.joined[half, at, :].astype(f32) + parts[half][at, :].astype(f32)
                self.joined[half, at, :] = total.astype(bf16)
                return 0

            lax.fori_loop(0, self.depth // tile, add, 0)
            hops.append(net.remote(self.joined.at[half], self.far.at[self.rows(half), :], peer))
        self.far_a, self.far_b = hops

    def prepare(self, buffers):
        net = self.net
        self.buffers = list(buffers)
        self.loads = [net.local(self.whole(), buffers[0])]
        for copy in (self.near_a, self.near_b):
            copy.wait_recv()
        if self.in_vmem:
            self.buffers[1:3] = [self.near, self.far]
        else:
            self.loads.append(net.local(self.near, buffers[1]))

    def finish(self, out):
        net, buffers = self.net, self.buffers
        last = []
        for half, copy in enumerate((self.far_a, self.far_b)):
            copy.wait_recv()
            if not self.in_vmem:
                rows = self.rows(half)
                last.append(net.local(self.far.at[rows, :], buffers[2].at[rows, :]))
        for copy in self.loads:
            copy.wait()
        tile = 64
        self.here, self.there = [], []
        for half in range(2):
            if last:
                last[half].wait()

            def add(n, _, half=half):
                at = span(half * self.depth + n * tile, tile)
                parts = [buffer[at, :].astype(f32) for buffer in buffers[:3]]
                buffers[3][at, :] = (parts[0] + parts[1] + parts[2]).astype(bf16)
                return 0

            lax.fori_loop(0, self.depth // tile, add, 0)
            source = buffers[3].at[self.rows(half), :]
            if self.by_rows:
                place = out.at[span(net.k * Q + half * self.depth, self.depth), :]
            else:
                place = out.at[self.rows(half), span(net.k * Q, Q)]
            self.here.append(net.local(source, place))
            self.there.append(net.remote(source, place, net.core))

    def done(self):
        for copy in self.here:
            copy.wait()
        for copy in self.there:
            copy.wait_recv()


def block_kernel(
    x, og, w_qkv, w_dense, w_fc, w_proj, t_turn,
    i_gain_1, i_bias_1, i_gain_2, i_bias_2, i_b_qkv, i_b_fc, i_b_dense, i_b_proj,
    o_proj, o_qkv, o_fc, o_dense, o_block, o_input, o_small,
    all_proj, r_proj, r_qkv, r_fc, r_dense, n_proj, f_proj, n_qkv, f_qkv, n_fc, f_fc,
    g_qkv, g_dense, g_fc, g_tail, xs, ys, pks, stats, rows, h1c, h1s, h2c, h2s, dyc, dys, xh,
    qb, kb, vb, probs, probs_low, oc, dob, dqc, gc, slope, dabt, stage,
    out_recv, hat_recv, j_proj, j_qkv, j_fc, j_dense, n_dense, f_dense, tables, vecs, bias, packs, small,
    gain_1, bias_1, gain_2, bias_2, b_qkv, b_fc, b_dense, b_proj,
    send_sems, recv_sems, local_sems, stage_sems,
):
    tok = x.shape[0]
    heads = qb.shape[0]
    width = gc.shape[1]
    scale = 1.0 / math.sqrt(HD)
    net = Net(send_sems, recv_sems, local_sems)
    net.barrier()
    qkv = Gather(net, w_qkv, g_qkv, True)
    dense = Gather(net, w_dense, g_dense, False)
    fc = Gather(net, w_fc, g_fc, True)
    proj = Gather(net, w_proj, all_proj, False)
    qkv.send_own()
    dense.send_own()
    load_x = net.local(x, probs.at[0])
    vectors = [
        net.local(i_gain_1, gain_1), net.local(i_bias_1, bias_1), net.local(i_gain_2, gain_2),
        net.local(i_bias_2, bias_2), net.local(i_b_qkv, b_qkv), net.local(i_b_fc, b_fc),
        net.local(i_b_dense, b_dense), net.local(i_b_proj, b_proj),
    ]
    load_og = net.local(og, probs.at[1])
    load_turn = net.local(t_turn, tables)
    tiles = Tiles(stage, stage_sems)
    mine = pl.ds(0, tok)
    theirs = pl.ds(tok, tok)

    step = 128
    lane = lax.broadcasted_iota(jnp.int32, (step, 128), 1)
    load_x.wait()

    def local_norm(n, _):
        at = span(n * step, step)
        block = probs[0, at, :]
        mean = jnp.mean(block, axis=1, keepdims=True)
        centred = block - mean
        var = jnp.mean(centred * centred, axis=1, keepdims=True)
        stats[at, :] = jnp.where(lane == 0, mean, jnp.where(lane == 1, var, 0.0))
        return 0

    lax.fori_loop(0, tok // step, local_norm, 0)
    pks[0] = stats[...].T[0:8]
    for copy in vectors:
        copy.wait()
    for n, vector in enumerate((gain_1, bias_1, gain_2, bias_2)):
        pks[0, 2 + n : 3 + n, :] = vector[...].reshape(1, 512)
    p_line = Line(net, pks)
    p_line.start()
    for weight in (qkv, dense, fc):
        weight.place_own()
    bias[...] = jnp.zeros_like(bias)
    bias[3:4, 0 : b_qkv.shape[0]] = b_qkv[...].reshape(1, b_qkv.shape[0])
    bias[4:5, :] = b_fc[...].reshape(1, width)
    bias[5:6, 0:512] = (b_dense[...] + b_proj[...]).reshape(1, 512)
    rows[...] = jnp.zeros_like(rows)
    load_og.wait()

    def local_grad(n, _):
        at = span(n * step, step)
        block = probs[1, at, :]
        ys[0, at, :] = block.astype(bf16)
        bias[1:2, 0:512] += jnp.sum(block, axis=0, keepdims=True)
        return 0

    lax.fori_loop(0, tok // step, local_grad, 0)
    for hop in range(3):
        p_line.step(hop)
    p_line.ready()
    means = [pks[j, 0:1, :] for j in range(4)]
    mu = (means[0] + means[1] + means[2] + means[3]) * 0.25
    spread = [pks[j, 1:2, :] + (means[j] - mu) * (means[j] - mu) for j in range(4)]
    rows[0:1, :] = mu
    rows[1:2, :] = lax.rsqrt((spread[0] + spread[1] + spread[2] + spread[3]) * 0.25 + epsilon)
    stats[...] = rows[...].T

    def own_norm(n, _):
        at = span(n * step, step)
        hats = (probs[0, at, :] - stats[at, 0:1]) * stats[at, 1:2]
        xs[0, at, :] = (hats * pks[0, 2:3, :] + pks[0, 3:4, :]).astype(bf16)
        return 0

    lax.fori_loop(0, tok // step, own_norm, 0)
    x_line = Line(net, xs)
    y_line = Line(net, ys)
    x_line.start()
    qkv.forward()
    x_line.step(0)
    x_line.step(1)
    fc.send_own()
    dense.forward()
    qkv.swap_near()
    x_line.step(2)
    y_line.start()
    dense.swap_near()
    qkv.swap_far()
    x_line.ready()
    fc.forward()
    proj.send_own()

    for s in range(2):
        for j in range(4):
            lanes = span(flip(s, net.k) * Q, Q)
            dest = span(net.mix(j) * Q, Q)
            wide = span(s * HALF + net.mix(j) * Q, Q)
            vecs[0:4, wide] = pks[j, 2:6, lanes]

            def norm(n, _, s=s, j=j, lanes=lanes, dest=dest, wide=wide):
                at = span(n * step, step)
                one = xs[j, at, lanes]
                hats = (one.astype(f32) - pks[j, 3:4, lanes]) * (1.0 / pks[j, 2:3, lanes])
                xh[at, wide] = hats.astype(bf16)
                (h1s if s else h1c)[at, dest] = one
                two = hats * pks[j, 4:5, lanes] + pks[j, 5:6, lanes]
                (h2s if s else h2c)[at, dest] = two.astype(bf16)
                return 0

            lax.fori_loop(0, tok // step, norm, 0)
    swap_h1 = net.remote(h1s, h1c.at[theirs, :], net.core)
    swap_h2 = net.remote(h2s, h2c.at[theirs, :], net.core)
    y_line.step(0)
    load_turn.wait()
    qkv.ready()

    def project(n, _):
        cols = span(n * 3 * HD, 3 * HD)
        acc = mm(h1c[mine, :], g_qkv[0:HALF, cols]) + mm(h1s[...], g_qkv[HALF:, cols])
        acc = acc + bias[3:4, cols]
        qb[n, :, 0:128] = turn(acc[:, 0:128], tables, 1.0).astype(bf16)
        qb[n, :, 128:HD] = acc[:, 128:HD].astype(bf16)
        kb[n, :, 0:128] = turn(acc[:, HD : HD + 128], tables, 1.0).astype(bf16)
        kb[n, :, 128:HD] = acc[:, HD + 128 : 2 * HD].astype(bf16)
        vb[n] = acc[:, 2 * HD :].astype(bf16)
        return 0

    lax.fori_loop(0, heads, project, 0)
    y_line.step(1)
    chunks = tok // step

    def attend(n, _):
        head, chunk = n // chunks, n % chunks
        at = span(chunk * step, step)
        scores = mm_nt(qb[head, at, :], kb[head]) * scale
        token = lax.broadcasted_iota(jnp.int32, (step, tok), 0) + chunk * step
        allowed = token >= lax.broadcasted_iota(jnp.int32, (step, tok), 1)
        scores = jnp.where(allowed, scores, -1e30)
        top = jnp.max(scores, axis=1, keepdims=True)
        raised = jnp.where(allowed, jnp.exp(scores - top), 0.0)
        weight = raised / jnp.sum(raised, axis=1, keepdims=True)
        probs[head, at, :] = weight
        low = weight.astype(bf16)
        probs_low[head, at, :] = low
        oc[at, span(head * HD, HD)] = mm(low, vb[head]).astype(bf16)
        return 0

    lax.fori_loop(0, heads * chunks, attend, 0)
    swap_o = net.remote(oc.at[mine, :], oc.at[theirs, :], net.core)
    dense.swap_far()
    fc.swap_near()
    y_line.step(2)
    fc.swap_far()
    fc.ready()

    def expand(n, _):
        cols = span(n * 512, 512)
        a = mm(h2c[mine, :], g_fc[0:HALF, cols]) + mm(h2s[...], g_fc[HALF:, cols])
        a = a + bias[4:5, cols]
        rise = 0.5 * (1.0 + lax.erf(a * 0.7071067811865476))
        gc[mine, cols] = (a * rise).astype(bf16)
        slope[:, cols] = (rise + a * 0.3989422804014327 * jnp.exp(-0.5 * a * a)).astype(bf16)
        return 0

    lax.fori_loop(0, width // 1024, expand, 0)
    proj.forward()
    lax.fori_loop(width // 1024, width // 512, expand, 0)
    swap_g = net.remote(gc.at[mine, :], gc.at[theirs, :], net.core)
    y_line.ready()
    for s in range(2):
        for j in range(4):
            lanes = span(flip(s, net.k) * Q, Q)
            dest = span(net.mix(j) * Q, Q)
            (dys if s else dyc)[mine, dest] = ys[j, :, lanes]
    swap_dy = net.remote(dys, dyc.at[theirs, :], net.core)
    dense.ready()
    dob[...] = (
        mm_nt(dyc[mine, :], g_dense[:, 0:HALF]) + mm_nt(dys[...], g_dense[:, HALF:])
    ).astype(bf16)

    red_proj = Reduce(net, r_proj, j_proj, n_proj, f_proj, False)
    red_qkv = Reduce(net, r_qkv, j_qkv, n_qkv, f_qkv, True)
    red_fc = Reduce(net, r_fc, j_fc, n_fc, f_fc, True)
    red_dense = Reduce(net, r_dense, j_dense, n_dense, f_dense, False, True)
    swap_g.wait_recv()
    swap_dy.wait_recv()
    tall = width // 2
    tiles.write(
        4,
        lambda n: mm_tn(gc[:, span(n // 2 * tall, tall)], dyc[:, span(n % 2 * 512, 512)]),
        lambda n: r_proj.at[span(n // 2 * tall, tall), span(n % 2 * 512, 512)],
        tall,
    )
    proj.swap_near()
    red_proj.start()

    def keep(head, part, at, value, rotated):
        base = head * 3 * HD + part * HD
        if rotated:
            low = turn(value[:, 0:128], [tables[t, at, :] for t in range(2)], -1.0)
            dqc[at, pl.ds(pl.multiple_of(base, 128), 128)] = low.astype(bf16)
            bias[0:1, pl.ds(pl.multiple_of(base, 128), 128)] += jnp.sum(low, axis=0, keepdims=True)
            value, base, size = value[:, 128:], base + 128, 128
        else:
            size = HD
        cols = pl.ds(pl.multiple_of(base, 128), size)
        dqc[at, cols] = value.astype(bf16)
        bias[0:1, cols] += jnp.sum(value, axis=0, keepdims=True)

    def attend_back(head, _):
        cols = span(head * HD, HD)

        def chunk_back(n, _):
            at = span(n * step, step)
            grad = dob[at, cols]
            delta = jnp.sum(grad.astype(f32) * oc[at, cols].astype(f32), axis=1, keepdims=True)
            spread = mm_nt(grad, vb[head]) - delta
            low = (probs[head, at, :] * spread * scale).astype(bf16)
            probs_low[head, at, :] = low
            keep(head, 0, at, mm(low, kb[head]), True)
            return 0

        keep(head, 2, mine, mm_tn(probs_low[head], dob[:, cols]), False)
        lax.fori_loop(0, chunks, chunk_back, 0)
        keep(head, 1, mine, mm_tn(probs_low[head], qb[head]), True)
        return 0

    lax.fori_loop(0, heads, attend_back, 0)
    proj.swap_far()
    swap_dq = net.remote(dqc.at[mine, :], dqc.at[theirs, :], net.core)
    net.sent(swap_h1)
    net.sent(swap_h2)
    for s in range(2):

        def back_first(n, _, s=s):
            wide = span(s * HALF + n * 512, 512)
            grad = mm_nt(dqc[mine, :], g_qkv[wide, :])
            (h2s if s else h1s)[:, span(n * 512, 512)] = (grad * vecs[0:1, wide]).astype(bf16)
            vecs[4:5, wide] = jnp.sum(grad * xh[:, wide].astype(f32), axis=0, keepdims=True)
            vecs[5:6, wide] = jnp.sum(grad, axis=0, keepdims=True)
            return 0

        lax.fori_loop(0, HALF // 512, back_first, 0)

    proj.ready()
    qkv.release()
    loads = [
        net.local(w_proj.at[:, span(net.k * Q, Q)], g_qkv.at[:, pl.ds(0, Q)]),
        net.local(w_proj.at[:, span((1 - net.k) * Q, Q)], g_qkv.at[:, pl.ds(HALF, Q)]),
        net.local(all_proj.at[:, pl.ds(Q, 3 * Q)], g_qkv.at[:, pl.ds(Q, 3 * Q)]),
        net.local(all_proj.at[:, pl.ds(5 * Q, Q)], g_qkv.at[:, pl.ds(5 * Q, Q)]),
        net.local(all_proj.at[:, pl.ds(6 * Q, 2 * Q)], g_tail),
    ]
    swap_o.wait_recv()
    attn = oc.shape[1]
    tiles.write(
        2,
        lambda n: mm_tn(oc[...], dyc[:, span(n * 512, 512)]),
        lambda n: r_dense.at[:, span(n * 512, 512)],
        attn,
    )
    swap_h1.wait_recv()
    swap_dq.wait_recv()
    tiles.write(
        dqc.shape[1] // 512,
        lambda n: mm_tn(h1c[...], dqc[:, span(n * 512, 512)]),
        lambda n: r_qkv.at[:, span(n * 512, 512)],
        HALF,
    )
    red_qkv.start()
    red_dense.start()

    for copy in loads:
        copy.wait()
    x_line.drain()
    y_line.drain()

    def put_out(p, product):
        s, i = p // 4, p % 4
        out = product + mm(oc[mine, :], g_dense[:, span(p * Q, Q)])
        xs[net.mix(i), :, span(flip(s, net.k) * Q, Q)] = out.astype(bf16)

    def project_head(p, _):
        put_out(p, mm(gc[mine, :], g_qkv[:, span(p * Q, Q)]))
        return 0

    def project_tail(p, _):
        put_out(6 + p, mm(gc[mine, :], g_tail[:, span(p * Q, Q)]))
        return 0

    lax.fori_loop(0, 6, project_head, 0)
    lax.fori_loop(0, 2, project_tail, 0)
    out_fold = Fold(net, xs, out_recv)
    out_fold.start(0, 2)

    def back_fc(n, _):
        cols = span(n * 512, 512)
        grad = mm_nt(dyc[mine, :], g_qkv[cols, 0:HALF])
        grad = grad + mm_nt(dys[:, 0:512], g_qkv[cols, HALF : 6 * Q])
        grad = grad + mm_nt(dys[:, 512:], g_tail[cols, :])
        grad = grad * slope[:, cols].astype(f32)
        bias[2:3, cols] = jnp.sum(grad, axis=0, keepdims=True)
        slope[:, cols] = grad.astype(bf16)
        return 0

    lax.fori_loop(0, width // 512, back_fc, 0)
    dab = slope
    swap_da = net.remote(dab, dabt, net.core)
    red_proj.join([g_tail.at[pl.ds(0, tall), pl.ds(0, Q)], g_tail.at[pl.ds(tall, tall), pl.ds(0, Q)]])
    stats[...] = jnp.zeros_like(stats)
    lane = lax.broadcasted_iota(jnp.int32, (tok, 128), 1)

    def back_norm(j, _):
        for s in range(2):
            lanes = span(flip(s, net.k) * Q, Q)
            dest = span(net.mix(j) * Q, Q)
            wide = span(s * HALF + net.mix(j) * Q, Q)
            grad = mm_nt(dab[...], g_fc[wide, :])
            hats = xh[:, wide].astype(f32)
            packs[j, 2:4, lanes] = vecs[4:6, wide]
            packs[j, 4:5, lanes] = jnp.sum(grad * hats, axis=0, keepdims=True)
            packs[j, 5:6, lanes] = jnp.sum(grad, axis=0, keepdims=True)
            joint = (h2s if s else h1s)[:, dest].astype(f32) + grad * vecs[2:3, wide]
            ys[j, :, lanes] = joint.astype(bf16)
            one = jnp.sum(joint, axis=1, keepdims=True)
            two = jnp.sum(joint * hats, axis=1, keepdims=True)
            stats[...] += jnp.where(lane == 0, one, jnp.where(lane == 1, two, 0.0))
        return 0

    lax.fori_loop(0, 4, back_norm, 0)

    fc.release()
    red_qkv.join(
        [g_fc.at[pl.ds(7 * Q + n * (Q // 2), Q // 2), pl.ds(0, 6 * Q)] for n in range(2)]
    )
    turned = stats[...].T
    for j in range(4):
        packs[j, 0:2, :] = turned[0:2]
        packs[j, 6:8, :] = jnp.zeros((2, tok), f32)
    pack_copies = [net.remote(packs.at[j], packs.at[3 + j], net.z[j]) for j in (1, 2, 3)]
    hat_fold = Fold(net, ys, hat_recv)
    hat_fold.start(0, 2)
    out_fold.start(2, 3)
    hat_fold.start(2, 3)
    out_fold.step(0)
    swap_h2.wait_recv()
    swap_da.wait_recv()

    def grad_fc(n):
        cols = span(n * 512, 512)
        return mm_tn(h2c[mine, :], dab[:, cols]) + mm_tn(h2c[theirs, :], dabt[:, cols])

    tiles.write(width // 512, grad_fc, lambda n: r_fc.at[:, span(n * 512, 512)], HALF)
    red_fc.start()
    out_fold.step(1)

    def strips(base, n, columns):
        return g_fc.at[pl.ds(base + n * Q, Q), pl.ds(0, columns)]

    out_fold.step(2)
    for copy in pack_copies:
        copy.wait_recv()
    total = packs[0] + packs[4] + packs[5] + packs[6]
    rows[2:4, :] = total[0:2, :]
    stats[...] = rows[...].T
    me = net.k * 4 + net.r
    small[me, 0:4, :] = total[2:6, :]
    for n in range(3):
        small[me, 4 + n : 5 + n, :] = bias[0:1, n * 512 : n * 512 + 512]
    for n in range(4):
        small[me, 7 + n : 8 + n, :] = bias[2:3, n * 512 : n * 512 + 512]
    small[me, 11:12, :] = bias[1:2, 0:512]
    small[me, 12:16, :] = jnp.zeros((4, 512), f32)
    small_copies = []
    for n in range(1, 8):
        row = flip(net.r % 2, n % 2) + 2 * flip(net.r // 2, n // 2 % 2)
        peer = (flip(net.k, n // 4), row, net.c)
        small_copies.append(net.remote(small.at[me], small.at[me], peer))
    reload_x = net.local(x, probs.at[1])
    red_proj.prepare([g_qkv.at[:, pl.ds(n * Q, Q)] for n in range(4)])
    red_proj.finish(o_proj)
    hat_fold.step(0)
    red_fc.join([g_fc.at[pl.ds(6 * Q + n * (Q // 2), Q // 2), :] for n in range(2)])
    hat_fold.step(1)
    hat_fold.step(2)
    reload_x.wait()

    def close_out(at, value):
        probs[0, at, :] = probs[1, at, :] + value + bias[5:6, 0:512]

    out_fold.total(close_out)
    keep_block = net.local(probs.at[0], o_block)
    keep_block.wait()
    reload_og = net.local(og, probs.at[0])
    red_qkv.prepare([strips(0, n, 6 * Q) for n in range(4)])
    red_qkv.finish(o_qkv)
    red_dense.join([g_tail.at[pl.ds(n * attn // 2, attn // 2), pl.ds(0, Q)] for n in range(2)])
    red_fc.prepare([strips(4 * Q, n, 8 * Q) for n in range(4)])
    red_dense.prepare([g_tail.at[pl.ds(n * attn, attn), pl.ds(Q, Q)] for n in range(4)])
    for copy in small_copies:
        copy.wait_recv()
    grand = small[0]
    for n in range(1, 8):
        grand = grand + small[n]
    small[8] = grand
    keep_small = net.local(small.at[8], o_small)
    reload_og.wait()

    def close_hat(at, value):
        mu, rstd = stats[at, 0:1], stats[at, 1:2]
        hats = (probs[1, at, :] - mu) * rstd
        mean, cross = stats[at, 2:3] * (1.0 / D), stats[at, 3:4] * (1.0 / D)
        probs[0, at, :] += rstd * (value - mean - hats * cross)

    hat_fold.total(close_hat)
    keep_input = net.local(probs.at[0], o_input)
    red_fc.finish(o_fc)
    red_dense.finish(o_dense)
    for weight in (red_proj, red_qkv, red_fc, red_dense):
        weight.done()
    keep_small.wait()
    keep_input.wait()
    p_line.drain()
    out_fold.drain()
    hat_fold.drain()
    net.drain()


def call_block(*args):
    x, w_qkv, w_dense, w_fc = args[0], args[2], args[3], args[4]
    tok = x.shape[0]
    n_qkv, n_attn, n_fc = w_qkv.shape[1], w_dense.shape[0], w_fc.shape[1]
    heads = n_attn // HD
    wide = 2 * HALF
    any_spec = pl.BlockSpec(memory_space=pl.ANY)
    shape = jax.ShapeDtypeStruct
    pieces = ((n_fc, Q), (Q, n_qkv), (Q, n_fc), (n_attn, Q))
    outs = [
        shape((n_fc, 2 * Q), bf16), shape((2 * Q, n_qkv), bf16),
        shape((2 * Q, n_fc), bf16), shape((n_attn, 2 * Q), bf16),
        shape((tok, 512), f32), shape((tok, 512), f32), shape((16, 512), f32),
        shape((n_fc, wide), bf16), shape((n_fc, HALF), bf16), shape((HALF, n_qkv), bf16),
        shape((HALF, n_fc), bf16), shape((n_attn, HALF), bf16),
    ]
    outs += [shape(piece, bf16) for piece in pieces[:3] for _ in range(2)]
    scratch = [
        VMEM((wide, n_qkv), bf16), VMEM((n_attn, wide), bf16), VMEM((wide, n_fc), bf16),
        VMEM((n_fc, 2 * Q), bf16),
        VMEM((4, tok, 512), bf16), VMEM((4, tok, 512), bf16), VMEM((4, 8, tok), f32),
        VMEM((tok, 128), f32), VMEM((128, tok), f32),
        VMEM((2 * tok, HALF), bf16), VMEM((tok, HALF), bf16),
        VMEM((2 * tok, HALF), bf16), VMEM((tok, HALF), bf16),
        VMEM((2 * tok, HALF), bf16), VMEM((tok, HALF), bf16), VMEM((tok, wide), bf16),
        VMEM((heads, tok, HD), bf16), VMEM((heads, tok, HD), bf16), VMEM((heads, tok, HD), bf16),
        VMEM((heads, tok, tok), f32), VMEM((heads, tok, tok), bf16),
        VMEM((2 * tok, n_attn), bf16), VMEM((tok, n_attn), bf16), VMEM((2 * tok, n_qkv), bf16),
        VMEM((2 * tok, n_fc), bf16), VMEM((tok, n_fc), bf16), VMEM((tok, n_fc), bf16),
        VMEM((2, HALF, 512), bf16),
        VMEM((5, tok, 512), bf16), VMEM((5, tok, 512), bf16),
    ]
    scratch += [VMEM((2,) + ((r // 2, c)), bf16) for r, c in pieces]
    scratch += [VMEM(pieces[3], bf16)] * 2
    scratch += [
        VMEM((2, tok, 128), f32),
        VMEM((8, wide), f32), VMEM((8, n_fc), f32), VMEM((7, 8, tok), f32), VMEM((9, 16, 512), f32),
        VMEM((512,), f32), VMEM((512,), f32), VMEM((512,), f32), VMEM((512,), f32),
        VMEM((n_qkv,), f32), VMEM((n_fc,), f32), VMEM((512,), f32), VMEM((512,), f32),
        pltpu.SemaphoreType.DMA((128,)), pltpu.SemaphoreType.DMA((128,)),
        pltpu.SemaphoreType.DMA((64,)), pltpu.SemaphoreType.DMA((2,)),
    ]
    return pl.pallas_call(
        block_kernel,
        name="block",
        out_shape=outs,
        in_specs=[any_spec] * 15,
        out_specs=[any_spec] * len(outs),
        scratch_shapes=scratch,
        compiler_params=pltpu.CompilerParams(
            collective_id=1, has_side_effects=True, vmem_limit_bytes=67043328
        ),
    )(*args)


def turn_tables(length):
    half_rot = ROT // 2
    frequency = (10000.0 ** (-np.arange(half_rot, dtype=np.float32) * (2.0 / ROT))).astype(np.float32)
    angles = np.arange(length, dtype=np.float32)[:, None] * frequency[None, :]
    tables = np.zeros((2, length, 128), np.float32)
    tables[0] = 1.0
    tables[0, :, :half_rot] = tables[0, :, half_rot:ROT] = np.cos(angles)
    tables[1, :, :half_rot] = -np.sin(angles)
    tables[1, :, half_rot:ROT] = np.sin(angles)
    return tables


def close_kernel(cuts, *refs):
    count = len(cuts)
    refs = list(refs)
    sources, small = [refs.pop(0) for _ in cuts], refs.pop(0)
    outs, vectors = [refs.pop(0) for _ in cuts], [refs.pop(0) for _ in range(8)]
    lows, sums = [refs.pop(0) for _ in cuts], refs.pop(0)
    wides, lines = [refs.pop(0) for _ in range(4)], [refs.pop(0) for _ in range(8)]
    in_sems, out_sems = refs
    loads, stores = [], []
    for n, cut in enumerate(cuts):
        rows = sources[n].shape[0] // cut
        for part in range(cut):
            at = pl.ds(part * rows, rows)
            number = len(loads)
            wide = wides[n] if n < len(wides) else lows[n]
            loads.append(
                pltpu.make_async_copy(sources[n].at[at, :], lows[n].at[at, :], in_sems.at[number])
            )
            stores.append(
                (n, at, pltpu.make_async_copy(wide.at[at, :], outs[n].at[at, :], out_sems.at[number]))
            )
    total = len(loads)
    load_small = pltpu.make_async_copy(small, sums, in_sems.at[total])
    for copy in loads:
        copy.start()
    load_small.start()
    for load, (n, at, store) in zip(loads, stores):
        load.wait()
        if n < len(wides):
            wides[n][at, :] = lows[n][at, :].astype(f32)
        store.start()
    load_small.wait()
    last = []
    for n, (row, line, vector) in enumerate(zip((0, 1, 2, 3, 4, 7, 11, 11), lines, vectors)):
        for part in range(line.shape[0] // 512):
            line[part * 512 : part * 512 + 512] = sums[row + part, :]
        last.append(pltpu.make_async_copy(line, vector, out_sems.at[total + n]))
        last[-1].start()
    for _, _, store in stores:
        store.wait()
    for copy in last:
        copy.wait()


def call_close(proj, qkv, fc, dense, block, grad, small):
    any_spec = pl.BlockSpec(memory_space=pl.ANY)
    shape = jax.ShapeDtypeStruct
    arrays = (fc, proj, qkv, dense, block, grad)
    cuts = (4, 4, 2, 1, 2, 2)
    outs = [shape(a.shape, f32) for a in arrays]
    lengths = [512] * 4 + [qkv.shape[1], fc.shape[1], 512, 512]
    outs += [shape((length,), f32) for length in lengths]
    return pl.pallas_call(
        functools.partial(close_kernel, cuts),
        name="close",
        out_shape=outs,
        in_specs=[any_spec] * 7,
        out_specs=[any_spec] * 14,
        scratch_shapes=[VMEM(a.shape, a.dtype) for a in (*arrays, small)]
        + [VMEM(a.shape, f32) for a in arrays[:4]]
        + [VMEM((length,), f32) for length in lengths]
        + [pltpu.SemaphoreType.DMA((sum(cuts) + 8,)), pltpu.SemaphoreType.DMA((sum(cuts) + 8,))],
        compiler_params=pltpu.CompilerParams(vmem_limit_bytes=60 << 20),
    )(*arrays, small)


def fused_shards(
    block_input, out_grad, ln1_gain, ln1_bias, ln2_gain, ln2_bias,
    w_qkv, b_qkv, w_dense, b_dense, w_fc, b_fc, w_proj, b_proj,
):
    results = call_block(
        block_input, out_grad, w_qkv, w_dense, w_fc, w_proj, turn_tables(SEQ),
        ln1_gain, ln1_bias, ln2_gain, ln2_bias, b_qkv, b_fc, b_dense, b_proj,
    )
    fc, proj, qkv, dense, block, grad, *vectors = call_close(*results[:7])
    gain_1, shift_1, gain_2, shift_2, qkv_bias, fc_bias, dense_bias, proj_bias = vectors
    return (
        block, grad, gain_1, shift_1, gain_2, shift_2, qkv, qkv_bias, dense, dense_bias,
        fc, fc_bias, proj, proj_bias,
    )


def solution(mesh):
    sizes = tuple(mesh.shape[name] for name in ("dp", "row", "col"))
    body = fused_shards if sizes == (2, 4, 4) else shards
    return jax.shard_map(
        body,
        mesh=mesh,
        in_specs=(
            P(("dp", "row"), "col"),
            P(("dp", "row"), "col"),
            P("col"),
            P("col"),
            P("col"),
            P("col"),
            P("row", "col"),
            P("col"),
            P("col", "row"),
            P("col"),
            P("row", "col"),
            P("col"),
            P("col", "row"),
            P("col"),
        ),
        out_specs=(
            P(("dp", "row"), "col"),
            P(("dp", "row"), "col"),
            P("col"),
            P("col"),
            P("col"),
            P("col"),
            P("row", "col"),
            P("col"),
            P("col", "row"),
            P("col"),
            P("row", "col"),
            P("col"),
            P("col", "row"),
            P("col"),
        ),
        check_vma=False,
    )
```

```python
import functools
import math

import jax
import jax.numpy as jnp
import numpy as np
from jax import lax
from jax.experimental import pallas as pl
from jax.experimental.pallas import tpu as pltpu
from jax.sharding import PartitionSpec as P

D = 2048
HD = 256
ROT = 64
SEQ = 512


epsilon = 1e-05
contract_last = (((1,), (1,)), ((), ()))
contract_first = (((0,), (0,)), ((), ()))


def angle_tables(length):
    half_rot = ROT // 2
    position = jnp.arange(length, dtype=jnp.float32)
    exponent = jnp.arange(half_rot, dtype=jnp.float32) * (2.0 / ROT)
    frequency = 10000.0 ** (-exponent)
    angles = position[:, None] * frequency[None, :]
    return (jnp.cos(angles), jnp.sin(angles))


def rotate_fwd(values, cosine, sine_vals):
    half_rot = ROT // 2
    first = values[..., :half_rot]
    second = values[..., half_rot:ROT]
    cos_part = cosine[:, None, :]
    sin_part = sine_vals[:, None, :]
    return jnp.concatenate(
        [
            first * cos_part - second * sin_part,
            second * cos_part + first * sin_part,
            values[..., ROT:],
        ],
        axis=-1,
    )


def rotate_back(grads, cosine, sine_vals):
    half_rot = ROT // 2
    first = grads[..., :half_rot]
    second = grads[..., half_rot:ROT]
    cos_part = cosine[:, None, :]
    sin_part = sine_vals[:, None, :]
    return jnp.concatenate(
        [
            first * cos_part + second * sin_part,
            second * cos_part - first * sin_part,
            grads[..., ROT:],
        ],
        axis=-1,
    )


def gelu_value(pre_act):
    return 0.5 * pre_act * (1.0 + lax.erf(pre_act * 0.7071067811865476))


def gelu_slope(pre_act):
    return 0.5 * (
        1.0 + lax.erf(pre_act * 0.7071067811865476)
    ) + pre_act * 0.3989422804014327 * jnp.exp(-0.5 * pre_act * pre_act)


def shards(
    block_input,
    out_grad,
    ln1_gain,
    ln1_bias,
    ln2_gain,
    ln2_bias,
    w_qkv,
    b_qkv,
    w_dense,
    b_dense,
    w_fc,
    b_fc,
    w_proj,
    b_proj,
):
    tok_rows = block_input.shape[0]
    seq_count = tok_rows // SEQ
    qkv_cols = w_qkv.shape[1]
    fc_cols = w_fc.shape[1]
    local_heads = qkv_cols // (3 * HD)
    head_cols = local_heads * HD
    scale = 1.0 / math.sqrt(HD)
    cosine, sine_vals = angle_tables(SEQ)
    causal = jnp.arange(SEQ)[:, None] >= jnp.arange(SEQ)[None, :]
    row_total, square_total = lax.psum(
        (jnp.sum(block_input, axis=1), jnp.sum(block_input * block_input, axis=1)), "col"
    )
    mean_row = (row_total / D)[:, None]
    var_row = (square_total / D)[:, None] - mean_row * mean_row
    inv_std = lax.rsqrt(var_row + epsilon)
    x_hat = (block_input - mean_row) * inv_std
    normed_one = (x_hat * ln1_gain + ln1_bias).astype(jnp.bfloat16)
    normed_two = (x_hat * ln2_gain + ln2_bias).astype(jnp.bfloat16)
    wide_one, wide_two = (
        lax.all_gather(normed_one, "col", axis=1, tiled=True),
        lax.all_gather(normed_two, "col", axis=1, tiled=True),
    )
    part_one = wide_one
    part_two = wide_two
    qkv_pre = jnp.dot(
        part_one,
        lax.all_gather(w_qkv, "row", axis=0, tiled=True),
        preferred_element_type=jnp.float32,
    )
    fc_pre = jnp.dot(
        part_two,
        lax.all_gather(w_fc, "row", axis=0, tiled=True),
        preferred_element_type=jnp.float32,
    )
    qkv_pre = qkv_pre + b_qkv
    fc_pre = fc_pre + b_fc

    def forward_seq(block):
        query = rotate_fwd(block[:, :, 0], cosine, sine_vals).astype(jnp.bfloat16)
        keys = rotate_fwd(block[:, :, 1], cosine, sine_vals).astype(jnp.bfloat16)
        values = block[:, :, 2].astype(jnp.bfloat16)
        scores = jnp.einsum("qhd,khd->hqk", query, keys, preferred_element_type=jnp.float32) * scale
        masked = jnp.where(causal[None], scores, -1e30)
        row_max = jnp.max(masked, axis=-1, keepdims=True)
        exp_sum = jnp.sum(
            jnp.where(causal[None], jnp.exp(masked - row_max), 0.0), axis=-1, keepdims=True
        )
        log_total = row_max + jnp.log(exp_sum)
        probs_low = jnp.where(causal[None], jnp.exp(masked - log_total), 0.0).astype(jnp.bfloat16)
        attended = jnp.einsum(
            "hqk,khd->qhd", probs_low, values, preferred_element_type=jnp.float32
        ).astype(jnp.bfloat16)
        return (query, keys, values, attended, log_total)

    query, keys, values, attended, log_total = lax.map(
        forward_seq, qkv_pre.reshape(seq_count, SEQ, local_heads, 3, HD)
    )
    attn_out = attended.reshape(tok_rows, head_cols)
    gelu_out = gelu_value(fc_pre).astype(jnp.bfloat16)
    out_stack = jnp.concatenate([w_dense, w_proj], axis=0)
    shard_piece = lax.all_gather(out_stack, "row", axis=1, tiled=True)
    mixed = jnp.dot(
        attn_out, shard_piece[:head_cols], preferred_element_type=jnp.float32
    ) + jnp.dot(gelu_out, shard_piece[head_cols:], preferred_element_type=jnp.float32)
    branch_sum = lax.psum_scatter(mixed, "col", scatter_dimension=1, tiled=True)
    block_output = block_input + branch_sum + b_dense + b_proj
    grad_low = out_grad.astype(jnp.bfloat16)
    wide_grad = lax.all_gather(grad_low, "col", axis=1, tiled=True)
    both_grad = lax.dot_general(
        wide_grad,
        lax.all_gather(out_stack, "row", axis=1, tiled=True),
        contract_last,
        preferred_element_type=jnp.float32,
    )
    attn_grad = both_grad[:, :head_cols]
    gelu_grad = both_grad[:, head_cols:]
    attn_grad_low = attn_grad.astype(jnp.bfloat16)
    fc_grad = gelu_grad * gelu_slope(fc_pre)
    fc_bias_grad = jnp.sum(fc_grad, axis=0)
    fc_grad_low = fc_grad.astype(jnp.bfloat16)

    def backward_seq(items):
        query_s, keys_s, values_s, attended_s, log_s, head_grad = items
        scores = (
            jnp.einsum("qhd,khd->hqk", query_s, keys_s, preferred_element_type=jnp.float32) * scale
        )
        probs = jnp.where(
            causal[None], jnp.exp(jnp.where(causal[None], scores, -1e30) - log_s), 0.0
        )
        probs_low = probs.astype(jnp.bfloat16)
        value_grad = jnp.einsum(
            "hqk,qhd->khd", probs_low, head_grad, preferred_element_type=jnp.float32
        )
        prob_grad = jnp.einsum(
            "qhd,khd->hqk", head_grad, values_s, preferred_element_type=jnp.float32
        )
        delta_row = jnp.transpose(
            jnp.sum(head_grad.astype(jnp.float32) * attended_s.astype(jnp.float32), axis=-1), (1, 0)
        )[:, :, None]
        score_grad = (probs * (prob_grad - delta_row) * scale).astype(jnp.bfloat16)
        query_grad = jnp.einsum(
            "hqk,khd->qhd", score_grad, keys_s, preferred_element_type=jnp.float32
        )
        key_grad = jnp.einsum(
            "hqk,qhd->khd", score_grad, query_s, preferred_element_type=jnp.float32
        )
        return jnp.stack(
            [
                rotate_back(query_grad, cosine, sine_vals),
                rotate_back(key_grad, cosine, sine_vals),
                value_grad,
            ],
            axis=2,
        )

    head_grads = attn_grad_low.reshape(seq_count, SEQ, local_heads, HD)
    qkv_grad = lax.map(
        backward_seq, (query, keys, values, attended, log_total, head_grads)
    ).reshape(tok_rows, qkv_cols)
    qkv_bias_grad = jnp.sum(qkv_grad, axis=0)
    qkv_grad_low = qkv_grad.astype(jnp.bfloat16)
    in_stack = jnp.concatenate([w_qkv, w_fc], axis=1)
    shard_piece = lax.all_gather(in_stack, "row", axis=0, tiled=True)
    norm_grads = jnp.stack(
        [
            lax.dot_general(
                qkv_grad_low,
                shard_piece[:, :qkv_cols],
                contract_last,
                preferred_element_type=jnp.float32,
            ),
            lax.dot_general(
                fc_grad_low,
                shard_piece[:, qkv_cols:],
                contract_last,
                preferred_element_type=jnp.float32,
            ),
        ]
    )
    part_one = wide_one
    part_two = wide_two
    row_part = lax.psum_scatter(
        jnp.concatenate(
            [
                lax.dot_general(
                    part_one, qkv_grad_low, contract_first, preferred_element_type=jnp.float32
                ),
                lax.dot_general(
                    part_two, fc_grad_low, contract_first, preferred_element_type=jnp.float32
                ),
                lax.dot_general(
                    wide_grad, attn_out, contract_first, preferred_element_type=jnp.float32
                ),
                lax.dot_general(
                    wide_grad, gelu_out, contract_first, preferred_element_type=jnp.float32
                ),
            ],
            axis=1,
        ),
        "row",
        scatter_dimension=0,
        tiled=True,
    )
    grad_rows = lax.psum(row_part, "dp")
    qkv_total = grad_rows[:, :qkv_cols]
    fc_total = grad_rows[:, qkv_cols : qkv_cols + fc_cols]
    dense_total = grad_rows[:, qkv_cols + fc_cols : qkv_cols + fc_cols + head_cols].T
    proj_total = grad_rows[:, qkv_cols + fc_cols + head_cols :].T
    norm_local = lax.psum_scatter(norm_grads, "col", scatter_dimension=2, tiled=True)
    grad_one = norm_local[0]
    grad_two = norm_local[1]
    hat_grad = grad_one * ln1_gain + grad_two * ln2_gain
    total_hat, total_cross = lax.psum(
        (jnp.sum(hat_grad, axis=1), jnp.sum(hat_grad * x_hat, axis=1)), "col"
    )
    input_grad = out_grad + inv_std * (
        hat_grad - (total_hat / D)[:, None] - x_hat * (total_cross / D)[:, None]
    )
    gain_one, shift_one, gain_two, shift_two, qkv_bias_total, fc_bias_total, out_bias_total = (
        lax.psum(
            (
                jnp.sum(grad_one * x_hat, axis=0),
                jnp.sum(grad_one, axis=0),
                jnp.sum(grad_two * x_hat, axis=0),
                jnp.sum(grad_two, axis=0),
                qkv_bias_grad,
                fc_bias_grad,
                jnp.sum(out_grad, axis=0),
            ),
            ("dp", "row"),
        )
    )
    return (
        block_output,
        input_grad,
        gain_one,
        shift_one,
        gain_two,
        shift_two,
        qkv_total,
        qkv_bias_total,
        dense_total,
        out_bias_total,
        fc_total,
        fc_bias_total,
        proj_total,
        out_bias_total,
    )


f32 = jnp.float32
bf16 = jnp.bfloat16
MESH = pl.DeviceIdType.MESH
VMEM = pltpu.VMEM
Q = 256
HALF = 4 * Q


def flip(a, b):
    return a + b - 2 * a * b


def span(start, size):
    return pl.ds(pl.multiple_of(start, size), size)


def mm(a, b):
    return jnp.dot(a, b, preferred_element_type=f32)


def mm_nt(a, b):
    return lax.dot_general(a, b, (((1,), (1,)), ((), ())), preferred_element_type=f32)


def mm_tn(a, b):
    return lax.dot_general(a, b, (((0,), (0,)), ((), ())), preferred_element_type=f32)


class Net:
    def __init__(self, send_sems, recv_sems, local_sems):
        self.k = lax.axis_index("dp")
        self.r = lax.axis_index("row")
        self.c = lax.axis_index("col")
        k, r, c = self.k, self.r, self.c
        self.core = (1 - k, r, c)
        self.x = (k, r + 1 - 2 * (r % 2), c)
        self.y = (k, r + 2 - 4 * (r // 2), c)
        near = c + 1 - 2 * (c % 2)
        self.z = (None, (k, r, near), (k, r, c + 2 - 4 * (c // 2)), (k, r, 3 - c))
        self.middle = flip(c % 2, c // 2) == 1
        self.send_sems, self.recv_sems, self.local_sems = send_sems, recv_sems, local_sems
        self.remote_count = 0
        self.local_count = 0
        self.pending = []

    def mix(self, j):
        return flip(j % 2, flip(self.c % 2, self.r % 2)) + 2 * flip(
            j // 2, flip(self.c // 2, self.r // 2)
        )

    def barrier(self):
        sem = pltpu.get_barrier_semaphore()

        def greet(peer):
            pl.semaphore_signal(sem, inc=1, device_id=peer, device_id_type=MESH)

        for peer in (self.x, self.y, self.core, self.z[1]):
            greet(peer)

        @pl.when(self.middle)
        def _():
            greet(self.z[3])
            pl.semaphore_wait(sem, 5)

        @pl.when(jnp.logical_not(self.middle))
        def _():
            pl.semaphore_wait(sem, 4)

    def slot(self):
        self.remote_count += 1
        return self.remote_count - 1

    def remote(self, src, dst, peer):
        slot = self.slot()
        copy = pltpu.make_async_remote_copy(
            src_ref=src,
            dst_ref=dst,
            send_sem=self.send_sems.at[slot],
            recv_sem=self.recv_sems.at[slot],
            device_id=peer,
            device_id_type=MESH,
        )
        copy.start()
        self.pending.append(copy)
        return copy

    def local(self, src, dst):
        copy = pltpu.make_async_copy(src, dst, self.local_sems.at[self.local_count])
        self.local_count += 1
        copy.start()
        return copy

    def sent(self, copy):
        copy.wait_send()
        self.pending = [other for other in self.pending if other is not copy]

    def drain(self):
        for copy in self.pending:
            copy.wait_send()


class Gather:
    def __init__(self, net, shard, full, by_rows):
        self.net, self.shard, self.full, self.by_rows = net, shard, full, by_rows
        self.depth = Q // 2 if by_rows else shard.shape[0] // 2
        self.placed = []

    def own(self, half, part=None):
        if self.by_rows:
            if part is None:
                return self.shard.at[span(half * Q, Q), :]
            return self.shard.at[span(half * Q + part * self.depth, self.depth), :]
        rows = slice(None) if part is None else pl.ds(part * self.depth, self.depth)
        return self.shard.at[rows, span(half * Q, Q)]

    def chunk(self, s, i, part=None):
        start = s * HALF + i * Q
        if self.by_rows:
            if part is None:
                return self.full.at[pl.ds(start, Q), :]
            return self.full.at[pl.ds(start + part * self.depth, self.depth), :]
        rows = slice(None) if part is None else pl.ds(part * self.depth, self.depth)
        return self.full.at[rows, pl.ds(start, Q)]

    def place_own(self):
        net = self.net
        self.placed = [
            net.local(self.own(net.k), self.chunk(0, 0)),
            net.local(self.own(1 - net.k), self.chunk(1, 0)),
        ]

    def send_own(self):
        net, k = self.net, self.net.k
        self.y0 = net.remote(self.own(k, 0), self.chunk(0, 2, 0), net.y)
        self.x1 = net.remote(self.own(k, 1), self.chunk(0, 1, 1), net.x)
        self.y1 = net.remote(self.own(k, 1), self.chunk(0, 2, 1), net.y)
        self.x0 = net.remote(self.own(k, 0), self.chunk(0, 1, 0), net.x)

    def forward(self):
        net = self.net
        self.y0.wait_recv()
        self.d0 = net.remote(self.chunk(0, 2, 0), self.chunk(0, 3, 0), net.x)
        self.x1.wait_recv()
        self.d1 = net.remote(self.chunk(0, 1, 1), self.chunk(0, 3, 1), net.y)

    def swap_near(self):
        net = self.net
        self.x0.wait_recv()
        self.c1 = net.remote(self.chunk(0, 1), self.chunk(1, 1), net.core)
        self.y1.wait_recv()
        self.c2 = net.remote(self.chunk(0, 2), self.chunk(1, 2), net.core)

    def swap_far(self):
        net = self.net
        self.d0.wait_recv()
        self.d1.wait_recv()
        self.c3 = net.remote(self.chunk(0, 3), self.chunk(1, 3), net.core)

    def ready(self):
        for copy in (self.c1, self.c2, self.c3):
            copy.wait_recv()
        for copy in self.placed:
            copy.wait()

    def release(self):
        for copy in (self.d0, self.d1, self.c1, self.c2, self.c3):
            self.net.sent(copy)


class Line:
    def __init__(self, net, slots):
        self.net, self.slots = net, slots
        self.ids = [None] + [net.slot() for _ in range(3)]
        self.sends = []

    def copy(self, src, dst, peer, send):
        net = self.net
        return pltpu.make_async_remote_copy(
            src_ref=self.slots.at[src],
            dst_ref=self.slots.at[dst],
            send_sem=net.send_sems.at[send],
            recv_sem=net.recv_sems.at[self.ids[dst]],
            device_id=peer,
            device_id_type=MESH,
        )

    def start(self):
        net = self.net
        self.first = self.copy(0, 1, net.z[1], self.ids[1])
        self.first.start()
        self.hops = [
            self.copy(0, 3, net.z[3], self.ids[2]),
            self.copy(1, 2, net.z[3], self.ids[3]),
            self.copy(3, 2, net.z[1], net.slot()),
            self.copy(2, 3, net.z[1], net.slot()),
        ]

        @pl.when(net.middle)
        def _():
            self.hops[0].start()

    def arrived(self, slot):
        return self.copy(0, slot, self.net.z[1], self.ids[slot])

    def step(self, number):
        slot = (1, 3, 2)[number]

        @pl.when(self.net.middle)
        def _():
            self.arrived(slot).wait_recv()
            self.hops[number + 1].start()

    def ready(self):
        @pl.when(jnp.logical_not(self.net.middle))
        def _():
            for slot in (1, 2, 3):
                self.arrived(slot).wait_recv()

    def drain(self):
        self.first.wait_send()

        @pl.when(self.net.middle)
        def _():
            for hop in self.hops:
                hop.wait_send()


class Fold:
    def __init__(self, net, blocks, inbox):
        self.net, self.blocks, self.inbox = net, blocks, inbox
        hops = ((3, None, 0), (2, None, 1), (1, None, 2), (None, 0, 3), (None, 1, 4), (None, 3, 0))
        self.copies = []
        for n, (block, slot, dest) in enumerate(hops):
            number = net.slot()
            self.copies.append(
                pltpu.make_async_remote_copy(
                    src_ref=blocks.at[block] if slot is None else inbox.at[slot],
                    dst_ref=inbox.at[dest],
                    send_sem=net.send_sems.at[number],
                    recv_sem=net.recv_sems.at[number],
                    device_id=net.z[3] if n in (3, 4) else net.z[1],
                    device_id_type=MESH,
                )
            )

    def start(self, first, last):
        @pl.when(jnp.logical_not(self.net.middle))
        def _():
            for copy in self.copies[first:last]:
                copy.start()

    def step(self, number):
        slot, block = ((0, 2), (1, 3), (3, 1))[number]
        inbox, blocks = self.inbox, self.blocks

        @pl.when(self.net.middle)
        def _():
            self.copies[(0, 1, 3)[number]].wait_recv()

            def add(n, _):
                at = span(n * 64, 64)
                total = inbox[slot, at, :].astype(f32) + blocks[block, at, :].astype(f32)
                inbox[slot, at, :] = total.astype(bf16)
                return 0

            lax.fori_loop(0, inbox.shape[1] // 64, add, 0)
            self.copies[3 + number].start()

    def total(self, use):
        def gather(*slots):
            def add(n, _):
                at = span(n * 64, 64)
                value = self.blocks[0, at, :].astype(f32)
                for slot in slots:
                    value = value + self.inbox[slot, at, :].astype(f32)
                use(at, value)
                return 0

            lax.fori_loop(0, self.inbox.shape[1] // 64, add, 0)

        @pl.when(self.net.middle)
        def _():
            self.copies[2].wait_recv()
            self.copies[4].wait_recv()
            gather(2, 4)

        @pl.when(jnp.logical_not(self.net.middle))
        def _():
            self.copies[5].wait_recv()
            gather(0)

    def drain(self):
        @pl.when(self.net.middle)
        def _():
            for copy in self.copies[3:]:
                copy.wait_send()

        @pl.when(jnp.logical_not(self.net.middle))
        def _():
            for copy in self.copies[:3]:
                copy.wait_send()


def turn(low, tables, sign):
    lane = lax.broadcasted_iota(jnp.int32, low.shape, 1)
    swung = jnp.where(lane < ROT // 2, pltpu.roll(low, 96, 1), pltpu.roll(low, 32, 1))
    return low * tables[0] + sign * (tables[1] * swung)


class Tiles:
    def __init__(self, slots, sems):
        self.slots, self.sems = slots, sems

    def write(self, count, product, place, depth):
        def body(n, _):
            slot = n % 2
            source = self.slots.at[slot, pl.ds(0, depth), :]
            copy = pltpu.make_async_copy(source, place(n), self.sems.at[slot])

            @pl.when(n >= 2)
            def _():
                copy.wait()

            self.slots[slot, 0:depth, :] = product(n).astype(bf16)
            copy.start()
            return 0

        lax.fori_loop(0, count, body, 0)
        for slot in range(2):
            source = self.slots.at[slot, pl.ds(0, depth), :]
            pltpu.make_async_copy(source, place(slot), self.sems.at[slot]).wait()


class Reduce:
    def __init__(self, net, partial, joined, near, far, by_rows, in_vmem=False):
        self.in_vmem = in_vmem
        self.net, self.partial, self.by_rows = net, partial, by_rows
        self.joined, self.near, self.far = joined, near, far
        self.depth = Q // 2 if by_rows else partial.shape[0] // 2

    def chunk(self, i, half):
        if self.by_rows:
            return self.partial.at[pl.ds(i * Q + half * self.depth, self.depth), :]
        return self.partial.at[pl.ds(half * self.depth, self.depth), pl.ds(i * Q, Q)]

    def whole(self):
        if self.by_rows:
            return self.partial.at[pl.ds(0, Q), :]
        return self.partial.at[:, pl.ds(0, Q)]

    def rows(self, half):
        return pl.ds(half * self.depth, self.depth)

    def start(self):
        net = self.net
        self.a = net.remote(self.chunk(3, 0), self.joined.at[0], net.x)
        self.b = net.remote(self.chunk(3, 1), self.joined.at[1], net.y)
        self.near_a = net.remote(self.chunk(1, 0), self.near.at[self.rows(0), :], net.x)
        self.near_b = net.remote(self.chunk(2, 1), self.near.at[self.rows(1), :], net.y)

    def join(self, parts):
        net = self.net
        loads = [net.local(self.chunk(2, 0), parts[0]), net.local(self.chunk(1, 1), parts[1])]
        hops = []
        for half, copy, peer in ((0, self.a, net.y), (1, self.b, net.x)):
            loads[half].wait()
            copy.wait_recv()
            tile = 64

            def add(n, _, half=half):
                at = span(n * tile, tile)
                total = self.joined[half, at, :].astype(f32) + parts[half][at, :].astype(f32)
                self.joined[half, at, :] = total.astype(bf16)
                return 0

            lax.fori_loop(0, self.depth // tile, add, 0)
            hops.append(net.remote(self.joined.at[half], self.far.at[self.rows(half), :], peer))
        self.far_a, self.far_b = hops

    def prepare(self, buffers):
        net = self.net
        self.buffers = list(buffers)
        self.loads = [net.local(self.whole(), buffers[0])]
        for copy in (self.near_a, self.near_b):
            copy.wait_recv()
        if self.in_vmem:
            self.buffers[1:3] = [self.near, self.far]
        else:
            self.loads.append(net.local(self.near, buffers[1]))

    def finish(self, out):
        net, buffers = self.net, self.buffers
        last = []
        for half, copy in enumerate((self.far_a, self.far_b)):
            copy.wait_recv()
            if not self.in_vmem:
                rows = self.rows(half)
                last.append(net.local(self.far.at[rows, :], buffers[2].at[rows, :]))
        for copy in self.loads:
            copy.wait()
        tile = 64
        self.here, self.there = [], []
        for half in range(2):
            if last:
                last[half].wait()

            def add(n, _, half=half):
                at = span(half * self.depth + n * tile, tile)
                parts = [buffer[at, :].astype(f32) for buffer in buffers[:3]]
                buffers[3][at, :] = (parts[0] + parts[1] + parts[2]).astype(bf16)
                return 0

            lax.fori_loop(0, self.depth // tile, add, 0)
            source = buffers[3].at[self.rows(half), :]
            if self.by_rows:
                place = out.at[span(net.k * Q + half * self.depth, self.depth), :]
            else:
                place = out.at[self.rows(half), span(net.k * Q, Q)]
            self.here.append(net.local(source, place))
            self.there.append(net.remote(source, place, net.core))

    def done(self):
        for copy in self.here:
            copy.wait()
        for copy in self.there:
            copy.wait_recv()


def block_kernel(
    x, og, w_qkv, w_dense, w_fc, w_proj, t_turn,
    i_gain_1, i_bias_1, i_gain_2, i_bias_2, i_b_qkv, i_b_fc, i_b_dense, i_b_proj,
    o_proj, o_qkv, o_fc, o_dense, o_block, o_input, o_small,
    all_proj, r_proj, r_qkv, r_fc, r_dense, n_proj, f_proj, n_qkv, f_qkv, n_fc, f_fc,
    g_qkv, g_dense, g_fc, g_tail, xs, ys, pks, stats, rows, h1c, h1s, h2c, h2s, dyc, dys, xh,
    qb, kb, vb, probs, probs_low, oc, dob, dqc, gc, slope, dabt, stage,
    out_recv, hat_recv, j_proj, j_qkv, j_fc, j_dense, n_dense, f_dense, tables, vecs, bias, packs, small,
    gain_1, bias_1, gain_2, bias_2, b_qkv, b_fc, b_dense, b_proj,
    send_sems, recv_sems, local_sems, stage_sems,
):
    tok = x.shape[0]
    heads = qb.shape[0]
    width = gc.shape[1]
    scale = 1.0 / math.sqrt(HD)
    net = Net(send_sems, recv_sems, local_sems)
    net.barrier()
    qkv = Gather(net, w_qkv, g_qkv, True)
    dense = Gather(net, w_dense, g_dense, False)
    fc = Gather(net, w_fc, g_fc, True)
    proj = Gather(net, w_proj, all_proj, False)
    qkv.send_own()
    dense.send_own()
    load_x = net.local(x, probs.at[0])
    vectors = [
        net.local(i_gain_1, gain_1), net.local(i_bias_1, bias_1), net.local(i_gain_2, gain_2),
        net.local(i_bias_2, bias_2), net.local(i_b_qkv, b_qkv), net.local(i_b_fc, b_fc),
        net.local(i_b_dense, b_dense), net.local(i_b_proj, b_proj),
    ]
    load_og = net.local(og, probs.at[1])
    load_turn = net.local(t_turn, tables)
    tiles = Tiles(stage, stage_sems)
    mine = pl.ds(0, tok)
    theirs = pl.ds(tok, tok)

    step = 128
    lane = lax.broadcasted_iota(jnp.int32, (step, 128), 1)
    load_x.wait()

    def local_norm(n, _):
        at = span(n * step, step)
        block = probs[0, at, :]
        mean = jnp.mean(block, axis=1, keepdims=True)
        centred = block - mean
        var = jnp.mean(centred * centred, axis=1, keepdims=True)
        stats[at, :] = jnp.where(lane == 0, mean, jnp.where(lane == 1, var, 0.0))
        return 0

    lax.fori_loop(0, tok // step, local_norm, 0)
    pks[0] = stats[...].T[0:8]
    for copy in vectors:
        copy.wait()
    for n, vector in enumerate((gain_1, bias_1, gain_2, bias_2)):
        pks[0, 2 + n : 3 + n, :] = vector[...].reshape(1, 512)
    p_line = Line(net, pks)
    p_line.start()
    for weight in (qkv, dense, fc):
        weight.place_own()
    bias[...] = jnp.zeros_like(bias)
    bias[3:4, 0 : b_qkv.shape[0]] = b_qkv[...].reshape(1, b_qkv.shape[0])
    bias[4:5, :] = b_fc[...].reshape(1, width)
    bias[5:6, 0:512] = (b_dense[...] + b_proj[...]).reshape(1, 512)
    rows[...] = jnp.zeros_like(rows)
    load_og.wait()

    def local_grad(n, _):
        at = span(n * step, step)
        block = probs[1, at, :]
        ys[0, at, :] = block.astype(bf16)
        bias[1:2, 0:512] += jnp.sum(block, axis=0, keepdims=True)
        return 0

    lax.fori_loop(0, tok // step, local_grad, 0)
    for hop in range(3):
        p_line.step(hop)
    p_line.ready()
    means = [pks[j, 0:1, :] for j in range(4)]
    mu = (means[0] + means[1] + means[2] + means[3]) * 0.25
    spread = [pks[j, 1:2, :] + (means[j] - mu) * (means[j] - mu) for j in range(4)]
    rows[0:1, :] = mu
    rows[1:2, :] = lax.rsqrt((spread[0] + spread[1] + spread[2] + spread[3]) * 0.25 + epsilon)
    stats[...] = rows[...].T

    def own_norm(n, _):
        at = span(n * step, step)
        hats = (probs[0, at, :] - stats[at, 0:1]) * stats[at, 1:2]
        xs[0, at, :] = (hats * pks[0, 2:3, :] + pks[0, 3:4, :]).astype(bf16)
        return 0

    lax.fori_loop(0, tok // step, own_norm, 0)
    x_line = Line(net, xs)
    y_line = Line(net, ys)
    x_line.start()
    qkv.forward()
    x_line.step(0)
    x_line.step(1)
    fc.send_own()
    dense.forward()
    qkv.swap_near()
    x_line.step(2)
    y_line.start()
    dense.swap_near()
    qkv.swap_far()
    x_line.ready()
    fc.forward()
    proj.send_own()

    for s in range(2):
        for j in range(4):
            lanes = span(flip(s, net.k) * Q, Q)
            dest = span(net.mix(j) * Q, Q)
            wide = span(s * HALF + net.mix(j) * Q, Q)
            vecs[0:4, wide] = pks[j, 2:6, lanes]

            def norm(n, _, s=s, j=j, lanes=lanes, dest=dest, wide=wide):
                at = span(n * step, step)
                one = xs[j, at, lanes]
                hats = (one.astype(f32) - pks[j, 3:4, lanes]) * (1.0 / pks[j, 2:3, lanes])
                xh[at, wide] = hats.astype(bf16)
                (h1s if s else h1c)[at, dest] = one
                two = hats * pks[j, 4:5, lanes] + pks[j, 5:6, lanes]
                (h2s if s else h2c)[at, dest] = two.astype(bf16)
                return 0

            lax.fori_loop(0, tok // step, norm, 0)
    swap_h1 = net.remote(h1s, h1c.at[theirs, :], net.core)
    swap_h2 = net.remote(h2s, h2c.at[theirs, :], net.core)
    y_line.step(0)
    load_turn.wait()
    qkv.ready()

    def project(n, _):
        cols = span(n * 3 * HD, 3 * HD)
        acc = mm(h1c[mine, :], g_qkv[0:HALF, cols]) + mm(h1s[...], g_qkv[HALF:, cols])
        acc = acc + bias[3:4, cols]
        qb[n, :, 0:128] = turn(acc[:, 0:128], tables, 1.0).astype(bf16)
        qb[n, :, 128:HD] = acc[:, 128:HD].astype(bf16)
        kb[n, :, 0:128] = turn(acc[:, HD : HD + 128], tables, 1.0).astype(bf16)
        kb[n, :, 128:HD] = acc[:, HD + 128 : 2 * HD].astype(bf16)
        vb[n] = acc[:, 2 * HD :].astype(bf16)
        return 0

    lax.fori_loop(0, heads, project, 0)
    y_line.step(1)
    chunks = tok // step

    def attend(n, _):
        head, chunk = n // chunks, n % chunks
        at = span(chunk * step, step)
        scores = mm_nt(qb[head, at, :], kb[head]) * scale
        token = lax.broadcasted_iota(jnp.int32, (step, tok), 0) + chunk * step
        allowed = token >= lax.broadcasted_iota(jnp.int32, (step, tok), 1)
        scores = jnp.where(allowed, scores, -1e30)
        top = jnp.max(scores, axis=1, keepdims=True)
        raised = jnp.where(allowed, jnp.exp(scores - top), 0.0)
        weight = raised / jnp.sum(raised, axis=1, keepdims=True)
        probs[head, at, :] = weight
        low = weight.astype(bf16)
        probs_low[head, at, :] = low
        oc[at, span(head * HD, HD)] = mm(low, vb[head]).astype(bf16)
        return 0

    lax.fori_loop(0, heads * chunks, attend, 0)
    swap_o = net.remote(oc.at[mine, :], oc.at[theirs, :], net.core)
    dense.swap_far()
    fc.swap_near()
    y_line.step(2)
    fc.swap_far()
    fc.ready()

    def expand(n, _):
        cols = span(n * 512, 512)
        a = mm(h2c[mine, :], g_fc[0:HALF, cols]) + mm(h2s[...], g_fc[HALF:, cols])
        a = a + bias[4:5, cols]
        rise = 0.5 * (1.0 + lax.erf(a * 0.7071067811865476))
        gc[mine, cols] = (a * rise).astype(bf16)
        slope[:, cols] = (rise + a * 0.3989422804014327 * jnp.exp(-0.5 * a * a)).astype(bf16)
        return 0

    lax.fori_loop(0, width // 1024, expand, 0)
    proj.forward()
    lax.fori_loop(width // 1024, width // 512, expand, 0)
    swap_g = net.remote(gc.at[mine, :], gc.at[theirs, :], net.core)
    y_line.ready()
    for s in range(2):
        for j in range(4):
            lanes = span(flip(s, net.k) * Q, Q)
            dest = span(net.mix(j) * Q, Q)
            (dys if s else dyc)[mine, dest] = ys[j, :, lanes]
    swap_dy = net.remote(dys, dyc.at[theirs, :], net.core)
    dense.ready()
    dob[...] = (
        mm_nt(dyc[mine, :], g_dense[:, 0:HALF]) + mm_nt(dys[...], g_dense[:, HALF:])
    ).astype(bf16)

    red_proj = Reduce(net, r_proj, j_proj, n_proj, f_proj, False)
    red_qkv = Reduce(net, r_qkv, j_qkv, n_qkv, f_qkv, True)
    red_fc = Reduce(net, r_fc, j_fc, n_fc, f_fc, True)
    red_dense = Reduce(net, r_dense, j_dense, n_dense, f_dense, False, True)
    swap_g.wait_recv()
    swap_dy.wait_recv()
    tall = width // 2
    tiles.write(
        4,
        lambda n: mm_tn(gc[:, span(n // 2 * tall, tall)], dyc[:, span(n % 2 * 512, 512)]),
        lambda n: r_proj.at[span(n // 2 * tall, tall), span(n % 2 * 512, 512)],
        tall,
    )
    proj.swap_near()
    red_proj.start()

    def keep(head, part, at, value, rotated):
        base = head * 3 * HD + part * HD
        if rotated:
            low = turn(value[:, 0:128], [tables[t, at, :] for t in range(2)], -1.0)
            dqc[at, pl.ds(pl.multiple_of(base, 128), 128)] = low.astype(bf16)
            bias[0:1, pl.ds(pl.multiple_of(base, 128), 128)] += jnp.sum(low, axis=0, keepdims=True)
            value, base, size = value[:, 128:], base + 128, 128
        else:
            size = HD
        cols = pl.ds(pl.multiple_of(base, 128), size)
        dqc[at, cols] = value.astype(bf16)
        bias[0:1, cols] += jnp.sum(value, axis=0, keepdims=True)

    def attend_back(head, _):
        cols = span(head * HD, HD)

        def chunk_back(n, _):
            at = span(n * step, step)
            grad = dob[at, cols]
            delta = jnp.sum(grad.astype(f32) * oc[at, cols].astype(f32), axis=1, keepdims=True)
            spread = mm_nt(grad, vb[head]) - delta
            low = (probs[head, at, :] * spread * scale).astype(bf16)
            probs_low[head, at, :] = low
            keep(head, 0, at, mm(low, kb[head]), True)
            return 0

        keep(head, 2, mine, mm_tn(probs_low[head], dob[:, cols]), False)
        lax.fori_loop(0, chunks, chunk_back, 0)
        keep(head, 1, mine, mm_tn(probs_low[head], qb[head]), True)
        return 0

    lax.fori_loop(0, heads, attend_back, 0)
    proj.swap_far()
    swap_dq = net.remote(dqc.at[mine, :], dqc.at[theirs, :], net.core)
    net.sent(swap_h1)
    net.sent(swap_h2)
    for s in range(2):

        def back_first(n, _, s=s):
            wide = span(s * HALF + n * 512, 512)
            grad = mm_nt(dqc[mine, :], g_qkv[wide, :])
            (h2s if s else h1s)[:, span(n * 512, 512)] = (grad * vecs[0:1, wide]).astype(bf16)
            vecs[4:5, wide] = jnp.sum(grad * xh[:, wide].astype(f32), axis=0, keepdims=True)
            vecs[5:6, wide] = jnp.sum(grad, axis=0, keepdims=True)
            return 0

        lax.fori_loop(0, HALF // 512, back_first, 0)

    proj.ready()
    qkv.release()
    loads = [
        net.local(w_proj.at[:, span(net.k * Q, Q)], g_qkv.at[:, pl.ds(0, Q)]),
        net.local(w_proj.at[:, span((1 - net.k) * Q, Q)], g_qkv.at[:, pl.ds(HALF, Q)]),
        net.local(all_proj.at[:, pl.ds(Q, 3 * Q)], g_qkv.at[:, pl.ds(Q, 3 * Q)]),
        net.local(all_proj.at[:, pl.ds(5 * Q, Q)], g_qkv.at[:, pl.ds(5 * Q, Q)]),
        net.local(all_proj.at[:, pl.ds(6 * Q, 2 * Q)], g_tail),
    ]
    swap_o.wait_recv()
    attn = oc.shape[1]
    tiles.write(
        2,
        lambda n: mm_tn(oc[...], dyc[:, span(n * 512, 512)]),
        lambda n: r_dense.at[:, span(n * 512, 512)],
        attn,
    )
    swap_h1.wait_recv()
    swap_dq.wait_recv()
    tiles.write(
        dqc.shape[1] // 512,
        lambda n: mm_tn(h1c[...], dqc[:, span(n * 512, 512)]),
        lambda n: r_qkv.at[:, span(n * 512, 512)],
        HALF,
    )
    red_qkv.start()
    red_dense.start()

    for copy in loads:
        copy.wait()
    x_line.drain()
    y_line.drain()

    def put_out(p, product):
        s, i = p // 4, p % 4
        out = product + mm(oc[mine, :], g_dense[:, span(p * Q, Q)])
        xs[net.mix(i), :, span(flip(s, net.k) * Q, Q)] = out.astype(bf16)

    def project_head(p, _):
        put_out(p, mm(gc[mine, :], g_qkv[:, span(p * Q, Q)]))
        return 0

    def project_tail(p, _):
        put_out(6 + p, mm(gc[mine, :], g_tail[:, span(p * Q, Q)]))
        return 0

    lax.fori_loop(0, 6, project_head, 0)
    lax.fori_loop(0, 2, project_tail, 0)
    out_fold = Fold(net, xs, out_recv)
    out_fold.start(0, 2)

    def back_fc(n, _):
        cols = span(n * 512, 512)
        grad = mm_nt(dyc[mine, :], g_qkv[cols, 0:HALF])
        grad = grad + mm_nt(dys[:, 0:512], g_qkv[cols, HALF : 6 * Q])
        grad = grad + mm_nt(dys[:, 512:], g_tail[cols, :])
        grad = grad * slope[:, cols].astype(f32)
        bias[2:3, cols] = jnp.sum(grad, axis=0, keepdims=True)
        slope[:, cols] = grad.astype(bf16)
        return 0

    lax.fori_loop(0, width // 512, back_fc, 0)
    dab = slope
    swap_da = net.remote(dab, dabt, net.core)
    red_proj.join([g_tail.at[pl.ds(0, tall), pl.ds(0, Q)], g_tail.at[pl.ds(tall, tall), pl.ds(0, Q)]])
    stats[...] = jnp.zeros_like(stats)
    lane = lax.broadcasted_iota(jnp.int32, (tok, 128), 1)

    def back_norm(j, _):
        for s in range(2):
            lanes = span(flip(s, net.k) * Q, Q)
            dest = span(net.mix(j) * Q, Q)
            wide = span(s * HALF + net.mix(j) * Q, Q)
            grad = mm_nt(dab[...], g_fc[wide, :])
            hats = xh[:, wide].astype(f32)
            packs[j, 2:4, lanes] = vecs[4:6, wide]
            packs[j, 4:5, lanes] = jnp.sum(grad * hats, axis=0, keepdims=True)
            packs[j, 5:6, lanes] = jnp.sum(grad, axis=0, keepdims=True)
            joint = (h2s if s else h1s)[:, dest].astype(f32) + grad * vecs[2:3, wide]
            ys[j, :, lanes] = joint.astype(bf16)
            one = jnp.sum(joint, axis=1, keepdims=True)
            two = jnp.sum(joint * hats, axis=1, keepdims=True)
            stats[...] += jnp.where(lane == 0, one, jnp.where(lane == 1, two, 0.0))
        return 0

    lax.fori_loop(0, 4, back_norm, 0)

    fc.release()
    red_qkv.join(
        [g_fc.at[pl.ds(7 * Q + n * (Q // 2), Q // 2), pl.ds(0, 6 * Q)] for n in range(2)]
    )
    turned = stats[...].T
    for j in range(4):
        packs[j, 0:2, :] = turned[0:2]
        packs[j, 6:8, :] = jnp.zeros((2, tok), f32)
    pack_copies = [net.remote(packs.at[j], packs.at[3 + j], net.z[j]) for j in (1, 2, 3)]
    hat_fold = Fold(net, ys, hat_recv)
    hat_fold.start(0, 2)
    out_fold.start(2, 3)
    hat_fold.start(2, 3)
    out_fold.step(0)
    swap_h2.wait_recv()
    swap_da.wait_recv()

    def grad_fc(n):
        cols = span(n * 512, 512)
        return mm_tn(h2c[mine, :], dab[:, cols]) + mm_tn(h2c[theirs, :], dabt[:, cols])

    tiles.write(width // 512, grad_fc, lambda n: r_fc.at[:, span(n * 512, 512)], HALF)
    red_fc.start()
    out_fold.step(1)

    def strips(base, n, columns):
        return g_fc.at[pl.ds(base + n * Q, Q), pl.ds(0, columns)]

    out_fold.step(2)
    for copy in pack_copies:
        copy.wait_recv()
    total = packs[0] + packs[4] + packs[5] + packs[6]
    rows[2:4, :] = total[0:2, :]
    stats[...] = rows[...].T
    small[0, 0:4, :] = total[2:6, :]
    for n in range(3):
        small[0, 4 + n : 5 + n, :] = bias[0:1, n * 512 : n * 512 + 512]
    for n in range(4):
        small[0, 7 + n : 8 + n, :] = bias[2:3, n * 512 : n * 512 + 512]
    small[0, 11:12, :] = bias[1:2, 0:512]
    small[0, 12:16, :] = jnp.zeros((4, 512), f32)
    net.remote(small.at[0], small.at[1], net.core).wait_recv()
    own_rows = span(net.k * 8, 8)
    small[2 + net.r, 0:8, :] = small[0, own_rows, :] + small[1, own_rows, :]
    place = small.at[2 + net.r, pl.ds(0, 8), :]
    across = (net.k, 3 - net.r, net.c)
    small_copies = [net.remote(place, place, peer) for peer in (net.x, net.y, across)]
    reload_x = net.local(x, probs.at[1])
    red_proj.prepare([g_qkv.at[:, pl.ds(n * Q, Q)] for n in range(4)])
    red_proj.finish(o_proj)
    hat_fold.step(0)
    red_fc.join([g_fc.at[pl.ds(6 * Q + n * (Q // 2), Q // 2), :] for n in range(2)])
    hat_fold.step(1)
    hat_fold.step(2)
    reload_x.wait()

    def close_out(at, value):
        probs[0, at, :] = probs[1, at, :] + value + bias[5:6, 0:512]

    out_fold.total(close_out)
    keep_block = net.local(probs.at[0], o_block)
    keep_block.wait()
    reload_og = net.local(og, probs.at[0])
    red_qkv.prepare([strips(0, n, 6 * Q) for n in range(4)])
    red_qkv.finish(o_qkv)
    red_dense.join([g_tail.at[pl.ds(n * attn // 2, attn // 2), pl.ds(0, Q)] for n in range(2)])
    red_fc.prepare([strips(4 * Q, n, 8 * Q) for n in range(4)])
    red_dense.prepare([g_tail.at[pl.ds(n * attn, attn), pl.ds(Q, Q)] for n in range(4)])
    for copy in small_copies:
        copy.wait_recv()
    small[6, own_rows, :] = small[2, 0:8] + small[3, 0:8] + small[4, 0:8] + small[5, 0:8]
    place = small.at[6, own_rows, :]
    swap_small = net.remote(place, place, net.core)
    reload_og.wait()

    def close_hat(at, value):
        mu, rstd = stats[at, 0:1], stats[at, 1:2]
        hats = (probs[1, at, :] - mu) * rstd
        mean, cross = stats[at, 2:3] * (1.0 / D), stats[at, 3:4] * (1.0 / D)
        probs[0, at, :] += rstd * (value - mean - hats * cross)

    hat_fold.total(close_hat)
    keep_input = net.local(probs.at[0], o_input)
    swap_small.wait_recv()
    keep_small = net.local(small.at[6], o_small)
    red_fc.finish(o_fc)
    red_dense.finish(o_dense)
    for weight in (red_proj, red_qkv, red_fc, red_dense):
        weight.done()
    keep_small.wait()
    keep_input.wait()
    p_line.drain()
    out_fold.drain()
    hat_fold.drain()
    net.drain()


def call_block(*args):
    x, w_qkv, w_dense, w_fc = args[0], args[2], args[3], args[4]
    tok = x.shape[0]
    n_qkv, n_attn, n_fc = w_qkv.shape[1], w_dense.shape[0], w_fc.shape[1]
    heads = n_attn // HD
    wide = 2 * HALF
    any_spec = pl.BlockSpec(memory_space=pl.ANY)
    shape = jax.ShapeDtypeStruct
    pieces = ((n_fc, Q), (Q, n_qkv), (Q, n_fc), (n_attn, Q))
    outs = [
        shape((n_fc, 2 * Q), bf16), shape((2 * Q, n_qkv), bf16),
        shape((2 * Q, n_fc), bf16), shape((n_attn, 2 * Q), bf16),
        shape((tok, 512), f32), shape((tok, 512), f32), shape((16, 512), f32),
        shape((n_fc, wide), bf16), shape((n_fc, HALF), bf16), shape((HALF, n_qkv), bf16),
        shape((HALF, n_fc), bf16), shape((n_attn, HALF), bf16),
    ]
    outs += [shape(piece, bf16) for piece in pieces[:3] for _ in range(2)]
    scratch = [
        VMEM((wide, n_qkv), bf16), VMEM((n_attn, wide), bf16), VMEM((wide, n_fc), bf16),
        VMEM((n_fc, 2 * Q), bf16),
        VMEM((4, tok, 512), bf16), VMEM((4, tok, 512), bf16), VMEM((4, 8, tok), f32),
        VMEM((tok, 128), f32), VMEM((128, tok), f32),
        VMEM((2 * tok, HALF), bf16), VMEM((tok, HALF), bf16),
        VMEM((2 * tok, HALF), bf16), VMEM((tok, HALF), bf16),
        VMEM((2 * tok, HALF), bf16), VMEM((tok, HALF), bf16), VMEM((tok, wide), bf16),
        VMEM((heads, tok, HD), bf16), VMEM((heads, tok, HD), bf16), VMEM((heads, tok, HD), bf16),
        VMEM((heads, tok, tok), f32), VMEM((heads, tok, tok), bf16),
        VMEM((2 * tok, n_attn), bf16), VMEM((tok, n_attn), bf16), VMEM((2 * tok, n_qkv), bf16),
        VMEM((2 * tok, n_fc), bf16), VMEM((tok, n_fc), bf16), VMEM((tok, n_fc), bf16),
        VMEM((2, HALF, 512), bf16),
        VMEM((5, tok, 512), bf16), VMEM((5, tok, 512), bf16),
    ]
    scratch += [VMEM((2,) + ((r // 2, c)), bf16) for r, c in pieces]
    scratch += [VMEM(pieces[3], bf16)] * 2
    scratch += [
        VMEM((2, tok, 128), f32),
        VMEM((8, wide), f32), VMEM((8, n_fc), f32), VMEM((7, 8, tok), f32), VMEM((7, 16, 512), f32),
        VMEM((512,), f32), VMEM((512,), f32), VMEM((512,), f32), VMEM((512,), f32),
        VMEM((n_qkv,), f32), VMEM((n_fc,), f32), VMEM((512,), f32), VMEM((512,), f32),
        pltpu.SemaphoreType.DMA((128,)), pltpu.SemaphoreType.DMA((128,)),
        pltpu.SemaphoreType.DMA((64,)), pltpu.SemaphoreType.DMA((2,)),
    ]
    return pl.pallas_call(
        block_kernel,
        name="block",
        out_shape=outs,
        in_specs=[any_spec] * 15,
        out_specs=[any_spec] * len(outs),
        scratch_shapes=scratch,
        compiler_params=pltpu.CompilerParams(
            collective_id=1, has_side_effects=True, vmem_limit_bytes=67043328
        ),
    )(*args)


def turn_tables(length):
    half_rot = ROT // 2
    frequency = (10000.0 ** (-np.arange(half_rot, dtype=np.float32) * (2.0 / ROT))).astype(np.float32)
    angles = np.arange(length, dtype=np.float32)[:, None] * frequency[None, :]
    tables = np.zeros((2, length, 128), np.float32)
    tables[0] = 1.0
    tables[0, :, :half_rot] = tables[0, :, half_rot:ROT] = np.cos(angles)
    tables[1, :, :half_rot] = -np.sin(angles)
    tables[1, :, half_rot:ROT] = np.sin(angles)
    return tables


def close_kernel(cuts, *refs):
    count = len(cuts)
    refs = list(refs)
    sources, small = [refs.pop(0) for _ in cuts], refs.pop(0)
    outs, vectors = [refs.pop(0) for _ in cuts], [refs.pop(0) for _ in range(8)]
    lows, sums = [refs.pop(0) for _ in cuts], refs.pop(0)
    wides, lines = [refs.pop(0) for _ in range(4)], [refs.pop(0) for _ in range(8)]
    in_sems, out_sems = refs
    loads, stores = [], []
    for n, cut in enumerate(cuts):
        rows = sources[n].shape[0] // cut
        for part in range(cut):
            at = pl.ds(part * rows, rows)
            number = len(loads)
            wide = wides[n] if n < len(wides) else lows[n]
            loads.append(
                pltpu.make_async_copy(sources[n].at[at, :], lows[n].at[at, :], in_sems.at[number])
            )
            stores.append(
                (n, at, pltpu.make_async_copy(wide.at[at, :], outs[n].at[at, :], out_sems.at[number]))
            )
    total = len(loads)
    load_small = pltpu.make_async_copy(small, sums, in_sems.at[total])
    for copy in loads:
        copy.start()
    load_small.start()
    for load, (n, at, store) in zip(loads, stores):
        load.wait()
        if n < len(wides):
            wides[n][at, :] = lows[n][at, :].astype(f32)
        store.start()
    load_small.wait()
    last = []
    for n, (row, line, vector) in enumerate(zip((0, 1, 2, 3, 4, 7, 11, 11), lines, vectors)):
        for part in range(line.shape[0] // 512):
            line[part * 512 : part * 512 + 512] = sums[row + part, :]
        last.append(pltpu.make_async_copy(line, vector, out_sems.at[total + n]))
        last[-1].start()
    for _, _, store in stores:
        store.wait()
    for copy in last:
        copy.wait()


def call_close(proj, qkv, fc, dense, block, grad, small):
    any_spec = pl.BlockSpec(memory_space=pl.ANY)
    shape = jax.ShapeDtypeStruct
    arrays = (fc, proj, qkv, dense, block, grad)
    cuts = (4, 4, 2, 1, 2, 2)
    outs = [shape(a.shape, f32) for a in arrays]
    lengths = [512] * 4 + [qkv.shape[1], fc.shape[1], 512, 512]
    outs += [shape((length,), f32) for length in lengths]
    return pl.pallas_call(
        functools.partial(close_kernel, cuts),
        name="close",
        out_shape=outs,
        in_specs=[any_spec] * 7,
        out_specs=[any_spec] * 14,
        scratch_shapes=[VMEM(a.shape, a.dtype) for a in (*arrays, small)]
        + [VMEM(a.shape, f32) for a in arrays[:4]]
        + [VMEM((length,), f32) for length in lengths]
        + [pltpu.SemaphoreType.DMA((sum(cuts) + 8,)), pltpu.SemaphoreType.DMA((sum(cuts) + 8,))],
        compiler_params=pltpu.CompilerParams(vmem_limit_bytes=60 << 20),
    )(*arrays, small)


def fused_shards(
    block_input, out_grad, ln1_gain, ln1_bias, ln2_gain, ln2_bias,
    w_qkv, b_qkv, w_dense, b_dense, w_fc, b_fc, w_proj, b_proj,
):
    results = call_block(
        block_input, out_grad, w_qkv, w_dense, w_fc, w_proj, turn_tables(SEQ),
        ln1_gain, ln1_bias, ln2_gain, ln2_bias, b_qkv, b_fc, b_dense, b_proj,
    )
    fc, proj, qkv, dense, block, grad, *vectors = call_close(*results[:7])
    gain_1, shift_1, gain_2, shift_2, qkv_bias, fc_bias, dense_bias, proj_bias = vectors
    return (
        block, grad, gain_1, shift_1, gain_2, shift_2, qkv, qkv_bias, dense, dense_bias,
        fc, fc_bias, proj, proj_bias,
    )


def solution(mesh):
    sizes = tuple(mesh.shape[name] for name in ("dp", "row", "col"))
    body = fused_shards if sizes == (2, 4, 4) else shards
    return jax.shard_map(
        body,
        mesh=mesh,
        in_specs=(
            P(("dp", "row"), "col"),
            P(("dp", "row"), "col"),
            P("col"),
            P("col"),
            P("col"),
            P("col"),
            P("row", "col"),
            P("col"),
            P("col", "row"),
            P("col"),
            P("row", "col"),
            P("col"),
            P("col", "row"),
            P("col"),
        ),
        out_specs=(
            P(("dp", "row"), "col"),
            P(("dp", "row"), "col"),
            P("col"),
            P("col"),
            P("col"),
            P("col"),
            P("row", "col"),
            P("col"),
            P("col", "row"),
            P("col"),
            P("row", "col"),
            P("col"),
            P("col", "row"),
            P("col"),
        ),
        check_vma=False,
    )
```

```python
import functools
import math

import jax
import jax.numpy as jnp
import numpy as np
from jax import lax
from jax.experimental import pallas as pl
from jax.experimental.pallas import tpu as pltpu
from jax.sharding import PartitionSpec as P

D = 2048
HD = 256
ROT = 64
SEQ = 512


epsilon = 1e-05
contract_last = (((1,), (1,)), ((), ()))
contract_first = (((0,), (0,)), ((), ()))


def angle_tables(length):
    half_rot = ROT // 2
    position = jnp.arange(length, dtype=jnp.float32)
    exponent = jnp.arange(half_rot, dtype=jnp.float32) * (2.0 / ROT)
    frequency = 10000.0 ** (-exponent)
    angles = position[:, None] * frequency[None, :]
    return (jnp.cos(angles), jnp.sin(angles))


def rotate_fwd(values, cosine, sine_vals):
    half_rot = ROT // 2
    first = values[..., :half_rot]
    second = values[..., half_rot:ROT]
    cos_part = cosine[:, None, :]
    sin_part = sine_vals[:, None, :]
    return jnp.concatenate(
        [
            first * cos_part - second * sin_part,
            second * cos_part + first * sin_part,
            values[..., ROT:],
        ],
        axis=-1,
    )


def rotate_back(grads, cosine, sine_vals):
    half_rot = ROT // 2
    first = grads[..., :half_rot]
    second = grads[..., half_rot:ROT]
    cos_part = cosine[:, None, :]
    sin_part = sine_vals[:, None, :]
    return jnp.concatenate(
        [
            first * cos_part + second * sin_part,
            second * cos_part - first * sin_part,
            grads[..., ROT:],
        ],
        axis=-1,
    )


def gelu_value(pre_act):
    return 0.5 * pre_act * (1.0 + lax.erf(pre_act * 0.7071067811865476))


def gelu_slope(pre_act):
    return 0.5 * (
        1.0 + lax.erf(pre_act * 0.7071067811865476)
    ) + pre_act * 0.3989422804014327 * jnp.exp(-0.5 * pre_act * pre_act)


def shards(
    block_input,
    out_grad,
    ln1_gain,
    ln1_bias,
    ln2_gain,
    ln2_bias,
    w_qkv,
    b_qkv,
    w_dense,
    b_dense,
    w_fc,
    b_fc,
    w_proj,
    b_proj,
):
    tok_rows = block_input.shape[0]
    seq_count = tok_rows // SEQ
    qkv_cols = w_qkv.shape[1]
    fc_cols = w_fc.shape[1]
    local_heads = qkv_cols // (3 * HD)
    head_cols = local_heads * HD
    scale = 1.0 / math.sqrt(HD)
    cosine, sine_vals = angle_tables(SEQ)
    causal = jnp.arange(SEQ)[:, None] >= jnp.arange(SEQ)[None, :]
    row_total, square_total = lax.psum(
        (jnp.sum(block_input, axis=1), jnp.sum(block_input * block_input, axis=1)), "col"
    )
    mean_row = (row_total / D)[:, None]
    var_row = (square_total / D)[:, None] - mean_row * mean_row
    inv_std = lax.rsqrt(var_row + epsilon)
    x_hat = (block_input - mean_row) * inv_std
    normed_one = (x_hat * ln1_gain + ln1_bias).astype(jnp.bfloat16)
    normed_two = (x_hat * ln2_gain + ln2_bias).astype(jnp.bfloat16)
    wide_one, wide_two = (
        lax.all_gather(normed_one, "col", axis=1, tiled=True),
        lax.all_gather(normed_two, "col", axis=1, tiled=True),
    )
    part_one = wide_one
    part_two = wide_two
    qkv_pre = jnp.dot(
        part_one,
        lax.all_gather(w_qkv, "row", axis=0, tiled=True),
        preferred_element_type=jnp.float32,
    )
    fc_pre = jnp.dot(
        part_two,
        lax.all_gather(w_fc, "row", axis=0, tiled=True),
        preferred_element_type=jnp.float32,
    )
    qkv_pre = qkv_pre + b_qkv
    fc_pre = fc_pre + b_fc

    def forward_seq(block):
        query = rotate_fwd(block[:, :, 0], cosine, sine_vals).astype(jnp.bfloat16)
        keys = rotate_fwd(block[:, :, 1], cosine, sine_vals).astype(jnp.bfloat16)
        values = block[:, :, 2].astype(jnp.bfloat16)
        scores = jnp.einsum("qhd,khd->hqk", query, keys, preferred_element_type=jnp.float32) * scale
        masked = jnp.where(causal[None], scores, -1e30)
        row_max = jnp.max(masked, axis=-1, keepdims=True)
        exp_sum = jnp.sum(
            jnp.where(causal[None], jnp.exp(masked - row_max), 0.0), axis=-1, keepdims=True
        )
        log_total = row_max + jnp.log(exp_sum)
        probs_low = jnp.where(causal[None], jnp.exp(masked - log_total), 0.0).astype(jnp.bfloat16)
        attended = jnp.einsum(
            "hqk,khd->qhd", probs_low, values, preferred_element_type=jnp.float32
        ).astype(jnp.bfloat16)
        return (query, keys, values, attended, log_total)

    query, keys, values, attended, log_total = lax.map(
        forward_seq, qkv_pre.reshape(seq_count, SEQ, local_heads, 3, HD)
    )
    attn_out = attended.reshape(tok_rows, head_cols)
    gelu_out = gelu_value(fc_pre).astype(jnp.bfloat16)
    out_stack = jnp.concatenate([w_dense, w_proj], axis=0)
    shard_piece = lax.all_gather(out_stack, "row", axis=1, tiled=True)
    mixed = jnp.dot(
        attn_out, shard_piece[:head_cols], preferred_element_type=jnp.float32
    ) + jnp.dot(gelu_out, shard_piece[head_cols:], preferred_element_type=jnp.float32)
    branch_sum = lax.psum_scatter(mixed, "col", scatter_dimension=1, tiled=True)
    block_output = block_input + branch_sum + b_dense + b_proj
    grad_low = out_grad.astype(jnp.bfloat16)
    wide_grad = lax.all_gather(grad_low, "col", axis=1, tiled=True)
    both_grad = lax.dot_general(
        wide_grad,
        lax.all_gather(out_stack, "row", axis=1, tiled=True),
        contract_last,
        preferred_element_type=jnp.float32,
    )
    attn_grad = both_grad[:, :head_cols]
    gelu_grad = both_grad[:, head_cols:]
    attn_grad_low = attn_grad.astype(jnp.bfloat16)
    fc_grad = gelu_grad * gelu_slope(fc_pre)
    fc_bias_grad = jnp.sum(fc_grad, axis=0)
    fc_grad_low = fc_grad.astype(jnp.bfloat16)

    def backward_seq(items):
        query_s, keys_s, values_s, attended_s, log_s, head_grad = items
        scores = (
            jnp.einsum("qhd,khd->hqk", query_s, keys_s, preferred_element_type=jnp.float32) * scale
        )
        probs = jnp.where(
            causal[None], jnp.exp(jnp.where(causal[None], scores, -1e30) - log_s), 0.0
        )
        probs_low = probs.astype(jnp.bfloat16)
        value_grad = jnp.einsum(
            "hqk,qhd->khd", probs_low, head_grad, preferred_element_type=jnp.float32
        )
        prob_grad = jnp.einsum(
            "qhd,khd->hqk", head_grad, values_s, preferred_element_type=jnp.float32
        )
        delta_row = jnp.transpose(
            jnp.sum(head_grad.astype(jnp.float32) * attended_s.astype(jnp.float32), axis=-1), (1, 0)
        )[:, :, None]
        score_grad = (probs * (prob_grad - delta_row) * scale).astype(jnp.bfloat16)
        query_grad = jnp.einsum(
            "hqk,khd->qhd", score_grad, keys_s, preferred_element_type=jnp.float32
        )
        key_grad = jnp.einsum(
            "hqk,qhd->khd", score_grad, query_s, preferred_element_type=jnp.float32
        )
        return jnp.stack(
            [
                rotate_back(query_grad, cosine, sine_vals),
                rotate_back(key_grad, cosine, sine_vals),
                value_grad,
            ],
            axis=2,
        )

    head_grads = attn_grad_low.reshape(seq_count, SEQ, local_heads, HD)
    qkv_grad = lax.map(
        backward_seq, (query, keys, values, attended, log_total, head_grads)
    ).reshape(tok_rows, qkv_cols)
    qkv_bias_grad = jnp.sum(qkv_grad, axis=0)
    qkv_grad_low = qkv_grad.astype(jnp.bfloat16)
    in_stack = jnp.concatenate([w_qkv, w_fc], axis=1)
    shard_piece = lax.all_gather(in_stack, "row", axis=0, tiled=True)
    norm_grads = jnp.stack(
        [
            lax.dot_general(
                qkv_grad_low,
                shard_piece[:, :qkv_cols],
                contract_last,
                preferred_element_type=jnp.float32,
            ),
            lax.dot_general(
                fc_grad_low,
                shard_piece[:, qkv_cols:],
                contract_last,
                preferred_element_type=jnp.float32,
            ),
        ]
    )
    part_one = wide_one
    part_two = wide_two
    row_part = lax.psum_scatter(
        jnp.concatenate(
            [
                lax.dot_general(
                    part_one, qkv_grad_low, contract_first, preferred_element_type=jnp.float32
                ),
                lax.dot_general(
                    part_two, fc_grad_low, contract_first, preferred_element_type=jnp.float32
                ),
                lax.dot_general(
                    wide_grad, attn_out, contract_first, preferred_element_type=jnp.float32
                ),
                lax.dot_general(
                    wide_grad, gelu_out, contract_first, preferred_element_type=jnp.float32
                ),
            ],
            axis=1,
        ),
        "row",
        scatter_dimension=0,
        tiled=True,
    )
    grad_rows = lax.psum(row_part, "dp")
    qkv_total = grad_rows[:, :qkv_cols]
    fc_total = grad_rows[:, qkv_cols : qkv_cols + fc_cols]
    dense_total = grad_rows[:, qkv_cols + fc_cols : qkv_cols + fc_cols + head_cols].T
    proj_total = grad_rows[:, qkv_cols + fc_cols + head_cols :].T
    norm_local = lax.psum_scatter(norm_grads, "col", scatter_dimension=2, tiled=True)
    grad_one = norm_local[0]
    grad_two = norm_local[1]
    hat_grad = grad_one * ln1_gain + grad_two * ln2_gain
    total_hat, total_cross = lax.psum(
        (jnp.sum(hat_grad, axis=1), jnp.sum(hat_grad * x_hat, axis=1)), "col"
    )
    input_grad = out_grad + inv_std * (
        hat_grad - (total_hat / D)[:, None] - x_hat * (total_cross / D)[:, None]
    )
    gain_one, shift_one, gain_two, shift_two, qkv_bias_total, fc_bias_total, out_bias_total = (
        lax.psum(
            (
                jnp.sum(grad_one * x_hat, axis=0),
                jnp.sum(grad_one, axis=0),
                jnp.sum(grad_two * x_hat, axis=0),
                jnp.sum(grad_two, axis=0),
                qkv_bias_grad,
                fc_bias_grad,
                jnp.sum(out_grad, axis=0),
            ),
            ("dp", "row"),
        )
    )
    return (
        block_output,
        input_grad,
        gain_one,
        shift_one,
        gain_two,
        shift_two,
        qkv_total,
        qkv_bias_total,
        dense_total,
        out_bias_total,
        fc_total,
        fc_bias_total,
        proj_total,
        out_bias_total,
    )


f32 = jnp.float32
bf16 = jnp.bfloat16
MESH = pl.DeviceIdType.MESH
VMEM = pltpu.VMEM
Q = 256
HALF = 4 * Q


def flip(a, b):
    return a + b - 2 * a * b


def span(start, size):
    return pl.ds(pl.multiple_of(start, size), size)


def mm(a, b):
    return jnp.dot(a, b, preferred_element_type=f32)


def mm_nt(a, b):
    return lax.dot_general(a, b, (((1,), (1,)), ((), ())), preferred_element_type=f32)


def mm_tn(a, b):
    return lax.dot_general(a, b, (((0,), (0,)), ((), ())), preferred_element_type=f32)


class Net:
    def __init__(self, send_sems, recv_sems, local_sems):
        self.k = lax.axis_index("dp")
        self.r = lax.axis_index("row")
        self.c = lax.axis_index("col")
        k, r, c = self.k, self.r, self.c
        self.core = (1 - k, r, c)
        self.x = (k, r + 1 - 2 * (r % 2), c)
        self.y = (k, r + 2 - 4 * (r // 2), c)
        near = c + 1 - 2 * (c % 2)
        self.z = (None, (k, r, near), (k, r, c + 2 - 4 * (c // 2)), (k, r, 3 - c))
        self.middle = flip(c % 2, c // 2) == 1
        self.send_sems, self.recv_sems, self.local_sems = send_sems, recv_sems, local_sems
        self.remote_count = 0
        self.local_count = 0
        self.pending = []

    def mix(self, j):
        return flip(j % 2, flip(self.c % 2, self.r % 2)) + 2 * flip(
            j // 2, flip(self.c // 2, self.r // 2)
        )

    def barrier(self):
        sem = pltpu.get_barrier_semaphore()

        def greet(peer):
            pl.semaphore_signal(sem, inc=1, device_id=peer, device_id_type=MESH)

        for peer in (self.x, self.y, self.core, self.z[1]):
            greet(peer)

        @pl.when(self.middle)
        def _():
            greet(self.z[3])
            pl.semaphore_wait(sem, 5)

        @pl.when(jnp.logical_not(self.middle))
        def _():
            pl.semaphore_wait(sem, 4)

    def slot(self):
        self.remote_count += 1
        return self.remote_count - 1

    def remote(self, src, dst, peer):
        slot = self.slot()
        copy = pltpu.make_async_remote_copy(
            src_ref=src,
            dst_ref=dst,
            send_sem=self.send_sems.at[slot],
            recv_sem=self.recv_sems.at[slot],
            device_id=peer,
            device_id_type=MESH,
        )
        copy.start()
        self.pending.append(copy)
        return copy

    def local(self, src, dst):
        copy = pltpu.make_async_copy(src, dst, self.local_sems.at[self.local_count])
        self.local_count += 1
        copy.start()
        return copy

    def sent(self, copy):
        copy.wait_send()
        self.pending = [other for other in self.pending if other is not copy]

    def drain(self):
        for copy in self.pending:
            copy.wait_send()


class Gather:
    def __init__(self, net, shard, full, by_rows):
        self.net, self.shard, self.full, self.by_rows = net, shard, full, by_rows
        self.depth = Q // 2 if by_rows else shard.shape[0] // 2
        self.placed = []

    def own(self, half, part=None):
        if self.by_rows:
            if part is None:
                return self.shard.at[span(half * Q, Q), :]
            return self.shard.at[span(half * Q + part * self.depth, self.depth), :]
        rows = slice(None) if part is None else pl.ds(part * self.depth, self.depth)
        return self.shard.at[rows, span(half * Q, Q)]

    def chunk(self, s, i, part=None):
        start = s * HALF + i * Q
        if self.by_rows:
            if part is None:
                return self.full.at[pl.ds(start, Q), :]
            return self.full.at[pl.ds(start + part * self.depth, self.depth), :]
        rows = slice(None) if part is None else pl.ds(part * self.depth, self.depth)
        return self.full.at[rows, pl.ds(start, Q)]

    def place_own(self):
        net = self.net
        self.placed = [
            net.local(self.own(net.k), self.chunk(0, 0)),
            net.local(self.own(1 - net.k), self.chunk(1, 0)),
        ]

    def send_own(self):
        net, k = self.net, self.net.k
        self.y0 = net.remote(self.own(k, 0), self.chunk(0, 2, 0), net.y)
        self.x1 = net.remote(self.own(k, 1), self.chunk(0, 1, 1), net.x)
        self.y1 = net.remote(self.own(k, 1), self.chunk(0, 2, 1), net.y)
        self.x0 = net.remote(self.own(k, 0), self.chunk(0, 1, 0), net.x)

    def forward(self):
        net = self.net
        self.y0.wait_recv()
        self.d0 = net.remote(self.chunk(0, 2, 0), self.chunk(0, 3, 0), net.x)
        self.x1.wait_recv()
        self.d1 = net.remote(self.chunk(0, 1, 1), self.chunk(0, 3, 1), net.y)

    def swap_near(self):
        net = self.net
        self.x0.wait_recv()
        self.c1 = net.remote(self.chunk(0, 1), self.chunk(1, 1), net.core)
        self.y1.wait_recv()
        self.c2 = net.remote(self.chunk(0, 2), self.chunk(1, 2), net.core)

    def swap_far(self):
        net = self.net
        self.d0.wait_recv()
        self.d1.wait_recv()
        self.c3 = net.remote(self.chunk(0, 3), self.chunk(1, 3), net.core)

    def ready(self):
        for copy in (self.c1, self.c2, self.c3):
            copy.wait_recv()
        for copy in self.placed:
            copy.wait()

    def release(self):
        for copy in (self.d0, self.d1, self.c1, self.c2, self.c3):
            self.net.sent(copy)


class Line:
    def __init__(self, net, slots):
        self.net, self.slots = net, slots
        self.ids = [None] + [net.slot() for _ in range(3)]
        self.sends = []

    def copy(self, src, dst, peer, send):
        net = self.net
        return pltpu.make_async_remote_copy(
            src_ref=self.slots.at[src],
            dst_ref=self.slots.at[dst],
            send_sem=net.send_sems.at[send],
            recv_sem=net.recv_sems.at[self.ids[dst]],
            device_id=peer,
            device_id_type=MESH,
        )

    def start(self):
        net = self.net
        self.first = self.copy(0, 1, net.z[1], self.ids[1])
        self.first.start()
        self.hops = [
            self.copy(0, 3, net.z[3], self.ids[2]),
            self.copy(1, 2, net.z[3], self.ids[3]),
            self.copy(3, 2, net.z[1], net.slot()),
            self.copy(2, 3, net.z[1], net.slot()),
        ]

        @pl.when(net.middle)
        def _():
            self.hops[0].start()

    def arrived(self, slot):
        return self.copy(0, slot, self.net.z[1], self.ids[slot])

    def step(self, number):
        slot = (1, 3, 2)[number]

        @pl.when(self.net.middle)
        def _():
            self.arrived(slot).wait_recv()
            self.hops[number + 1].start()

    def ready(self):
        @pl.when(jnp.logical_not(self.net.middle))
        def _():
            for slot in (1, 2, 3):
                self.arrived(slot).wait_recv()

    def drain(self):
        self.first.wait_send()

        @pl.when(self.net.middle)
        def _():
            for hop in self.hops:
                hop.wait_send()


class Fold:
    def __init__(self, net, blocks, inbox):
        self.net, self.blocks, self.inbox = net, blocks, inbox
        hops = ((3, None, 0), (2, None, 1), (1, None, 2), (None, 0, 3), (None, 1, 4), (None, 3, 0))
        self.copies = []
        for n, (block, slot, dest) in enumerate(hops):
            number = net.slot()
            self.copies.append(
                pltpu.make_async_remote_copy(
                    src_ref=blocks.at[block] if slot is None else inbox.at[slot],
                    dst_ref=inbox.at[dest],
                    send_sem=net.send_sems.at[number],
                    recv_sem=net.recv_sems.at[number],
                    device_id=net.z[3] if n in (3, 4) else net.z[1],
                    device_id_type=MESH,
                )
            )

    def start(self, first, last):
        @pl.when(jnp.logical_not(self.net.middle))
        def _():
            for copy in self.copies[first:last]:
                copy.start()

    def step(self, number):
        slot, block = ((0, 2), (1, 3), (3, 1))[number]
        inbox, blocks = self.inbox, self.blocks

        @pl.when(self.net.middle)
        def _():
            self.copies[(0, 1, 3)[number]].wait_recv()

            def add(n, _):
                at = span(n * 64, 64)
                total = inbox[slot, at, :].astype(f32) + blocks[block, at, :].astype(f32)
                inbox[slot, at, :] = total.astype(bf16)
                return 0

            lax.fori_loop(0, inbox.shape[1] // 64, add, 0)
            self.copies[3 + number].start()

    def total(self, use):
        def gather(*slots):
            def add(n, _):
                at = span(n * 64, 64)
                value = self.blocks[0, at, :].astype(f32)
                for slot in slots:
                    value = value + self.inbox[slot, at, :].astype(f32)
                use(at, value)
                return 0

            lax.fori_loop(0, self.inbox.shape[1] // 64, add, 0)

        @pl.when(self.net.middle)
        def _():
            self.copies[2].wait_recv()
            self.copies[4].wait_recv()
            gather(2, 4)

        @pl.when(jnp.logical_not(self.net.middle))
        def _():
            self.copies[5].wait_recv()
            gather(0)

    def drain(self):
        @pl.when(self.net.middle)
        def _():
            for copy in self.copies[3:]:
                copy.wait_send()

        @pl.when(jnp.logical_not(self.net.middle))
        def _():
            for copy in self.copies[:3]:
                copy.wait_send()


def turn(low, tables, sign):
    lane = lax.broadcasted_iota(jnp.int32, low.shape, 1)
    swung = jnp.where(lane < ROT // 2, pltpu.roll(low, 96, 1), pltpu.roll(low, 32, 1))
    return low * tables[0] + sign * (tables[1] * swung)


class Tiles:
    def __init__(self, slots, sems):
        self.slots, self.sems = slots, sems

    def write(self, count, product, place, depth):
        def body(n, _):
            slot = n % 2
            source = self.slots.at[slot, pl.ds(0, depth), :]
            copy = pltpu.make_async_copy(source, place(n), self.sems.at[slot])

            @pl.when(n >= 2)
            def _():
                copy.wait()

            self.slots[slot, 0:depth, :] = product(n).astype(bf16)
            copy.start()
            return 0

        lax.fori_loop(0, count, body, 0)
        for slot in range(2):
            source = self.slots.at[slot, pl.ds(0, depth), :]
            pltpu.make_async_copy(source, place(slot), self.sems.at[slot]).wait()


class Reduce:
    def __init__(self, net, partial, joined, near, far, by_rows, in_vmem=False):
        self.in_vmem = in_vmem
        self.net, self.partial, self.by_rows = net, partial, by_rows
        self.joined, self.near, self.far = joined, near, far
        self.depth = Q // 2 if by_rows else partial.shape[0] // 2

    def chunk(self, i, half):
        if self.by_rows:
            return self.partial.at[pl.ds(i * Q + half * self.depth, self.depth), :]
        return self.partial.at[pl.ds(half * self.depth, self.depth), pl.ds(i * Q, Q)]

    def whole(self):
        if self.by_rows:
            return self.partial.at[pl.ds(0, Q), :]
        return self.partial.at[:, pl.ds(0, Q)]

    def rows(self, half):
        return pl.ds(half * self.depth, self.depth)

    def start(self):
        net = self.net
        self.a = net.remote(self.chunk(3, 0), self.joined.at[0], net.x)
        self.b = net.remote(self.chunk(3, 1), self.joined.at[1], net.y)
        self.near_a = net.remote(self.chunk(1, 0), self.near.at[self.rows(0), :], net.x)
        self.near_b = net.remote(self.chunk(2, 1), self.near.at[self.rows(1), :], net.y)

    def join(self, parts):
        net = self.net
        loads = [net.local(self.chunk(2, 0), parts[0]), net.local(self.chunk(1, 1), parts[1])]
        hops = []
        for half, copy, peer in ((0, self.a, net.y), (1, self.b, net.x)):
            loads[half].wait()
            copy.wait_recv()
            tile = 64

            def add(n, _, half=half):
                at = span(n * tile, tile)
                total = self.joined[half, at, :].astype(f32) + parts[half][at, :].astype(f32)
                self.joined[half, at, :] = total.astype(bf16)
                return 0

            lax.fori_loop(0, self.depth // tile, add, 0)
            hops.append(net.remote(self.joined.at[half], self.far.at[self.rows(half), :], peer))
        self.far_a, self.far_b = hops

    def prepare(self, buffers):
        net = self.net
        self.buffers = list(buffers)
        self.loads = [net.local(self.whole(), buffers[0])]
        for copy in (self.near_a, self.near_b):
            copy.wait_recv()
        if self.in_vmem:
            self.buffers[1:3] = [self.near, self.far]
        else:
            self.loads.append(net.local(self.near, buffers[1]))

    def finish(self, out):
        net, buffers = self.net, self.buffers
        last = []
        for half, copy in enumerate((self.far_a, self.far_b)):
            copy.wait_recv()
            if not self.in_vmem:
                rows = self.rows(half)
                last.append(net.local(self.far.at[rows, :], buffers[2].at[rows, :]))
        for copy in self.loads:
            copy.wait()
        tile = 64
        self.here, self.there = [], []
        for half in range(2):
            if last:
                last[half].wait()

            def add(n, _, half=half):
                at = span(half * self.depth + n * tile, tile)
                parts = [buffer[at, :].astype(f32) for buffer in buffers[:3]]
                buffers[3][at, :] = (parts[0] + parts[1] + parts[2]).astype(bf16)
                return 0

            lax.fori_loop(0, self.depth // tile, add, 0)
            source = buffers[3].at[self.rows(half), :]
            if self.by_rows:
                place = out.at[span(net.k * Q + half * self.depth, self.depth), :]
            else:
                place = out.at[self.rows(half), span(net.k * Q, Q)]
            self.here.append(net.local(source, place))
            self.there.append(net.remote(source, place, net.core))

    def done(self):
        for copy in self.here:
            copy.wait()
        for copy in self.there:
            copy.wait_recv()


def block_kernel(
    x, og, w_qkv, w_dense, w_fc, w_proj, t_turn,
    i_gain_1, i_bias_1, i_gain_2, i_bias_2, i_b_qkv, i_b_fc, i_b_dense, i_b_proj,
    o_proj, o_qkv, o_fc, o_dense, o_block, o_input, o_small,
    all_proj, r_proj, r_qkv, r_fc, r_dense, n_proj, f_proj, n_qkv, f_qkv, n_fc, f_fc,
    g_qkv, g_dense, g_fc, g_tail, xs, ys, pks, stats, rows, h1c, h1s, h2c, h2s, dyc, dys, xh,
    qb, kb, vb, probs, probs_low, oc, dob, dqc, gc, slope, dabt, stage,
    out_recv, hat_recv, j_proj, j_qkv, j_fc, j_dense, n_dense, f_dense, tables, vecs, bias, packs, small,
    gain_1, bias_1, gain_2, bias_2, b_qkv, b_fc, b_dense, b_proj,
    send_sems, recv_sems, local_sems, stage_sems,
):
    tok = x.shape[0]
    heads = qb.shape[0]
    width = gc.shape[1]
    scale = 1.0 / math.sqrt(HD)
    net = Net(send_sems, recv_sems, local_sems)
    net.barrier()
    qkv = Gather(net, w_qkv, g_qkv, True)
    dense = Gather(net, w_dense, g_dense, False)
    fc = Gather(net, w_fc, g_fc, True)
    proj = Gather(net, w_proj, all_proj, False)
    qkv.send_own()
    dense.send_own()
    load_x = net.local(x, probs.at[0])
    vectors = [
        net.local(i_gain_1, gain_1), net.local(i_bias_1, bias_1), net.local(i_gain_2, gain_2),
        net.local(i_bias_2, bias_2), net.local(i_b_qkv, b_qkv), net.local(i_b_fc, b_fc),
        net.local(i_b_dense, b_dense), net.local(i_b_proj, b_proj),
    ]
    load_og = net.local(og, probs.at[1])
    load_turn = net.local(t_turn, tables)
    tiles = Tiles(stage, stage_sems)
    mine = pl.ds(0, tok)
    theirs = pl.ds(tok, tok)

    step = 128
    lane = lax.broadcasted_iota(jnp.int32, (step, 128), 1)
    load_x.wait()

    def local_norm(n, _):
        at = span(n * step, step)
        block = probs[0, at, :]
        mean = jnp.mean(block, axis=1, keepdims=True)
        centred = block - mean
        var = jnp.mean(centred * centred, axis=1, keepdims=True)
        stats[at, :] = jnp.where(lane == 0, mean, jnp.where(lane == 1, var, 0.0))
        return 0

    lax.fori_loop(0, tok // step, local_norm, 0)
    pks[0] = stats[...].T[0:8]
    for copy in vectors:
        copy.wait()
    for n, vector in enumerate((gain_1, bias_1, gain_2, bias_2)):
        pks[0, 2 + n : 3 + n, :] = vector[...].reshape(1, 512)
    p_line = Line(net, pks)
    p_line.start()
    for weight in (qkv, dense, fc):
        weight.place_own()
    bias[...] = jnp.zeros_like(bias)
    bias[3:4, 0 : b_qkv.shape[0]] = b_qkv[...].reshape(1, b_qkv.shape[0])
    bias[4:5, :] = b_fc[...].reshape(1, width)
    bias[5:6, 0:512] = (b_dense[...] + b_proj[...]).reshape(1, 512)
    rows[...] = jnp.zeros_like(rows)
    load_og.wait()

    def local_grad(n, _):
        at = span(n * step, step)
        block = probs[1, at, :]
        ys[0, at, :] = block.astype(bf16)
        bias[1:2, 0:512] += jnp.sum(block, axis=0, keepdims=True)
        return 0

    lax.fori_loop(0, tok // step, local_grad, 0)
    for hop in range(3):
        p_line.step(hop)
    p_line.ready()
    means = [pks[j, 0:1, :] for j in range(4)]
    mu = (means[0] + means[1] + means[2] + means[3]) * 0.25
    spread = [pks[j, 1:2, :] + (means[j] - mu) * (means[j] - mu) for j in range(4)]
    rows[0:1, :] = mu
    rows[1:2, :] = lax.rsqrt((spread[0] + spread[1] + spread[2] + spread[3]) * 0.25 + epsilon)
    stats[...] = rows[...].T

    def own_norm(n, _):
        at = span(n * step, step)
        hats = (probs[0, at, :] - stats[at, 0:1]) * stats[at, 1:2]
        xs[0, at, :] = (hats * pks[0, 2:3, :] + pks[0, 3:4, :]).astype(bf16)
        return 0

    lax.fori_loop(0, tok // step, own_norm, 0)
    x_line = Line(net, xs)
    y_line = Line(net, ys)
    x_line.start()
    qkv.forward()
    x_line.step(0)
    x_line.step(1)
    fc.send_own()
    dense.forward()
    qkv.swap_near()
    x_line.step(2)
    y_line.start()
    dense.swap_near()
    qkv.swap_far()
    x_line.ready()
    fc.forward()
    proj.send_own()

    for s in range(2):
        for j in range(4):
            lanes = span(flip(s, net.k) * Q, Q)
            dest = span(net.mix(j) * Q, Q)
            wide = span(s * HALF + net.mix(j) * Q, Q)
            vecs[0:4, wide] = pks[j, 2:6, lanes]

            def norm(n, _, s=s, j=j, lanes=lanes, dest=dest, wide=wide):
                at = span(n * step, step)
                one = xs[j, at, lanes]
                hats = (one.astype(f32) - pks[j, 3:4, lanes]) * (1.0 / pks[j, 2:3, lanes])
                xh[at, wide] = hats.astype(bf16)
                (h1s if s else h1c)[at, dest] = one
                two = hats * pks[j, 4:5, lanes] + pks[j, 5:6, lanes]
                (h2s if s else h2c)[at, dest] = two.astype(bf16)
                return 0

            lax.fori_loop(0, tok // step, norm, 0)
    swap_h1 = net.remote(h1s, h1c.at[theirs, :], net.core)
    swap_h2 = net.remote(h2s, h2c.at[theirs, :], net.core)
    y_line.step(0)
    load_turn.wait()
    qkv.ready()

    def project(n, _):
        cols = span(n * 3 * HD, 3 * HD)
        acc = mm(h1c[mine, :], g_qkv[0:HALF, cols]) + mm(h1s[...], g_qkv[HALF:, cols])
        acc = acc + bias[3:4, cols]
        qb[n, :, 0:128] = turn(acc[:, 0:128], tables, 1.0).astype(bf16)
        qb[n, :, 128:HD] = acc[:, 128:HD].astype(bf16)
        kb[n, :, 0:128] = turn(acc[:, HD : HD + 128], tables, 1.0).astype(bf16)
        kb[n, :, 128:HD] = acc[:, HD + 128 : 2 * HD].astype(bf16)
        vb[n] = acc[:, 2 * HD :].astype(bf16)
        return 0

    lax.fori_loop(0, heads, project, 0)
    y_line.step(1)
    chunks = tok // step

    def attend(n, _):
        head, chunk = n // chunks, n % chunks
        at = span(chunk * step, step)
        scores = mm_nt(qb[head, at, :], kb[head]) * scale
        token = lax.broadcasted_iota(jnp.int32, (step, tok), 0) + chunk * step
        allowed = token >= lax.broadcasted_iota(jnp.int32, (step, tok), 1)
        scores = jnp.where(allowed, scores, -1e30)
        top = jnp.max(scores, axis=1, keepdims=True)
        raised = jnp.where(allowed, jnp.exp(scores - top), 0.0)
        weight = raised / jnp.sum(raised, axis=1, keepdims=True)
        probs[head, at, :] = weight
        low = weight.astype(bf16)
        probs_low[head, at, :] = low
        oc[at, span(head * HD, HD)] = mm(low, vb[head]).astype(bf16)
        return 0

    lax.fori_loop(0, heads * chunks, attend, 0)
    swap_o = net.remote(oc.at[mine, :], oc.at[theirs, :], net.core)
    dense.swap_far()
    fc.swap_near()
    y_line.step(2)
    fc.swap_far()
    fc.ready()

    def expand(n, _):
        cols = span(n * 512, 512)
        a = mm(h2c[mine, :], g_fc[0:HALF, cols]) + mm(h2s[...], g_fc[HALF:, cols])
        a = a + bias[4:5, cols]
        rise = 0.5 * (1.0 + lax.erf(a * 0.7071067811865476))
        gc[mine, cols] = (a * rise).astype(bf16)
        slope[:, cols] = (rise + a * 0.3989422804014327 * jnp.exp(-0.5 * a * a)).astype(bf16)
        return 0

    lax.fori_loop(0, width // 1024, expand, 0)
    proj.forward()
    lax.fori_loop(width // 1024, width // 512, expand, 0)
    swap_g = net.remote(gc.at[mine, :], gc.at[theirs, :], net.core)
    y_line.ready()
    for s in range(2):
        for j in range(4):
            lanes = span(flip(s, net.k) * Q, Q)
            dest = span(net.mix(j) * Q, Q)
            (dys if s else dyc)[mine, dest] = ys[j, :, lanes]
    swap_dy = net.remote(dys, dyc.at[theirs, :], net.core)
    dense.ready()
    dob[...] = (
        mm_nt(dyc[mine, :], g_dense[:, 0:HALF]) + mm_nt(dys[...], g_dense[:, HALF:])
    ).astype(bf16)

    red_proj = Reduce(net, r_proj, j_proj, n_proj, f_proj, False)
    red_qkv = Reduce(net, r_qkv, j_qkv, n_qkv, f_qkv, True)
    red_fc = Reduce(net, r_fc, j_fc, n_fc, f_fc, True)
    red_dense = Reduce(net, r_dense, j_dense, n_dense, f_dense, False, True)
    swap_g.wait_recv()
    swap_dy.wait_recv()
    tall = width // 2
    tiles.write(
        4,
        lambda n: mm_tn(gc[:, span(n // 2 * tall, tall)], dyc[:, span(n % 2 * 512, 512)]),
        lambda n: r_proj.at[span(n // 2 * tall, tall), span(n % 2 * 512, 512)],
        tall,
    )
    proj.swap_near()
    red_proj.start()

    def keep(head, part, at, value, rotated):
        base = head * 3 * HD + part * HD
        if rotated:
            low = turn(value[:, 0:128], [tables[t, at, :] for t in range(2)], -1.0)
            dqc[at, pl.ds(pl.multiple_of(base, 128), 128)] = low.astype(bf16)
            bias[0:1, pl.ds(pl.multiple_of(base, 128), 128)] += jnp.sum(low, axis=0, keepdims=True)
            value, base, size = value[:, 128:], base + 128, 128
        else:
            size = HD
        cols = pl.ds(pl.multiple_of(base, 128), size)
        dqc[at, cols] = value.astype(bf16)
        bias[0:1, cols] += jnp.sum(value, axis=0, keepdims=True)

    def attend_back(head, _):
        cols = span(head * HD, HD)

        def chunk_back(n, _):
            at = span(n * step, step)
            grad = dob[at, cols]
            delta = jnp.sum(grad.astype(f32) * oc[at, cols].astype(f32), axis=1, keepdims=True)
            spread = mm_nt(grad, vb[head]) - delta
            low = (probs[head, at, :] * spread * scale).astype(bf16)
            probs_low[head, at, :] = low
            keep(head, 0, at, mm(low, kb[head]), True)
            return 0

        keep(head, 2, mine, mm_tn(probs_low[head], dob[:, cols]), False)
        lax.fori_loop(0, chunks, chunk_back, 0)
        keep(head, 1, mine, mm_tn(probs_low[head], qb[head]), True)
        return 0

    lax.fori_loop(0, heads, attend_back, 0)
    proj.swap_far()
    swap_dq = net.remote(dqc.at[mine, :], dqc.at[theirs, :], net.core)
    net.sent(swap_h1)
    net.sent(swap_h2)
    for s in range(2):

        def back_first(n, _, s=s):
            wide = span(s * HALF + n * 512, 512)
            grad = mm_nt(dqc[mine, :], g_qkv[wide, :])
            (h2s if s else h1s)[:, span(n * 512, 512)] = (grad * vecs[0:1, wide]).astype(bf16)
            vecs[4:5, wide] = jnp.sum(grad * xh[:, wide].astype(f32), axis=0, keepdims=True)
            vecs[5:6, wide] = jnp.sum(grad, axis=0, keepdims=True)
            return 0

        lax.fori_loop(0, HALF // 512, back_first, 0)

    proj.ready()
    qkv.release()
    loads = [
        net.local(w_proj.at[:, span(net.k * Q, Q)], g_qkv.at[:, pl.ds(0, Q)]),
        net.local(w_proj.at[:, span((1 - net.k) * Q, Q)], g_qkv.at[:, pl.ds(HALF, Q)]),
        net.local(all_proj.at[:, pl.ds(Q, 3 * Q)], g_qkv.at[:, pl.ds(Q, 3 * Q)]),
        net.local(all_proj.at[:, pl.ds(5 * Q, Q)], g_qkv.at[:, pl.ds(5 * Q, Q)]),
        net.local(all_proj.at[:, pl.ds(6 * Q, 2 * Q)], g_tail),
    ]
    swap_o.wait_recv()
    attn = oc.shape[1]
    tiles.write(
        2,
        lambda n: mm_tn(oc[...], dyc[:, span(n * 512, 512)]),
        lambda n: r_dense.at[:, span(n * 512, 512)],
        attn,
    )
    swap_h1.wait_recv()
    swap_dq.wait_recv()
    tiles.write(
        dqc.shape[1] // 512,
        lambda n: mm_tn(h1c[...], dqc[:, span(n * 512, 512)]),
        lambda n: r_qkv.at[:, span(n * 512, 512)],
        HALF,
    )
    red_qkv.start()
    red_dense.start()

    for copy in loads:
        copy.wait()
    x_line.drain()
    y_line.drain()

    def put_out(p, product):
        s, i = p // 4, p % 4
        out = product + mm(oc[mine, :], g_dense[:, span(p * Q, Q)])
        xs[net.mix(i), :, span(flip(s, net.k) * Q, Q)] = out.astype(bf16)

    def project_head(p, _):
        put_out(p, mm(gc[mine, :], g_qkv[:, span(p * Q, Q)]))
        return 0

    def project_tail(p, _):
        put_out(6 + p, mm(gc[mine, :], g_tail[:, span(p * Q, Q)]))
        return 0

    lax.fori_loop(0, 6, project_head, 0)
    lax.fori_loop(0, 2, project_tail, 0)
    out_fold = Fold(net, xs, out_recv)
    out_fold.start(0, 2)

    def back_fc(n, _):
        cols = span(n * 512, 512)
        grad = mm_nt(dyc[mine, :], g_qkv[cols, 0:HALF])
        grad = grad + mm_nt(dys[:, 0:512], g_qkv[cols, HALF : 6 * Q])
        grad = grad + mm_nt(dys[:, 512:], g_tail[cols, :])
        grad = grad * slope[:, cols].astype(f32)
        bias[2:3, cols] = jnp.sum(grad, axis=0, keepdims=True)
        slope[:, cols] = grad.astype(bf16)
        return 0

    lax.fori_loop(0, width // 512, back_fc, 0)
    dab = slope
    swap_da = net.remote(dab, dabt, net.core)
    red_proj.join([g_tail.at[pl.ds(0, tall), pl.ds(0, Q)], g_tail.at[pl.ds(tall, tall), pl.ds(0, Q)]])
    stats[...] = jnp.zeros_like(stats)
    lane = lax.broadcasted_iota(jnp.int32, (tok, 128), 1)

    def back_norm(j, _):
        for s in range(2):
            lanes = span(flip(s, net.k) * Q, Q)
            dest = span(net.mix(j) * Q, Q)
            wide = span(s * HALF + net.mix(j) * Q, Q)
            grad = mm_nt(dab[...], g_fc[wide, :])
            hats = xh[:, wide].astype(f32)
            packs[j, 2:4, lanes] = vecs[4:6, wide]
            packs[j, 4:5, lanes] = jnp.sum(grad * hats, axis=0, keepdims=True)
            packs[j, 5:6, lanes] = jnp.sum(grad, axis=0, keepdims=True)
            joint = (h2s if s else h1s)[:, dest].astype(f32) + grad * vecs[2:3, wide]
            ys[j, :, lanes] = joint.astype(bf16)
            one = jnp.sum(joint, axis=1, keepdims=True)
            two = jnp.sum(joint * hats, axis=1, keepdims=True)
            stats[...] += jnp.where(lane == 0, one, jnp.where(lane == 1, two, 0.0))
        return 0

    lax.fori_loop(0, 4, back_norm, 0)

    fc.release()
    turned = stats[...].T
    for j in range(4):
        packs[j, 0:2, :] = turned[0:2]
        packs[j, 6:8, :] = jnp.zeros((2, tok), f32)
    pack_copies = [net.remote(packs.at[j], packs.at[3 + j], net.z[j]) for j in (1, 2, 3)]
    hat_fold = Fold(net, ys, hat_recv)
    hat_fold.start(0, 2)
    out_fold.start(2, 3)
    hat_fold.start(2, 3)
    out_fold.step(0)
    swap_h2.wait_recv()
    swap_da.wait_recv()

    def grad_fc(n):
        cols = span(n * 512, 512)
        return mm_tn(h2c[mine, :], dab[:, cols]) + mm_tn(h2c[theirs, :], dabt[:, cols])

    tiles.write(width // 512, grad_fc, lambda n: r_fc.at[:, span(n * 512, 512)], HALF)
    red_fc.start()
    out_fold.step(1)

    def strips(base, n, columns):
        return g_fc.at[pl.ds(base + n * Q, Q), pl.ds(0, columns)]

    out_fold.step(2)
    for copy in pack_copies:
        copy.wait_recv()
    total = packs[0] + packs[4] + packs[5] + packs[6]
    rows[2:4, :] = total[0:2, :]
    stats[...] = rows[...].T
    small[0, 0:4, :] = total[2:6, :]
    for n in range(3):
        small[0, 4 + n : 5 + n, :] = bias[0:1, n * 512 : n * 512 + 512]
    for n in range(4):
        small[0, 7 + n : 8 + n, :] = bias[2:3, n * 512 : n * 512 + 512]
    small[0, 11:12, :] = bias[1:2, 0:512]
    small[0, 12:16, :] = jnp.zeros((4, 512), f32)
    net.remote(small.at[0], small.at[1], net.core).wait_recv()
    own_rows = span(net.k * 8, 8)
    small[2 + net.r, 0:8, :] = small[0, own_rows, :] + small[1, own_rows, :]
    place = small.at[2 + net.r, pl.ds(0, 8), :]
    across = (net.k, 3 - net.r, net.c)
    small_copies = [net.remote(place, place, peer) for peer in (net.x, net.y, across)]
    reload_x = net.local(x, probs.at[1])
    red_proj.prepare([g_qkv.at[:, pl.ds(n * Q, Q)] for n in range(4)])
    red_proj.finish(o_proj)
    hat_fold.step(0)
    red_fc.join([g_fc.at[pl.ds(6 * Q + n * (Q // 2), Q // 2), :] for n in range(2)])
    red_qkv.join(
        [g_fc.at[pl.ds(7 * Q + n * (Q // 2), Q // 2), pl.ds(0, 6 * Q)] for n in range(2)]
    )
    hat_fold.step(1)
    hat_fold.step(2)
    reload_x.wait()

    def close_out(at, value):
        probs[0, at, :] = probs[1, at, :] + value + bias[5:6, 0:512]

    out_fold.total(close_out)
    keep_block = net.local(probs.at[0], o_block)
    keep_block.wait()
    reload_og = net.local(og, probs.at[0])
    red_dense.join([g_tail.at[pl.ds(n * attn // 2, attn // 2), pl.ds(0, Q)] for n in range(2)])
    red_fc.prepare([strips(4 * Q, n, 8 * Q) for n in range(4)])
    red_qkv.prepare([strips(0, n, 6 * Q) for n in range(4)])
    red_dense.prepare([g_tail.at[pl.ds(n * attn, attn), pl.ds(Q, Q)] for n in range(4)])
    for copy in small_copies:
        copy.wait_recv()
    small[6, own_rows, :] = small[2, 0:8] + small[3, 0:8] + small[4, 0:8] + small[5, 0:8]
    place = small.at[6, own_rows, :]
    swap_small = net.remote(place, place, net.core)
    reload_og.wait()

    def close_hat(at, value):
        mu, rstd = stats[at, 0:1], stats[at, 1:2]
        hats = (probs[1, at, :] - mu) * rstd
        mean, cross = stats[at, 2:3] * (1.0 / D), stats[at, 3:4] * (1.0 / D)
        probs[0, at, :] += rstd * (value - mean - hats * cross)

    hat_fold.total(close_hat)
    keep_input = net.local(probs.at[0], o_input)
    swap_small.wait_recv()
    keep_small = net.local(small.at[6], o_small)
    red_fc.finish(o_fc)
    red_qkv.finish(o_qkv)
    red_dense.finish(o_dense)
    for weight in (red_proj, red_qkv, red_fc, red_dense):
        weight.done()
    keep_small.wait()
    keep_input.wait()
    p_line.drain()
    out_fold.drain()
    hat_fold.drain()
    net.drain()


def call_block(*args):
    x, w_qkv, w_dense, w_fc = args[0], args[2], args[3], args[4]
    tok = x.shape[0]
    n_qkv, n_attn, n_fc = w_qkv.shape[1], w_dense.shape[0], w_fc.shape[1]
    heads = n_attn // HD
    wide = 2 * HALF
    any_spec = pl.BlockSpec(memory_space=pl.ANY)
    shape = jax.ShapeDtypeStruct
    pieces = ((n_fc, Q), (Q, n_qkv), (Q, n_fc), (n_attn, Q))
    outs = [
        shape((n_fc, 2 * Q), bf16), shape((2 * Q, n_qkv), bf16),
        shape((2 * Q, n_fc), bf16), shape((n_attn, 2 * Q), bf16),
        shape((tok, 512), f32), shape((tok, 512), f32), shape((16, 512), f32),
        shape((n_fc, wide), bf16), shape((n_fc, HALF), bf16), shape((HALF, n_qkv), bf16),
        shape((HALF, n_fc), bf16), shape((n_attn, HALF), bf16),
    ]
    outs += [shape(piece, bf16) for piece in pieces[:3] for _ in range(2)]
    scratch = [
        VMEM((wide, n_qkv), bf16), VMEM((n_attn, wide), bf16), VMEM((wide, n_fc), bf16),
        VMEM((n_fc, 2 * Q), bf16),
        VMEM((4, tok, 512), bf16), VMEM((4, tok, 512), bf16), VMEM((4, 8, tok), f32),
        VMEM((tok, 128), f32), VMEM((128, tok), f32),
        VMEM((2 * tok, HALF), bf16), VMEM((tok, HALF), bf16),
        VMEM((2 * tok, HALF), bf16), VMEM((tok, HALF), bf16),
        VMEM((2 * tok, HALF), bf16), VMEM((tok, HALF), bf16), VMEM((tok, wide), bf16),
        VMEM((heads, tok, HD), bf16), VMEM((heads, tok, HD), bf16), VMEM((heads, tok, HD), bf16),
        VMEM((heads, tok, tok), f32), VMEM((heads, tok, tok), bf16),
        VMEM((2 * tok, n_attn), bf16), VMEM((tok, n_attn), bf16), VMEM((2 * tok, n_qkv), bf16),
        VMEM((2 * tok, n_fc), bf16), VMEM((tok, n_fc), bf16), VMEM((tok, n_fc), bf16),
        VMEM((2, HALF, 512), bf16),
        VMEM((5, tok, 512), bf16), VMEM((5, tok, 512), bf16),
    ]
    scratch += [VMEM((2,) + ((r // 2, c)), bf16) for r, c in pieces]
    scratch += [VMEM(pieces[3], bf16)] * 2
    scratch += [
        VMEM((2, tok, 128), f32),
        VMEM((8, wide), f32), VMEM((8, n_fc), f32), VMEM((7, 8, tok), f32), VMEM((7, 16, 512), f32),
        VMEM((512,), f32), VMEM((512,), f32), VMEM((512,), f32), VMEM((512,), f32),
        VMEM((n_qkv,), f32), VMEM((n_fc,), f32), VMEM((512,), f32), VMEM((512,), f32),
        pltpu.SemaphoreType.DMA((128,)), pltpu.SemaphoreType.DMA((128,)),
        pltpu.SemaphoreType.DMA((64,)), pltpu.SemaphoreType.DMA((2,)),
    ]
    return pl.pallas_call(
        block_kernel,
        name="block",
        out_shape=outs,
        in_specs=[any_spec] * 15,
        out_specs=[any_spec] * len(outs),
        scratch_shapes=scratch,
        compiler_params=pltpu.CompilerParams(
            collective_id=1, has_side_effects=True, vmem_limit_bytes=67043328
        ),
    )(*args)


def turn_tables(length):
    half_rot = ROT // 2
    frequency = (10000.0 ** (-np.arange(half_rot, dtype=np.float32) * (2.0 / ROT))).astype(np.float32)
    angles = np.arange(length, dtype=np.float32)[:, None] * frequency[None, :]
    tables = np.zeros((2, length, 128), np.float32)
    tables[0] = 1.0
    tables[0, :, :half_rot] = tables[0, :, half_rot:ROT] = np.cos(angles)
    tables[1, :, :half_rot] = -np.sin(angles)
    tables[1, :, half_rot:ROT] = np.sin(angles)
    return tables


def close_kernel(cuts, *refs):
    count = len(cuts)
    refs = list(refs)
    sources, small = [refs.pop(0) for _ in cuts], refs.pop(0)
    outs, vectors = [refs.pop(0) for _ in cuts], [refs.pop(0) for _ in range(8)]
    lows, sums = [refs.pop(0) for _ in cuts], refs.pop(0)
    wides, lines = [refs.pop(0) for _ in range(4)], [refs.pop(0) for _ in range(8)]
    in_sems, out_sems = refs
    loads, stores = [], []
    for n, cut in enumerate(cuts):
        rows = sources[n].shape[0] // cut
        for part in range(cut):
            at = pl.ds(part * rows, rows)
            number = len(loads)
            wide = wides[n] if n < len(wides) else lows[n]
            loads.append(
                pltpu.make_async_copy(sources[n].at[at, :], lows[n].at[at, :], in_sems.at[number])
            )
            stores.append(
                (n, at, pltpu.make_async_copy(wide.at[at, :], outs[n].at[at, :], out_sems.at[number]))
            )
    total = len(loads)
    load_small = pltpu.make_async_copy(small, sums, in_sems.at[total])
    for copy in loads:
        copy.start()
    load_small.start()
    for load, (n, at, store) in zip(loads, stores):
        load.wait()
        if n < len(wides):
            wides[n][at, :] = lows[n][at, :].astype(f32)
        store.start()
    load_small.wait()
    last = []
    for n, (row, line, vector) in enumerate(zip((0, 1, 2, 3, 4, 7, 11, 11), lines, vectors)):
        for part in range(line.shape[0] // 512):
            line[part * 512 : part * 512 + 512] = sums[row + part, :]
        last.append(pltpu.make_async_copy(line, vector, out_sems.at[total + n]))
        last[-1].start()
    for _, _, store in stores:
        store.wait()
    for copy in last:
        copy.wait()


def call_close(proj, qkv, fc, dense, block, grad, small):
    any_spec = pl.BlockSpec(memory_space=pl.ANY)
    shape = jax.ShapeDtypeStruct
    arrays = (fc, proj, qkv, dense, block, grad)
    cuts = (2, 2, 2, 1, 1, 1)
    outs = [shape(a.shape, f32) for a in arrays]
    lengths = [512] * 4 + [qkv.shape[1], fc.shape[1], 512, 512]
    outs += [shape((length,), f32) for length in lengths]
    return pl.pallas_call(
        functools.partial(close_kernel, cuts),
        name="close",
        out_shape=outs,
        in_specs=[any_spec] * 7,
        out_specs=[any_spec] * 14,
        scratch_shapes=[VMEM(a.shape, a.dtype) for a in (*arrays, small)]
        + [VMEM(a.shape, f32) for a in arrays[:4]]
        + [VMEM((length,), f32) for length in lengths]
        + [pltpu.SemaphoreType.DMA((sum(cuts) + 8,)), pltpu.SemaphoreType.DMA((sum(cuts) + 8,))],
        compiler_params=pltpu.CompilerParams(vmem_limit_bytes=60 << 20),
    )(*arrays, small)


def fused_shards(
    block_input, out_grad, ln1_gain, ln1_bias, ln2_gain, ln2_bias,
    w_qkv, b_qkv, w_dense, b_dense, w_fc, b_fc, w_proj, b_proj,
):
    results = call_block(
        block_input, out_grad, w_qkv, w_dense, w_fc, w_proj, turn_tables(SEQ),
        ln1_gain, ln1_bias, ln2_gain, ln2_bias, b_qkv, b_fc, b_dense, b_proj,
    )
    fc, proj, qkv, dense, block, grad, *vectors = call_close(*results[:7])
    gain_1, shift_1, gain_2, shift_2, qkv_bias, fc_bias, dense_bias, proj_bias = vectors
    return (
        block, grad, gain_1, shift_1, gain_2, shift_2, qkv, qkv_bias, dense, dense_bias,
        fc, fc_bias, proj, proj_bias,
    )


def solution(mesh):
    sizes = tuple(mesh.shape[name] for name in ("dp", "row", "col"))
    body = fused_shards if sizes == (2, 4, 4) else shards
    return jax.shard_map(
        body,
        mesh=mesh,
        in_specs=(
            P(("dp", "row"), "col"),
            P(("dp", "row"), "col"),
            P("col"),
            P("col"),
            P("col"),
            P("col"),
            P("row", "col"),
            P("col"),
            P("col", "row"),
            P("col"),
            P("row", "col"),
            P("col"),
            P("col", "row"),
            P("col"),
        ),
        out_specs=(
            P(("dp", "row"), "col"),
            P(("dp", "row"), "col"),
            P("col"),
            P("col"),
            P("col"),
            P("col"),
            P("row", "col"),
            P("col"),
            P("col", "row"),
            P("col"),
            P("row", "col"),
            P("col"),
            P("col", "row"),
            P("col"),
        ),
        check_vma=False,
    )
```

```python
import functools
import math

import jax
import jax.numpy as jnp
import numpy as np
from jax import lax
from jax.experimental import pallas as pl
from jax.experimental.pallas import tpu as pltpu
from jax.sharding import PartitionSpec as P

D = 2048
HD = 256
ROT = 64
SEQ = 512


epsilon = 1e-05
contract_last = (((1,), (1,)), ((), ()))
contract_first = (((0,), (0,)), ((), ()))


def angle_tables(length):
    half_rot = ROT // 2
    position = jnp.arange(length, dtype=jnp.float32)
    exponent = jnp.arange(half_rot, dtype=jnp.float32) * (2.0 / ROT)
    frequency = 10000.0 ** (-exponent)
    angles = position[:, None] * frequency[None, :]
    return (jnp.cos(angles), jnp.sin(angles))


def rotate_fwd(values, cosine, sine_vals):
    half_rot = ROT // 2
    first = values[..., :half_rot]
    second = values[..., half_rot:ROT]
    cos_part = cosine[:, None, :]
    sin_part = sine_vals[:, None, :]
    return jnp.concatenate(
        [
            first * cos_part - second * sin_part,
            second * cos_part + first * sin_part,
            values[..., ROT:],
        ],
        axis=-1,
    )


def rotate_back(grads, cosine, sine_vals):
    half_rot = ROT // 2
    first = grads[..., :half_rot]
    second = grads[..., half_rot:ROT]
    cos_part = cosine[:, None, :]
    sin_part = sine_vals[:, None, :]
    return jnp.concatenate(
        [
            first * cos_part + second * sin_part,
            second * cos_part - first * sin_part,
            grads[..., ROT:],
        ],
        axis=-1,
    )


def gelu_value(pre_act):
    return 0.5 * pre_act * (1.0 + lax.erf(pre_act * 0.7071067811865476))


def gelu_slope(pre_act):
    return 0.5 * (
        1.0 + lax.erf(pre_act * 0.7071067811865476)
    ) + pre_act * 0.3989422804014327 * jnp.exp(-0.5 * pre_act * pre_act)


def shards(
    block_input,
    out_grad,
    ln1_gain,
    ln1_bias,
    ln2_gain,
    ln2_bias,
    w_qkv,
    b_qkv,
    w_dense,
    b_dense,
    w_fc,
    b_fc,
    w_proj,
    b_proj,
):
    tok_rows = block_input.shape[0]
    seq_count = tok_rows // SEQ
    qkv_cols = w_qkv.shape[1]
    fc_cols = w_fc.shape[1]
    local_heads = qkv_cols // (3 * HD)
    head_cols = local_heads * HD
    scale = 1.0 / math.sqrt(HD)
    cosine, sine_vals = angle_tables(SEQ)
    causal = jnp.arange(SEQ)[:, None] >= jnp.arange(SEQ)[None, :]
    row_total, square_total = lax.psum(
        (jnp.sum(block_input, axis=1), jnp.sum(block_input * block_input, axis=1)), "col"
    )
    mean_row = (row_total / D)[:, None]
    var_row = (square_total / D)[:, None] - mean_row * mean_row
    inv_std = lax.rsqrt(var_row + epsilon)
    x_hat = (block_input - mean_row) * inv_std
    normed_one = (x_hat * ln1_gain + ln1_bias).astype(jnp.bfloat16)
    normed_two = (x_hat * ln2_gain + ln2_bias).astype(jnp.bfloat16)
    wide_one, wide_two = (
        lax.all_gather(normed_one, "col", axis=1, tiled=True),
        lax.all_gather(normed_two, "col", axis=1, tiled=True),
    )
    part_one = wide_one
    part_two = wide_two
    qkv_pre = jnp.dot(
        part_one,
        lax.all_gather(w_qkv, "row", axis=0, tiled=True),
        preferred_element_type=jnp.float32,
    )
    fc_pre = jnp.dot(
        part_two,
        lax.all_gather(w_fc, "row", axis=0, tiled=True),
        preferred_element_type=jnp.float32,
    )
    qkv_pre = qkv_pre + b_qkv
    fc_pre = fc_pre + b_fc

    def forward_seq(block):
        query = rotate_fwd(block[:, :, 0], cosine, sine_vals).astype(jnp.bfloat16)
        keys = rotate_fwd(block[:, :, 1], cosine, sine_vals).astype(jnp.bfloat16)
        values = block[:, :, 2].astype(jnp.bfloat16)
        scores = jnp.einsum("qhd,khd->hqk", query, keys, preferred_element_type=jnp.float32) * scale
        masked = jnp.where(causal[None], scores, -1e30)
        row_max = jnp.max(masked, axis=-1, keepdims=True)
        exp_sum = jnp.sum(
            jnp.where(causal[None], jnp.exp(masked - row_max), 0.0), axis=-1, keepdims=True
        )
        log_total = row_max + jnp.log(exp_sum)
        probs_low = jnp.where(causal[None], jnp.exp(masked - log_total), 0.0).astype(jnp.bfloat16)
        attended = jnp.einsum(
            "hqk,khd->qhd", probs_low, values, preferred_element_type=jnp.float32
        ).astype(jnp.bfloat16)
        return (query, keys, values, attended, log_total)

    query, keys, values, attended, log_total = lax.map(
        forward_seq, qkv_pre.reshape(seq_count, SEQ, local_heads, 3, HD)
    )
    attn_out = attended.reshape(tok_rows, head_cols)
    gelu_out = gelu_value(fc_pre).astype(jnp.bfloat16)
    out_stack = jnp.concatenate([w_dense, w_proj], axis=0)
    shard_piece = lax.all_gather(out_stack, "row", axis=1, tiled=True)
    mixed = jnp.dot(
        attn_out, shard_piece[:head_cols], preferred_element_type=jnp.float32
    ) + jnp.dot(gelu_out, shard_piece[head_cols:], preferred_element_type=jnp.float32)
    branch_sum = lax.psum_scatter(mixed, "col", scatter_dimension=1, tiled=True)
    block_output = block_input + branch_sum + b_dense + b_proj
    grad_low = out_grad.astype(jnp.bfloat16)
    wide_grad = lax.all_gather(grad_low, "col", axis=1, tiled=True)
    both_grad = lax.dot_general(
        wide_grad,
        lax.all_gather(out_stack, "row", axis=1, tiled=True),
        contract_last,
        preferred_element_type=jnp.float32,
    )
    attn_grad = both_grad[:, :head_cols]
    gelu_grad = both_grad[:, head_cols:]
    attn_grad_low = attn_grad.astype(jnp.bfloat16)
    fc_grad = gelu_grad * gelu_slope(fc_pre)
    fc_bias_grad = jnp.sum(fc_grad, axis=0)
    fc_grad_low = fc_grad.astype(jnp.bfloat16)

    def backward_seq(items):
        query_s, keys_s, values_s, attended_s, log_s, head_grad = items
        scores = (
            jnp.einsum("qhd,khd->hqk", query_s, keys_s, preferred_element_type=jnp.float32) * scale
        )
        probs = jnp.where(
            causal[None], jnp.exp(jnp.where(causal[None], scores, -1e30) - log_s), 0.0
        )
        probs_low = probs.astype(jnp.bfloat16)
        value_grad = jnp.einsum(
            "hqk,qhd->khd", probs_low, head_grad, preferred_element_type=jnp.float32
        )
        prob_grad = jnp.einsum(
            "qhd,khd->hqk", head_grad, values_s, preferred_element_type=jnp.float32
        )
        delta_row = jnp.transpose(
            jnp.sum(head_grad.astype(jnp.float32) * attended_s.astype(jnp.float32), axis=-1), (1, 0)
        )[:, :, None]
        score_grad = (probs * (prob_grad - delta_row) * scale).astype(jnp.bfloat16)
        query_grad = jnp.einsum(
            "hqk,khd->qhd", score_grad, keys_s, preferred_element_type=jnp.float32
        )
        key_grad = jnp.einsum(
            "hqk,qhd->khd", score_grad, query_s, preferred_element_type=jnp.float32
        )
        return jnp.stack(
            [
                rotate_back(query_grad, cosine, sine_vals),
                rotate_back(key_grad, cosine, sine_vals),
                value_grad,
            ],
            axis=2,
        )

    head_grads = attn_grad_low.reshape(seq_count, SEQ, local_heads, HD)
    qkv_grad = lax.map(
        backward_seq, (query, keys, values, attended, log_total, head_grads)
    ).reshape(tok_rows, qkv_cols)
    qkv_bias_grad = jnp.sum(qkv_grad, axis=0)
    qkv_grad_low = qkv_grad.astype(jnp.bfloat16)
    in_stack = jnp.concatenate([w_qkv, w_fc], axis=1)
    shard_piece = lax.all_gather(in_stack, "row", axis=0, tiled=True)
    norm_grads = jnp.stack(
        [
            lax.dot_general(
                qkv_grad_low,
                shard_piece[:, :qkv_cols],
                contract_last,
                preferred_element_type=jnp.float32,
            ),
            lax.dot_general(
                fc_grad_low,
                shard_piece[:, qkv_cols:],
                contract_last,
                preferred_element_type=jnp.float32,
            ),
        ]
    )
    part_one = wide_one
    part_two = wide_two
    row_part = lax.psum_scatter(
        jnp.concatenate(
            [
                lax.dot_general(
                    part_one, qkv_grad_low, contract_first, preferred_element_type=jnp.float32
                ),
                lax.dot_general(
                    part_two, fc_grad_low, contract_first, preferred_element_type=jnp.float32
                ),
                lax.dot_general(
                    wide_grad, attn_out, contract_first, preferred_element_type=jnp.float32
                ),
                lax.dot_general(
                    wide_grad, gelu_out, contract_first, preferred_element_type=jnp.float32
                ),
            ],
            axis=1,
        ),
        "row",
        scatter_dimension=0,
        tiled=True,
    )
    grad_rows = lax.psum(row_part, "dp")
    qkv_total = grad_rows[:, :qkv_cols]
    fc_total = grad_rows[:, qkv_cols : qkv_cols + fc_cols]
    dense_total = grad_rows[:, qkv_cols + fc_cols : qkv_cols + fc_cols + head_cols].T
    proj_total = grad_rows[:, qkv_cols + fc_cols + head_cols :].T
    norm_local = lax.psum_scatter(norm_grads, "col", scatter_dimension=2, tiled=True)
    grad_one = norm_local[0]
    grad_two = norm_local[1]
    hat_grad = grad_one * ln1_gain + grad_two * ln2_gain
    total_hat, total_cross = lax.psum(
        (jnp.sum(hat_grad, axis=1), jnp.sum(hat_grad * x_hat, axis=1)), "col"
    )
    input_grad = out_grad + inv_std * (
        hat_grad - (total_hat / D)[:, None] - x_hat * (total_cross / D)[:, None]
    )
    gain_one, shift_one, gain_two, shift_two, qkv_bias_total, fc_bias_total, out_bias_total = (
        lax.psum(
            (
                jnp.sum(grad_one * x_hat, axis=0),
                jnp.sum(grad_one, axis=0),
                jnp.sum(grad_two * x_hat, axis=0),
                jnp.sum(grad_two, axis=0),
                qkv_bias_grad,
                fc_bias_grad,
                jnp.sum(out_grad, axis=0),
            ),
            ("dp", "row"),
        )
    )
    return (
        block_output,
        input_grad,
        gain_one,
        shift_one,
        gain_two,
        shift_two,
        qkv_total,
        qkv_bias_total,
        dense_total,
        out_bias_total,
        fc_total,
        fc_bias_total,
        proj_total,
        out_bias_total,
    )


f32 = jnp.float32
bf16 = jnp.bfloat16
MESH = pl.DeviceIdType.MESH
VMEM = pltpu.VMEM
Q = 256
HALF = 4 * Q


def flip(a, b):
    return a + b - 2 * a * b


def span(start, size):
    return pl.ds(pl.multiple_of(start, size), size)


def mm(a, b):
    return jnp.dot(a, b, preferred_element_type=f32)


def mm_nt(a, b):
    return lax.dot_general(a, b, (((1,), (1,)), ((), ())), preferred_element_type=f32)


def mm_tn(a, b):
    return lax.dot_general(a, b, (((0,), (0,)), ((), ())), preferred_element_type=f32)


class Net:
    def __init__(self, send_sems, recv_sems, local_sems):
        self.k = lax.axis_index("dp")
        self.r = lax.axis_index("row")
        self.c = lax.axis_index("col")
        k, r, c = self.k, self.r, self.c
        self.core = (1 - k, r, c)
        self.x = (k, r + 1 - 2 * (r % 2), c)
        self.y = (k, r + 2 - 4 * (r // 2), c)
        near = c + 1 - 2 * (c % 2)
        self.z = (None, (k, r, near), (k, r, c + 2 - 4 * (c // 2)), (k, r, 3 - c))
        self.middle = flip(c % 2, c // 2) == 1
        self.send_sems, self.recv_sems, self.local_sems = send_sems, recv_sems, local_sems
        self.remote_count = 0
        self.local_count = 0
        self.pending = []

    def mix(self, j):
        return flip(j % 2, flip(self.c % 2, self.r % 2)) + 2 * flip(
            j // 2, flip(self.c // 2, self.r // 2)
        )

    def barrier(self):
        sem = pltpu.get_barrier_semaphore()

        def greet(peer):
            pl.semaphore_signal(sem, inc=1, device_id=peer, device_id_type=MESH)

        for peer in (self.x, self.y, self.core, self.z[1]):
            greet(peer)

        @pl.when(self.middle)
        def _():
            greet(self.z[3])
            pl.semaphore_wait(sem, 5)

        @pl.when(jnp.logical_not(self.middle))
        def _():
            pl.semaphore_wait(sem, 4)

    def slot(self):
        self.remote_count += 1
        return self.remote_count - 1

    def remote(self, src, dst, peer):
        slot = self.slot()
        copy = pltpu.make_async_remote_copy(
            src_ref=src,
            dst_ref=dst,
            send_sem=self.send_sems.at[slot],
            recv_sem=self.recv_sems.at[slot],
            device_id=peer,
            device_id_type=MESH,
        )
        copy.start()
        self.pending.append(copy)
        return copy

    def local(self, src, dst):
        copy = pltpu.make_async_copy(src, dst, self.local_sems.at[self.local_count])
        self.local_count += 1
        copy.start()
        return copy

    def sent(self, copy):
        copy.wait_send()
        self.pending = [other for other in self.pending if other is not copy]

    def drain(self):
        for copy in self.pending:
            copy.wait_send()


class Gather:
    def __init__(self, net, shard, full, by_rows):
        self.net, self.shard, self.full, self.by_rows = net, shard, full, by_rows
        self.depth = Q // 2 if by_rows else shard.shape[0] // 2
        self.placed = []

    def own(self, half, part=None):
        if self.by_rows:
            if part is None:
                return self.shard.at[span(half * Q, Q), :]
            return self.shard.at[span(half * Q + part * self.depth, self.depth), :]
        rows = slice(None) if part is None else pl.ds(part * self.depth, self.depth)
        return self.shard.at[rows, span(half * Q, Q)]

    def chunk(self, s, i, part=None):
        start = s * HALF + i * Q
        if self.by_rows:
            if part is None:
                return self.full.at[pl.ds(start, Q), :]
            return self.full.at[pl.ds(start + part * self.depth, self.depth), :]
        rows = slice(None) if part is None else pl.ds(part * self.depth, self.depth)
        return self.full.at[rows, pl.ds(start, Q)]

    def place_own(self):
        net = self.net
        self.placed = [
            net.local(self.own(net.k), self.chunk(0, 0)),
            net.local(self.own(1 - net.k), self.chunk(1, 0)),
        ]

    def send_own(self):
        net, k = self.net, self.net.k
        self.y0 = net.remote(self.own(k, 0), self.chunk(0, 2, 0), net.y)
        self.x1 = net.remote(self.own(k, 1), self.chunk(0, 1, 1), net.x)
        self.y1 = net.remote(self.own(k, 1), self.chunk(0, 2, 1), net.y)
        self.x0 = net.remote(self.own(k, 0), self.chunk(0, 1, 0), net.x)

    def forward(self):
        net = self.net
        self.y0.wait_recv()
        self.d0 = net.remote(self.chunk(0, 2, 0), self.chunk(0, 3, 0), net.x)
        self.x1.wait_recv()
        self.d1 = net.remote(self.chunk(0, 1, 1), self.chunk(0, 3, 1), net.y)

    def swap_near(self):
        net = self.net
        self.x0.wait_recv()
        self.c1 = net.remote(self.chunk(0, 1), self.chunk(1, 1), net.core)
        self.y1.wait_recv()
        self.c2 = net.remote(self.chunk(0, 2), self.chunk(1, 2), net.core)

    def swap_far(self):
        net = self.net
        self.d0.wait_recv()
        self.d1.wait_recv()
        self.c3 = net.remote(self.chunk(0, 3), self.chunk(1, 3), net.core)

    def ready(self):
        for copy in (self.c1, self.c2, self.c3):
            copy.wait_recv()
        for copy in self.placed:
            copy.wait()

    def release(self):
        for copy in (self.d0, self.d1, self.c1, self.c2, self.c3):
            self.net.sent(copy)


class Line:
    def __init__(self, net, slots):
        self.net, self.slots = net, slots
        self.ids = [None] + [net.slot() for _ in range(3)]
        self.sends = []

    def copy(self, src, dst, peer, send):
        net = self.net
        return pltpu.make_async_remote_copy(
            src_ref=self.slots.at[src],
            dst_ref=self.slots.at[dst],
            send_sem=net.send_sems.at[send],
            recv_sem=net.recv_sems.at[self.ids[dst]],
            device_id=peer,
            device_id_type=MESH,
        )

    def start(self):
        net = self.net
        self.first = self.copy(0, 1, net.z[1], self.ids[1])
        self.first.start()
        self.hops = [
            self.copy(0, 3, net.z[3], self.ids[2]),
            self.copy(1, 2, net.z[3], self.ids[3]),
            self.copy(3, 2, net.z[1], net.slot()),
            self.copy(2, 3, net.z[1], net.slot()),
        ]

        @pl.when(net.middle)
        def _():
            self.hops[0].start()

    def arrived(self, slot):
        return self.copy(0, slot, self.net.z[1], self.ids[slot])

    def step(self, number):
        slot = (1, 3, 2)[number]

        @pl.when(self.net.middle)
        def _():
            self.arrived(slot).wait_recv()
            self.hops[number + 1].start()

    def ready(self):
        @pl.when(jnp.logical_not(self.net.middle))
        def _():
            for slot in (1, 2, 3):
                self.arrived(slot).wait_recv()

    def drain(self):
        self.first.wait_send()

        @pl.when(self.net.middle)
        def _():
            for hop in self.hops:
                hop.wait_send()


class Fold:
    def __init__(self, net, blocks, inbox):
        self.net, self.blocks, self.inbox = net, blocks, inbox
        hops = ((3, None, 0), (2, None, 1), (1, None, 2), (None, 0, 3), (None, 1, 4), (None, 3, 0))
        self.copies = []
        for n, (block, slot, dest) in enumerate(hops):
            number = net.slot()
            self.copies.append(
                pltpu.make_async_remote_copy(
                    src_ref=blocks.at[block] if slot is None else inbox.at[slot],
                    dst_ref=inbox.at[dest],
                    send_sem=net.send_sems.at[number],
                    recv_sem=net.recv_sems.at[number],
                    device_id=net.z[3] if n in (3, 4) else net.z[1],
                    device_id_type=MESH,
                )
            )

    def start(self, first, last):
        @pl.when(jnp.logical_not(self.net.middle))
        def _():
            for copy in self.copies[first:last]:
                copy.start()

    def step(self, number):
        slot, block = ((0, 2), (1, 3), (3, 1))[number]
        inbox, blocks = self.inbox, self.blocks

        @pl.when(self.net.middle)
        def _():
            self.copies[(0, 1, 3)[number]].wait_recv()

            def add(n, _):
                at = span(n * 64, 64)
                total = inbox[slot, at, :].astype(f32) + blocks[block, at, :].astype(f32)
                inbox[slot, at, :] = total.astype(bf16)
                return 0

            lax.fori_loop(0, inbox.shape[1] // 64, add, 0)
            self.copies[3 + number].start()

    def total(self, use):
        def gather(*slots):
            def add(n, _):
                at = span(n * 64, 64)
                value = self.blocks[0, at, :].astype(f32)
                for slot in slots:
                    value = value + self.inbox[slot, at, :].astype(f32)
                use(at, value)
                return 0

            lax.fori_loop(0, self.inbox.shape[1] // 64, add, 0)

        @pl.when(self.net.middle)
        def _():
            self.copies[2].wait_recv()
            self.copies[4].wait_recv()
            gather(2, 4)

        @pl.when(jnp.logical_not(self.net.middle))
        def _():
            self.copies[5].wait_recv()
            gather(0)

    def drain(self):
        @pl.when(self.net.middle)
        def _():
            for copy in self.copies[3:]:
                copy.wait_send()

        @pl.when(jnp.logical_not(self.net.middle))
        def _():
            for copy in self.copies[:3]:
                copy.wait_send()


def turn(low, tables, sign):
    lane = lax.broadcasted_iota(jnp.int32, low.shape, 1)
    swung = jnp.where(lane < ROT // 2, pltpu.roll(low, 96, 1), pltpu.roll(low, 32, 1))
    return low * tables[0] + sign * (tables[1] * swung)


class Tiles:
    def __init__(self, slots, sems):
        self.slots, self.sems = slots, sems

    def write(self, count, product, place, depth):
        def body(n, _):
            slot = n % 2
            source = self.slots.at[slot, pl.ds(0, depth), :]
            copy = pltpu.make_async_copy(source, place(n), self.sems.at[slot])

            @pl.when(n >= 2)
            def _():
                copy.wait()

            self.slots[slot, 0:depth, :] = product(n).astype(bf16)
            copy.start()
            return 0

        lax.fori_loop(0, count, body, 0)
        for slot in range(2):
            source = self.slots.at[slot, pl.ds(0, depth), :]
            pltpu.make_async_copy(source, place(slot), self.sems.at[slot]).wait()


class Reduce:
    def __init__(self, net, partial, joined, near, far, by_rows, in_vmem=False):
        self.in_vmem = in_vmem
        self.net, self.partial, self.by_rows = net, partial, by_rows
        self.joined, self.near, self.far = joined, near, far
        self.depth = Q // 2 if by_rows else partial.shape[0] // 2

    def chunk(self, i, half):
        if self.by_rows:
            return self.partial.at[pl.ds(i * Q + half * self.depth, self.depth), :]
        return self.partial.at[pl.ds(half * self.depth, self.depth), pl.ds(i * Q, Q)]

    def whole(self):
        if self.by_rows:
            return self.partial.at[pl.ds(0, Q), :]
        return self.partial.at[:, pl.ds(0, Q)]

    def rows(self, half):
        return pl.ds(half * self.depth, self.depth)

    def start(self):
        net = self.net
        self.a = net.remote(self.chunk(3, 0), self.joined.at[0], net.x)
        self.b = net.remote(self.chunk(3, 1), self.joined.at[1], net.y)
        self.near_a = net.remote(self.chunk(1, 0), self.near.at[self.rows(0), :], net.x)
        self.near_b = net.remote(self.chunk(2, 1), self.near.at[self.rows(1), :], net.y)

    def join(self, parts):
        net = self.net
        loads = [net.local(self.chunk(2, 0), parts[0]), net.local(self.chunk(1, 1), parts[1])]
        hops = []
        for half, copy, peer in ((0, self.a, net.y), (1, self.b, net.x)):
            loads[half].wait()
            copy.wait_recv()
            tile = 64

            def add(n, _, half=half):
                at = span(n * tile, tile)
                total = self.joined[half, at, :].astype(f32) + parts[half][at, :].astype(f32)
                self.joined[half, at, :] = total.astype(bf16)
                return 0

            lax.fori_loop(0, self.depth // tile, add, 0)
            hops.append(net.remote(self.joined.at[half], self.far.at[self.rows(half), :], peer))
        self.far_a, self.far_b = hops

    def prepare(self, buffers):
        net = self.net
        self.buffers = list(buffers)
        self.loads = [net.local(self.whole(), buffers[0])]
        for copy in (self.near_a, self.near_b):
            copy.wait_recv()
        if self.in_vmem:
            self.buffers[1:3] = [self.near, self.far]
        else:
            self.loads.append(net.local(self.near, buffers[1]))

    def finish(self, out):
        net, buffers = self.net, self.buffers
        arrivals = (self.far_a, self.far_b)
        last = []
        if not self.in_vmem:
            for half, copy in enumerate(arrivals):
                copy.wait_recv()
                rows = self.rows(half)
                last.append(net.local(self.far.at[rows, :], buffers[2].at[rows, :]))
        for copy in self.loads:
            copy.wait()
        tile = 64
        self.here, self.there = [], []
        for half in range(2):
            if self.in_vmem:
                arrivals[half].wait_recv()
            else:
                last[half].wait()

            def add(n, _, half=half):
                at = span(half * self.depth + n * tile, tile)
                parts = [buffer[at, :].astype(f32) for buffer in buffers[:3]]
                buffers[3][at, :] = (parts[0] + parts[1] + parts[2]).astype(bf16)
                return 0

            lax.fori_loop(0, self.depth // tile, add, 0)
            source = buffers[3].at[self.rows(half), :]
            if self.by_rows:
                place = out.at[span(net.k * Q + half * self.depth, self.depth), :]
            else:
                place = out.at[self.rows(half), span(net.k * Q, Q)]
            self.here.append(net.local(source, place))
            self.there.append(net.remote(source, place, net.core))

    def done(self):
        for copy in self.here:
            copy.wait()
        for copy in self.there:
            copy.wait_recv()


def block_kernel(
    x, og, w_qkv, w_dense, w_fc, w_proj, t_turn,
    i_gain_1, i_bias_1, i_gain_2, i_bias_2, i_b_qkv, i_b_fc, i_b_dense, i_b_proj,
    o_proj, o_qkv, o_fc, o_dense, o_block, o_input, o_small,
    all_proj, r_proj, r_qkv, r_fc, r_dense, n_proj, f_proj, n_qkv, f_qkv, n_fc, f_fc,
    g_qkv, g_dense, g_fc, g_tail, xs, ys, pks, stats, rows, h1c, h1s, h2c, h2s, dyc, dys, xh,
    qb, kb, vb, probs, probs_low, oc, dob, dqc, gc, slope, dabt, stage,
    out_recv, hat_recv, j_proj, j_qkv, j_fc, j_dense, n_dense, f_dense, tables, vecs, bias, packs, small,
    gain_1, bias_1, gain_2, bias_2, b_qkv, b_fc, b_dense, b_proj,
    send_sems, recv_sems, local_sems, stage_sems,
):
    tok = x.shape[0]
    heads = qb.shape[0]
    width = gc.shape[1]
    scale = 1.0 / math.sqrt(HD)
    net = Net(send_sems, recv_sems, local_sems)
    net.barrier()
    qkv = Gather(net, w_qkv, g_qkv, True)
    dense = Gather(net, w_dense, g_dense, False)
    fc = Gather(net, w_fc, g_fc, True)
    proj = Gather(net, w_proj, all_proj, False)
    qkv.send_own()
    dense.send_own()
    load_x = net.local(x, probs.at[0])
    vectors = [
        net.local(i_gain_1, gain_1), net.local(i_bias_1, bias_1), net.local(i_gain_2, gain_2),
        net.local(i_bias_2, bias_2), net.local(i_b_qkv, b_qkv), net.local(i_b_fc, b_fc),
        net.local(i_b_dense, b_dense), net.local(i_b_proj, b_proj),
    ]
    load_og = net.local(og, probs.at[1])
    load_turn = net.local(t_turn, tables)
    tiles = Tiles(stage, stage_sems)
    mine = pl.ds(0, tok)
    theirs = pl.ds(tok, tok)

    step = 128
    lane = lax.broadcasted_iota(jnp.int32, (step, 128), 1)
    load_x.wait()

    def local_norm(n, _):
        at = span(n * step, step)
        block = probs[0, at, :]
        mean = jnp.mean(block, axis=1, keepdims=True)
        centred = block - mean
        var = jnp.mean(centred * centred, axis=1, keepdims=True)
        stats[at, :] = jnp.where(lane == 0, mean, jnp.where(lane == 1, var, 0.0))
        return 0

    lax.fori_loop(0, tok // step, local_norm, 0)
    pks[0] = stats[...].T[0:8]
    for copy in vectors:
        copy.wait()
    for n, vector in enumerate((gain_1, bias_1, gain_2, bias_2)):
        pks[0, 2 + n : 3 + n, :] = vector[...].reshape(1, 512)
    p_line = Line(net, pks)
    p_line.start()
    for weight in (qkv, dense, fc):
        weight.place_own()
    bias[...] = jnp.zeros_like(bias)
    bias[3:4, 0 : b_qkv.shape[0]] = b_qkv[...].reshape(1, b_qkv.shape[0])
    bias[4:5, :] = b_fc[...].reshape(1, width)
    bias[5:6, 0:512] = (b_dense[...] + b_proj[...]).reshape(1, 512)
    rows[...] = jnp.zeros_like(rows)
    load_og.wait()

    def local_grad(n, _):
        at = span(n * step, step)
        block = probs[1, at, :]
        ys[0, at, :] = block.astype(bf16)
        bias[1:2, 0:512] += jnp.sum(block, axis=0, keepdims=True)
        return 0

    lax.fori_loop(0, tok // step, local_grad, 0)
    for hop in range(3):
        p_line.step(hop)
    p_line.ready()
    means = [pks[j, 0:1, :] for j in range(4)]
    mu = (means[0] + means[1] + means[2] + means[3]) * 0.25
    spread = [pks[j, 1:2, :] + (means[j] - mu) * (means[j] - mu) for j in range(4)]
    rows[0:1, :] = mu
    rows[1:2, :] = lax.rsqrt((spread[0] + spread[1] + spread[2] + spread[3]) * 0.25 + epsilon)
    stats[...] = rows[...].T

    def own_norm(n, _):
        at = span(n * step, step)
        hats = (probs[0, at, :] - stats[at, 0:1]) * stats[at, 1:2]
        xs[0, at, :] = (hats * pks[0, 2:3, :] + pks[0, 3:4, :]).astype(bf16)
        return 0

    lax.fori_loop(0, tok // step, own_norm, 0)
    x_line = Line(net, xs)
    y_line = Line(net, ys)
    x_line.start()
    qkv.forward()
    x_line.step(0)
    x_line.step(1)
    fc.send_own()
    dense.forward()
    qkv.swap_near()
    x_line.step(2)
    y_line.start()
    dense.swap_near()
    qkv.swap_far()
    x_line.ready()
    fc.forward()
    proj.send_own()

    for s in range(2):
        for j in range(4):
            lanes = span(flip(s, net.k) * Q, Q)
            dest = span(net.mix(j) * Q, Q)
            wide = span(s * HALF + net.mix(j) * Q, Q)
            vecs[0:4, wide] = pks[j, 2:6, lanes]

            def norm(n, _, s=s, j=j, lanes=lanes, dest=dest, wide=wide):
                at = span(n * step, step)
                one = xs[j, at, lanes]
                hats = (one.astype(f32) - pks[j, 3:4, lanes]) * (1.0 / pks[j, 2:3, lanes])
                xh[at, wide] = hats.astype(bf16)
                (h1s if s else h1c)[at, dest] = one
                two = hats * pks[j, 4:5, lanes] + pks[j, 5:6, lanes]
                (h2s if s else h2c)[at, dest] = two.astype(bf16)
                return 0

            lax.fori_loop(0, tok // step, norm, 0)
    swap_h1 = net.remote(h1s, h1c.at[theirs, :], net.core)
    swap_h2 = net.remote(h2s, h2c.at[theirs, :], net.core)
    y_line.step(0)
    load_turn.wait()
    qkv.ready()

    def project(n, _):
        cols = span(n * 3 * HD, 3 * HD)
        acc = mm(h1c[mine, :], g_qkv[0:HALF, cols]) + mm(h1s[...], g_qkv[HALF:, cols])
        acc = acc + bias[3:4, cols]
        qb[n, :, 0:128] = turn(acc[:, 0:128], tables, 1.0).astype(bf16)
        qb[n, :, 128:HD] = acc[:, 128:HD].astype(bf16)
        kb[n, :, 0:128] = turn(acc[:, HD : HD + 128], tables, 1.0).astype(bf16)
        kb[n, :, 128:HD] = acc[:, HD + 128 : 2 * HD].astype(bf16)
        vb[n] = acc[:, 2 * HD :].astype(bf16)
        return 0

    lax.fori_loop(0, heads, project, 0)
    y_line.step(1)
    chunks = tok // step

    def attend(n, _):
        head, chunk = n // chunks, n % chunks
        at = span(chunk * step, step)
        scores = mm_nt(qb[head, at, :], kb[head]) * scale
        token = lax.broadcasted_iota(jnp.int32, (step, tok), 0) + chunk * step
        allowed = token >= lax.broadcasted_iota(jnp.int32, (step, tok), 1)
        scores = jnp.where(allowed, scores, -1e30)
        top = jnp.max(scores, axis=1, keepdims=True)
        raised = jnp.where(allowed, jnp.exp(scores - top), 0.0)
        weight = raised / jnp.sum(raised, axis=1, keepdims=True)
        probs[head, at, :] = weight
        low = weight.astype(bf16)
        probs_low[head, at, :] = low
        oc[at, span(head * HD, HD)] = mm(low, vb[head]).astype(bf16)
        return 0

    lax.fori_loop(0, heads * chunks, attend, 0)
    swap_o = net.remote(oc.at[mine, :], oc.at[theirs, :], net.core)
    dense.swap_far()
    fc.swap_near()
    y_line.step(2)
    fc.swap_far()
    fc.ready()

    def expand(n, _):
        cols = span(n * 512, 512)
        a = mm(h2c[mine, :], g_fc[0:HALF, cols]) + mm(h2s[...], g_fc[HALF:, cols])
        a = a + bias[4:5, cols]
        rise = 0.5 * (1.0 + lax.erf(a * 0.7071067811865476))
        gc[mine, cols] = (a * rise).astype(bf16)
        slope[:, cols] = (rise + a * 0.3989422804014327 * jnp.exp(-0.5 * a * a)).astype(bf16)
        return 0

    lax.fori_loop(0, width // 1024, expand, 0)
    proj.forward()
    lax.fori_loop(width // 1024, width // 512, expand, 0)
    swap_g = net.remote(gc.at[mine, :], gc.at[theirs, :], net.core)
    y_line.ready()
    for s in range(2):
        for j in range(4):
            lanes = span(flip(s, net.k) * Q, Q)
            dest = span(net.mix(j) * Q, Q)
            (dys if s else dyc)[mine, dest] = ys[j, :, lanes]
    swap_dy = net.remote(dys, dyc.at[theirs, :], net.core)
    dense.ready()
    dob[...] = (
        mm_nt(dyc[mine, :], g_dense[:, 0:HALF]) + mm_nt(dys[...], g_dense[:, HALF:])
    ).astype(bf16)

    red_proj = Reduce(net, r_proj, j_proj, n_proj, f_proj, False)
    red_qkv = Reduce(net, r_qkv, j_qkv, n_qkv, f_qkv, True)
    red_fc = Reduce(net, r_fc, j_fc, n_fc, f_fc, True)
    red_dense = Reduce(net, r_dense, j_dense, n_dense, f_dense, False, True)
    swap_g.wait_recv()
    swap_dy.wait_recv()
    tall = width // 2
    tiles.write(
        4,
        lambda n: mm_tn(gc[:, span(n // 2 * tall, tall)], dyc[:, span(n % 2 * 512, 512)]),
        lambda n: r_proj.at[span(n // 2 * tall, tall), span(n % 2 * 512, 512)],
        tall,
    )
    proj.swap_near()
    red_proj.start()

    def keep(head, part, at, value, rotated):
        base = head * 3 * HD + part * HD
        if rotated:
            low = turn(value[:, 0:128], [tables[t, at, :] for t in range(2)], -1.0)
            dqc[at, pl.ds(pl.multiple_of(base, 128), 128)] = low.astype(bf16)
            bias[0:1, pl.ds(pl.multiple_of(base, 128), 128)] += jnp.sum(low, axis=0, keepdims=True)
            value, base, size = value[:, 128:], base + 128, 128
        else:
            size = HD
        cols = pl.ds(pl.multiple_of(base, 128), size)
        dqc[at, cols] = value.astype(bf16)
        bias[0:1, cols] += jnp.sum(value, axis=0, keepdims=True)

    def attend_back(head, _):
        cols = span(head * HD, HD)

        def chunk_back(n, _):
            at = span(n * step, step)
            grad = dob[at, cols]
            delta = jnp.sum(grad.astype(f32) * oc[at, cols].astype(f32), axis=1, keepdims=True)
            spread = mm_nt(grad, vb[head]) - delta
            low = (probs[head, at, :] * spread * scale).astype(bf16)
            probs_low[head, at, :] = low
            keep(head, 0, at, mm(low, kb[head]), True)
            return 0

        keep(head, 2, mine, mm_tn(probs_low[head], dob[:, cols]), False)
        lax.fori_loop(0, chunks, chunk_back, 0)
        keep(head, 1, mine, mm_tn(probs_low[head], qb[head]), True)
        return 0

    lax.fori_loop(0, heads, attend_back, 0)
    proj.swap_far()
    swap_dq = net.remote(dqc.at[mine, :], dqc.at[theirs, :], net.core)
    net.sent(swap_h1)
    net.sent(swap_h2)
    for s in range(2):

        def back_first(n, _, s=s):
            wide = span(s * HALF + n * 512, 512)
            grad = mm_nt(dqc[mine, :], g_qkv[wide, :])
            (h2s if s else h1s)[:, span(n * 512, 512)] = (grad * vecs[0:1, wide]).astype(bf16)
            vecs[4:5, wide] = jnp.sum(grad * xh[:, wide].astype(f32), axis=0, keepdims=True)
            vecs[5:6, wide] = jnp.sum(grad, axis=0, keepdims=True)
            return 0

        lax.fori_loop(0, HALF // 512, back_first, 0)

    proj.ready()
    qkv.release()
    loads = [
        net.local(w_proj.at[:, span(net.k * Q, Q)], g_qkv.at[:, pl.ds(0, Q)]),
        net.local(w_proj.at[:, span((1 - net.k) * Q, Q)], g_qkv.at[:, pl.ds(HALF, Q)]),
        net.local(all_proj.at[:, pl.ds(Q, 3 * Q)], g_qkv.at[:, pl.ds(Q, 3 * Q)]),
        net.local(all_proj.at[:, pl.ds(5 * Q, Q)], g_qkv.at[:, pl.ds(5 * Q, Q)]),
        net.local(all_proj.at[:, pl.ds(6 * Q, 2 * Q)], g_tail),
    ]
    swap_o.wait_recv()
    attn = oc.shape[1]
    tiles.write(
        2,
        lambda n: mm_tn(oc[...], dyc[:, span(n * 512, 512)]),
        lambda n: r_dense.at[:, span(n * 512, 512)],
        attn,
    )
    swap_h1.wait_recv()
    swap_dq.wait_recv()
    tiles.write(
        dqc.shape[1] // 512,
        lambda n: mm_tn(h1c[...], dqc[:, span(n * 512, 512)]),
        lambda n: r_qkv.at[:, span(n * 512, 512)],
        HALF,
    )
    red_qkv.start()
    red_dense.start()

    for copy in loads:
        copy.wait()
    x_line.drain()
    y_line.drain()

    def put_out(p, product):
        s, i = p // 4, p % 4
        out = product + mm(oc[mine, :], g_dense[:, span(p * Q, Q)])
        xs[net.mix(i), :, span(flip(s, net.k) * Q, Q)] = out.astype(bf16)

    def project_head(p, _):
        put_out(p, mm(gc[mine, :], g_qkv[:, span(p * Q, Q)]))
        return 0

    def project_tail(p, _):
        put_out(6 + p, mm(gc[mine, :], g_tail[:, span(p * Q, Q)]))
        return 0

    lax.fori_loop(0, 6, project_head, 0)
    lax.fori_loop(0, 2, project_tail, 0)
    out_fold = Fold(net, xs, out_recv)
    out_fold.start(0, 2)

    def back_fc(n, _):
        cols = span(n * 512, 512)
        grad = mm_nt(dyc[mine, :], g_qkv[cols, 0:HALF])
        grad = grad + mm_nt(dys[:, 0:512], g_qkv[cols, HALF : 6 * Q])
        grad = grad + mm_nt(dys[:, 512:], g_tail[cols, :])
        grad = grad * slope[:, cols].astype(f32)
        bias[2:3, cols] = jnp.sum(grad, axis=0, keepdims=True)
        slope[:, cols] = grad.astype(bf16)
        return 0

    lax.fori_loop(0, width // 512, back_fc, 0)
    dab = slope
    swap_da = net.remote(dab, dabt, net.core)
    red_proj.join([g_tail.at[pl.ds(0, tall), pl.ds(0, Q)], g_tail.at[pl.ds(tall, tall), pl.ds(0, Q)]])
    stats[...] = jnp.zeros_like(stats)
    lane = lax.broadcasted_iota(jnp.int32, (tok, 128), 1)

    def back_norm(j, _):
        for s in range(2):
            lanes = span(flip(s, net.k) * Q, Q)
            dest = span(net.mix(j) * Q, Q)
            wide = span(s * HALF + net.mix(j) * Q, Q)
            grad = mm_nt(dab[...], g_fc[wide, :])
            hats = xh[:, wide].astype(f32)
            packs[j, 2:4, lanes] = vecs[4:6, wide]
            packs[j, 4:5, lanes] = jnp.sum(grad * hats, axis=0, keepdims=True)
            packs[j, 5:6, lanes] = jnp.sum(grad, axis=0, keepdims=True)
            joint = (h2s if s else h1s)[:, dest].astype(f32) + grad * vecs[2:3, wide]
            ys[j, :, lanes] = joint.astype(bf16)
            one = jnp.sum(joint, axis=1, keepdims=True)
            two = jnp.sum(joint * hats, axis=1, keepdims=True)
            stats[...] += jnp.where(lane == 0, one, jnp.where(lane == 1, two, 0.0))
        return 0

    lax.fori_loop(0, 4, back_norm, 0)

    fc.release()
    turned = stats[...].T
    for j in range(4):
        packs[j, 0:2, :] = turned[0:2]
        packs[j, 6:8, :] = jnp.zeros((2, tok), f32)
    pack_copies = [net.remote(packs.at[j], packs.at[3 + j], net.z[j]) for j in (1, 2, 3)]
    hat_fold = Fold(net, ys, hat_recv)
    hat_fold.start(0, 2)
    out_fold.start(2, 3)
    hat_fold.start(2, 3)
    out_fold.step(0)
    swap_h2.wait_recv()
    swap_da.wait_recv()

    def grad_fc(n):
        cols = span(n * 512, 512)
        return mm_tn(h2c[mine, :], dab[:, cols]) + mm_tn(h2c[theirs, :], dabt[:, cols])

    tiles.write(width // 512, grad_fc, lambda n: r_fc.at[:, span(n * 512, 512)], HALF)
    red_fc.start()
    out_fold.step(1)

    def strips(base, n, columns):
        return g_fc.at[pl.ds(base + n * Q, Q), pl.ds(0, columns)]

    out_fold.step(2)
    for copy in pack_copies:
        copy.wait_recv()
    total = packs[0] + packs[4] + packs[5] + packs[6]
    rows[2:4, :] = total[0:2, :]
    stats[...] = rows[...].T
    small[0, 0:4, :] = total[2:6, :]
    for n in range(3):
        small[0, 4 + n : 5 + n, :] = bias[0:1, n * 512 : n * 512 + 512]
    for n in range(4):
        small[0, 7 + n : 8 + n, :] = bias[2:3, n * 512 : n * 512 + 512]
    small[0, 11:12, :] = bias[1:2, 0:512]
    small[0, 12:16, :] = jnp.zeros((4, 512), f32)
    net.remote(small.at[0], small.at[1], net.core).wait_recv()
    own_rows = span(net.k * 8, 8)
    small[2 + net.r, 0:8, :] = small[0, own_rows, :] + small[1, own_rows, :]
    place = small.at[2 + net.r, pl.ds(0, 8), :]
    across = (net.k, 3 - net.r, net.c)
    small_copies = [net.remote(place, place, peer) for peer in (net.x, net.y, across)]
    reload_x = net.local(x, probs.at[1])
    red_proj.prepare([g_qkv.at[:, pl.ds(n * Q, Q)] for n in range(4)])
    red_proj.finish(o_proj)
    hat_fold.step(0)
    red_fc.join([g_fc.at[pl.ds(6 * Q + n * (Q // 2), Q // 2), :] for n in range(2)])
    red_qkv.join(
        [g_fc.at[pl.ds(7 * Q + n * (Q // 2), Q // 2), pl.ds(0, 6 * Q)] for n in range(2)]
    )
    hat_fold.step(1)
    hat_fold.step(2)
    reload_x.wait()

    def close_out(at, value):
        probs[0, at, :] = probs[1, at, :] + value + bias[5:6, 0:512]

    out_fold.total(close_out)
    keep_block = net.local(probs.at[0], o_block)
    keep_block.wait()
    reload_og = net.local(og, probs.at[0])
    red_dense.join([g_tail.at[pl.ds(n * attn // 2, attn // 2), pl.ds(0, Q)] for n in range(2)])
    red_fc.prepare([strips(4 * Q, n, 8 * Q) for n in range(4)])
    red_qkv.prepare([strips(0, n, 6 * Q) for n in range(4)])
    red_dense.prepare([g_tail.at[pl.ds(n * attn, attn), pl.ds(Q, Q)] for n in range(4)])
    for copy in small_copies:
        copy.wait_recv()
    small[6, own_rows, :] = small[2, 0:8] + small[3, 0:8] + small[4, 0:8] + small[5, 0:8]
    place = small.at[6, own_rows, :]
    swap_small = net.remote(place, place, net.core)
    reload_og.wait()

    def close_hat(at, value):
        mu, rstd = stats[at, 0:1], stats[at, 1:2]
        hats = (probs[1, at, :] - mu) * rstd
        mean, cross = stats[at, 2:3] * (1.0 / D), stats[at, 3:4] * (1.0 / D)
        probs[0, at, :] += rstd * (value - mean - hats * cross)

    hat_fold.total(close_hat)
    keep_input = net.local(probs.at[0], o_input)
    swap_small.wait_recv()
    keep_small = net.local(small.at[6], o_small)
    red_fc.finish(o_fc)
    red_qkv.finish(o_qkv)
    red_dense.finish(o_dense)
    for weight in (red_proj, red_qkv, red_fc, red_dense):
        weight.done()
    keep_small.wait()
    keep_input.wait()
    p_line.drain()
    out_fold.drain()
    hat_fold.drain()
    net.drain()


def call_block(*args):
    x, w_qkv, w_dense, w_fc = args[0], args[2], args[3], args[4]
    tok = x.shape[0]
    n_qkv, n_attn, n_fc = w_qkv.shape[1], w_dense.shape[0], w_fc.shape[1]
    heads = n_attn // HD
    wide = 2 * HALF
    any_spec = pl.BlockSpec(memory_space=pl.ANY)
    shape = jax.ShapeDtypeStruct
    pieces = ((n_fc, Q), (Q, n_qkv), (Q, n_fc), (n_attn, Q))
    outs = [
        shape((n_fc, 2 * Q), bf16), shape((2 * Q, n_qkv), bf16),
        shape((2 * Q, n_fc), bf16), shape((n_attn, 2 * Q), bf16),
        shape((tok, 512), f32), shape((tok, 512), f32), shape((16, 512), f32),
        shape((n_fc, wide), bf16), shape((n_fc, HALF), bf16), shape((HALF, n_qkv), bf16),
        shape((HALF, n_fc), bf16), shape((n_attn, HALF), bf16),
    ]
    outs += [shape(piece, bf16) for piece in pieces[:3] for _ in range(2)]
    scratch = [
        VMEM((wide, n_qkv), bf16), VMEM((n_attn, wide), bf16), VMEM((wide, n_fc), bf16),
        VMEM((n_fc, 2 * Q), bf16),
        VMEM((4, tok, 512), bf16), VMEM((4, tok, 512), bf16), VMEM((4, 8, tok), f32),
        VMEM((tok, 128), f32), VMEM((128, tok), f32),
        VMEM((2 * tok, HALF), bf16), VMEM((tok, HALF), bf16),
        VMEM((2 * tok, HALF), bf16), VMEM((tok, HALF), bf16),
        VMEM((2 * tok, HALF), bf16), VMEM((tok, HALF), bf16), VMEM((tok, wide), bf16),
        VMEM((heads, tok, HD), bf16), VMEM((heads, tok, HD), bf16), VMEM((heads, tok, HD), bf16),
        VMEM((heads, tok, tok), f32), VMEM((heads, tok, tok), bf16),
        VMEM((2 * tok, n_attn), bf16), VMEM((tok, n_attn), bf16), VMEM((2 * tok, n_qkv), bf16),
        VMEM((2 * tok, n_fc), bf16), VMEM((tok, n_fc), bf16), VMEM((tok, n_fc), bf16),
        VMEM((2, HALF, 512), bf16),
        VMEM((5, tok, 512), bf16), VMEM((5, tok, 512), bf16),
    ]
    scratch += [VMEM((2,) + ((r // 2, c)), bf16) for r, c in pieces]
    scratch += [VMEM(pieces[3], bf16)] * 2
    scratch += [
        VMEM((2, tok, 128), f32),
        VMEM((8, wide), f32), VMEM((8, n_fc), f32), VMEM((7, 8, tok), f32), VMEM((7, 16, 512), f32),
        VMEM((512,), f32), VMEM((512,), f32), VMEM((512,), f32), VMEM((512,), f32),
        VMEM((n_qkv,), f32), VMEM((n_fc,), f32), VMEM((512,), f32), VMEM((512,), f32),
        pltpu.SemaphoreType.DMA((128,)), pltpu.SemaphoreType.DMA((128,)),
        pltpu.SemaphoreType.DMA((64,)), pltpu.SemaphoreType.DMA((2,)),
    ]
    return pl.pallas_call(
        block_kernel,
        name="block",
        out_shape=outs,
        in_specs=[any_spec] * 15,
        out_specs=[any_spec] * len(outs),
        scratch_shapes=scratch,
        compiler_params=pltpu.CompilerParams(
            collective_id=1, has_side_effects=True, vmem_limit_bytes=67043328
        ),
    )(*args)


def turn_tables(length):
    half_rot = ROT // 2
    frequency = (10000.0 ** (-np.arange(half_rot, dtype=np.float32) * (2.0 / ROT))).astype(np.float32)
    angles = np.arange(length, dtype=np.float32)[:, None] * frequency[None, :]
    tables = np.zeros((2, length, 128), np.float32)
    tables[0] = 1.0
    tables[0, :, :half_rot] = tables[0, :, half_rot:ROT] = np.cos(angles)
    tables[1, :, :half_rot] = -np.sin(angles)
    tables[1, :, half_rot:ROT] = np.sin(angles)
    return tables


def close_kernel(cuts, *refs):
    count = len(cuts)
    refs = list(refs)
    sources, small = [refs.pop(0) for _ in cuts], refs.pop(0)
    outs, vectors = [refs.pop(0) for _ in cuts], [refs.pop(0) for _ in range(8)]
    lows, sums = [refs.pop(0) for _ in cuts], refs.pop(0)
    wides, lines = [refs.pop(0) for _ in range(4)], [refs.pop(0) for _ in range(8)]
    in_sems, out_sems = refs
    loads, stores = [], []
    for n, cut in enumerate(cuts):
        rows = sources[n].shape[0] // cut
        for part in range(cut):
            at = pl.ds(part * rows, rows)
            number = len(loads)
            wide = wides[n] if n < len(wides) else lows[n]
            loads.append(
                pltpu.make_async_copy(sources[n].at[at, :], lows[n].at[at, :], in_sems.at[number])
            )
            stores.append(
                (n, at, pltpu.make_async_copy(wide.at[at, :], outs[n].at[at, :], out_sems.at[number]))
            )
    total = len(loads)
    load_small = pltpu.make_async_copy(small, sums, in_sems.at[total])
    for copy in loads:
        copy.start()
    load_small.start()
    for load, (n, at, store) in zip(loads, stores):
        load.wait()
        if n < len(wides):
            wides[n][at, :] = lows[n][at, :].astype(f32)
        store.start()
    load_small.wait()
    last = []
    for n, (row, line, vector) in enumerate(zip((0, 1, 2, 3, 4, 7, 11, 11), lines, vectors)):
        for part in range(line.shape[0] // 512):
            line[part * 512 : part * 512 + 512] = sums[row + part, :]
        last.append(pltpu.make_async_copy(line, vector, out_sems.at[total + n]))
        last[-1].start()
    for _, _, store in stores:
        store.wait()
    for copy in last:
        copy.wait()


def call_close(proj, qkv, fc, dense, block, grad, small):
    any_spec = pl.BlockSpec(memory_space=pl.ANY)
    shape = jax.ShapeDtypeStruct
    arrays = (fc, proj, qkv, dense, block, grad)
    cuts = (2, 2, 2, 1, 1, 1)
    outs = [shape(a.shape, f32) for a in arrays]
    lengths = [512] * 4 + [qkv.shape[1], fc.shape[1], 512, 512]
    outs += [shape((length,), f32) for length in lengths]
    return pl.pallas_call(
        functools.partial(close_kernel, cuts),
        name="close",
        out_shape=outs,
        in_specs=[any_spec] * 7,
        out_specs=[any_spec] * 14,
        scratch_shapes=[VMEM(a.shape, a.dtype) for a in (*arrays, small)]
        + [VMEM(a.shape, f32) for a in arrays[:4]]
        + [VMEM((length,), f32) for length in lengths]
        + [pltpu.SemaphoreType.DMA((sum(cuts) + 8,)), pltpu.SemaphoreType.DMA((sum(cuts) + 8,))],
        compiler_params=pltpu.CompilerParams(vmem_limit_bytes=60 << 20),
    )(*arrays, small)


def fused_shards(
    block_input, out_grad, ln1_gain, ln1_bias, ln2_gain, ln2_bias,
    w_qkv, b_qkv, w_dense, b_dense, w_fc, b_fc, w_proj, b_proj,
):
    results = call_block(
        block_input, out_grad, w_qkv, w_dense, w_fc, w_proj, turn_tables(SEQ),
        ln1_gain, ln1_bias, ln2_gain, ln2_bias, b_qkv, b_fc, b_dense, b_proj,
    )
    fc, proj, qkv, dense, block, grad, *vectors = call_close(*results[:7])
    gain_1, shift_1, gain_2, shift_2, qkv_bias, fc_bias, dense_bias, proj_bias = vectors
    return (
        block, grad, gain_1, shift_1, gain_2, shift_2, qkv, qkv_bias, dense, dense_bias,
        fc, fc_bias, proj, proj_bias,
    )


def solution(mesh):
    sizes = tuple(mesh.shape[name] for name in ("dp", "row", "col"))
    body = fused_shards if sizes == (2, 4, 4) else shards
    return jax.shard_map(
        body,
        mesh=mesh,
        in_specs=(
            P(("dp", "row"), "col"),
            P(("dp", "row"), "col"),
            P("col"),
            P("col"),
            P("col"),
            P("col"),
            P("row", "col"),
            P("col"),
            P("col", "row"),
            P("col"),
            P("row", "col"),
            P("col"),
            P("col", "row"),
            P("col"),
        ),
        out_specs=(
            P(("dp", "row"), "col"),
            P(("dp", "row"), "col"),
            P("col"),
            P("col"),
            P("col"),
            P("col"),
            P("row", "col"),
            P("col"),
            P("col", "row"),
            P("col"),
            P("row", "col"),
            P("col"),
            P("col", "row"),
            P("col"),
        ),
        check_vma=False,
    )
```

```python
import functools
import math

import jax
import jax.numpy as jnp
import numpy as np
from jax import lax
from jax.experimental import pallas as pl
from jax.experimental.pallas import tpu as pltpu
from jax.sharding import PartitionSpec as P

D = 2048
HD = 256
ROT = 64
SEQ = 512


epsilon = 1e-05
contract_last = (((1,), (1,)), ((), ()))
contract_first = (((0,), (0,)), ((), ()))


def angle_tables(length):
    half_rot = ROT // 2
    position = jnp.arange(length, dtype=jnp.float32)
    exponent = jnp.arange(half_rot, dtype=jnp.float32) * (2.0 / ROT)
    frequency = 10000.0 ** (-exponent)
    angles = position[:, None] * frequency[None, :]
    return (jnp.cos(angles), jnp.sin(angles))


def rotate_fwd(values, cosine, sine_vals):
    half_rot = ROT // 2
    first = values[..., :half_rot]
    second = values[..., half_rot:ROT]
    cos_part = cosine[:, None, :]
    sin_part = sine_vals[:, None, :]
    return jnp.concatenate(
        [
            first * cos_part - second * sin_part,
            second * cos_part + first * sin_part,
            values[..., ROT:],
        ],
        axis=-1,
    )


def rotate_back(grads, cosine, sine_vals):
    half_rot = ROT // 2
    first = grads[..., :half_rot]
    second = grads[..., half_rot:ROT]
    cos_part = cosine[:, None, :]
    sin_part = sine_vals[:, None, :]
    return jnp.concatenate(
        [
            first * cos_part + second * sin_part,
            second * cos_part - first * sin_part,
            grads[..., ROT:],
        ],
        axis=-1,
    )


def gelu_value(pre_act):
    return 0.5 * pre_act * (1.0 + lax.erf(pre_act * 0.7071067811865476))


def gelu_slope(pre_act):
    return 0.5 * (
        1.0 + lax.erf(pre_act * 0.7071067811865476)
    ) + pre_act * 0.3989422804014327 * jnp.exp(-0.5 * pre_act * pre_act)


def shards(
    block_input,
    out_grad,
    ln1_gain,
    ln1_bias,
    ln2_gain,
    ln2_bias,
    w_qkv,
    b_qkv,
    w_dense,
    b_dense,
    w_fc,
    b_fc,
    w_proj,
    b_proj,
):
    tok_rows = block_input.shape[0]
    seq_count = tok_rows // SEQ
    qkv_cols = w_qkv.shape[1]
    fc_cols = w_fc.shape[1]
    local_heads = qkv_cols // (3 * HD)
    head_cols = local_heads * HD
    scale = 1.0 / math.sqrt(HD)
    cosine, sine_vals = angle_tables(SEQ)
    causal = jnp.arange(SEQ)[:, None] >= jnp.arange(SEQ)[None, :]
    row_total, square_total = lax.psum(
        (jnp.sum(block_input, axis=1), jnp.sum(block_input * block_input, axis=1)), "col"
    )
    mean_row = (row_total / D)[:, None]
    var_row = (square_total / D)[:, None] - mean_row * mean_row
    inv_std = lax.rsqrt(var_row + epsilon)
    x_hat = (block_input - mean_row) * inv_std
    normed_one = (x_hat * ln1_gain + ln1_bias).astype(jnp.bfloat16)
    normed_two = (x_hat * ln2_gain + ln2_bias).astype(jnp.bfloat16)
    wide_one, wide_two = (
        lax.all_gather(normed_one, "col", axis=1, tiled=True),
        lax.all_gather(normed_two, "col", axis=1, tiled=True),
    )
    part_one = wide_one
    part_two = wide_two
    qkv_pre = jnp.dot(
        part_one,
        lax.all_gather(w_qkv, "row", axis=0, tiled=True),
        preferred_element_type=jnp.float32,
    )
    fc_pre = jnp.dot(
        part_two,
        lax.all_gather(w_fc, "row", axis=0, tiled=True),
        preferred_element_type=jnp.float32,
    )
    qkv_pre = qkv_pre + b_qkv
    fc_pre = fc_pre + b_fc

    def forward_seq(block):
        query = rotate_fwd(block[:, :, 0], cosine, sine_vals).astype(jnp.bfloat16)
        keys = rotate_fwd(block[:, :, 1], cosine, sine_vals).astype(jnp.bfloat16)
        values = block[:, :, 2].astype(jnp.bfloat16)
        scores = jnp.einsum("qhd,khd->hqk", query, keys, preferred_element_type=jnp.float32) * scale
        masked = jnp.where(causal[None], scores, -1e30)
        row_max = jnp.max(masked, axis=-1, keepdims=True)
        exp_sum = jnp.sum(
            jnp.where(causal[None], jnp.exp(masked - row_max), 0.0), axis=-1, keepdims=True
        )
        log_total = row_max + jnp.log(exp_sum)
        probs_low = jnp.where(causal[None], jnp.exp(masked - log_total), 0.0).astype(jnp.bfloat16)
        attended = jnp.einsum(
            "hqk,khd->qhd", probs_low, values, preferred_element_type=jnp.float32
        ).astype(jnp.bfloat16)
        return (query, keys, values, attended, log_total)

    query, keys, values, attended, log_total = lax.map(
        forward_seq, qkv_pre.reshape(seq_count, SEQ, local_heads, 3, HD)
    )
    attn_out = attended.reshape(tok_rows, head_cols)
    gelu_out = gelu_value(fc_pre).astype(jnp.bfloat16)
    out_stack = jnp.concatenate([w_dense, w_proj], axis=0)
    shard_piece = lax.all_gather(out_stack, "row", axis=1, tiled=True)
    mixed = jnp.dot(
        attn_out, shard_piece[:head_cols], preferred_element_type=jnp.float32
    ) + jnp.dot(gelu_out, shard_piece[head_cols:], preferred_element_type=jnp.float32)
    branch_sum = lax.psum_scatter(mixed, "col", scatter_dimension=1, tiled=True)
    block_output = block_input + branch_sum + b_dense + b_proj
    grad_low = out_grad.astype(jnp.bfloat16)
    wide_grad = lax.all_gather(grad_low, "col", axis=1, tiled=True)
    both_grad = lax.dot_general(
        wide_grad,
        lax.all_gather(out_stack, "row", axis=1, tiled=True),
        contract_last,
        preferred_element_type=jnp.float32,
    )
    attn_grad = both_grad[:, :head_cols]
    gelu_grad = both_grad[:, head_cols:]
    attn_grad_low = attn_grad.astype(jnp.bfloat16)
    fc_grad = gelu_grad * gelu_slope(fc_pre)
    fc_bias_grad = jnp.sum(fc_grad, axis=0)
    fc_grad_low = fc_grad.astype(jnp.bfloat16)

    def backward_seq(items):
        query_s, keys_s, values_s, attended_s, log_s, head_grad = items
        scores = (
            jnp.einsum("qhd,khd->hqk", query_s, keys_s, preferred_element_type=jnp.float32) * scale
        )
        probs = jnp.where(
            causal[None], jnp.exp(jnp.where(causal[None], scores, -1e30) - log_s), 0.0
        )
        probs_low = probs.astype(jnp.bfloat16)
        value_grad = jnp.einsum(
            "hqk,qhd->khd", probs_low, head_grad, preferred_element_type=jnp.float32
        )
        prob_grad = jnp.einsum(
            "qhd,khd->hqk", head_grad, values_s, preferred_element_type=jnp.float32
        )
        delta_row = jnp.transpose(
            jnp.sum(head_grad.astype(jnp.float32) * attended_s.astype(jnp.float32), axis=-1), (1, 0)
        )[:, :, None]
        score_grad = (probs * (prob_grad - delta_row) * scale).astype(jnp.bfloat16)
        query_grad = jnp.einsum(
            "hqk,khd->qhd", score_grad, keys_s, preferred_element_type=jnp.float32
        )
        key_grad = jnp.einsum(
            "hqk,qhd->khd", score_grad, query_s, preferred_element_type=jnp.float32
        )
        return jnp.stack(
            [
                rotate_back(query_grad, cosine, sine_vals),
                rotate_back(key_grad, cosine, sine_vals),
                value_grad,
            ],
            axis=2,
        )

    head_grads = attn_grad_low.reshape(seq_count, SEQ, local_heads, HD)
    qkv_grad = lax.map(
        backward_seq, (query, keys, values, attended, log_total, head_grads)
    ).reshape(tok_rows, qkv_cols)
    qkv_bias_grad = jnp.sum(qkv_grad, axis=0)
    qkv_grad_low = qkv_grad.astype(jnp.bfloat16)
    in_stack = jnp.concatenate([w_qkv, w_fc], axis=1)
    shard_piece = lax.all_gather(in_stack, "row", axis=0, tiled=True)
    norm_grads = jnp.stack(
        [
            lax.dot_general(
                qkv_grad_low,
                shard_piece[:, :qkv_cols],
                contract_last,
                preferred_element_type=jnp.float32,
            ),
            lax.dot_general(
                fc_grad_low,
                shard_piece[:, qkv_cols:],
                contract_last,
                preferred_element_type=jnp.float32,
            ),
        ]
    )
    part_one = wide_one
    part_two = wide_two
    row_part = lax.psum_scatter(
        jnp.concatenate(
            [
                lax.dot_general(
                    part_one, qkv_grad_low, contract_first, preferred_element_type=jnp.float32
                ),
                lax.dot_general(
                    part_two, fc_grad_low, contract_first, preferred_element_type=jnp.float32
                ),
                lax.dot_general(
                    wide_grad, attn_out, contract_first, preferred_element_type=jnp.float32
                ),
                lax.dot_general(
                    wide_grad, gelu_out, contract_first, preferred_element_type=jnp.float32
                ),
            ],
            axis=1,
        ),
        "row",
        scatter_dimension=0,
        tiled=True,
    )
    grad_rows = lax.psum(row_part, "dp")
    qkv_total = grad_rows[:, :qkv_cols]
    fc_total = grad_rows[:, qkv_cols : qkv_cols + fc_cols]
    dense_total = grad_rows[:, qkv_cols + fc_cols : qkv_cols + fc_cols + head_cols].T
    proj_total = grad_rows[:, qkv_cols + fc_cols + head_cols :].T
    norm_local = lax.psum_scatter(norm_grads, "col", scatter_dimension=2, tiled=True)
    grad_one = norm_local[0]
    grad_two = norm_local[1]
    hat_grad = grad_one * ln1_gain + grad_two * ln2_gain
    total_hat, total_cross = lax.psum(
        (jnp.sum(hat_grad, axis=1), jnp.sum(hat_grad * x_hat, axis=1)), "col"
    )
    input_grad = out_grad + inv_std * (
        hat_grad - (total_hat / D)[:, None] - x_hat * (total_cross / D)[:, None]
    )
    gain_one, shift_one, gain_two, shift_two, qkv_bias_total, fc_bias_total, out_bias_total = (
        lax.psum(
            (
                jnp.sum(grad_one * x_hat, axis=0),
                jnp.sum(grad_one, axis=0),
                jnp.sum(grad_two * x_hat, axis=0),
                jnp.sum(grad_two, axis=0),
                qkv_bias_grad,
                fc_bias_grad,
                jnp.sum(out_grad, axis=0),
            ),
            ("dp", "row"),
        )
    )
    return (
        block_output,
        input_grad,
        gain_one,
        shift_one,
        gain_two,
        shift_two,
        qkv_total,
        qkv_bias_total,
        dense_total,
        out_bias_total,
        fc_total,
        fc_bias_total,
        proj_total,
        out_bias_total,
    )


f32 = jnp.float32
bf16 = jnp.bfloat16
MESH = pl.DeviceIdType.MESH
VMEM = pltpu.VMEM
Q = 256
HALF = 4 * Q


def flip(a, b):
    return a + b - 2 * a * b


def span(start, size):
    return pl.ds(pl.multiple_of(start, size), size)


def mm(a, b):
    return jnp.dot(a, b, preferred_element_type=f32)


def mm_nt(a, b):
    return lax.dot_general(a, b, (((1,), (1,)), ((), ())), preferred_element_type=f32)


def mm_tn(a, b):
    return lax.dot_general(a, b, (((0,), (0,)), ((), ())), preferred_element_type=f32)


class Net:
    def __init__(self, send_sems, recv_sems, local_sems):
        self.k = lax.axis_index("dp")
        self.r = lax.axis_index("row")
        self.c = lax.axis_index("col")
        k, r, c = self.k, self.r, self.c
        self.core = (1 - k, r, c)
        self.x = (k, r + 1 - 2 * (r % 2), c)
        self.y = (k, r + 2 - 4 * (r // 2), c)
        near = c + 1 - 2 * (c % 2)
        self.z = (None, (k, r, near), (k, r, c + 2 - 4 * (c // 2)), (k, r, 3 - c))
        self.middle = flip(c % 2, c // 2) == 1
        self.send_sems, self.recv_sems, self.local_sems = send_sems, recv_sems, local_sems
        self.remote_count = 0
        self.local_count = 0
        self.pending = []

    def mix(self, j):
        return flip(j % 2, flip(self.c % 2, self.r % 2)) + 2 * flip(
            j // 2, flip(self.c // 2, self.r // 2)
        )

    def barrier(self):
        sem = pltpu.get_barrier_semaphore()

        def greet(peer):
            pl.semaphore_signal(sem, inc=1, device_id=peer, device_id_type=MESH)

        for peer in (self.x, self.y, self.core, self.z[1]):
            greet(peer)

        @pl.when(self.middle)
        def _():
            greet(self.z[3])
            pl.semaphore_wait(sem, 5)

        @pl.when(jnp.logical_not(self.middle))
        def _():
            pl.semaphore_wait(sem, 4)

    def slot(self):
        self.remote_count += 1
        return self.remote_count - 1

    def remote(self, src, dst, peer):
        slot = self.slot()
        copy = pltpu.make_async_remote_copy(
            src_ref=src,
            dst_ref=dst,
            send_sem=self.send_sems.at[slot],
            recv_sem=self.recv_sems.at[slot],
            device_id=peer,
            device_id_type=MESH,
        )
        copy.start()
        self.pending.append(copy)
        return copy

    def local(self, src, dst):
        copy = pltpu.make_async_copy(src, dst, self.local_sems.at[self.local_count])
        self.local_count += 1
        copy.start()
        return copy

    def sent(self, copy):
        copy.wait_send()
        self.pending = [other for other in self.pending if other is not copy]

    def drain(self):
        for copy in self.pending:
            copy.wait_send()


class Gather:
    def __init__(self, net, shard, full, by_rows):
        self.net, self.shard, self.full, self.by_rows = net, shard, full, by_rows
        self.depth = Q // 2 if by_rows else shard.shape[0] // 2
        self.placed = []

    def own(self, half, part=None):
        if self.by_rows:
            if part is None:
                return self.shard.at[span(half * Q, Q), :]
            return self.shard.at[span(half * Q + part * self.depth, self.depth), :]
        rows = slice(None) if part is None else pl.ds(part * self.depth, self.depth)
        return self.shard.at[rows, span(half * Q, Q)]

    def chunk(self, s, i, part=None):
        start = s * HALF + i * Q
        if self.by_rows:
            if part is None:
                return self.full.at[pl.ds(start, Q), :]
            return self.full.at[pl.ds(start + part * self.depth, self.depth), :]
        rows = slice(None) if part is None else pl.ds(part * self.depth, self.depth)
        return self.full.at[rows, pl.ds(start, Q)]

    def place_own(self):
        net = self.net
        self.placed = [
            net.local(self.own(net.k), self.chunk(0, 0)),
            net.local(self.own(1 - net.k), self.chunk(1, 0)),
        ]

    def send_own(self):
        net, k = self.net, self.net.k
        self.y0 = net.remote(self.own(k, 0), self.chunk(0, 2, 0), net.y)
        self.x1 = net.remote(self.own(k, 1), self.chunk(0, 1, 1), net.x)
        self.y1 = net.remote(self.own(k, 1), self.chunk(0, 2, 1), net.y)
        self.x0 = net.remote(self.own(k, 0), self.chunk(0, 1, 0), net.x)

    def forward(self):
        net = self.net
        self.y0.wait_recv()
        self.d0 = net.remote(self.chunk(0, 2, 0), self.chunk(0, 3, 0), net.x)
        self.x1.wait_recv()
        self.d1 = net.remote(self.chunk(0, 1, 1), self.chunk(0, 3, 1), net.y)

    def swap_near(self):
        net = self.net
        self.x0.wait_recv()
        self.c1 = net.remote(self.chunk(0, 1), self.chunk(1, 1), net.core)
        self.y1.wait_recv()
        self.c2 = net.remote(self.chunk(0, 2), self.chunk(1, 2), net.core)

    def swap_far(self):
        net = self.net
        self.d0.wait_recv()
        self.d1.wait_recv()
        self.c3 = net.remote(self.chunk(0, 3), self.chunk(1, 3), net.core)

    def ready(self):
        for copy in (self.c1, self.c2, self.c3):
            copy.wait_recv()
        for copy in self.placed:
            copy.wait()

    def release(self):
        for copy in (self.d0, self.d1, self.c1, self.c2, self.c3):
            self.net.sent(copy)


class Line:
    def __init__(self, net, slots):
        self.net, self.slots = net, slots
        self.ids = [None] + [net.slot() for _ in range(3)]
        self.sends = []

    def copy(self, src, dst, peer, send):
        net = self.net
        return pltpu.make_async_remote_copy(
            src_ref=self.slots.at[src],
            dst_ref=self.slots.at[dst],
            send_sem=net.send_sems.at[send],
            recv_sem=net.recv_sems.at[self.ids[dst]],
            device_id=peer,
            device_id_type=MESH,
        )

    def start(self):
        net = self.net
        self.first = self.copy(0, 1, net.z[1], self.ids[1])
        self.first.start()
        self.hops = [
            self.copy(0, 3, net.z[3], self.ids[2]),
            self.copy(1, 2, net.z[3], self.ids[3]),
            self.copy(3, 2, net.z[1], net.slot()),
            self.copy(2, 3, net.z[1], net.slot()),
        ]

        @pl.when(net.middle)
        def _():
            self.hops[0].start()

    def arrived(self, slot):
        return self.copy(0, slot, self.net.z[1], self.ids[slot])

    def step(self, number):
        slot = (1, 3, 2)[number]

        @pl.when(self.net.middle)
        def _():
            self.arrived(slot).wait_recv()
            self.hops[number + 1].start()

    def ready(self):
        @pl.when(jnp.logical_not(self.net.middle))
        def _():
            for slot in (1, 2, 3):
                self.arrived(slot).wait_recv()

    def drain(self):
        self.first.wait_send()

        @pl.when(self.net.middle)
        def _():
            for hop in self.hops:
                hop.wait_send()


class Fold:
    def __init__(self, net, blocks, inbox):
        self.net, self.blocks, self.inbox = net, blocks, inbox
        hops = ((3, None, 0), (2, None, 1), (1, None, 2), (None, 0, 3), (None, 1, 4), (None, 3, 0))
        self.copies = []
        for n, (block, slot, dest) in enumerate(hops):
            number = net.slot()
            self.copies.append(
                pltpu.make_async_remote_copy(
                    src_ref=blocks.at[block] if slot is None else inbox.at[slot],
                    dst_ref=inbox.at[dest],
                    send_sem=net.send_sems.at[number],
                    recv_sem=net.recv_sems.at[number],
                    device_id=net.z[3] if n in (3, 4) else net.z[1],
                    device_id_type=MESH,
                )
            )

    def start(self, first, last):
        @pl.when(jnp.logical_not(self.net.middle))
        def _():
            for copy in self.copies[first:last]:
                copy.start()

    def step(self, number):
        slot, block = ((0, 2), (1, 3), (3, 1))[number]
        inbox, blocks = self.inbox, self.blocks

        @pl.when(self.net.middle)
        def _():
            self.copies[(0, 1, 3)[number]].wait_recv()

            def add(n, _):
                at = span(n * 64, 64)
                total = inbox[slot, at, :].astype(f32) + blocks[block, at, :].astype(f32)
                inbox[slot, at, :] = total.astype(bf16)
                return 0

            lax.fori_loop(0, inbox.shape[1] // 64, add, 0)
            self.copies[3 + number].start()

    def total(self, use):
        def gather(*slots):
            def add(n, _):
                at = span(n * 64, 64)
                value = self.blocks[0, at, :].astype(f32)
                for slot in slots:
                    value = value + self.inbox[slot, at, :].astype(f32)
                use(at, value)
                return 0

            lax.fori_loop(0, self.inbox.shape[1] // 64, add, 0)

        @pl.when(self.net.middle)
        def _():
            self.copies[2].wait_recv()
            self.copies[4].wait_recv()
            gather(2, 4)

        @pl.when(jnp.logical_not(self.net.middle))
        def _():
            self.copies[5].wait_recv()
            gather(0)

    def drain(self):
        @pl.when(self.net.middle)
        def _():
            for copy in self.copies[3:]:
                copy.wait_send()

        @pl.when(jnp.logical_not(self.net.middle))
        def _():
            for copy in self.copies[:3]:
                copy.wait_send()


def turn(low, tables, sign):
    lane = lax.broadcasted_iota(jnp.int32, low.shape, 1)
    swung = jnp.where(lane < ROT // 2, pltpu.roll(low, 96, 1), pltpu.roll(low, 32, 1))
    return low * tables[0] + sign * (tables[1] * swung)


class Tiles:
    def __init__(self, slots, sems):
        self.slots, self.sems = slots, sems

    def write(self, count, product, place, depth):
        def body(n, _):
            slot = n % 2
            source = self.slots.at[slot, pl.ds(0, depth), :]
            copy = pltpu.make_async_copy(source, place(n), self.sems.at[slot])

            @pl.when(n >= 2)
            def _():
                copy.wait()

            self.slots[slot, 0:depth, :] = product(n).astype(bf16)
            copy.start()
            return 0

        lax.fori_loop(0, count, body, 0)
        for slot in range(2):
            source = self.slots.at[slot, pl.ds(0, depth), :]
            pltpu.make_async_copy(source, place(slot), self.sems.at[slot]).wait()


class Reduce:
    def __init__(self, net, partial, joined, near, far, by_rows, in_vmem=False):
        self.in_vmem = in_vmem
        self.net, self.partial, self.by_rows = net, partial, by_rows
        self.joined, self.near, self.far = joined, near, far
        self.depth = Q // 2 if by_rows else partial.shape[0] // 2

    def chunk(self, i, half):
        if self.by_rows:
            return self.partial.at[pl.ds(i * Q + half * self.depth, self.depth), :]
        return self.partial.at[pl.ds(half * self.depth, self.depth), pl.ds(i * Q, Q)]

    def whole(self):
        if self.by_rows:
            return self.partial.at[pl.ds(0, Q), :]
        return self.partial.at[:, pl.ds(0, Q)]

    def rows(self, half):
        return pl.ds(half * self.depth, self.depth)

    def start(self):
        net = self.net
        self.a = net.remote(self.chunk(3, 0), self.joined.at[0], net.x)
        self.b = net.remote(self.chunk(3, 1), self.joined.at[1], net.y)
        self.near_a = net.remote(self.chunk(1, 0), self.near.at[self.rows(0), :], net.x)
        self.near_b = net.remote(self.chunk(2, 1), self.near.at[self.rows(1), :], net.y)

    def join(self, parts):
        net = self.net
        loads = [net.local(self.chunk(2, 0), parts[0]), net.local(self.chunk(1, 1), parts[1])]
        hops = []
        for half, copy, peer in ((0, self.a, net.y), (1, self.b, net.x)):
            loads[half].wait()
            copy.wait_recv()
            tile = 64

            def add(n, _, half=half):
                at = span(n * tile, tile)
                total = self.joined[half, at, :].astype(f32) + parts[half][at, :].astype(f32)
                self.joined[half, at, :] = total.astype(bf16)
                return 0

            lax.fori_loop(0, self.depth // tile, add, 0)
            hops.append(net.remote(self.joined.at[half], self.far.at[self.rows(half), :], peer))
        self.far_a, self.far_b = hops

    def prepare(self, buffers):
        net = self.net
        self.buffers = list(buffers)
        self.loads = [net.local(self.whole(), buffers[0])]
        for copy in (self.near_a, self.near_b):
            copy.wait_recv()
        if self.in_vmem:
            self.buffers[1:3] = [self.near, self.far]
        else:
            self.loads.append(net.local(self.near, buffers[1]))

    def finish(self, out):
        net, buffers = self.net, self.buffers
        last = []
        for half, copy in enumerate((self.far_a, self.far_b)):
            copy.wait_recv()
            if not self.in_vmem:
                rows = self.rows(half)
                last.append(net.local(self.far.at[rows, :], buffers[2].at[rows, :]))
        for copy in self.loads:
            copy.wait()
        tile = 64
        self.here, self.there = [], []
        for half in range(2):
            if last:
                last[half].wait()

            def add(n, _, half=half):
                at = span(half * self.depth + n * tile, tile)
                parts = [buffer[at, :].astype(f32) for buffer in buffers[:3]]
                buffers[3][at, :] = (parts[0] + parts[1] + parts[2]).astype(bf16)
                return 0

            lax.fori_loop(0, self.depth // tile, add, 0)
            source = buffers[3].at[self.rows(half), :]
            if self.by_rows:
                place = out.at[span(net.k * Q + half * self.depth, self.depth), :]
            else:
                place = out.at[self.rows(half), span(net.k * Q, Q)]
            self.here.append(net.local(source, place))
            self.there.append(net.remote(source, place, net.core))

    def done(self):
        for copy in self.here:
            copy.wait()
        for copy in self.there:
            copy.wait_recv()


def block_kernel(
    x, og, w_qkv, w_dense, w_fc, w_proj, t_turn,
    i_gain_1, i_bias_1, i_gain_2, i_bias_2, i_b_qkv, i_b_fc, i_b_dense, i_b_proj,
    o_proj, o_qkv, o_fc, o_dense, o_block, o_input, o_small,
    all_proj, r_proj, r_qkv, r_fc, r_dense, n_proj, f_proj, n_qkv, f_qkv, n_fc, f_fc,
    g_qkv, g_dense, g_fc, g_tail, xs, ys, pks, stats, rows, h1c, h1s, h2c, h2s, dyc, dys, xh,
    qb, kb, vb, probs, probs_low, oc, dob, dqc, gc, slope, dabt, stage,
    out_recv, hat_recv, j_proj, j_qkv, j_fc, j_dense, n_dense, f_dense, tables, vecs, bias, packs, small,
    gain_1, bias_1, gain_2, bias_2, b_qkv, b_fc, b_dense, b_proj,
    send_sems, recv_sems, local_sems, stage_sems,
):
    tok = x.shape[0]
    heads = qb.shape[0]
    width = gc.shape[1]
    scale = 1.0 / math.sqrt(HD)
    net = Net(send_sems, recv_sems, local_sems)
    net.barrier()
    qkv = Gather(net, w_qkv, g_qkv, True)
    dense = Gather(net, w_dense, g_dense, False)
    fc = Gather(net, w_fc, g_fc, True)
    proj = Gather(net, w_proj, all_proj, False)
    qkv.send_own()
    dense.send_own()
    load_x = net.local(x, probs.at[0])
    vectors = [
        net.local(i_gain_1, gain_1), net.local(i_bias_1, bias_1), net.local(i_gain_2, gain_2),
        net.local(i_bias_2, bias_2), net.local(i_b_qkv, b_qkv), net.local(i_b_fc, b_fc),
        net.local(i_b_dense, b_dense), net.local(i_b_proj, b_proj),
    ]
    load_og = net.local(og, probs.at[1])
    load_turn = net.local(t_turn, tables)
    tiles = Tiles(stage, stage_sems)
    mine = pl.ds(0, tok)
    theirs = pl.ds(tok, tok)

    step = 128
    lane = lax.broadcasted_iota(jnp.int32, (step, 128), 1)
    load_x.wait()

    def local_norm(n, _):
        at = span(n * step, step)
        block = probs[0, at, :]
        mean = jnp.mean(block, axis=1, keepdims=True)
        centred = block - mean
        var = jnp.mean(centred * centred, axis=1, keepdims=True)
        stats[at, :] = jnp.where(lane == 0, mean, jnp.where(lane == 1, var, 0.0))
        return 0

    lax.fori_loop(0, tok // step, local_norm, 0)
    pks[0] = stats[...].T[0:8]
    for copy in vectors:
        copy.wait()
    for n, vector in enumerate((gain_1, bias_1, gain_2, bias_2)):
        pks[0, 2 + n : 3 + n, :] = vector[...].reshape(1, 512)
    p_line = Line(net, pks)
    p_line.start()
    for weight in (qkv, dense, fc):
        weight.place_own()
    bias[...] = jnp.zeros_like(bias)
    bias[3:4, 0 : b_qkv.shape[0]] = b_qkv[...].reshape(1, b_qkv.shape[0])
    bias[4:5, :] = b_fc[...].reshape(1, width)
    bias[5:6, 0:512] = (b_dense[...] + b_proj[...]).reshape(1, 512)
    rows[...] = jnp.zeros_like(rows)
    load_og.wait()

    def local_grad(n, _):
        at = span(n * step, step)
        block = probs[1, at, :]
        ys[0, at, :] = block.astype(bf16)
        bias[1:2, 0:512] += jnp.sum(block, axis=0, keepdims=True)
        return 0

    lax.fori_loop(0, tok // step, local_grad, 0)
    for hop in range(3):
        p_line.step(hop)
    p_line.ready()
    means = [pks[j, 0:1, :] for j in range(4)]
    mu = (means[0] + means[1] + means[2] + means[3]) * 0.25
    spread = [pks[j, 1:2, :] + (means[j] - mu) * (means[j] - mu) for j in range(4)]
    rows[0:1, :] = mu
    rows[1:2, :] = lax.rsqrt((spread[0] + spread[1] + spread[2] + spread[3]) * 0.25 + epsilon)
    stats[...] = rows[...].T

    def own_norm(n, _):
        at = span(n * step, step)
        hats = (probs[0, at, :] - stats[at, 0:1]) * stats[at, 1:2]
        xs[0, at, :] = (hats * pks[0, 2:3, :] + pks[0, 3:4, :]).astype(bf16)
        return 0

    lax.fori_loop(0, tok // step, own_norm, 0)
    x_line = Line(net, xs)
    y_line = Line(net, ys)
    x_line.start()
    qkv.forward()
    x_line.step(0)
    x_line.step(1)
    fc.send_own()
    dense.forward()
    qkv.swap_near()
    x_line.step(2)
    y_line.start()
    dense.swap_near()
    qkv.swap_far()
    x_line.ready()
    fc.forward()
    proj.send_own()

    for s in range(2):
        for j in range(4):
            lanes = span(flip(s, net.k) * Q, Q)
            dest = span(net.mix(j) * Q, Q)
            wide = span(s * HALF + net.mix(j) * Q, Q)
            vecs[0:4, wide] = pks[j, 2:6, lanes]

            def norm(n, _, s=s, j=j, lanes=lanes, dest=dest, wide=wide):
                at = span(n * step, step)
                one = xs[j, at, lanes]
                hats = (one.astype(f32) - pks[j, 3:4, lanes]) * (1.0 / pks[j, 2:3, lanes])
                xh[at, wide] = hats.astype(bf16)
                (h1s if s else h1c)[at, dest] = one
                two = hats * pks[j, 4:5, lanes] + pks[j, 5:6, lanes]
                (h2s if s else h2c)[at, dest] = two.astype(bf16)
                return 0

            lax.fori_loop(0, tok // step, norm, 0)
    swap_h1 = net.remote(h1s, h1c.at[theirs, :], net.core)
    swap_h2 = net.remote(h2s, h2c.at[theirs, :], net.core)
    y_line.step(0)
    load_turn.wait()
    qkv.ready()

    def project(n, _):
        cols = span(n * 3 * HD, 3 * HD)
        acc = mm(h1c[mine, :], g_qkv[0:HALF, cols]) + mm(h1s[...], g_qkv[HALF:, cols])
        acc = acc + bias[3:4, cols]
        qb[n, :, 0:128] = turn(acc[:, 0:128], tables, 1.0).astype(bf16)
        qb[n, :, 128:HD] = acc[:, 128:HD].astype(bf16)
        kb[n, :, 0:128] = turn(acc[:, HD : HD + 128], tables, 1.0).astype(bf16)
        kb[n, :, 128:HD] = acc[:, HD + 128 : 2 * HD].astype(bf16)
        vb[n] = acc[:, 2 * HD :].astype(bf16)
        return 0

    lax.fori_loop(0, heads, project, 0)
    y_line.step(1)
    chunks = tok // step

    def attend(n, _):
        head, chunk = n // chunks, n % chunks
        at = span(chunk * step, step)
        scores = mm_nt(qb[head, at, :], kb[head]) * scale
        token = lax.broadcasted_iota(jnp.int32, (step, tok), 0) + chunk * step
        allowed = token >= lax.broadcasted_iota(jnp.int32, (step, tok), 1)
        scores = jnp.where(allowed, scores, -1e30)
        top = jnp.max(scores, axis=1, keepdims=True)
        raised = jnp.where(allowed, jnp.exp(scores - top), 0.0)
        weight = raised / jnp.sum(raised, axis=1, keepdims=True)
        probs[head, at, :] = weight
        low = weight.astype(bf16)
        probs_low[head, at, :] = low
        oc[at, span(head * HD, HD)] = mm(low, vb[head]).astype(bf16)
        return 0

    lax.fori_loop(0, heads * chunks, attend, 0)
    swap_o = net.remote(oc.at[mine, :], oc.at[theirs, :], net.core)
    dense.swap_far()
    fc.swap_near()
    y_line.step(2)
    fc.swap_far()
    fc.ready()

    def expand(n, _):
        cols = span(n * 512, 512)
        a = mm(h2c[mine, :], g_fc[0:HALF, cols]) + mm(h2s[...], g_fc[HALF:, cols])
        a = a + bias[4:5, cols]
        rise = 0.5 * (1.0 + lax.erf(a * 0.7071067811865476))
        gc[mine, cols] = (a * rise).astype(bf16)
        slope[:, cols] = (rise + a * 0.3989422804014327 * jnp.exp(-0.5 * a * a)).astype(bf16)
        return 0

    lax.fori_loop(0, width // 1024, expand, 0)
    proj.forward()
    lax.fori_loop(width // 1024, width // 512, expand, 0)
    swap_g = net.remote(gc.at[mine, :], gc.at[theirs, :], net.core)
    y_line.ready()
    for s in range(2):
        for j in range(4):
            lanes = span(flip(s, net.k) * Q, Q)
            dest = span(net.mix(j) * Q, Q)
            (dys if s else dyc)[mine, dest] = ys[j, :, lanes]
    swap_dy = net.remote(dys, dyc.at[theirs, :], net.core)
    dense.ready()
    dob[...] = (
        mm_nt(dyc[mine, :], g_dense[:, 0:HALF]) + mm_nt(dys[...], g_dense[:, HALF:])
    ).astype(bf16)

    red_proj = Reduce(net, r_proj, j_proj, n_proj, f_proj, False)
    red_qkv = Reduce(net, r_qkv, j_qkv, n_qkv, f_qkv, True)
    red_fc = Reduce(net, r_fc, j_fc, n_fc, f_fc, True)
    red_dense = Reduce(net, r_dense, j_dense, n_dense, f_dense, False, True)
    swap_g.wait_recv()
    swap_dy.wait_recv()
    tall = width // 2
    tiles.write(
        4,
        lambda n: mm_tn(gc[:, span(n // 2 * tall, tall)], dyc[:, span(n % 2 * 512, 512)]),
        lambda n: r_proj.at[span(n // 2 * tall, tall), span(n % 2 * 512, 512)],
        tall,
    )
    proj.swap_near()
    red_proj.start()

    def keep(head, part, at, value, rotated):
        base = head * 3 * HD + part * HD
        if rotated:
            low = turn(value[:, 0:128], [tables[t, at, :] for t in range(2)], -1.0)
            dqc[at, pl.ds(pl.multiple_of(base, 128), 128)] = low.astype(bf16)
            bias[0:1, pl.ds(pl.multiple_of(base, 128), 128)] += jnp.sum(low, axis=0, keepdims=True)
            value, base, size = value[:, 128:], base + 128, 128
        else:
            size = HD
        cols = pl.ds(pl.multiple_of(base, 128), size)
        dqc[at, cols] = value.astype(bf16)
        bias[0:1, cols] += jnp.sum(value, axis=0, keepdims=True)

    def attend_back(head, _):
        cols = span(head * HD, HD)

        def chunk_back(n, _):
            at = span(n * step, step)
            grad = dob[at, cols]
            delta = jnp.sum(grad.astype(f32) * oc[at, cols].astype(f32), axis=1, keepdims=True)
            spread = mm_nt(grad, vb[head]) - delta
            low = (probs[head, at, :] * spread * scale).astype(bf16)
            probs_low[head, at, :] = low
            keep(head, 0, at, mm(low, kb[head]), True)
            return 0

        keep(head, 2, mine, mm_tn(probs_low[head], dob[:, cols]), False)
        lax.fori_loop(0, chunks, chunk_back, 0)
        keep(head, 1, mine, mm_tn(probs_low[head], qb[head]), True)
        return 0

    lax.fori_loop(0, heads, attend_back, 0)
    proj.swap_far()
    swap_dq = net.remote(dqc.at[mine, :], dqc.at[theirs, :], net.core)
    net.sent(swap_h1)
    net.sent(swap_h2)
    for s in range(2):

        def back_first(n, _, s=s):
            wide = span(s * HALF + n * 512, 512)
            grad = mm_nt(dqc[mine, :], g_qkv[wide, :])
            (h2s if s else h1s)[:, span(n * 512, 512)] = (grad * vecs[0:1, wide]).astype(bf16)
            vecs[4:5, wide] = jnp.sum(grad * xh[:, wide].astype(f32), axis=0, keepdims=True)
            vecs[5:6, wide] = jnp.sum(grad, axis=0, keepdims=True)
            return 0

        lax.fori_loop(0, HALF // 512, back_first, 0)

    proj.ready()
    qkv.release()
    loads = [
        net.local(w_proj.at[:, span(net.k * Q, Q)], g_qkv.at[:, pl.ds(0, Q)]),
        net.local(w_proj.at[:, span((1 - net.k) * Q, Q)], g_qkv.at[:, pl.ds(HALF, Q)]),
        net.local(all_proj.at[:, pl.ds(Q, 3 * Q)], g_qkv.at[:, pl.ds(Q, 3 * Q)]),
        net.local(all_proj.at[:, pl.ds(5 * Q, Q)], g_qkv.at[:, pl.ds(5 * Q, Q)]),
        net.local(all_proj.at[:, pl.ds(6 * Q, 2 * Q)], g_tail),
    ]
    swap_o.wait_recv()
    attn = oc.shape[1]
    tiles.write(
        2,
        lambda n: mm_tn(oc[...], dyc[:, span(n * 512, 512)]),
        lambda n: r_dense.at[:, span(n * 512, 512)],
        attn,
    )
    swap_h1.wait_recv()
    swap_dq.wait_recv()
    tiles.write(
        dqc.shape[1] // 512,
        lambda n: mm_tn(h1c[...], dqc[:, span(n * 512, 512)]),
        lambda n: r_qkv.at[:, span(n * 512, 512)],
        HALF,
    )
    red_qkv.start()
    red_dense.start()

    for copy in loads:
        copy.wait()
    x_line.drain()
    y_line.drain()

    def put_out(p, product):
        s, i = p // 4, p % 4
        out = product + mm(oc[mine, :], g_dense[:, span(p * Q, Q)])
        xs[net.mix(i), :, span(flip(s, net.k) * Q, Q)] = out.astype(bf16)

    def project_head(p, _):
        put_out(p, mm(gc[mine, :], g_qkv[:, span(p * Q, Q)]))
        return 0

    def project_tail(p, _):
        put_out(6 + p, mm(gc[mine, :], g_tail[:, span(p * Q, Q)]))
        return 0

    lax.fori_loop(0, 6, project_head, 0)
    lax.fori_loop(0, 2, project_tail, 0)
    out_fold = Fold(net, xs, out_recv)
    out_fold.start(0, 2)

    def back_fc(n, _):
        cols = span(n * 512, 512)
        grad = mm_nt(dyc[mine, :], g_qkv[cols, 0:HALF])
        grad = grad + mm_nt(dys[:, 0:512], g_qkv[cols, HALF : 6 * Q])
        grad = grad + mm_nt(dys[:, 512:], g_tail[cols, :])
        grad = grad * slope[:, cols].astype(f32)
        bias[2:3, cols] = jnp.sum(grad, axis=0, keepdims=True)
        slope[:, cols] = grad.astype(bf16)
        return 0

    lax.fori_loop(0, width // 512, back_fc, 0)
    dab = slope
    swap_da = net.remote(dab, dabt, net.core)
    red_proj.join([g_tail.at[pl.ds(0, tall), pl.ds(0, Q)], g_tail.at[pl.ds(tall, tall), pl.ds(0, Q)]])
    stats[...] = jnp.zeros_like(stats)
    lane = lax.broadcasted_iota(jnp.int32, (tok, 128), 1)

    def back_norm(j, _):
        for s in range(2):
            lanes = span(flip(s, net.k) * Q, Q)
            dest = span(net.mix(j) * Q, Q)
            wide = span(s * HALF + net.mix(j) * Q, Q)
            grad = mm_nt(dab[...], g_fc[wide, :])
            hats = xh[:, wide].astype(f32)
            packs[j, 2:4, lanes] = vecs[4:6, wide]
            packs[j, 4:5, lanes] = jnp.sum(grad * hats, axis=0, keepdims=True)
            packs[j, 5:6, lanes] = jnp.sum(grad, axis=0, keepdims=True)
            joint = (h2s if s else h1s)[:, dest].astype(f32) + grad * vecs[2:3, wide]
            ys[j, :, lanes] = joint.astype(bf16)
            one = jnp.sum(joint, axis=1, keepdims=True)
            two = jnp.sum(joint * hats, axis=1, keepdims=True)
            stats[...] += jnp.where(lane == 0, one, jnp.where(lane == 1, two, 0.0))
        return 0

    lax.fori_loop(0, 4, back_norm, 0)

    fc.release()
    turned = stats[...].T
    for j in range(4):
        packs[j, 0:2, :] = turned[0:2]
        packs[j, 6:8, :] = jnp.zeros((2, tok), f32)
    pack_copies = [net.remote(packs.at[j], packs.at[3 + j], net.z[j]) for j in (1, 2, 3)]
    hat_fold = Fold(net, ys, hat_recv)
    hat_fold.start(0, 2)
    out_fold.start(2, 3)
    hat_fold.start(2, 3)
    out_fold.step(0)
    swap_h2.wait_recv()
    swap_da.wait_recv()

    def grad_fc(n):
        cols = span(n * 512, 512)
        return mm_tn(h2c[mine, :], dab[:, cols]) + mm_tn(h2c[theirs, :], dabt[:, cols])

    tiles.write(width // 512, grad_fc, lambda n: r_fc.at[:, span(n * 512, 512)], HALF)
    red_fc.start()
    out_fold.step(1)

    def strips(base, n, columns):
        return g_fc.at[pl.ds(base + n * Q, Q), pl.ds(0, columns)]

    out_fold.step(2)
    for copy in pack_copies:
        copy.wait_recv()
    total = packs[0] + packs[4] + packs[5] + packs[6]
    rows[2:4, :] = total[0:2, :]
    stats[...] = rows[...].T
    small[0, 0:4, :] = total[2:6, :]
    for n in range(3):
        small[0, 4 + n : 5 + n, :] = bias[0:1, n * 512 : n * 512 + 512]
    for n in range(4):
        small[0, 7 + n : 8 + n, :] = bias[2:3, n * 512 : n * 512 + 512]
    small[0, 11:12, :] = bias[1:2, 0:512]
    small[0, 12:16, :] = jnp.zeros((4, 512), f32)
    net.remote(small.at[0], small.at[1], net.core).wait_recv()
    own_rows = span(net.k * 8, 8)
    small[2 + net.r, 0:8, :] = small[0, own_rows, :] + small[1, own_rows, :]
    place = small.at[2 + net.r, pl.ds(0, 8), :]
    across = (net.k, 3 - net.r, net.c)
    small_copies = [net.remote(place, place, peer) for peer in (net.x, net.y, across)]
    reload_x = net.local(x, probs.at[1])
    red_proj.prepare([g_qkv.at[:, pl.ds(n * Q, Q)] for n in range(4)])
    red_proj.finish(o_proj)
    hat_fold.step(0)
    red_fc.join([g_fc.at[pl.ds(6 * Q + n * (Q // 2), Q // 2), :] for n in range(2)])
    red_qkv.join(
        [g_fc.at[pl.ds(7 * Q + n * (Q // 2), Q // 2), pl.ds(0, 6 * Q)] for n in range(2)]
    )
    hat_fold.step(1)
    hat_fold.step(2)
    reload_x.wait()

    def close_out(at, value):
        probs[0, at, :] = probs[1, at, :] + value + bias[5:6, 0:512]

    out_fold.total(close_out)
    keep_block = net.local(probs.at[0], o_block)
    keep_block.wait()
    reload_og = net.local(og, probs.at[0])
    red_dense.join([g_tail.at[pl.ds(n * attn // 2, attn // 2), pl.ds(0, Q)] for n in range(2)])
    red_fc.prepare([strips(4 * Q, n, 8 * Q) for n in range(4)])
    red_qkv.prepare([strips(0, n, 6 * Q) for n in range(4)])
    red_dense.prepare([g_tail.at[pl.ds(n * attn, attn), pl.ds(Q, Q)] for n in range(4)])
    for copy in small_copies:
        copy.wait_recv()
    small[6, own_rows, :] = small[2, 0:8] + small[3, 0:8] + small[4, 0:8] + small[5, 0:8]
    place = small.at[6, own_rows, :]
    swap_small = net.remote(place, place, net.core)
    reload_og.wait()

    def close_hat(at, value):
        mu, rstd = stats[at, 0:1], stats[at, 1:2]
        hats = (probs[1, at, :] - mu) * rstd
        mean, cross = stats[at, 2:3] * (1.0 / D), stats[at, 3:4] * (1.0 / D)
        probs[0, at, :] += rstd * (value - mean - hats * cross)

    hat_fold.total(close_hat)
    keep_input = net.local(probs.at[0], o_input)
    swap_small.wait_recv()
    keep_small = net.local(small.at[6], o_small)
    red_fc.finish(o_fc)
    red_qkv.finish(o_qkv)
    red_dense.finish(o_dense)
    for weight in (red_proj, red_qkv, red_fc, red_dense):
        weight.done()
    keep_small.wait()
    keep_input.wait()
    p_line.drain()
    out_fold.drain()
    hat_fold.drain()
    net.drain()


def call_block(*args):
    x, w_qkv, w_dense, w_fc = args[0], args[2], args[3], args[4]
    tok = x.shape[0]
    n_qkv, n_attn, n_fc = w_qkv.shape[1], w_dense.shape[0], w_fc.shape[1]
    heads = n_attn // HD
    wide = 2 * HALF
    any_spec = pl.BlockSpec(memory_space=pl.ANY)
    shape = jax.ShapeDtypeStruct
    pieces = ((n_fc, Q), (Q, n_qkv), (Q, n_fc), (n_attn, Q))
    outs = [
        shape((n_fc, 2 * Q), bf16), shape((2 * Q, n_qkv), bf16),
        shape((2 * Q, n_fc), bf16), shape((n_attn, 2 * Q), bf16),
        shape((tok, 512), f32), shape((tok, 512), f32), shape((16, 512), f32),
        shape((n_fc, wide), bf16), shape((n_fc, HALF), bf16), shape((HALF, n_qkv), bf16),
        shape((HALF, n_fc), bf16), shape((n_attn, HALF), bf16),
    ]
    outs += [shape(piece, bf16) for piece in pieces[:3] for _ in range(2)]
    scratch = [
        VMEM((wide, n_qkv), bf16), VMEM((n_attn, wide), bf16), VMEM((wide, n_fc), bf16),
        VMEM((n_fc, 2 * Q), bf16),
        VMEM((4, tok, 512), bf16), VMEM((4, tok, 512), bf16), VMEM((4, 8, tok), f32),
        VMEM((tok, 128), f32), VMEM((128, tok), f32),
        VMEM((2 * tok, HALF), bf16), VMEM((tok, HALF), bf16),
        VMEM((2 * tok, HALF), bf16), VMEM((tok, HALF), bf16),
        VMEM((2 * tok, HALF), bf16), VMEM((tok, HALF), bf16), VMEM((tok, wide), bf16),
        VMEM((heads, tok, HD), bf16), VMEM((heads, tok, HD), bf16), VMEM((heads, tok, HD), bf16),
        VMEM((heads, tok, tok), f32), VMEM((heads, tok, tok), bf16),
        VMEM((2 * tok, n_attn), bf16), VMEM((tok, n_attn), bf16), VMEM((2 * tok, n_qkv), bf16),
        VMEM((2 * tok, n_fc), bf16), VMEM((tok, n_fc), bf16), VMEM((tok, n_fc), bf16),
        VMEM((2, HALF, 512), bf16),
        VMEM((5, tok, 512), bf16), VMEM((5, tok, 512), bf16),
    ]
    scratch += [VMEM((2,) + ((r // 2, c)), bf16) for r, c in pieces]
    scratch += [VMEM(pieces[3], bf16)] * 2
    scratch += [
        VMEM((2, tok, 128), f32),
        VMEM((8, wide), f32), VMEM((8, n_fc), f32), VMEM((7, 8, tok), f32), VMEM((7, 16, 512), f32),
        VMEM((512,), f32), VMEM((512,), f32), VMEM((512,), f32), VMEM((512,), f32),
        VMEM((n_qkv,), f32), VMEM((n_fc,), f32), VMEM((512,), f32), VMEM((512,), f32),
        pltpu.SemaphoreType.DMA((128,)), pltpu.SemaphoreType.DMA((128,)),
        pltpu.SemaphoreType.DMA((64,)), pltpu.SemaphoreType.DMA((2,)),
    ]
    return pl.pallas_call(
        block_kernel,
        name="block",
        out_shape=outs,
        in_specs=[any_spec] * 15,
        out_specs=[any_spec] * len(outs),
        scratch_shapes=scratch,
        compiler_params=pltpu.CompilerParams(
            collective_id=1, has_side_effects=True, vmem_limit_bytes=67043328
        ),
    )(*args)


def turn_tables(length):
    half_rot = ROT // 2
    frequency = (10000.0 ** (-np.arange(half_rot, dtype=np.float32) * (2.0 / ROT))).astype(np.float32)
    angles = np.arange(length, dtype=np.float32)[:, None] * frequency[None, :]
    tables = np.zeros((2, length, 128), np.float32)
    tables[0] = 1.0
    tables[0, :, :half_rot] = tables[0, :, half_rot:ROT] = np.cos(angles)
    tables[1, :, :half_rot] = -np.sin(angles)
    tables[1, :, half_rot:ROT] = np.sin(angles)
    return tables


def close_kernel(cuts, *refs):
    count = len(cuts)
    refs = list(refs)
    sources, small = [refs.pop(0) for _ in cuts], refs.pop(0)
    outs, vectors = [refs.pop(0) for _ in cuts], [refs.pop(0) for _ in range(8)]
    lows, sums = [refs.pop(0) for _ in cuts], refs.pop(0)
    wides, lines = [refs.pop(0) for _ in range(4)], [refs.pop(0) for _ in range(8)]
    in_sems, out_sems = refs
    loads, stores = [], []
    for n, cut in enumerate(cuts):
        rows = sources[n].shape[0] // cut
        for part in range(cut):
            at = pl.ds(part * rows, rows)
            number = len(loads)
            wide = wides[n] if n < len(wides) else lows[n]
            loads.append(
                pltpu.make_async_copy(sources[n].at[at, :], lows[n].at[at, :], in_sems.at[number])
            )
            stores.append(
                (n, at, pltpu.make_async_copy(wide.at[at, :], outs[n].at[at, :], out_sems.at[number]))
            )
    total = len(loads)
    load_small = pltpu.make_async_copy(small, sums, in_sems.at[total])
    for copy in loads:
        copy.start()
    load_small.start()
    for load, (n, at, store) in zip(loads, stores):
        load.wait()
        if n < len(wides):
            wides[n][at, :] = lows[n][at, :].astype(f32)
        store.start()
    load_small.wait()
    last = []
    for n, (row, line, vector) in enumerate(zip((0, 1, 2, 3, 4, 7, 11, 11), lines, vectors)):
        for part in range(line.shape[0] // 512):
            line[part * 512 : part * 512 + 512] = sums[row + part, :]
        last.append(pltpu.make_async_copy(line, vector, out_sems.at[total + n]))
        last[-1].start()
    for _, _, store in stores:
        store.wait()
    for copy in last:
        copy.wait()


def call_close(proj, qkv, fc, dense, block, grad, small):
    any_spec = pl.BlockSpec(memory_space=pl.ANY)
    shape = jax.ShapeDtypeStruct
    arrays = (dense, qkv, fc, proj, block, grad)
    cuts = (1, 2, 2, 2, 1, 1)
    outs = [shape(a.shape, f32) for a in arrays]
    lengths = [512] * 4 + [qkv.shape[1], fc.shape[1], 512, 512]
    outs += [shape((length,), f32) for length in lengths]
    return pl.pallas_call(
        functools.partial(close_kernel, cuts),
        name="close",
        out_shape=outs,
        in_specs=[any_spec] * 7,
        out_specs=[any_spec] * 14,
        scratch_shapes=[VMEM(a.shape, a.dtype) for a in (*arrays, small)]
        + [VMEM(a.shape, f32) for a in arrays[:4]]
        + [VMEM((length,), f32) for length in lengths]
        + [pltpu.SemaphoreType.DMA((sum(cuts) + 8,)), pltpu.SemaphoreType.DMA((sum(cuts) + 8,))],
        compiler_params=pltpu.CompilerParams(vmem_limit_bytes=60 << 20),
    )(*arrays, small)


def fused_shards(
    block_input, out_grad, ln1_gain, ln1_bias, ln2_gain, ln2_bias,
    w_qkv, b_qkv, w_dense, b_dense, w_fc, b_fc, w_proj, b_proj,
):
    results = call_block(
        block_input, out_grad, w_qkv, w_dense, w_fc, w_proj, turn_tables(SEQ),
        ln1_gain, ln1_bias, ln2_gain, ln2_bias, b_qkv, b_fc, b_dense, b_proj,
    )
    dense, qkv, fc, proj, block, grad, *vectors = call_close(*results[:7])
    gain_1, shift_1, gain_2, shift_2, qkv_bias, fc_bias, dense_bias, proj_bias = vectors
    return (
        block, grad, gain_1, shift_1, gain_2, shift_2, qkv, qkv_bias, dense, dense_bias,
        fc, fc_bias, proj, proj_bias,
    )


def solution(mesh):
    sizes = tuple(mesh.shape[name] for name in ("dp", "row", "col"))
    body = fused_shards if sizes == (2, 4, 4) else shards
    return jax.shard_map(
        body,
        mesh=mesh,
        in_specs=(
            P(("dp", "row"), "col"),
            P(("dp", "row"), "col"),
            P("col"),
            P("col"),
            P("col"),
            P("col"),
            P("row", "col"),
            P("col"),
            P("col", "row"),
            P("col"),
            P("row", "col"),
            P("col"),
            P("col", "row"),
            P("col"),
        ),
        out_specs=(
            P(("dp", "row"), "col"),
            P(("dp", "row"), "col"),
            P("col"),
            P("col"),
            P("col"),
            P("col"),
            P("row", "col"),
            P("col"),
            P("col", "row"),
            P("col"),
            P("row", "col"),
            P("col"),
            P("col", "row"),
            P("col"),
        ),
        check_vma=False,
    )
```
